32 devices in a mesh: gx: 4 (over z), gy: 4 (over x, core), gz: 2 (over y).
Axes of the slice: x: 2, y: 2, z: 4, core: 2. Of those that a mesh axis runs over, the one named last changes fastest.
Arguments:
- source: float32 [64, 32, 512], P('gx', 'gz', 'gy'), may hold values from -0.6 to 0.6
- shift: float32 [1], replicated, may hold values from 1e-05 to 0.0001
Outputs:
- solution: float32 [64, 32, 512], P('gx', 'gz', 'gy')
The draws below stay inside these ranges and needn't reach their ends.
All inputs are finite; a program needn't handle non-finite values.
Results may differ from the reference program's by a relative error of at most 0.0004.
Values sent between devices are 32-bit elements; how exact they have to be, the bound alone decides.
A program may use at most 64 MiB of HBM per device.

```python
import math
import jax
import jax.numpy as jnp
from jax import lax

LEVELS = 4
NU_PRE = 1
NU_POST = 1
N0 = 64
N1 = 32
N2 = 512


MEAN_LEVEL = 1e-06


def draw_source(key, part):
    rough_key = jax.random.fold_in(jax.random.fold_in(key, 11), 0)
    rough = jnp.clip(0.1 * jax.random.normal(rough_key, (N0, N1, N2), jnp.float32), -0.59, 0.59)
    return rough - jnp.mean(rough) + MEAN_LEVEL


def setup_inputs(seed: int = 0) -> dict:
    streams_of = jax.random.split(jax.random.key(seed), 3)
    source = draw_source(jax.random.fold_in(streams_of[2], 71), 0)
    shift = jnp.clip(jnp.exp(jax.random.uniform(streams_of[1], (1,), jnp.float32, math.log(9.999999747378752e-06), math.log(0.0001))), 9.999999747378752e-06, 0.0001)
    return {"source": source, "shift": shift}


DAMPING = 6.0 / 7.0
PRECISE = lax.Precision.HIGHEST
CUBIC_EVEN = (-5.0 / 128.0, 35.0 / 128.0, 105.0 / 128.0, -7.0 / 128.0)
CUBIC_ODD = (-7.0 / 128.0, 105.0 / 128.0, 35.0 / 128.0, -5.0 / 128.0)
LINEAR_EVEN = (0.25, 0.75)
LINEAR_ODD = (0.75, 0.25)


def wrapped(values, width):
    return jnp.pad(values, width, mode="wrap")


def neighbours(padded):
    center = padded[1:-1, 1:-1, 1:-1]
    beside_all = padded[2:, 1:-1, 1:-1] + padded[:-2, 1:-1, 1:-1]
    beside_all = beside_all + padded[1:-1, 2:, 1:-1] + padded[1:-1, :-2, 1:-1]
    beside_all = beside_all + padded[1:-1, 1:-1, 2:] + padded[1:-1, 1:-1, :-2]
    return center, beside_all


def defect(padded, forcing, weight_nb, diagonal):
    center, beside_all = neighbours(padded)
    return forcing - (diagonal * center - weight_nb * beside_all)


def relaxed(padded, forcing, weight_nb, diagonal):
    center, beside_all = neighbours(padded)
    return center + DAMPING * (forcing - (diagonal * center - weight_nb * beside_all)) / diagonal


def coarsen(values):
    values = values[0::2] + values[1::2]
    values = values[:, 0::2] + values[:, 1::2]
    values = values[:, :, 0::2] + values[:, :, 1::2]
    return 0.125 * values


def refine_axis(padded, dimension, even_weights, odd_weights):
    margin = len(even_weights) // 2
    length = padded.shape[dimension] - 2 * margin
    even_cells = even_weights[0] * lax.slice_in_dim(padded, 0, length, axis=dimension)
    odd_cells = odd_weights[0] * lax.slice_in_dim(padded, 1, 1 + length, axis=dimension)
    for offset in range(1, len(even_weights)):
        even_cells = even_cells + even_weights[offset] * lax.slice_in_dim(padded, offset, offset + length, axis=dimension)
        odd_cells = odd_cells + odd_weights[offset] * lax.slice_in_dim(padded, offset + 1, offset + 1 + length, axis=dimension)
    stacked = jnp.stack([even_cells, odd_cells], axis=dimension + 1)
    new_shape = list(even_cells.shape)
    new_shape[dimension] = 2 * length
    return stacked.reshape(new_shape)


def refine(padded, even_weights, odd_weights):
    for dimension in range(3):
        padded = refine_axis(padded, dimension, even_weights, odd_weights)
    return padded


def tables(cells_count):
    indices = jnp.arange(cells_count, dtype=jnp.int32)
    angles = ((indices[:, None] * indices[None, :]) % cells_count).astype(jnp.float32) * (2.0 * math.pi / cells_count)
    return jnp.cos(angles), jnp.sin(angles)


def along_axis(matrix, values, dimension):
    product = jnp.tensordot(matrix, values, axes=([1], [dimension]), precision=PRECISE)
    return jnp.moveaxis(product, 0, dimension)


def coarse_solve(forcing, shift_value, weight_nb):
    cosine_table, sine_table = tables(forcing.shape[0])
    real_part = along_axis(cosine_table, forcing, 0)
    imag_part = -along_axis(sine_table, forcing, 0)
    for dimension in (1, 2):
        cosine_table, sine_table = tables(forcing.shape[dimension])
        real_next = along_axis(cosine_table, real_part, dimension) + along_axis(sine_table, imag_part, dimension)
        imag_part = along_axis(cosine_table, imag_part, dimension) - along_axis(sine_table, real_part, dimension)
        real_part = real_next
    cosines = [jnp.cos(jnp.arange(cells_count, dtype=jnp.float32) * (2.0 * math.pi / cells_count)) for cells_count in forcing.shape]
    eigenvalue = weight_nb * (6.0 - 2.0 * cosines[0][:, None, None] - 2.0 * cosines[1][None, :, None] - 2.0 * cosines[2][None, None, :]) + shift_value
    real_part = real_part / eigenvalue
    imag_part = imag_part / eigenvalue
    for dimension in (0, 1):
        cosine_table, sine_table = tables(forcing.shape[dimension])
        real_next = along_axis(cosine_table, real_part, dimension) - along_axis(sine_table, imag_part, dimension)
        imag_part = along_axis(cosine_table, imag_part, dimension) + along_axis(sine_table, real_part, dimension)
        real_part = real_next
    cosine_table, sine_table = tables(forcing.shape[2])
    real_part = along_axis(cosine_table, real_part, 2) - along_axis(sine_table, imag_part, 2)
    return real_part / float(forcing.size)


def vcycle(grid_level, iterate, forcing, shift_value):
    weight_nb = 0.25 ** grid_level
    diagonal = 6.0 * weight_nb + shift_value
    for sweep_index in range(NU_PRE):
        iterate = relaxed(wrapped(iterate, 1), forcing, weight_nb, diagonal)
    residue = coarsen(defect(wrapped(iterate, 1), forcing, weight_nb, diagonal))
    if grid_level + 1 == LEVELS - 1:
        correction = coarse_solve(residue, shift_value, 0.25 ** (grid_level + 1))
    else:
        correction = vcycle(grid_level + 1, jnp.zeros_like(residue), residue, shift_value)
    iterate = iterate + refine(wrapped(correction, 1), LINEAR_EVEN, LINEAR_ODD)
    for sweep_index in range(NU_POST):
        iterate = relaxed(wrapped(iterate, 1), forcing, weight_nb, diagonal)
    return iterate


def reference(source, shift):
    shift_value = shift[0]
    sources = [source]
    for grid_level in range(1, LEVELS):
        sources.append(coarsen(sources[-1]))
    iterate = coarse_solve(sources[-1], shift_value, 0.25 ** (LEVELS - 1))
    for grid_level in range(LEVELS - 2, -1, -1):
        iterate = refine(wrapped(iterate, 2), CUBIC_EVEN, CUBIC_ODD)
        iterate = vcycle(grid_level, iterate, sources[grid_level], shift_value)
    return iterate
```

```python
import functools

import jax
import jax.numpy as jnp
import numpy as np
from jax import lax
from jax.experimental import pallas as pl
from jax.experimental.pallas import tpu as pltpu
from jax.sharding import PartitionSpec as P

LEVELS = 4
DAMPING = 6.0 / 7.0
PRECISE = lax.Precision.HIGHEST
CUBIC = (
    {-2: -5.0 / 128.0, -1: 35.0 / 128.0, 0: 105.0 / 128.0, 1: -7.0 / 128.0},
    {-1: -7.0 / 128.0, 0: 105.0 / 128.0, 1: 35.0 / 128.0, 2: -5.0 / 128.0},
)
LINEAR = ({-1: 0.25, 0: 0.75}, {0: 0.75, 1: 0.25})
NAMES = ("gx", "gy", "gz")
MESH = pl.DeviceIdType.MESH


def basis(count):
    cells = np.arange(count)
    columns, cosines = [], []
    for m in range(count):
        k = (m + 1) // 2
        angle = 2.0 * np.pi * k * cells / count
        column = np.cos(angle) if m % 2 == 1 or m == 0 else np.sin(angle)
        columns.append(column / np.sqrt(np.sum(column**2)))
        cosines.append(np.cos(2.0 * np.pi * k / count))
    return np.stack(columns, axis=1), np.array(cosines, np.float32)


def interpolation(coarse_count, fine_cells, weights):
    matrix = np.zeros((len(fine_cells), coarse_count))
    for row, cell in enumerate(fine_cells):
        for offset, weight in weights[cell % 2].items():
            matrix[row, (cell // 2 + offset) % coarse_count] += weight
    return matrix


def pairs(coarse_count):
    return np.kron(np.eye(coarse_count), np.ones((1, 2)))


def blocked(matrix):
    count = max(1, 128 // matrix.shape[1])
    return np.kron(np.eye(count), matrix)


def constants(block, sizes):
    b0, b1, b2 = block
    m0, m1, m2 = (size // 2 for size in sizes)
    q0, q1, q2 = (size // 4 for size in sizes)
    c0, c1, c2 = (size // 8 for size in sizes)
    table = {}
    table["own_rows"] = np.kron(np.eye(b0 // 2), pairs(b1 // 2))
    lanes = 0.125 * pairs(b2 // 2).T
    table["own_lo"] = np.concatenate([lanes, np.zeros_like(lanes)], axis=1)
    table["own_hi"] = np.concatenate([np.zeros_like(lanes), lanes], axis=1)
    table["down_rows"] = blocked(pairs(q1))
    table["down_lanes"] = 0.125 * pairs(q2).T
    window_lanes = [b2 + j for j in range(b2 // 2)] + [j - b2 for j in range(b2 // 2, 2 * b2)]
    window_rows = [j - 8 for j in range(b1 + 16)]
    for name, weights in (("cubic", CUBIC), ("linear", LINEAR)):
        table[name + "_rows1"] = blocked(interpolation(q1, range(m1), weights))
        table[name + "_lanes1"] = interpolation(q2, range(m2), weights).T
        table[name + "_rows0"] = blocked(interpolation(m1, window_rows, weights))
        table[name + "_lanes0"] = interpolation(m2, window_lanes, weights).T
    (u0, cos0), (u1, cos1), (u2, cos2) = basis(c0), basis(c1), basis(c2)
    table["spectrum_rows"] = np.kron(u0.T @ pairs(c0), u1.T @ pairs(c1))
    table["spectrum_lanes"] = 0.125 * pairs(c2).T @ u2
    for name, weights in (("cubic", CUBIC), ("linear", LINEAR)):
        table[name + "_rows2"] = np.kron(
            interpolation(c0, range(q0), weights) @ u0, interpolation(c1, range(q1), weights) @ u1
        )
        table[name + "_lanes2"] = u2.T @ interpolation(c2, range(q2), weights).T
    two = np.float32(2.0)
    eigen = (
        np.float32(6.0)
        - two * cos0[:, None, None]
        - two * cos1[None, :, None]
        - two * cos2[None, None, :]
    )
    table["eigen"] = (np.float32(0.25 ** (LEVELS - 1)) * eigen).reshape(c0 * c1, c2)
    wide = ("spectrum_rows", "spectrum_lanes", "eigen")
    return {
        name: np.asarray(
            value, np.float32 if name in wide or name.endswith("2") else jnp.bfloat16
        )
        for name, value in table.items()
    }


def dot(a, b):
    return jnp.dot(a, b, precision=PRECISE, preferred_element_type=jnp.float32)


def parts_of(values, pieces):
    parts = []
    for n in range(pieces):
        parts.append(values.astype(jnp.bfloat16))
        if n + 1 < pieces:
            values = values - parts[-1].astype(jnp.float32)
    return parts[::-1]


def right(values, matrix, pieces):
    terms = [
        jnp.dot(part, matrix, preferred_element_type=jnp.float32)
        for part in parts_of(values, pieces)
    ]
    return sum(terms[1:], terms[0])


def left(matrix, values, pieces):
    terms = [
        jnp.dot(matrix, part, preferred_element_type=jnp.float32)
        for part in parts_of(values, pieces)
    ]
    return sum(terms[1:], terms[0])


def around(plane):
    rows, lanes = plane.shape
    total = pltpu.roll(plane, 1, 0) + pltpu.roll(plane, rows - 1, 0)
    return total + (pltpu.roll(plane, 1, 1) + pltpu.roll(plane, lanes - 1, 1))


def around_all(values):
    first = jnp.concatenate([values[1:], values[:1]], axis=0)
    first = first + jnp.concatenate([values[-1:], values[:-1]], axis=0)
    for axis in (1, 2):
        first = first + pltpu.roll(values, 1, axis)
        first = first + pltpu.roll(values, values.shape[axis] - 1, axis)
    return first


def row_blocks(matrix, values, pieces):
    depth = matrix.shape[1]
    return jnp.concatenate(
        [left(matrix, values[i : i + depth], pieces) for i in range(0, values.shape[0], depth)], axis=0
    )


def loop(count, body):
    def step(i, carry):
        body(i)
        return carry

    lax.fori_loop(0, count, step, 0, unroll=4 if count % 4 == 0 else 2)


def close(ref):
    count = ref.shape[0] - 2
    ref[0] = ref[count]
    ref[count + 1] = ref[1]


def defect_plane(v, p, g, weight, diagonal):
    center = v[p]
    beside = v[p - 1] + v[p + 1] + around(center)
    return center, g - (diagonal * center - weight * beside)


def restrict_own(k, summed):
    b_half, rows, lanes = summed.shape
    folded = left(k["own_rows"][...], summed.reshape(b_half * rows, lanes), 3)
    half = folded.shape[0] // 2
    return right(folded[:half], k["own_lo"][...], 3) + right(folded[half:], k["own_hi"][...], 3)


def unpack(gathered, counts, g):
    nx, ny, nz = counts
    x, y, z = (lax.axis_index(name) for name in NAMES)
    half, rows, lanes = gathered.shape[1:]
    low = lax.broadcasted_iota(jnp.int32, (half, rows, lanes), 2) < lanes // 2
    for dx in range(nx):
        for dz in range(nz):
            for pair in range(ny // 2):
                parts = []
                for dy in (2 * pair, 2 * pair + 1):
                    index = (lax.rem(x + dx, nx) * ny + lax.rem(y + dy, ny)) * nz
                    parts.append(gathered[index + lax.rem(z + dz, nz)])
                turned = [pltpu.roll(part, lanes // 2, 2) for part in parts]
                where = (pl.ds(dz * rows, rows), pl.ds(pair * lanes, lanes))
                start = 2 * half * dx
                g[(pl.ds(start, half), *where)] = jnp.where(low, parts[0], turned[1])
                g[(pl.ds(start + half, half), *where)] = jnp.where(low, turned[0], parts[1])


def solve(k, kind, values, shift):
    shape = values.shape
    flat = values.reshape(shape[0] * shape[1], shape[2])
    spectrum = dot(k["spectrum_rows"][...], dot(flat, k["spectrum_lanes"][...]))
    spectrum = spectrum / (k["eigen"][...] + shift)
    fine = dot(k[kind + "_rows2"][...], dot(spectrum, k[kind + "_lanes2"][...]))
    return fine.reshape(shape)


def cycle2(k, v, g, shift):
    weight = 0.25**2
    diagonal = 6.0 * weight + shift
    damp = DAMPING / diagonal
    if v is None:
        v = damp * g
    else:
        v = v + damp * (g - (diagonal * v - weight * around_all(v)))
    v = v + solve(k, "linear", g - (diagonal * v - weight * around_all(v)), shift)
    return v + damp * (g - (diagonal * v - weight * around_all(v)))


def down(k, t, shape2):
    flat = row_blocks(k["down_rows"][...], t[...].reshape(-1, t.shape[2]), 3)
    return right(flat, k["down_lanes"][...], 3).reshape(shape2)


def up(k, kind, level, values, z):
    flat = right(values, k[kind + "_lanes" + level][...], 2)
    z[...] = row_blocks(k[kind + "_rows" + level][...], flat, 2).reshape(z.shape)


def blend(z, i, weights, count):
    total = None
    for offset, weight in weights.items():
        index = i + offset
        index = index if count is None else lax.rem(index + count, count)
        term = weight * z[index]
        total = term if total is None else total + term
    return total


def up1(k, kind, values, z, v, add):
    count = z.shape[0]
    up(k, kind, "1", values.reshape(-1, values.shape[2]), z)
    weights = CUBIC if kind == "cubic" else LINEAR

    def body(i):
        for odd in (0, 1):
            p = 2 * i + odd + 1
            value = blend(z, i, weights[odd], count)
            v[p] = v[p] + value if add else value

    loop(count, body)
    close(v)


def cycle1(k, v, u, g, t, z, shift, zero, shape2):
    weight = 0.25
    diagonal = 6.0 * weight + shift
    damp = DAMPING / diagonal
    count = g.shape[0]

    def before(p):
        if zero:
            u[p + 1] = damp * g[p]
        else:
            center, rest = defect_plane(v, p + 1, g[p], weight, diagonal)
            u[p + 1] = center + damp * rest

    loop(count, before)
    close(u)

    def residue(i):
        t[i] = (
            defect_plane(u, 2 * i + 1, g[2 * i], weight, diagonal)[1]
            + defect_plane(u, 2 * i + 2, g[2 * i + 1], weight, diagonal)[1]
        )

    loop(count // 2, residue)
    correction = cycle2(k, None, down(k, t, shape2), shift)
    up1(k, "linear", correction, z, u, True)

    def after(p):
        center, rest = defect_plane(u, p + 1, g[p], weight, diagonal)
        v[p + 1] = center + damp * rest

    loop(count, after)
    close(v)


def window(k, kind, v, zw, span, write):
    count = v.shape[0] - 2
    values = jnp.concatenate([v[count - 3 : count + 1], v[1 : span - 3]], axis=0)
    up(k, kind, "0", values.reshape(-1, values.shape[2]), zw)
    weights = CUBIC if kind == "cubic" else LINEAR

    def body(i):
        for odd in (0, 1):
            write(2 * i + odd, blend(zw, i + 3, weights[odd], None))

    loop(span - 6, body)


def own_defect(v, p, f, weight, diagonal):
    rows, lanes = f.shape
    inside = (pl.ds(8, rows), pl.ds(lanes, lanes))
    wide = v[p + 1, pl.ds(8, rows), :]
    center = wide[:, lanes:]
    beside = v[(p, *inside)] + v[(p + 2, *inside)]
    beside = beside + v[p + 1, pl.ds(7, rows), pl.ds(lanes, lanes)]
    beside = beside + v[p + 1, pl.ds(9, rows), pl.ds(lanes, lanes)]
    beside = beside + pltpu.roll(wide, 1, 1)[:, lanes:]
    beside = beside + pltpu.roll(wide, 2 * lanes - 1, 1)[:, lanes:]
    return center, f - (diagonal * center - weight * beside)


def position():
    return tuple(lax.axis_index(name) for name in NAMES)


def partner_of(place):
    x, y, z = place
    return (x, y + 1 - 2 * lax.rem(y, 2), z)


def shifted(place, counts, offset):
    return tuple(
        lax.rem(at + step + count, count) for at, step, count in zip(place, offset, counts)
    )


def slot(place, counts):
    return (place[0] * counts[1] + place[1]) * counts[2] + place[2]


def chip_offsets(counts):
    nx, ny, nz = counts
    offsets = [
        (dx, dy, dz) for dx in range(nx) for dy in range(0, ny, 2) for dz in range(nz)
    ]

    def hops(offset):
        return sum(min(step, count - step) for step, count in zip(offset, (nx, ny, nz)))

    return sorted(offsets[1:], key=hops, reverse=True)


def face_offsets(counts):
    faces = []
    for axis in range(3):
        for side, step in ((0, -1), (1, 1)):
            offset = [0, 0, 0]
            offset[axis] = step
            faces.append((tuple(offset), axis, side))
    return faces


def greet(barrier, places):
    for place in places:
        pl.semaphore_signal(barrier, inc=1, device_id=place, device_id_type=MESH)


def remote(src, dst, send, recv, place):
    return pltpu.make_async_remote_copy(
        src_ref=src, dst_ref=dst, send_sem=send, recv_sem=recv, device_id=place, device_id_type=MESH
    )


def spread(counts, block, gathered, sems):
    send, recv, relay_send, relay_recv = sems
    me = position()
    partner = partner_of(me)
    along, across = stages(counts)
    number = {offset: n for n, offset in enumerate(chip_offsets(counts))}
    mine = gathered.at[slot(me, counts)]
    copies, relays = {}, []

    def pass_on(offset, source, target, place):
        n = number[offset]
        copies[offset] = remote(source, target, send.at[n], recv.at[n], place)
        copies[offset].start()

    def relay(n, source, target):
        relays.append(remote(source, target, relay_send.at[n], relay_recv.at[n], partner))
        relays[-1].start()

    for offset in along + across:
        pass_on(offset, block, mine, shifted(me, counts, offset))
    relay(len(number), block, mine)

    def arrival(offset):
        copies[offset].wait_recv()
        source = shifted(me, counts, tuple(-step for step in offset))
        return gathered.at[slot(source, counts)]

    def finish():
        gathered[slot(me, counts)] = block[...]
        for first in along[::-1]:
            arrived = arrival(first)
            for second in across:
                place = shifted(me, counts, second)
                pass_on((first[0], second[1], second[2]), arrived, arrived, place)
            relay(number[first], arrived, arrived)
        for first in ((0, 0, 0), *along[::-1]):
            for second in across[::-1]:
                offset = (first[0], second[1], second[2])
                arrived = arrival(offset)
                relay(number[offset], arrived, arrived)
        for copy in copies.values():
            copy.wait_send()
        for copy in relays:
            copy.wait()

    return finish


def stages(counts):
    offsets = chip_offsets(counts)
    along = [offset for offset in offsets if offset[1:] == (0, 0)]
    across = [offset for offset in offsets if offset[0] == 0]
    return along, across


def gather_places(counts):
    me = position()
    along, across = stages(counts)
    return [shifted(me, counts, offset) for offset in along + across] + [partner_of(me)]


def first_part(k, counts, source, f, gathered, halos, block, owns, sems, face_sems):
    own_planes, own_rows, own_columns = owns
    planes, rows, columns = halos
    face_send, face_recv = face_sems
    me = position()
    barrier = pltpu.get_barrier_semaphore()
    faces = face_offsets(counts)
    places = gather_places(counts) + [shifted(me, counts, offset) for offset, _, _ in faces]
    greet(barrier, places)
    b0, b1, b2 = source.shape
    summed = source[...].reshape(b0 // 2, 2, b1, b2)
    block[...] = restrict_own(k, summed[:, 0] + summed[:, 1]).reshape(block.shape)
    own_planes[0] = source[0]
    own_planes[1] = source[b0 - 1]
    own_rows[0] = source[:, pl.ds(0, 1), :]
    own_rows[1] = source[:, pl.ds(b1 - 1, 1), :]
    turned = source[...].reshape(b0 * b1, b2).T
    own_columns[0] = turned[:8]
    own_columns[1] = turned[b2 - 8 :]
    pl.semaphore_wait(barrier, len(places))
    finish = spread(counts, block, gathered, sems)
    buffers = ((own_planes, planes), (own_rows, rows), (own_columns, columns))
    order = (0, 2, 1)
    copies = []
    for n, (offset, axis, side) in enumerate(faces):
        own, halo = buffers[order[axis]]
        place = shifted(me, counts, offset)
        copies.append(
            remote(own.at[side], halo.at[1 - side], face_send.at[n], face_recv.at[n], place)
        )
        copies[-1].start()
    f[...] = jnp.zeros_like(f)
    f[1 : b0 + 1, pl.ds(8, b1), pl.ds(b2, b2)] = source[...]
    finish()
    for copy in copies:
        copy.wait()


def second_part(k, counts, shape2, span, shift, gathered, source, halos, out, buffers):
    g, v, u, t, z, zw, v0, v1, f, summed = buffers
    plane_halo, row_halo, column_halo = halos
    unpack(gathered, counts, g)
    b0, b1, b2 = source.shape
    rows, lanes = pl.ds(8, b1), pl.ds(b2, b2)
    f[0, rows, lanes] = plane_halo[0]
    f[b0 + 1, rows, lanes] = plane_halo[1]
    f[1 : b0 + 1, pl.ds(7, 1), lanes] = row_halo[0]
    f[1 : b0 + 1, pl.ds(8 + b1, 1), lanes] = row_halo[1]
    middle = jnp.zeros((b2 - 16, b0 * b1), jnp.float32)
    turned = jnp.concatenate([column_halo[1], middle, column_halo[0]], axis=0)
    f[1 : b0 + 1, rows, pl.ds(0, b2)] = turned.T.reshape(b0, b1, b2)
    def pair_sum(i):
        t[i] = g[2 * i] + g[2 * i + 1]

    loop(g.shape[0] // 2, pair_sum)
    forcing2 = down(k, t, shape2)
    iterate2 = cycle2(k, solve(k, "cubic", forcing2, shift), forcing2, shift)
    up1(k, "cubic", iterate2, z, v, False)
    cycle1(k, v, u, g, t, z, shift, False, shape2)

    def put(p, value):
        v0[p] = value

    window(k, "cubic", v, zw, span, put)
    diagonal = 6.0 + shift
    damp = DAMPING / diagonal

    def before(p):
        center, rest = defect_plane(v0, p + 1, f[p], 1.0, diagonal)
        v1[p] = center + damp * rest

    loop(b0 + 2, before)

    def residue(i):
        summed[i] = (
            own_defect(v1, 2 * i, source[2 * i], 1.0, diagonal)[1]
            + own_defect(v1, 2 * i + 1, source[2 * i + 1], 1.0, diagonal)[1]
        )

    loop(b0 // 2, residue)
    out[...] = restrict_own(k, summed[...]).reshape(out.shape)


def third_part(k, counts, shape2, span, shift, gathered, source, out, buffers):
    g, v, u, t, z, zw, w, v1 = buffers[:8]
    unpack(gathered, counts, g)
    cycle1(k, v, u, g, t, z, shift, True, shape2)
    b0 = source.shape[0]

    def put(p, value):
        w[p] = value

    window(k, "linear", v, zw, span, put)

    def add(p):
        w[p] = v1[p] + w[p + 1]

    loop(b0 + 2, add)
    diagonal = 6.0 + shift
    damp = DAMPING / diagonal

    def after(p):
        center, rest = own_defect(w, p, source[p], 1.0, diagonal)
        out[p] = center + damp * rest

    loop(b0, after)


def kernel(names, counts, shape2, span, *refs):
    k = dict(zip(names, refs))
    shift_ref, source, out, *rest = refs[len(names) :]
    shift = shift_ref[0]
    landing, later, *halos = rest[:5]
    block, block_later, *owns = rest[5:10]
    buffers = rest[10:20]
    sems, sems_later, face_sems = rest[20:24], rest[24:28], rest[28:30]
    f = buffers[8]
    first_part(k, counts, source, f, landing, halos, block, owns, sems, face_sems)
    second_part(k, counts, shape2, span, shift, landing, source, halos, block_later, buffers)
    spread(counts, block_later, later, sems_later)()
    third_part(k, counts, shape2, span, shift, later, source, out, buffers)


def per_device(counts, source, shift):
    nx, ny, nz = counts
    b0, b1, b2 = source.shape
    sizes = (b0 * nx, b1 * nz, b2 * ny)
    table = constants(source.shape, sizes)
    m0, m1, m2 = (size // 2 for size in sizes)
    shape2 = tuple(size // 4 for size in sizes)
    span = b0 // 2 + 8
    wide = (b1 + 16, 2 * b2)
    packed = (b0 // 4, b1 // 2, b2)
    devices = nx * ny * nz
    chips = devices // 2
    vmem = pl.BlockSpec(memory_space=pltpu.VMEM)

    def field(*shape):
        return pltpu.VMEM(shape, jnp.float32)

    faces = [field(2, b1, b2), field(2, b0, 1, b2), field(2, 8, b0 * b1)]
    buffers = [
        field(m0, m1, m2),
        field(m0 + 2, m1, m2),
        field(m0 + 2, m1, m2),
        field(m0 // 2, m1, m2),
        field(m0 // 2, m1, m2),
        field(span, *wide),
        field(b0 + 4, *wide),
        field(b0 + 2, *wide),
        field(b0 + 2, *wide),
        field(b0 // 2, b1, b2),
    ]
    sems = [pltpu.SemaphoreType.DMA((max(chips - 1, 1),))] * 2
    sems += [pltpu.SemaphoreType.DMA((chips,))] * 2
    landing = [field(devices, *packed)] * 2 + faces
    names = tuple(table)
    return pl.pallas_call(
        functools.partial(kernel, names, counts, shape2, span),
        out_shape=jax.ShapeDtypeStruct(source.shape, jnp.float32),
        in_specs=[vmem] * len(names) + [pl.BlockSpec(memory_space=pltpu.SMEM), vmem],
        out_specs=vmem,
        scratch_shapes=landing
        + [field(*packed)] * 2
        + faces
        + buffers
        + sems * 2
        + [pltpu.SemaphoreType.DMA((6,))] * 2,
        compiler_params=pltpu.CompilerParams(
            vmem_limit_bytes=60 * 1024 * 1024, collective_id=0, has_side_effects=True
        ),
    )(*[jnp.asarray(table[name]) for name in names], shift, source)


def modes(count, depth):
    if depth == 0:
        return [(0, k) for k in range(count // 2)] + [(1, k) for k in range(1, count // 2 + 1)]
    half = count // 2
    low = modes(half, depth - 1)
    high = []
    for kind, k in low:
        if kind == 0:
            high.append((0, half - k if k else half // 2))
        else:
            high.append((1, half - k if k < half // 2 else half))
    return low + high


def waves(count, order):
    cells = (np.arange(count) + 0.5) * (2.0 * np.pi / count)
    return np.stack([np.sin(k * cells) if kind else np.cos(k * cells) for kind, k in order], axis=1)


def analysis(waves_):
    return waves_.T / np.sum(waves_**2, axis=0)[:, None]


def two_blocks(matrix, axis):
    first, second = np.split(matrix, 2, axis=axis)
    return np.concatenate([np.diag(first), np.diag(second)])


def factors(m):
    orders = modes(m, 2), modes(m // 2, 1), modes(m // 4, 0)
    bases = [waves(len(order), order) for order in orders]
    t = {"waves": bases[0]}
    for level, fine, coarse in (("1", bases[0], bases[1]), ("2", bases[1], bases[2])):
        n = fine.shape[0]
        t["r" + level] = two_blocks(analysis(coarse) @ (0.5 * pairs(n // 2)) @ fine, 1)
        for name, weights in (("p", LINEAR), ("q", CUBIC)):
            matrix = interpolation(n // 2, range(n), weights)
            t[name + level] = two_blocks(analysis(fine) @ matrix @ coarse, 0)
        order = orders[int(level) - 1]
        t["e" + level] = np.array([2.0 - 2.0 * np.cos(2.0 * np.pi * k / n) for _, k in order])
    t["c3"] = np.array([np.cos(2.0 * np.pi * k / (m // 4)) for _, k in orders[2]], np.float32)
    fine = np.eye(2 * m)
    lap = 2.0 * fine - np.roll(fine, 1, 0) - np.roll(fine, -1, 0)
    current = interpolation(m, range(2 * m), CUBIC) @ bases[0]
    for i in range(3):
        t[f"m{i}"] = np.sum(analysis(bases[0]).T * ((0.5 * pairs(m)) @ current), axis=0)
        current = lap @ current
    return t


def window_cells(count, reach):
    return [j if j < count + reach else None for j in range(count)] + [
        count + j if j < reach else (j - 8 if j >= 8 - reach else None) for j in range(8)
    ]


def synthesis(t, cells, weights):
    m = t["waves"].shape[0]
    rows = interpolation(m, [0 if cell is None else cell for cell in cells], weights)
    rows[[cell is None for cell in cells]] = 0.0
    return rows @ t["waves"]


def halves(matrix, axis):
    high = np.asarray(matrix, jnp.bfloat16)
    low = np.asarray(matrix - high.astype(np.float64), jnp.bfloat16)
    return np.concatenate([high, low], axis=axis)


def fast_constants(block, sizes):
    b0, b1, b2 = block
    m0, m1, m2 = (size // 2 for size in sizes)
    t0, t1, t2 = (factors(m) for m in (m0, m1, m2))
    index = np.arange(m0 * m1).reshape(2, 2, m0 // 4, 2, 2, m1 // 4).transpose(0, 3, 1, 4, 2, 5).reshape(-1)
    i0, i1 = index // m1, index % m1
    rows2 = m0 * m1 // 4
    j0, j1 = i0[:rows2], i1[:rows2]

    def across(name, k, l, op=np.multiply):
        return op(t0[name][k], t1[name][l])

    def joint(a, c):
        return t0[a][i0] * t1[c][i1]

    columns = [across("r1", i0, i1), across("p1", i0, i1), across("q1", i0, i1), across("e1", i0, i1, np.add)]
    columns += [joint("m0", "m0"), joint("m1", "m0") + joint("m0", "m1")]
    columns += [joint("m2", "m0") + joint("m0", "m2") + 2.0 * joint("m1", "m1")]
    by_row = np.zeros((m0 * m1, 128))
    by_row[:, : len(columns)] = np.stack(columns, axis=1)
    for n, name in enumerate(("r2", "p2", "q2", "e2")):
        by_row[:rows2, 8 + n] = across(name, j0, j1, np.add if name == "e2" else np.multiply)
    by_lane = np.zeros((16, m2))
    for n, name in enumerate(("r1", "p1", "q1", "e1", "m0", "m1", "m2")):
        by_lane[n] = t2[name]
    for n, name in enumerate(("r2", "p2", "q2", "e2")):
        by_lane[8 + n, : m2 // 2] = t2[name]
    two = np.float32(2.0)
    eigen = np.float32(6.0) - two * t0["c3"][:, None, None]
    eigen = eigen - two * t1["c3"][None, :, None] - two * t2["c3"][None, None, :]
    eigen = (np.float32(0.25 ** (LEVELS - 1)) * eigen).reshape(rows2 // 4, m2 // 4)
    table = {"by_row": by_row, "by_lane": by_lane, "eigen": np.concatenate([eigen, eigen], axis=1)}
    table = {name: np.asarray(value, np.float32) for name, value in table.items()}

    half = b2 // 2
    own = np.zeros((2, b2, 3, 2, half))
    four = sum(np.roll(np.kron(np.eye(half), np.eye(2)[:, :1]), s, axis=0) for s in (-1, 0, 1, 2))
    four[b2 - 1, 0] = 0.0
    four[0, half - 1] = 0.0
    beside = np.zeros((b2, half))
    beside[b2 - 1, 0] = beside[0, half - 1] = 1.0
    for n, part in enumerate((pairs(half).T, beside, four)):
        for s in range(2):
            own[s, :, n, s] = 0.125 * part
    table = {"own": np.asarray(own.reshape(2 * b2, 3 * b2), jnp.bfloat16), **table}

    forward = analysis(t0["waves"])[i0][:, :, None] * analysis(t1["waves"])[i1][:, None, :]
    table["forward_rows"] = halves(forward.reshape(m0 * m1, m0 * m1), 1)
    table["forward_lanes"] = halves(analysis(t2["waves"]).T, 0)
    lane_cells = [j if j < b2 + b2 // 2 else j - 2 * b2 for j in range(2 * b2)]
    for name, weights, reach in (("cubic", CUBIC, 2), ("linear", LINEAR, 1)):
        planes = synthesis(t0, range(-reach, b0 + reach), weights)[:, i0]
        rows = synthesis(t1, window_cells(b1, reach), weights)[:, i1]
        full = planes[:, None, :] * rows[None, :, :]
        table[name + "_rows"] = halves(full.reshape(-1, m0 * m1), 1)
        table[name + "_lanes"] = halves(synthesis(t2, lane_cells, weights).T, 0)
    return table


def split(values):
    high = values.astype(jnp.bfloat16)
    return high, (values - high.astype(jnp.float32)).astype(jnp.bfloat16)


def by_right(values, table):
    high, low = split(values)
    depth = values.shape[1]
    first, second = table[:depth], table[depth:]
    return jnp.dot(
        jnp.concatenate([high, low, high], axis=1),
        jnp.concatenate([first, first, second], axis=0),
        preferred_element_type=jnp.float32,
    )


def by_left(table, values):
    high, low = split(values)
    depth = values.shape[0]
    first, second = table[:, :depth], table[:, depth:]
    return jnp.dot(
        jnp.concatenate([first, first, second], axis=1),
        jnp.concatenate([high, low, high], axis=0),
        preferred_element_type=jnp.float32,
    )


def fold(values):
    rows = values.shape[0] // 4
    total = (values[:rows] + values[rows : 2 * rows]) + (values[2 * rows : 3 * rows] + values[3 * rows :])
    return total + pltpu.roll(total, total.shape[1] // 2, 1)


def unfold(values):
    return jnp.concatenate([values] * 4, axis=0)


def own_parts(source, own, outs, alpha, beta):
    block, across, along_rows, along_planes, rest = outs
    b0, b1, b2 = source.shape
    h0, h1 = b0 // 2, b1 // 2
    first = [source[p, pl.ds(0, h1, stride=2), :] for p in range(b0)]
    second = [source[p, pl.ds(1, h1, stride=2), :] for p in range(b0)]
    summed = [a + b for a, b in zip(first, second)]
    row = lax.broadcasted_iota(jnp.int32, (h1, b2), 0)
    zero = jnp.zeros((h1, b2), jnp.float32)
    whole, faces, inner = [], [], []
    for c in range(h0):
        total = summed[2 * c] + summed[2 * c + 1]
        down = pltpu.roll(second[2 * c] + second[2 * c + 1], 1, 0)
        up = pltpu.roll(first[2 * c] + first[2 * c + 1], h1 - 1, 0)
        whole.append(total)
        faces.append(jnp.where(row == 0, down, jnp.where(row == h1 - 1, up, zero)))
        near = 2.0 * total + jnp.where(row > 0, down, zero) + jnp.where(row < h1 - 1, up, zero)
        if c > 0:
            near = near + summed[2 * c - 1]
        if c < h0 - 1:
            near = near + summed[2 * c + 2]
        inner.append(near)

    def pack(planes):
        half = len(planes) // 2
        return [jnp.concatenate([planes[i], planes[i + half]], axis=1) for i in range(half)]

    ends = [jnp.concatenate([summed[b0 - 1], summed[0]], axis=1)]
    stacked = jnp.concatenate(pack(whole) + pack(faces) + pack(inner) + ends + [jnp.zeros((8, 2 * b2), jnp.float32)], axis=0)
    parts = parts_of(stacked, 3)
    weights = own[...]
    result = jnp.dot(
        jnp.concatenate(parts, axis=1),
        jnp.concatenate([weights] * 3, axis=0),
        preferred_element_type=jnp.float32,
    )
    n = h0 // 2 * h1
    shape = block.shape
    mine = result[:n, :b2]
    block[...] = mine.reshape(shape)
    across[...] = result[:n, b2 : 2 * b2].reshape(shape)
    along_rows[...] = result[n : 2 * n, :b2].reshape(shape)
    along_planes[...] = result[3 * n : 3 * n + h1, :b2]
    rest[...] = (alpha * mine + beta * (result[2 * n : 3 * n, :b2] + result[:n, 2 * b2 :])).reshape(shape)


def beyond(place, counts):
    x, y, z = place
    return (x, lax.rem(y - 1 + 2 * lax.rem(y, 2) + counts[1], counts[1]), z)


def send_all(counts, block, landing, sems):
    send, recv, relay_send, relay_recv = sems
    me = position()
    mine = landing.at[slot(me, counts)]
    copies = []
    for n, offset in enumerate(chip_offsets(counts)):
        copies.append(remote(block, mine, send.at[n], recv.at[n], shifted(me, counts, offset)))
        copies[-1].start()
    n = len(copies)
    relays = [remote(block, mine, relay_send.at[n], relay_recv.at[n], partner_of(me))]
    relays[-1].start()
    return copies, relays


def relay_all(counts, started, landing, sems):
    relay_send, relay_recv = sems[2:]
    me = position()
    copies, relays = started
    for n, offset in enumerate(chip_offsets(counts)):
        copies[n].wait_recv()
        source = shifted(me, counts, tuple(-step for step in offset))
        arrived = landing.at[slot(source, counts)]
        relays.append(remote(arrived, arrived, relay_send.at[n], relay_recv.at[n], partner_of(me)))
        relays[-1].start()


def end_all(counts, started, block, landing):
    copies, relays = started
    landing[slot(position(), counts)] = block[...]
    for copy in copies:
        copy.wait_send()
    for copy in relays:
        copy.wait()


def prepare(k, many, few, shift):
    diagonal0, diagonal1, diagonal2 = (6.0 * 0.25**level + shift for level in range(3))
    sigma0, sigma1, sigma2 = diagonal0 - 6.0, diagonal1 - 1.5, diagonal2 - 0.375
    damp0, damp1, damp2 = DAMPING / diagonal0, DAMPING / diagonal1, DAMPING / diagonal2
    down, pre, fine_q, out_q, out_g, out_e, cross = many
    by_row, by_lane = k["by_row"], k["by_lane"]
    lanes = by_lane.shape[1]

    def level1(i):
        rows = pl.ds(pl.multiple_of(8 * i, 8), 8)
        column = by_row[rows, :]

        def tall(n):
            return jnp.broadcast_to(column[:, n : n + 1], (8, lanes))

        def wide(n):
            return jnp.broadcast_to(by_lane[n : n + 1, :], (8, lanes))

        r, p, q = (tall(n) * wide(n) for n in range(3))
        a = 0.25 * (tall(3) + wide(3)) + sigma1
        s = 1.0 - damp1 * a
        down[rows, :] = r
        pre[rows, :] = r * s
        fine_q[rows, :] = a * q
        out_q[rows, :] = s * s * q
        out_g[rows, :] = damp1 * (1.0 + s)
        out_e[rows, :] = s * p
        c0, c1, c2 = tall(4), tall(5), tall(6)
        first = sigma0 * c0 + c1 - damp0 * ((sigma0 * sigma0) * c0 + (2.0 * sigma0) * c1 + c2)
        second = c0 - (2.0 * damp0) * (sigma0 * c0 + c1)
        cross[rows, :] = first * wide(4) + second * wide(5) - (damp0 * c0) * wide(6)

    loop(by_row.shape[0] // 8, level1)
    rows2, lanes2 = few[0].shape
    column = by_row[:rows2, :]

    def tall(n):
        return jnp.broadcast_to(column[:, n : n + 1], (rows2, lanes2))

    def wide(n):
        return jnp.broadcast_to(by_lane[n : n + 1, :lanes2], (rows2, lanes2))

    r, p, q = (tall(n) * wide(n) for n in (8, 9, 10))
    a = 0.0625 * (tall(11) + wide(11)) + sigma2
    s = 1.0 - damp2 * a
    values = (r, r * s, a * q, s * s * q, damp2 * (1.0 + s), s * p)
    for ref, value in zip(few, values):
        ref[...] = value
    k["inverse"][...] = 1.0 / (k["eigen"][...] + shift)


def level2(k, few, g):
    down, pre, fine_q, out_q, out_g, out_e = few
    e = unfold(fold(pre[...] * g) * k["inverse"][...])
    return out_g[...] * g + out_e[...] * e


def level2_full(k, few, g):
    down, pre, fine_q, out_q, out_g, out_e = few
    start = unfold(fold(down[...] * g) * k["inverse"][...])
    e = unfold(fold(pre[...] * (g - fine_q[...] * start)) * k["inverse"][...])
    return out_q[...] * start + out_g[...] * g + out_e[...] * e


def blocks_of(spectrum, i):
    rows2, lanes2 = spectrum.shape[0] // 4, spectrum.shape[1] // 2
    for a in range(4):
        start = pl.multiple_of(a * rows2 + 8 * i, 8)
        for c in range(2):
            yield (pl.ds(start, 8), pl.ds(c * lanes2, lanes2))


def spectral_u(k, many, few, spectrum, coupled, coarse):
    down, pre, fine_q, out_q, out_g, out_e, cross = many
    first, second, third = coarse
    steps = first.shape[0] // 8

    def at(i):
        return pl.ds(pl.multiple_of(8 * i, 8), 8)

    def restrict(i):
        first[at(i), :] = sum(down[w] * spectrum[w] for w in blocks_of(spectrum, i))

    loop(steps, restrict)
    second[...] = level2_full(k, few, first[...])

    def residue(i):
        u = second[at(i), :]
        first[at(i), :] = sum(pre[w] * (spectrum[w] - fine_q[w] * u) for w in blocks_of(spectrum, i))

    loop(steps, residue)
    third[...] = level2(k, few, first[...])

    def finish(i):
        u, e = second[at(i), :], third[at(i), :]
        for w in blocks_of(spectrum, i):
            value = out_q[w] * u + out_g[w] * spectrum[w] + out_e[w] * e
            spectrum[w] = value
            coupled[w] = cross[w] * value

    loop(steps, finish)


def spectral_e(k, many, few, spectrum, coupled, coarse):
    pre, out_g, out_e = many[1], many[4], many[5]
    first, second = coarse[:2]
    steps = first.shape[0] // 8

    def at(i):
        return pl.ds(pl.multiple_of(8 * i, 8), 8)

    def residue(i):
        total = None
        for w in blocks_of(spectrum, i):
            value = spectrum[w] - coupled[w]
            spectrum[w] = value
            total = pre[w] * value if total is None else total + pre[w] * value
        first[at(i), :] = total

    loop(steps, residue)
    second[...] = level2(k, few, first[...])

    def finish(i):
        e = second[at(i), :]
        for w in blocks_of(spectrum, i):
            spectrum[w] = out_g[w] * spectrum[w] + out_e[w] * e

    loop(steps, finish)


def transform(k, counts, landing, g, spectrum):
    unpack(landing, counts, g)
    m0, m1, m2 = g.shape
    spectrum[...] = by_left(k["forward_rows"], by_right(g[...].reshape(m0 * m1, m2), k["forward_lanes"]))


def evaluate(k, kind, spectrum, out):
    values = by_right(by_left(k[kind + "_rows"], spectrum[...]), k[kind + "_lanes"])
    out[...] = values.reshape(out.shape)


def neighbours_of(v, p):
    center = v[p]
    return center, v[p - 1] + v[p + 1] + around(center)


def fast_kernel(names, counts, *refs):
    count = len(names)
    outside = dict(zip(names, refs))
    shift_ref, source_ref, out, *rest = refs[count:]
    k = dict(zip(names, rest[:count]))
    rest = rest[count:]
    landing_f, landing_h = rest[:2]
    faces_in = rest[2:8]
    halos = rest[8:11]
    block_f, block_h, across, along_rows, along_planes, local = rest[11:17]
    own_planes, own_rows, own_columns = rest[17:20]
    many, few, coarse = rest[20:27], rest[27:33], rest[33:36]
    k["inverse"], g, spectrum, coupled, wide, w, f, source = rest[36:44]
    table_sems, face_send, face_recv, halo_send, halo_recv = rest[44:49]
    sems_f, sems_h = rest[49:53], rest[53:57]

    shift = shift_ref[0]
    me = position()
    barrier = pltpu.get_barrier_semaphore()
    places = [shifted(me, counts, offset) for offset in chip_offsets(counts)]
    places += [partner_of(me), beyond(me, counts)]
    greet(barrier, places)
    loads = {"source": pltpu.make_async_copy(source_ref, source, table_sems.at[count])}
    loads["source"].start()
    for n, name in enumerate(names):
        loads[name] = pltpu.make_async_copy(outside[name], k[name], table_sems.at[n])
        loads[name].start()

    b0, b1, b2 = source.shape
    diagonal = 6.0 + shift
    damp = DAMPING / diagonal
    loads["source"].wait()
    loads["own"].wait()
    parts = (block_f, across, along_rows, along_planes, local)
    own_parts(source, k["own"], parts, 1.0 - damp * diagonal, damp)
    own_planes[0] = source[0]
    own_planes[1] = source[b0 - 1]
    own_rows[0] = source[:, pl.ds(0, 1), :]
    own_rows[1] = source[:, pl.ds(b1 - 1, 1), :]
    turned = source[...].reshape(b0 * b1, b2).T
    own_columns[0] = turned[:8]
    own_columns[1] = turned[b2 - 8 :]
    pl.semaphore_wait(barrier, len(places))

    faces = face_offsets(counts)
    order = (0, 2, 1)
    sent = (along_planes, along_rows, across)
    first = []
    for n, (offset, axis, side) in enumerate(faces):
        place = shifted(me, counts, offset)
        copy = remote(sent[order[axis]], faces_in[2 * order[axis] + 1 - side], face_send.at[n], face_recv.at[n], place)
        copy.start()
        first.append(copy)
    started_f = send_all(counts, block_f, landing_f, sems_f)
    buffers = ((own_planes, halos[0]), (own_rows, halos[1]), (own_columns, halos[2]))
    last = []
    for n, (offset, axis, side) in enumerate(faces):
        mine, halo = buffers[order[axis]]
        place = shifted(me, counts, offset)
        last.append(remote(mine.at[side], halo.at[1 - side], halo_send.at[n], halo_recv.at[n], place))
        last[-1].start()

    for name in ("by_row", "by_lane", "eigen"):
        loads[name].wait()
    prepare(k, many, few, shift)
    for copy in first:
        copy.wait()
    shape = local.shape
    lane = lax.rem(lax.broadcasted_iota(jnp.int32, shape, 2), b2 // 2)
    row = lax.broadcasted_iota(jnp.int32, shape, 1)
    from_planes, from_rows, from_lanes = faces_in[:2], faces_in[2:4], faces_in[4:6]
    total = jnp.where(lane == 0, from_lanes[0][...], 0.0) + jnp.where(lane == b2 // 2 - 1, from_lanes[1][...], 0.0)
    total = total + jnp.where(row == 0, from_rows[0][...], 0.0) + jnp.where(row == shape[1] - 1, from_rows[1][...], 0.0)
    block_h[...] = local[...] + damp * total
    low = lax.broadcasted_iota(jnp.int32, shape[1:], 1) < b2 // 2
    block_h[0] = block_h[0] + damp * jnp.where(low, from_planes[0][...], 0.0)
    end = shape[0] - 1
    block_h[end] = block_h[end] + damp * jnp.where(low, 0.0, from_planes[1][...])
    started_h = send_all(counts, block_h, landing_h, sems_h)

    relay_all(counts, started_f, landing_f, sems_f)
    for copy in last:
        copy.wait()
    f[...] = jnp.zeros_like(f)
    rows, lanes = pl.ds(0, b1), pl.ds(0, b2)
    f[1 : b0 + 1, rows, lanes] = source[...]
    f[0, rows, lanes] = halos[0][0]
    f[b0 + 1, rows, lanes] = halos[0][1]
    f[1 : b0 + 1, pl.ds(b1, 1), lanes] = halos[1][1]
    f[1 : b0 + 1, pl.ds(b1 + 7, 1), lanes] = halos[1][0]
    middle = jnp.zeros((b2 - 16, b0 * b1), jnp.float32)
    turned = jnp.concatenate([halos[2][1], middle, halos[2][0]], axis=0)
    f[1 : b0 + 1, rows, pl.ds(b2, b2)] = turned.T.reshape(b0, b1, b2)
    end_all(counts, started_f, block_f, landing_f)
    for name in names:
        if name not in ("own", "by_row", "by_lane", "eigen"):
            loads[name].wait()
    transform(k, counts, landing_f, g, spectrum)
    spectral_u(k, many, few, spectrum, coupled, coarse)

    relay_all(counts, started_h, landing_h, sems_h)
    evaluate(k, "cubic", spectrum, wide)
    keep = 1.0 - damp * diagonal

    def before(p):
        center, beside = neighbours_of(wide, p + 1)
        f[p] = keep * center + damp * (beside + f[p])

    loop(b0 + 2, before)
    end_all(counts, started_h, block_h, landing_h)
    transform(k, counts, landing_h, g, spectrum)
    spectral_e(k, many, few, spectrum, coupled, coarse)
    evaluate(k, "linear", spectrum, w)

    def add(p):
        w[p] = w[p] + f[p]

    loop(b0 + 2, add)

    def after(p):
        center, beside = neighbours_of(w, p + 1)
        out[p] = (keep * center + damp * beside)[:b1, :b2] + damp * source[p]

    loop(b0, after)


def fast_per_device(counts, source, shift):
    nx, ny, nz = counts
    b0, b1, b2 = source.shape
    sizes = (b0 * nx, b1 * nz, b2 * ny)
    table = fast_constants(source.shape, sizes)
    m0, m1, m2 = (size // 2 for size in sizes)
    rows = m0 * m1
    packed = (b0 // 4, b1 // 2, b2)
    devices = nx * ny * nz
    chips = devices // 2
    vmem = pl.BlockSpec(memory_space=pltpu.VMEM)

    def field(*shape):
        return pltpu.VMEM(shape, jnp.float32)

    def in_hbm(value):
        return pltpu.with_memory_space_constraint(value, pltpu.HBM)

    names = tuple(table)
    scratch = [pltpu.VMEM(table[name].shape, table[name].dtype) for name in names]
    scratch += [field(devices, *packed)] * 2
    scratch += [field(*packed[1:])] * 2 + [field(*packed)] * 4
    scratch += [field(2, b1, b2), field(2, b0, 1, b2), field(2, 8, b0 * b1)]
    scratch += [field(*packed)] * 4 + [field(*packed[1:]), field(*packed)]
    scratch += [field(2, b1, b2), field(2, b0, 1, b2), field(2, 8, b0 * b1)]
    scratch += [field(rows, m2)] * 7 + [field(rows // 4, m2 // 2)] * 9
    scratch += [field(rows // 16, m2 // 2), field(m0, m1, m2), field(rows, m2), field(rows, m2)]
    scratch += [field(b0 + 4, b1 + 8, 2 * b2), field(b0 + 2, b1 + 8, 2 * b2), field(b0 + 2, b1 + 8, 2 * b2)]
    scratch += [field(*source.shape)]
    dma = pltpu.SemaphoreType.DMA
    scratch += [dma((len(names) + 1,))] + [dma((6,))] * 4
    scratch += ([dma((max(chips - 1, 1),))] * 2 + [dma((chips,))] * 2) * 2
    return pl.pallas_call(
        functools.partial(fast_kernel, names, counts),
        out_shape=jax.ShapeDtypeStruct(source.shape, jnp.float32),
        in_specs=[pl.BlockSpec(memory_space=pltpu.HBM)] * len(names)
        + [pl.BlockSpec(memory_space=pltpu.SMEM), pl.BlockSpec(memory_space=pltpu.HBM)],
        out_specs=vmem,
        scratch_shapes=scratch,
        compiler_params=pltpu.CompilerParams(
            vmem_limit_bytes=40 * 1024 * 1024, collective_id=0, has_side_effects=True
        ),
    )(*[in_hbm(jnp.asarray(table[name])) for name in names], shift, in_hbm(source))


def small_enough(counts, block):
    (nx, ny, nz), (b0, b1, b2) = counts, block
    rows = (b0 * nx // 2) * (b1 * nz // 2)
    return rows <= 512 and rows % 128 == 0 and b2 == 128 and b1 == 16 and b0 % 4 == 0 and ny * b2 % 512 == 0 and min(counts) > 1


def dispatch(counts, source, shift):
    run = fast_per_device if small_enough(counts, source.shape) else per_device
    return run(counts, source, shift)


def solution(mesh):
    counts = tuple(mesh.shape[name] for name in NAMES)
    return jax.shard_map(
        functools.partial(dispatch, counts),
        mesh=mesh,
        in_specs=(P("gx", "gz", "gy"), P()),
        out_specs=P("gx", "gz", "gy"),
        check_vma=False,
    )
```

```python
import functools

import jax
import jax.numpy as jnp
import numpy as np
from jax import lax
from jax.experimental import pallas as pl
from jax.experimental.pallas import tpu as pltpu
from jax.sharding import PartitionSpec as P

LEVELS = 4
DAMPING = 6.0 / 7.0
PRECISE = lax.Precision.HIGHEST
CUBIC = (
    {-2: -5.0 / 128.0, -1: 35.0 / 128.0, 0: 105.0 / 128.0, 1: -7.0 / 128.0},
    {-1: -7.0 / 128.0, 0: 105.0 / 128.0, 1: 35.0 / 128.0, 2: -5.0 / 128.0},
)
LINEAR = ({-1: 0.25, 0: 0.75}, {0: 0.75, 1: 0.25})
NAMES = ("gx", "gy", "gz")
MESH = pl.DeviceIdType.MESH


def basis(count):
    cells = np.arange(count)
    columns, cosines = [], []
    for m in range(count):
        k = (m + 1) // 2
        angle = 2.0 * np.pi * k * cells / count
        column = np.cos(angle) if m % 2 == 1 or m == 0 else np.sin(angle)
        columns.append(column / np.sqrt(np.sum(column**2)))
        cosines.append(np.cos(2.0 * np.pi * k / count))
    return np.stack(columns, axis=1), np.array(cosines, np.float32)


def interpolation(coarse_count, fine_cells, weights):
    matrix = np.zeros((len(fine_cells), coarse_count))
    for row, cell in enumerate(fine_cells):
        for offset, weight in weights[cell % 2].items():
            matrix[row, (cell // 2 + offset) % coarse_count] += weight
    return matrix


def pairs(coarse_count):
    return np.kron(np.eye(coarse_count), np.ones((1, 2)))


def blocked(matrix):
    count = max(1, 128 // matrix.shape[1])
    return np.kron(np.eye(count), matrix)


def constants(block, sizes):
    b0, b1, b2 = block
    m0, m1, m2 = (size // 2 for size in sizes)
    q0, q1, q2 = (size // 4 for size in sizes)
    c0, c1, c2 = (size // 8 for size in sizes)
    table = {}
    table["own_rows"] = np.kron(np.eye(b0 // 2), pairs(b1 // 2))
    lanes = 0.125 * pairs(b2 // 2).T
    table["own_lo"] = np.concatenate([lanes, np.zeros_like(lanes)], axis=1)
    table["own_hi"] = np.concatenate([np.zeros_like(lanes), lanes], axis=1)
    table["down_rows"] = blocked(pairs(q1))
    table["down_lanes"] = 0.125 * pairs(q2).T
    window_lanes = [b2 + j for j in range(b2 // 2)] + [j - b2 for j in range(b2 // 2, 2 * b2)]
    window_rows = [j - 8 for j in range(b1 + 16)]
    for name, weights in (("cubic", CUBIC), ("linear", LINEAR)):
        table[name + "_rows1"] = blocked(interpolation(q1, range(m1), weights))
        table[name + "_lanes1"] = interpolation(q2, range(m2), weights).T
        table[name + "_rows0"] = blocked(interpolation(m1, window_rows, weights))
        table[name + "_lanes0"] = interpolation(m2, window_lanes, weights).T
    (u0, cos0), (u1, cos1), (u2, cos2) = basis(c0), basis(c1), basis(c2)
    table["spectrum_rows"] = np.kron(u0.T @ pairs(c0), u1.T @ pairs(c1))
    table["spectrum_lanes"] = 0.125 * pairs(c2).T @ u2
    for name, weights in (("cubic", CUBIC), ("linear", LINEAR)):
        table[name + "_rows2"] = np.kron(
            interpolation(c0, range(q0), weights) @ u0, interpolation(c1, range(q1), weights) @ u1
        )
        table[name + "_lanes2"] = u2.T @ interpolation(c2, range(q2), weights).T
    two = np.float32(2.0)
    eigen = (
        np.float32(6.0)
        - two * cos0[:, None, None]
        - two * cos1[None, :, None]
        - two * cos2[None, None, :]
    )
    table["eigen"] = (np.float32(0.25 ** (LEVELS - 1)) * eigen).reshape(c0 * c1, c2)
    wide = ("spectrum_rows", "spectrum_lanes", "eigen")
    return {
        name: np.asarray(
            value, np.float32 if name in wide or name.endswith("2") else jnp.bfloat16
        )
        for name, value in table.items()
    }


def dot(a, b):
    return jnp.dot(a, b, precision=PRECISE, preferred_element_type=jnp.float32)


def parts_of(values, pieces):
    parts = []
    for n in range(pieces):
        parts.append(values.astype(jnp.bfloat16))
        if n + 1 < pieces:
            values = values - parts[-1].astype(jnp.float32)
    return parts[::-1]


def right(values, matrix, pieces):
    terms = [
        jnp.dot(part, matrix, preferred_element_type=jnp.float32)
        for part in parts_of(values, pieces)
    ]
    return sum(terms[1:], terms[0])


def left(matrix, values, pieces):
    terms = [
        jnp.dot(matrix, part, preferred_element_type=jnp.float32)
        for part in parts_of(values, pieces)
    ]
    return sum(terms[1:], terms[0])


def around(plane):
    rows, lanes = plane.shape
    total = pltpu.roll(plane, 1, 0) + pltpu.roll(plane, rows - 1, 0)
    return total + (pltpu.roll(plane, 1, 1) + pltpu.roll(plane, lanes - 1, 1))


def around_all(values):
    first = jnp.concatenate([values[1:], values[:1]], axis=0)
    first = first + jnp.concatenate([values[-1:], values[:-1]], axis=0)
    for axis in (1, 2):
        first = first + pltpu.roll(values, 1, axis)
        first = first + pltpu.roll(values, values.shape[axis] - 1, axis)
    return first


def row_blocks(matrix, values, pieces):
    depth = matrix.shape[1]
    return jnp.concatenate(
        [left(matrix, values[i : i + depth], pieces) for i in range(0, values.shape[0], depth)], axis=0
    )


def loop(count, body):
    def step(i, carry):
        body(i)
        return carry

    lax.fori_loop(0, count, step, 0, unroll=4 if count % 4 == 0 else 2)


def close(ref):
    count = ref.shape[0] - 2
    ref[0] = ref[count]
    ref[count + 1] = ref[1]


def defect_plane(v, p, g, weight, diagonal):
    center = v[p]
    beside = v[p - 1] + v[p + 1] + around(center)
    return center, g - (diagonal * center - weight * beside)


def restrict_own(k, summed):
    b_half, rows, lanes = summed.shape
    folded = left(k["own_rows"][...], summed.reshape(b_half * rows, lanes), 3)
    half = folded.shape[0] // 2
    return right(folded[:half], k["own_lo"][...], 3) + right(folded[half:], k["own_hi"][...], 3)


def unpack(gathered, counts, g):
    nx, ny, nz = counts
    x, y, z = (lax.axis_index(name) for name in NAMES)
    half, rows, lanes = gathered.shape[1:]
    low = lax.broadcasted_iota(jnp.int32, (half, rows, lanes), 2) < lanes // 2
    for dx in range(nx):
        for dz in range(nz):
            for pair in range(ny // 2):
                parts = []
                for dy in (2 * pair, 2 * pair + 1):
                    index = (lax.rem(x + dx, nx) * ny + lax.rem(y + dy, ny)) * nz
                    parts.append(gathered[index + lax.rem(z + dz, nz)])
                turned = [pltpu.roll(part, lanes // 2, 2) for part in parts]
                where = (pl.ds(dz * rows, rows), pl.ds(pair * lanes, lanes))
                start = 2 * half * dx
                g[(pl.ds(start, half), *where)] = jnp.where(low, parts[0], turned[1])
                g[(pl.ds(start + half, half), *where)] = jnp.where(low, turned[0], parts[1])


def solve(k, kind, values, shift):
    shape = values.shape
    flat = values.reshape(shape[0] * shape[1], shape[2])
    spectrum = dot(k["spectrum_rows"][...], dot(flat, k["spectrum_lanes"][...]))
    spectrum = spectrum / (k["eigen"][...] + shift)
    fine = dot(k[kind + "_rows2"][...], dot(spectrum, k[kind + "_lanes2"][...]))
    return fine.reshape(shape)


def cycle2(k, v, g, shift):
    weight = 0.25**2
    diagonal = 6.0 * weight + shift
    damp = DAMPING / diagonal
    if v is None:
        v = damp * g
    else:
        v = v + damp * (g - (diagonal * v - weight * around_all(v)))
    v = v + solve(k, "linear", g - (diagonal * v - weight * around_all(v)), shift)
    return v + damp * (g - (diagonal * v - weight * around_all(v)))


def down(k, t, shape2):
    flat = row_blocks(k["down_rows"][...], t[...].reshape(-1, t.shape[2]), 3)
    return right(flat, k["down_lanes"][...], 3).reshape(shape2)


def up(k, kind, level, values, z):
    flat = right(values, k[kind + "_lanes" + level][...], 2)
    z[...] = row_blocks(k[kind + "_rows" + level][...], flat, 2).reshape(z.shape)


def blend(z, i, weights, count):
    total = None
    for offset, weight in weights.items():
        index = i + offset
        index = index if count is None else lax.rem(index + count, count)
        term = weight * z[index]
        total = term if total is None else total + term
    return total


def up1(k, kind, values, z, v, add):
    count = z.shape[0]
    up(k, kind, "1", values.reshape(-1, values.shape[2]), z)
    weights = CUBIC if kind == "cubic" else LINEAR

    def body(i):
        for odd in (0, 1):
            p = 2 * i + odd + 1
            value = blend(z, i, weights[odd], count)
            v[p] = v[p] + value if add else value

    loop(count, body)
    close(v)


def cycle1(k, v, u, g, t, z, shift, zero, shape2):
    weight = 0.25
    diagonal = 6.0 * weight + shift
    damp = DAMPING / diagonal
    count = g.shape[0]

    def before(p):
        if zero:
            u[p + 1] = damp * g[p]
        else:
            center, rest = defect_plane(v, p + 1, g[p], weight, diagonal)
            u[p + 1] = center + damp * rest

    loop(count, before)
    close(u)

    def residue(i):
        t[i] = (
            defect_plane(u, 2 * i + 1, g[2 * i], weight, diagonal)[1]
            + defect_plane(u, 2 * i + 2, g[2 * i + 1], weight, diagonal)[1]
        )

    loop(count // 2, residue)
    correction = cycle2(k, None, down(k, t, shape2), shift)
    up1(k, "linear", correction, z, u, True)

    def after(p):
        center, rest = defect_plane(u, p + 1, g[p], weight, diagonal)
        v[p + 1] = center + damp * rest

    loop(count, after)
    close(v)


def window(k, kind, v, zw, span, write):
    count = v.shape[0] - 2
    values = jnp.concatenate([v[count - 3 : count + 1], v[1 : span - 3]], axis=0)
    up(k, kind, "0", values.reshape(-1, values.shape[2]), zw)
    weights = CUBIC if kind == "cubic" else LINEAR

    def body(i):
        for odd in (0, 1):
            write(2 * i + odd, blend(zw, i + 3, weights[odd], None))

    loop(span - 6, body)


def own_defect(v, p, f, weight, diagonal):
    rows, lanes = f.shape
    inside = (pl.ds(8, rows), pl.ds(lanes, lanes))
    wide = v[p + 1, pl.ds(8, rows), :]
    center = wide[:, lanes:]
    beside = v[(p, *inside)] + v[(p + 2, *inside)]
    beside = beside + v[p + 1, pl.ds(7, rows), pl.ds(lanes, lanes)]
    beside = beside + v[p + 1, pl.ds(9, rows), pl.ds(lanes, lanes)]
    beside = beside + pltpu.roll(wide, 1, 1)[:, lanes:]
    beside = beside + pltpu.roll(wide, 2 * lanes - 1, 1)[:, lanes:]
    return center, f - (diagonal * center - weight * beside)


def position():
    return tuple(lax.axis_index(name) for name in NAMES)


def partner_of(place):
    x, y, z = place
    return (x, y + 1 - 2 * lax.rem(y, 2), z)


def shifted(place, counts, offset):
    return tuple(
        lax.rem(at + step + count, count) for at, step, count in zip(place, offset, counts)
    )


def slot(place, counts):
    return (place[0] * counts[1] + place[1]) * counts[2] + place[2]


def chip_offsets(counts):
    nx, ny, nz = counts
    offsets = [
        (dx, dy, dz) for dx in range(nx) for dy in range(0, ny, 2) for dz in range(nz)
    ]

    def hops(offset):
        return sum(min(step, count - step) for step, count in zip(offset, (nx, ny, nz)))

    return sorted(offsets[1:], key=hops, reverse=True)


def face_offsets(counts):
    faces = []
    for axis in range(3):
        for side, step in ((0, -1), (1, 1)):
            offset = [0, 0, 0]
            offset[axis] = step
            faces.append((tuple(offset), axis, side))
    return faces


def greet(barrier, places):
    for place in places:
        pl.semaphore_signal(barrier, inc=1, device_id=place, device_id_type=MESH)


def remote(src, dst, send, recv, place):
    return pltpu.make_async_remote_copy(
        src_ref=src, dst_ref=dst, send_sem=send, recv_sem=recv, device_id=place, device_id_type=MESH
    )


def spread(counts, block, gathered, sems):
    send, recv, relay_send, relay_recv = sems
    me = position()
    partner = partner_of(me)
    along, across = stages(counts)
    number = {offset: n for n, offset in enumerate(chip_offsets(counts))}
    mine = gathered.at[slot(me, counts)]
    copies, relays = {}, []

    def pass_on(offset, source, target, place):
        n = number[offset]
        copies[offset] = remote(source, target, send.at[n], recv.at[n], place)
        copies[offset].start()

    def relay(n, source, target):
        relays.append(remote(source, target, relay_send.at[n], relay_recv.at[n], partner))
        relays[-1].start()

    for offset in along + across:
        pass_on(offset, block, mine, shifted(me, counts, offset))
    relay(len(number), block, mine)

    def arrival(offset):
        copies[offset].wait_recv()
        source = shifted(me, counts, tuple(-step for step in offset))
        return gathered.at[slot(source, counts)]

    def finish():
        gathered[slot(me, counts)] = block[...]
        for first in along[::-1]:
            arrived = arrival(first)
            for second in across:
                place = shifted(me, counts, second)
                pass_on((first[0], second[1], second[2]), arrived, arrived, place)
            relay(number[first], arrived, arrived)
        for first in ((0, 0, 0), *along[::-1]):
            for second in across[::-1]:
                offset = (first[0], second[1], second[2])
                arrived = arrival(offset)
                relay(number[offset], arrived, arrived)
        for copy in copies.values():
            copy.wait_send()
        for copy in relays:
            copy.wait()

    return finish


def stages(counts):
    offsets = chip_offsets(counts)
    along = [offset for offset in offsets if offset[1:] == (0, 0)]
    across = [offset for offset in offsets if offset[0] == 0]
    return along, across


def gather_places(counts):
    me = position()
    along, across = stages(counts)
    return [shifted(me, counts, offset) for offset in along + across] + [partner_of(me)]


def first_part(k, counts, source, f, gathered, halos, block, owns, sems, face_sems):
    own_planes, own_rows, own_columns = owns
    planes, rows, columns = halos
    face_send, face_recv = face_sems
    me = position()
    barrier = pltpu.get_barrier_semaphore()
    faces = face_offsets(counts)
    places = gather_places(counts) + [shifted(me, counts, offset) for offset, _, _ in faces]
    greet(barrier, places)
    b0, b1, b2 = source.shape
    summed = source[...].reshape(b0 // 2, 2, b1, b2)
    block[...] = restrict_own(k, summed[:, 0] + summed[:, 1]).reshape(block.shape)
    own_planes[0] = source[0]
    own_planes[1] = source[b0 - 1]
    own_rows[0] = source[:, pl.ds(0, 1), :]
    own_rows[1] = source[:, pl.ds(b1 - 1, 1), :]
    turned = source[...].reshape(b0 * b1, b2).T
    own_columns[0] = turned[:8]
    own_columns[1] = turned[b2 - 8 :]
    pl.semaphore_wait(barrier, len(places))
    finish = spread(counts, block, gathered, sems)
    buffers = ((own_planes, planes), (own_rows, rows), (own_columns, columns))
    order = (0, 2, 1)
    copies = []
    for n, (offset, axis, side) in enumerate(faces):
        own, halo = buffers[order[axis]]
        place = shifted(me, counts, offset)
        copies.append(
            remote(own.at[side], halo.at[1 - side], face_send.at[n], face_recv.at[n], place)
        )
        copies[-1].start()
    f[...] = jnp.zeros_like(f)
    f[1 : b0 + 1, pl.ds(8, b1), pl.ds(b2, b2)] = source[...]
    finish()
    for copy in copies:
        copy.wait()


def second_part(k, counts, shape2, span, shift, gathered, source, halos, out, buffers):
    g, v, u, t, z, zw, v0, v1, f, summed = buffers
    plane_halo, row_halo, column_halo = halos
    unpack(gathered, counts, g)
    b0, b1, b2 = source.shape
    rows, lanes = pl.ds(8, b1), pl.ds(b2, b2)
    f[0, rows, lanes] = plane_halo[0]
    f[b0 + 1, rows, lanes] = plane_halo[1]
    f[1 : b0 + 1, pl.ds(7, 1), lanes] = row_halo[0]
    f[1 : b0 + 1, pl.ds(8 + b1, 1), lanes] = row_halo[1]
    middle = jnp.zeros((b2 - 16, b0 * b1), jnp.float32)
    turned = jnp.concatenate([column_halo[1], middle, column_halo[0]], axis=0)
    f[1 : b0 + 1, rows, pl.ds(0, b2)] = turned.T.reshape(b0, b1, b2)
    def pair_sum(i):
        t[i] = g[2 * i] + g[2 * i + 1]

    loop(g.shape[0] // 2, pair_sum)
    forcing2 = down(k, t, shape2)
    iterate2 = cycle2(k, solve(k, "cubic", forcing2, shift), forcing2, shift)
    up1(k, "cubic", iterate2, z, v, False)
    cycle1(k, v, u, g, t, z, shift, False, shape2)

    def put(p, value):
        v0[p] = value

    window(k, "cubic", v, zw, span, put)
    diagonal = 6.0 + shift
    damp = DAMPING / diagonal

    def before(p):
        center, rest = defect_plane(v0, p + 1, f[p], 1.0, diagonal)
        v1[p] = center + damp * rest

    loop(b0 + 2, before)

    def residue(i):
        summed[i] = (
            own_defect(v1, 2 * i, source[2 * i], 1.0, diagonal)[1]
            + own_defect(v1, 2 * i + 1, source[2 * i + 1], 1.0, diagonal)[1]
        )

    loop(b0 // 2, residue)
    out[...] = restrict_own(k, summed[...]).reshape(out.shape)


def third_part(k, counts, shape2, span, shift, gathered, source, out, buffers):
    g, v, u, t, z, zw, w, v1 = buffers[:8]
    unpack(gathered, counts, g)
    cycle1(k, v, u, g, t, z, shift, True, shape2)
    b0 = source.shape[0]

    def put(p, value):
        w[p] = value

    window(k, "linear", v, zw, span, put)

    def add(p):
        w[p] = v1[p] + w[p + 1]

    loop(b0 + 2, add)
    diagonal = 6.0 + shift
    damp = DAMPING / diagonal

    def after(p):
        center, rest = own_defect(w, p, source[p], 1.0, diagonal)
        out[p] = center + damp * rest

    loop(b0, after)


def kernel(names, counts, shape2, span, *refs):
    k = dict(zip(names, refs))
    shift_ref, source, out, *rest = refs[len(names) :]
    shift = shift_ref[0]
    landing, later, *halos = rest[:5]
    block, block_later, *owns = rest[5:10]
    buffers = rest[10:20]
    sems, sems_later, face_sems = rest[20:24], rest[24:28], rest[28:30]
    f = buffers[8]
    first_part(k, counts, source, f, landing, halos, block, owns, sems, face_sems)
    second_part(k, counts, shape2, span, shift, landing, source, halos, block_later, buffers)
    spread(counts, block_later, later, sems_later)()
    third_part(k, counts, shape2, span, shift, later, source, out, buffers)


def per_device(counts, source, shift):
    nx, ny, nz = counts
    b0, b1, b2 = source.shape
    sizes = (b0 * nx, b1 * nz, b2 * ny)
    table = constants(source.shape, sizes)
    m0, m1, m2 = (size // 2 for size in sizes)
    shape2 = tuple(size // 4 for size in sizes)
    span = b0 // 2 + 8
    wide = (b1 + 16, 2 * b2)
    packed = (b0 // 4, b1 // 2, b2)
    devices = nx * ny * nz
    chips = devices // 2
    vmem = pl.BlockSpec(memory_space=pltpu.VMEM)

    def field(*shape):
        return pltpu.VMEM(shape, jnp.float32)

    faces = [field(2, b1, b2), field(2, b0, 1, b2), field(2, 8, b0 * b1)]
    buffers = [
        field(m0, m1, m2),
        field(m0 + 2, m1, m2),
        field(m0 + 2, m1, m2),
        field(m0 // 2, m1, m2),
        field(m0 // 2, m1, m2),
        field(span, *wide),
        field(b0 + 4, *wide),
        field(b0 + 2, *wide),
        field(b0 + 2, *wide),
        field(b0 // 2, b1, b2),
    ]
    sems = [pltpu.SemaphoreType.DMA((max(chips - 1, 1),))] * 2
    sems += [pltpu.SemaphoreType.DMA((chips,))] * 2
    landing = [field(devices, *packed)] * 2 + faces
    names = tuple(table)
    return pl.pallas_call(
        functools.partial(kernel, names, counts, shape2, span),
        out_shape=jax.ShapeDtypeStruct(source.shape, jnp.float32),
        in_specs=[vmem] * len(names) + [pl.BlockSpec(memory_space=pltpu.SMEM), vmem],
        out_specs=vmem,
        scratch_shapes=landing
        + [field(*packed)] * 2
        + faces
        + buffers
        + sems * 2
        + [pltpu.SemaphoreType.DMA((6,))] * 2,
        compiler_params=pltpu.CompilerParams(
            vmem_limit_bytes=60 * 1024 * 1024, collective_id=0, has_side_effects=True
        ),
    )(*[jnp.asarray(table[name]) for name in names], shift, source)


def modes(count, depth):
    if depth == 0:
        return [(0, k) for k in range(count // 2)] + [(1, k) for k in range(1, count // 2 + 1)]
    half = count // 2
    low = modes(half, depth - 1)
    high = []
    for kind, k in low:
        if kind == 0:
            high.append((0, half - k if k else half // 2))
        else:
            high.append((1, half - k if k < half // 2 else half))
    return low + high


def waves(count, order):
    cells = (np.arange(count) + 0.5) * (2.0 * np.pi / count)
    return np.stack([np.sin(k * cells) if kind else np.cos(k * cells) for kind, k in order], axis=1)


def analysis(waves_):
    return waves_.T / np.sum(waves_**2, axis=0)[:, None]


def two_blocks(matrix, axis):
    first, second = np.split(matrix, 2, axis=axis)
    return np.concatenate([np.diag(first), np.diag(second)])


def factors(m):
    orders = modes(m, 2), modes(m // 2, 1), modes(m // 4, 0)
    bases = [waves(len(order), order) for order in orders]
    t = {"waves": bases[0]}
    for level, fine, coarse in (("1", bases[0], bases[1]), ("2", bases[1], bases[2])):
        n = fine.shape[0]
        t["r" + level] = two_blocks(analysis(coarse) @ (0.5 * pairs(n // 2)) @ fine, 1)
        for name, weights in (("p", LINEAR), ("q", CUBIC)):
            matrix = interpolation(n // 2, range(n), weights)
            t[name + level] = two_blocks(analysis(fine) @ matrix @ coarse, 0)
        order = orders[int(level) - 1]
        t["e" + level] = np.array([2.0 - 2.0 * np.cos(2.0 * np.pi * k / n) for _, k in order])
    t["c3"] = np.array([np.cos(2.0 * np.pi * k / (m // 4)) for _, k in orders[2]], np.float32)
    fine = np.eye(2 * m)
    lap = 2.0 * fine - np.roll(fine, 1, 0) - np.roll(fine, -1, 0)
    current = interpolation(m, range(2 * m), CUBIC) @ bases[0]
    for i in range(3):
        t[f"m{i}"] = np.sum(analysis(bases[0]).T * ((0.5 * pairs(m)) @ current), axis=0)
        current = lap @ current
    return t


def near(matrix, axis=0):
    return np.roll(matrix, 1, axis) + np.roll(matrix, -1, axis)


def synthesis(t, cells, weights, powers):
    m = t["waves"].shape[0]
    matrix = interpolation(m, range(2 * m), weights) @ t["waves"]
    result = []
    for _ in range(powers):
        result.append(matrix[np.array(cells) % (2 * m)])
        matrix = near(matrix)
    return result


def pick(matrix, rows, columns):
    return matrix[np.array(rows) % matrix.shape[0]][:, np.array(columns) % matrix.shape[1]]


def late_kinds(m, rows, columns):
    plain = interpolation(m, range(2 * m), LINEAR)
    return [pick(kind, rows, columns) for kind in (plain, near(plain), near(plain, 1), near(near(plain), 1))]


def mixed(p, r):
    return [
        np.kron(p[0], r[0]),
        np.kron(p[1], r[0]) + np.kron(p[0], r[1]),
        np.kron(p[2], r[0]) + np.kron(p[0], r[2]),
        np.kron(p[3], r[0]) + np.kron(p[0], r[3]) + np.kron(p[2], r[1]) + np.kron(p[1], r[2]),
    ]


def exact(matrix):
    result = np.asarray(matrix, jnp.bfloat16)
    assert np.all(result.astype(np.float64) == matrix)
    return result


def halves(matrix, axis):
    high = np.asarray(matrix, jnp.bfloat16)
    low = np.asarray(matrix - high.astype(np.float64), jnp.bfloat16)
    return np.concatenate([high, low], axis=axis)


def halved_rows(m0, m1):
    index = np.arange(m0 * m1).reshape(2, 2, 2, m0 // 8, 2, 2, m1 // 4)
    index = index.transpose(2, 0, 4, 1, 5, 3, 6).reshape(2, 4, -1)
    return index, index[:, 0].reshape(-1), index.reshape(-1)


def own_table(half):
    count = 2 * half
    four = sum(np.roll(np.kron(np.eye(half), np.eye(2)[:, :1]), s, axis=0) for s in (-1, 0, 1, 2))
    four[count - 1, 0] = 0.0
    four[0, half - 1] = 0.0
    beside = np.zeros((count, half))
    beside[count - 1, 0] = beside[0, half - 1] = 1.0
    own = np.zeros((2, count, 3, 2, half))
    for n, part in enumerate((pairs(half).T, beside, four)):
        for s in range(2):
            own[s, :, n, s] = 0.125 * part
    return np.asarray(own.reshape(2 * count, 3 * count), jnp.bfloat16)


def two_levels(count):
    whole = 2 * count
    fine, half = np.eye(whole), np.eye(whole // 2)
    near, near1 = (np.roll(e, 1, 0) + np.roll(e, -1, 0) for e in (fine, half))
    down, down1 = pairs(whole // 2), pairs(whole // 4)
    start = count // 2
    rows = range(start // 4 - 1, (start + count) // 4 + 1)
    kinds = (down1 @ down, down1 @ down @ near, down1 @ near1 @ down, down1 @ near1 @ down @ near)
    return [kind[rows, start : start + count] for kind in kinds]


def early_tables(block):
    b0, b1, b2 = block
    (p, r, c) = ([*two_levels(size)] for size in block)
    full = mixed(p, r)
    rows = np.zeros((4, 3, 16, b0 * b1))
    rows[:, :, : 2 * r[0].shape[0]] = np.stack(full).reshape(4, 3, 2 * r[0].shape[0], b0 * b1)
    lanes = np.zeros((4, b2, b2))
    for n in range(4):
        lanes[n, :, : c[n].shape[0]] = c[n].T / 64.0
    return exact(rows.reshape(-1, b0 * b1)), exact(lanes.reshape(-1, b2))


def fast_constants(counts, block, sizes):
    nx, ny, nz = counts
    b0, b1, b2 = block
    m0, m1, m2 = (size // 2 for size in sizes)
    t0, t1, t2 = (factors(m) for m in (m0, m1, m2))
    parts, index2, index1 = halved_rows(m0, m1)
    i0, i1 = index1 // m1, index1 % m1
    j0, j1 = index2 // m1, index2 % m1
    rows2 = len(index2)

    def across(name, k, l, op=np.multiply):
        return op(t0[name][k], t1[name][l])

    def joint(a, c):
        return t0[a][i0] * t1[c][i1]

    columns = [across("r1", i0, i1), across("p1", i0, i1), across("q1", i0, i1), across("e1", i0, i1, np.add)]
    columns += [joint("m0", "m0"), joint("m1", "m0") + joint("m0", "m1")]
    columns += [joint("m2", "m0") + joint("m0", "m2") + 2.0 * joint("m1", "m1")]
    by_row = np.zeros((m0 * m1, 128))
    by_row[:, : len(columns)] = np.stack(columns, axis=1)
    for n, name in enumerate(("r2", "p2", "q2", "e2")):
        by_row[:rows2, 8 + n] = across(name, j0, j1, np.add if name == "e2" else np.multiply)
    by_lane = np.zeros((16, m2))
    for n, name in enumerate(("r1", "p1", "q1", "e1", "m0", "m1", "m2")):
        by_lane[n] = t2[name]
    for n, name in enumerate(("r2", "p2", "q2", "e2")):
        by_lane[8 + n, : m2 // 2] = t2[name]
    two = np.float32(2.0)
    eigen = np.float32(6.0) - two * t0["c3"][:, None, None]
    eigen = eigen - two * t1["c3"][None, :, None] - two * t2["c3"][None, None, :]
    eigen = (np.float32(0.25 ** (LEVELS - 1)) * eigen).reshape(rows2 // 4, m2 // 4)
    early_rows, early_lanes = early_tables(block)
    table = {"own": own_table(b2 // 2), "early_rows": early_rows, "early_lanes": early_lanes}
    small = {"by_row": by_row, "by_lane": by_lane, "eigen": np.concatenate([eigen, eigen], axis=1)}
    table.update({name: np.asarray(value, np.float32) for name, value in small.items()})

    a0, a1 = (analysis(waves(m // 2, modes(m // 2, 1))) for m in (m0, m1))
    a2 = analysis(waves(m2 // 2, modes(m2 // 2, 1)))
    p0, p1, p2 = b0 // 4, b1 // 4, b2 // 4
    wide = p2 + 2
    lanes = np.zeros((ny, b2, 3, m2 // 2))
    for dy in range(ny):
        for n in range(3):
            lanes[dy, 42 * n : 42 * n + wide, n] = a2[:, np.arange(p2 * dy - 1, p2 * dy + p2 + 1) % (m2 // 2)].T
    table["level2_lanes"] = halves(lanes.reshape(ny * b2, -1), 0)
    n, dx, dz, c, r = np.meshgrid(*(range(k) for k in (3, nx, nz, 2, p1 + 2)), indexing="ij")
    planes = (p0 * dx + 2 * n + c - 1 - p0 // 2) % (m0 // 2)
    rows = (p1 * dz + r - 1) % (m1 // 2)
    full = np.zeros((rows2, 3, nx, nz, 16))
    full[..., : 2 * (p1 + 2)] = (a0[j0][:, planes] * a1[j1][:, rows]).reshape(rows2, 3, nx, nz, -1)
    table["level2_rows"] = halves(full.reshape(rows2, -1), 1)

    forward = analysis(t0["waves"])[i0][:, : m0 // 2, None] * analysis(t1["waves"])[i1][:, None, :]
    table["forward_rows"] = halves(forward.reshape(2, m0 * m1 // 2, -1), 2)
    table["forward_lanes"] = halves(analysis(t2["waves"]).T, 0)
    for name, weights, powers in (("cubic", CUBIC, 3), ("linear", LINEAR, 2)):
        p = synthesis(t0, range(b0 // 2), weights, powers)
        r = synthesis(t1, range(b1), weights, powers)
        full = []
        for part in parts.reshape(2, -1):
            q0 = [matrix[:, part // m1][:, None, :] for matrix in p]
            q1 = [matrix[:, part % m1][None, :, :] for matrix in r]
            kinds = [q0[0] * q1[0], q0[1] * q1[0] + q0[0] * q1[1]]
            if powers == 3:
                kinds.append(q0[2] * q1[0] + 2.0 * q0[1] * q1[1] + q0[0] * q1[2])
            full.append(np.stack(kinds).reshape(-1, part.size))
        table[name + "_rows"] = halves(np.stack(full), 2)
        lanes = [matrix.T for matrix in synthesis(t2, range(b2), weights, powers)]
        table[name + "_lanes"] = halves(np.concatenate(lanes), 0)
    p = late_kinds(m0, range(b0), range(-2, b0 // 2 + 2))
    r = late_kinds(m1, range(b1), range(m1))
    table["late_rows"] = exact(np.concatenate(mixed(p, r), axis=1))
    table["late_lanes"] = exact(np.concatenate([c.T for c in late_kinds(m2, range(b2), range(m2))], axis=1))
    return table


def split(values):
    high = values.astype(jnp.bfloat16)
    return high, (values - high.astype(jnp.float32)).astype(jnp.bfloat16)


def by_right(values, table):
    high, low = split(values)
    depth = values.shape[1]
    first, second = table[:depth], table[depth:]
    return jnp.dot(
        jnp.concatenate([high, low, high], axis=1),
        jnp.concatenate([first, first, second], axis=0),
        preferred_element_type=jnp.float32,
    )


def by_left(table, values):
    high, low = split(values)
    depth = values.shape[0]
    first, second = table[:, :depth], table[:, depth:]
    return jnp.dot(
        jnp.concatenate([first, first, second], axis=1),
        jnp.concatenate([high, low, high], axis=0),
        preferred_element_type=jnp.float32,
    )


def fold(values):
    n = values.shape[0] // 8
    parts = []
    for kind in range(2):
        quarter = [values[(4 * kind + i) * n : (4 * kind + i + 1) * n] for i in range(4)]
        parts.append((quarter[0] + quarter[1]) + (quarter[2] + quarter[3]))
    total = jnp.concatenate(parts, axis=0)
    return total + pltpu.roll(total, total.shape[1] // 2, 1)


def unfold(values):
    n = values.shape[0] // 2
    return jnp.concatenate([values[:n]] * 4 + [values[n:]] * 4, axis=0)


def own_parts(source, own, outs, alpha, beta):
    block, across, along_rows, along_planes, rest = outs
    b0, b1, b2 = source.shape
    h0, h1 = b0 // 2, b1 // 2
    first = [source[p, pl.ds(0, h1, stride=2), :] for p in range(b0)]
    second = [source[p, pl.ds(1, h1, stride=2), :] for p in range(b0)]
    summed = [a + b for a, b in zip(first, second)]
    row = lax.broadcasted_iota(jnp.int32, (h1, b2), 0)
    zero = jnp.zeros((h1, b2), jnp.float32)
    whole, faces, inner = [], [], []
    for c in range(h0):
        total = summed[2 * c] + summed[2 * c + 1]
        down = pltpu.roll(second[2 * c] + second[2 * c + 1], 1, 0)
        up = pltpu.roll(first[2 * c] + first[2 * c + 1], h1 - 1, 0)
        whole.append(total)
        faces.append(jnp.where(row == 0, down, jnp.where(row == h1 - 1, up, zero)))
        near = 2.0 * total + jnp.where(row > 0, down, zero) + jnp.where(row < h1 - 1, up, zero)
        if c > 0:
            near = near + summed[2 * c - 1]
        if c < h0 - 1:
            near = near + summed[2 * c + 2]
        inner.append(near)

    def pack(planes):
        half = len(planes) // 2
        return [jnp.concatenate([planes[i], planes[i + half]], axis=1) for i in range(half)]

    ends = [jnp.concatenate([summed[b0 - 1], summed[0]], axis=1)]
    stacked = jnp.concatenate(pack(whole) + pack(faces) + pack(inner) + ends + [jnp.zeros((8, 2 * b2), jnp.float32)], axis=0)
    parts = parts_of(stacked, 3)
    weights = own[...]
    result = jnp.dot(
        jnp.concatenate(parts, axis=1),
        jnp.concatenate([weights] * 3, axis=0),
        preferred_element_type=jnp.float32,
    )
    n = h0 // 2 * h1
    shape = block.shape
    mine = result[:n, :b2]
    block[...] = mine.reshape(shape)
    across[...] = result[:n, b2 : 2 * b2].reshape(shape)
    along_rows[...] = result[n : 2 * n, :b2].reshape(shape)
    along_planes[...] = result[3 * n : 3 * n + h1, :b2]
    rest[...] = (alpha * mine + beta * (result[2 * n : 3 * n, :b2] + result[:n, 2 * b2 :])).reshape(shape)


def early_part(source, rows_table, lanes_table, weights):
    keep0, near0, keep1, near1 = weights
    b0, b1, b2 = source.shape
    result = jnp.dot(
        jnp.concatenate([rows_table[...]] * 3, axis=1),
        jnp.concatenate(parts_of(source[...].reshape(b0 * b1, b2), 3), axis=0),
        preferred_element_type=jnp.float32,
    )
    n = result.shape[0] // 4
    plain, first, second, both = (result[i * n : (i + 1) * n] for i in range(4))
    joint = near0 * near1
    columns = (
        (keep0 * keep1) * plain + (keep1 * near0) * first + (keep0 * near1) * second + joint * both,
        (keep1 * near0) * plain + joint * second,
        (keep0 * near1) * plain + joint * first,
        joint * plain,
    )
    result = jnp.dot(
        jnp.concatenate(parts_of(jnp.concatenate(columns, axis=1), 3), axis=1),
        jnp.concatenate([lanes_table[...]] * 3, axis=0),
        preferred_element_type=jnp.float32,
    )
    total = result[:16] + pltpu.roll(result[16:32], 42, 1)
    return (total + pltpu.roll(result[32:], 84, 1)).reshape(2, 8, b2)


def beyond(place, counts):
    x, y, z = place
    return (x, lax.rem(y - 1 + 2 * lax.rem(y, 2) + counts[1], counts[1]), z)


def close_by(counts):
    chosen = []
    for offset in chip_offsets(counts):
        step = offset[0]
        if min(step, counts[0] - step) <= 1:
            part = 0 if step == 0 or counts[0] == 2 else (1 if step == 1 else -1)
            chosen.append((offset, part))
    return chosen


def everywhere(counts):
    return [(offset, 0) for offset in chip_offsets(counts)]


def piece(ref, part):
    if part == 0:
        return ref
    half = ref.shape[0] // 2
    return ref.at[pl.ds(half if part == 1 else 0, half)]


def send_all(counts, chosen, block, landing, sems):
    send, recv, relay_send, relay_recv = sems
    me = position()
    mine = landing.at[slot(me, counts)]
    copies = []
    for n, (offset, part) in enumerate(chosen):
        place = shifted(me, counts, offset)
        copies.append(remote(piece(block, part), piece(mine, part), send.at[n], recv.at[n], place))
        copies[-1].start()
    n = len(copies)
    relays = [remote(block, mine, relay_send.at[n], relay_recv.at[n], partner_of(me))]
    relays[-1].start()
    return copies, relays


def relay_all(counts, chosen, started, landing, sems):
    relay_send, relay_recv = sems[2:]
    me = position()
    copies, relays = started
    for n, (offset, part) in enumerate(chosen):
        copies[n].wait_recv()
        source = shifted(me, counts, tuple(-step for step in offset))
        arrived = piece(landing.at[slot(source, counts)], part)
        relays.append(remote(arrived, arrived, relay_send.at[n], relay_recv.at[n], partner_of(me)))
        relays[-1].start()


def end_all(counts, started, block, landing):
    copies, relays = started
    landing[slot(position(), counts)] = block[...]
    for copy in copies:
        copy.wait_send()
    for copy in relays:
        copy.wait()


def exchange(counts, sent, received, send, recv):
    me = position()
    order = (0, 2, 1)
    copies = []
    for n, (offset, axis, side) in enumerate(face_offsets(counts)):
        which = order[axis]
        mine = sent[which] if len(sent[which]) == 1 else [sent[which][side]]
        place = shifted(me, counts, offset)
        copies.append(remote(mine[0], received[2 * which + 1 - side], send.at[n], recv.at[n], place))
        copies[-1].start()
    return copies


def prepare(k, many, few, shift):
    diagonal0, diagonal1, diagonal2 = (6.0 * 0.25**level + shift for level in range(3))
    sigma0, sigma1, sigma2 = diagonal0 - 6.0, diagonal1 - 1.5, diagonal2 - 0.375
    damp0, damp1, damp2 = DAMPING / diagonal0, DAMPING / diagonal1, DAMPING / diagonal2
    down, pre, fine_q, out_q, out_g, out_e, cross = many
    by_row, by_lane = k["by_row"], k["by_lane"]
    lanes = by_lane.shape[1]

    def level1(i):
        rows = pl.ds(pl.multiple_of(8 * i, 8), 8)
        column = by_row[rows, :]

        def tall(n):
            return jnp.broadcast_to(column[:, n : n + 1], (8, lanes))

        def wide(n):
            return jnp.broadcast_to(by_lane[n : n + 1, :], (8, lanes))

        r, p, q = (tall(n) * wide(n) for n in range(3))
        a = 0.25 * (tall(3) + wide(3)) + sigma1
        s = 1.0 - damp1 * a
        down[rows, :] = r
        pre[rows, :] = r * s
        fine_q[rows, :] = a * q
        out_q[rows, :] = s * s * q
        out_g[rows, :] = damp1 * (1.0 + s)
        out_e[rows, :] = s * p
        c0, c1, c2 = tall(4), tall(5), tall(6)
        first = sigma0 * c0 + c1 - damp0 * ((sigma0 * sigma0) * c0 + (2.0 * sigma0) * c1 + c2)
        second = c0 - (2.0 * damp0) * (sigma0 * c0 + c1)
        cross[rows, :] = first * wide(4) + second * wide(5) - (damp0 * c0) * wide(6)

    loop(by_row.shape[0] // 8, level1)
    rows2, lanes2 = few[0].shape
    column = by_row[:rows2, :]

    def tall(n):
        return jnp.broadcast_to(column[:, n : n + 1], (rows2, lanes2))

    def wide(n):
        return jnp.broadcast_to(by_lane[n : n + 1, :lanes2], (rows2, lanes2))

    r, p, q = (tall(n) * wide(n) for n in (8, 9, 10))
    a = 0.0625 * (tall(11) + wide(11)) + sigma2
    s = 1.0 - damp2 * a
    values = (r, r * s, a * q, s * s * q, damp2 * (1.0 + s), s * p)
    for ref, value in zip(few, values):
        ref[...] = value
    k["inverse"][...] = 1.0 / (k["eigen"][...] + shift)


def level2(k, few, g):
    down, pre, fine_q, out_q, out_g, out_e = few
    e = unfold(fold(pre[...] * g) * k["inverse"][...])
    return out_g[...] * g + out_e[...] * e


def level2_full(k, few, g):
    down, pre, fine_q, out_q, out_g, out_e = few
    start = unfold(fold(down[...] * g) * k["inverse"][...])
    e = unfold(fold(pre[...] * (g - fine_q[...] * start)) * k["inverse"][...])
    return out_q[...] * start + out_g[...] * g + out_e[...] * e


def blocks_of(spectrum, i):
    rows2, lanes2 = spectrum.shape[0] // 4, spectrum.shape[1] // 2
    half = rows2 // 2
    base = 8 * i + 3 * half * lax.div(i, half // 8)
    for a in range(4):
        start = pl.multiple_of(base + a * half, 8)
        for c in range(2):
            yield (pl.ds(start, 8), pl.ds(c * lanes2, lanes2))


def spectral_u(k, many, few, spectrum, coupled, coarse):
    down, pre, fine_q, out_q, out_g, out_e, cross = many
    first, second, third = coarse
    steps = first.shape[0] // 8

    def at(i):
        return pl.ds(pl.multiple_of(8 * i, 8), 8)

    def restrict(i):
        first[at(i), :] = sum(down[w] * spectrum[w] for w in blocks_of(spectrum, i))

    loop(steps, restrict)
    second[...] = level2_full(k, few, first[...])

    def residue(i):
        u = second[at(i), :]
        first[at(i), :] = sum(pre[w] * (spectrum[w] - fine_q[w] * u) for w in blocks_of(spectrum, i))

    loop(steps, residue)
    third[...] = level2(k, few, first[...])

    def finish(i):
        u, e = second[at(i), :], third[at(i), :]
        total = None
        for w in blocks_of(spectrum, i):
            value = out_q[w] * u + out_g[w] * spectrum[w] + out_e[w] * e
            spectrum[w] = value
            value = cross[w] * value
            coupled[w] = value
            total = pre[w] * value if total is None else total + pre[w] * value
        first[at(i), :] = total

    loop(steps, finish)


def spectral_e(many, spectrum, coupled, e2):
    out_g, out_e = many[4], many[5]

    def finish(i):
        e = e2[pl.ds(pl.multiple_of(8 * i, 8), 8), :]
        for w in blocks_of(spectrum, i):
            spectrum[w] = out_e[w] * e - out_g[w] * coupled[w]

    loop(e2.shape[0] // 8, finish)


def unpack_centred(gathered, counts, g):
    nx, ny, nz = counts
    me = position()
    half, rows, lanes = gathered.shape[1:]
    planes = g.shape[0]
    low = lax.broadcasted_iota(jnp.int32, (half, rows, lanes), 2) < lanes // 2
    for dx in range(nx):
        for dz in range(nz):
            for pair in range(ny // 2):
                parts = [
                    gathered[slot(shifted(me, counts, (dx, dy, dz)), counts)] for dy in (2 * pair, 2 * pair + 1)
                ]
                turned = [pltpu.roll(part, lanes // 2, 2) for part in parts]
                where = (pl.ds(dz * rows, rows), pl.ds(pair * lanes, lanes))
                start = (2 * half * dx - half) % planes
                g[(pl.ds(start, half), *where)] = jnp.where(low, parts[0], turned[1])
                g[(pl.ds(2 * half * dx, half), *where)] = jnp.where(low, turned[0], parts[1])


def transform(k, counts, landing, g, spectrum):
    unpack_centred(landing, counts, g)
    m0, m1, m2 = g.shape
    half = m0 // 2
    depth = half * m1
    for kind in range(2):
        rows = [g[p] - g[m0 - 1 - p] if kind else g[p] + g[m0 - 1 - p] for p in range(half)]
        values = by_left(k["forward_rows"][kind], jnp.concatenate(rows, axis=0))
        spectrum[kind * depth : (kind + 1) * depth, :] = by_right(values, k["forward_lanes"])


def transform2(k, counts, landing):
    nx, ny, nz = counts
    me = position()
    columns = []
    for dy in range(ny):
        rows = [
            landing[slot(shifted(me, counts, (dx, dy, dz)), counts)].reshape(16, -1)
            for dx in range(nx)
            for dz in range(nz)
        ]
        columns.append(jnp.concatenate(rows, axis=0))
    values = by_right(jnp.concatenate(columns, axis=1), k["level2_lanes"])
    width = values.shape[1] // 3
    parts = [values[:, n * width : (n + 1) * width] for n in range(3)]
    return by_left(k["level2_rows"], jnp.concatenate(parts, axis=0))


def evaluate(k, kind, spectrum, mix, out):
    planes, rows, lanes = out.shape
    half = planes // 2
    depth = spectrum.shape[0] // 2
    parts = []
    for n in range(2):
        values = by_left(k[kind + "_rows"][n], spectrum[n * depth : (n + 1) * depth, :])
        pieces = [values[i : i + half * rows] for i in range(0, values.shape[0], half * rows)]
        columns = [sum(c * pieces[i] for i, c in enumerate(line) if c is not None) for line in mix]
        parts.append(by_right(jnp.concatenate(columns, axis=1), k[kind + "_lanes"]).reshape(half, rows, lanes))
    even, odd = parts
    for p in range(half):
        for index, value in ((half + p, even[p] + odd[p]), (half - 1 - p, even[p] - odd[p])):
            out[index] = out[index] + value


def unpack_near(gathered, counts, g):
    nx, ny, nz = counts
    me = position()
    half, rows, lanes = gathered.shape[1:]
    for dx, first, last in ((nx - 1, half - 2, half), (0, 0, half), (1, 0, 2)):
        shape = (last - first, rows, lanes)
        low = lax.broadcasted_iota(jnp.int32, shape, 2) < lanes // 2
        for dz in range(nz):
            for pair in range(ny // 2):
                parts = [
                    gathered[slot(shifted(me, counts, (dx, dy, dz)), counts), pl.ds(first, last - first)]
                    for dy in (2 * pair, 2 * pair + 1)
                ]
                turned = [pltpu.roll(part, lanes // 2, 2) for part in parts]
                where = (pl.ds(dz * rows, rows), pl.ds(pair * lanes, lanes))
                if dx != nx - 1:
                    start = 2 if dx == 0 else 2 + 2 * half
                    g[(pl.ds(start, last - first), *where)] = jnp.where(low, parts[0], turned[1])
                if dx != 1:
                    start = 2 + half if dx == 0 else 0
                    g[(pl.ds(start, last - first), *where)] = jnp.where(low, turned[0], parts[1])


def late_part(k, g, weights):
    keep0, near0, keep1, near1 = weights
    planes, m1, m2 = g.shape
    pieces = split(g[...].reshape(planes * m1, m2))
    table = k["late_lanes"][...]
    values = jnp.dot(
        jnp.concatenate(pieces, axis=1),
        jnp.concatenate([table, table], axis=0),
        preferred_element_type=jnp.float32,
    )
    lanes = values.shape[1] // 4
    a, b, c, d = (values[:, i * lanes : (i + 1) * lanes] for i in range(4))
    joint = near0 * near1
    stacked = (
        (keep0 * keep1) * a + (near0 * keep1) * b + (keep0 * near1) * c + joint * d,
        (near0 * keep1) * a + joint * c,
        (keep0 * near1) * a + joint * b,
        joint * a,
    )
    table = k["late_rows"][...]
    values = jnp.dot(
        jnp.concatenate([table, table], axis=1),
        jnp.concatenate(split(jnp.concatenate(stacked, axis=0)), axis=0),
        preferred_element_type=jnp.float32,
    )
    return values


def own_sweep(f, source, keep, damp, out):
    rows, lanes = source.shape[1:]

    def body(p):
        beside = f[p] + f[p + 2] + around(f[p + 1])
        out[p] = damp * ((1.0 + keep) * source[p] + damp * beside[:rows, :lanes])

    loop(source.shape[0], body)


def fast_kernel(names, counts, *refs):
    count = len(names)
    outside = dict(zip(names, refs))
    shift_ref, source_ref, out, *rest = refs[count:]

    def take(number):
        taken = rest[:number]
        del rest[:number]
        return taken

    k = dict(zip(names, take(count)))
    (source,) = take(1)
    landing_f, landing_h, landing_j = take(3)
    faces_in, halos = take(6), take(3)
    block_f, block_h, across, along_rows, local, along_planes = take(6)
    (block_j,) = take(1)
    own_planes, own_rows, own_columns = take(3)
    many, few, coarse = take(7), take(6), take(3)
    k["inverse"], g, near_h, spectrum, coupled, f = take(6)
    table_sems, *face_sems = take(5)
    sems_f, sems_h, sems_j = take(4), take(4), take(4)

    shift = shift_ref[0]
    me = position()
    barrier = pltpu.get_barrier_semaphore()
    places = [shifted(me, counts, offset) for offset in chip_offsets(counts)]
    places += [partner_of(me), beyond(me, counts)]
    greet(barrier, places)
    loads = {"source": pltpu.make_async_copy(source_ref, source, table_sems.at[count])}
    loads["source"].start()
    for n, name in enumerate(names):
        loads[name] = pltpu.make_async_copy(outside[name], k[name], table_sems.at[n])
        loads[name].start()

    b0, b1, b2 = source.shape
    diagonal, diagonal1 = 6.0 + shift, 1.5 + shift
    damp, damp1 = DAMPING / diagonal, DAMPING / diagonal1
    loads["source"].wait()
    loads["own"].wait()
    parts = (block_f, across, along_rows, along_planes, local)
    own_parts(source, k["own"], parts, 1.0 - damp * diagonal, damp)
    own_planes[0] = source[0]
    own_planes[1] = source[b0 - 1]
    own_rows[0] = source[:, pl.ds(0, 1), :]
    own_rows[1] = source[:, pl.ds(b1 - 1, 1), :]
    turned = source[...].reshape(b0 * b1, b2).T
    own_columns[0] = turned[:8]
    own_columns[1] = turned[b2 - 8 :]
    for name in ("early_rows", "early_lanes"):
        loads[name].wait()
    weights = (1.0 - damp * diagonal, damp, 1.0 - damp1 * diagonal1, 0.25 * damp1)
    block_j[...] = early_part(source, k["early_rows"], k["early_lanes"], weights)
    pl.semaphore_wait(barrier, len(places))

    first = exchange(counts, ([along_planes], [along_rows], [across]), faces_in, *face_sems[:2])
    started_f = send_all(counts, everywhere(counts), block_f, landing_f, sems_f)
    started_j = send_all(counts, everywhere(counts), block_j, landing_j, sems_j)

    for name in ("by_row", "by_lane", "eigen"):
        loads[name].wait()
    prepare(k, many, few, shift)
    for copy in first:
        copy.wait()
    shape = local.shape
    lane = lax.rem(lax.broadcasted_iota(jnp.int32, shape, 2), b2 // 2)
    row = lax.broadcasted_iota(jnp.int32, shape, 1)
    from_planes, from_rows, from_lanes = faces_in[:2], faces_in[2:4], faces_in[4:6]
    total = jnp.where(lane == 0, from_lanes[0][...], 0.0) + jnp.where(lane == b2 // 2 - 1, from_lanes[1][...], 0.0)
    total = total + jnp.where(row == 0, from_rows[0][...], 0.0) + jnp.where(row == shape[1] - 1, from_rows[1][...], 0.0)
    block_h[...] = local[...] + damp * total
    low = lax.broadcasted_iota(jnp.int32, shape[1:], 1) < b2 // 2
    block_h[0] = block_h[0] + damp * jnp.where(low, from_planes[0][...], 0.0)
    end = shape[0] - 1
    block_h[end] = block_h[end] + damp * jnp.where(low, 0.0, from_planes[1][...])

    mine = [[own.at[side] for side in range(2)] for own in (own_planes, own_rows, own_columns)]
    last = exchange(counts, mine, [halo.at[side] for halo in halos for side in range(2)], *face_sems[2:4])
    started_h = send_all(counts, close_by(counts), block_h, landing_h, sems_h)
    relay_all(counts, everywhere(counts), started_f, landing_f, sems_f)
    for copy in last:
        copy.wait()
    f[...] = jnp.zeros_like(f)
    rows, lanes = pl.ds(0, b1), pl.ds(0, b2)
    f[1 : b0 + 1, rows, lanes] = source[...]
    f[0, rows, lanes] = halos[0][0]
    f[b0 + 1, rows, lanes] = halos[0][1]
    f[1 : b0 + 1, pl.ds(b1, 1), lanes] = halos[1][1]
    f[1 : b0 + 1, pl.ds(b1 + 7, 1), lanes] = halos[1][0]
    middle = jnp.zeros((b2 - 16, b0 * b1), jnp.float32)
    turned = jnp.concatenate([halos[2][1], middle, halos[2][0]], axis=0)
    f[1 : b0 + 1, rows, pl.ds(b2, b2)] = turned.T.reshape(b0, b1, b2)
    keep = 1.0 - damp * diagonal
    own_sweep(f, source, keep, damp, out)
    end_all(counts, started_f, block_f, landing_f)
    for name in names:
        if name not in ("own", "early_rows", "early_lanes", "by_row", "by_lane", "eigen"):
            loads[name].wait()
    transform(k, counts, landing_f, g, spectrum)
    spectral_u(k, many, few, spectrum, coupled, coarse)
    relay_all(counts, everywhere(counts), started_j, landing_j, sems_j)
    relay_all(counts, close_by(counts), started_h, landing_h, sems_h)
    double = 2.0 * keep * damp
    square = damp * damp
    mix = ((keep * keep, double, square), (double, 2.0 * square, None), (square, None, None))
    evaluate(k, "cubic", spectrum, mix, out)
    end_all(counts, started_h, block_h, landing_h)
    end_all(counts, started_j, block_j, landing_j)
    unpack_near(landing_h, counts, near_h)
    keep1 = 1.0 - damp1 * diagonal1
    coarse[1][...] = level2(k, few, transform2(k, counts, landing_j) - coarse[0][...])
    late = late_part(k, near_h, (keep, damp, damp1 * (1.0 + keep1), 0.25 * damp1 * damp1))
    out[...] = out[...] + late.reshape(out.shape)
    spectral_e(many, spectrum, coupled, coarse[1])
    evaluate(k, "linear", spectrum, ((keep, damp), (damp, None)), out)


def fast_per_device(counts, source, shift):
    nx, ny, nz = counts
    b0, b1, b2 = source.shape
    sizes = (b0 * nx, b1 * nz, b2 * ny)
    table = fast_constants(counts, source.shape, sizes)
    m0, m1, m2 = (size // 2 for size in sizes)
    rows = m0 * m1
    packed = (b0 // 4, b1 // 2, b2)
    devices = nx * ny * nz

    def field(*shape):
        return pltpu.VMEM(shape, jnp.float32)

    def in_hbm(value):
        return pltpu.with_memory_space_constraint(value, pltpu.HBM)

    names = tuple(table)
    tile = packed[1:]
    fine = [field(2, b1, b2), field(2, b0, 1, b2), field(2, 8, b0 * b1)]
    scratch = [pltpu.VMEM(table[name].shape, table[name].dtype) for name in names]
    scratch += [field(*source.shape), field(devices, *packed), field(devices, *packed), field(devices, 2, *tile)]
    scratch += [field(*tile)] * 2 + [field(*packed)] * 4 + fine
    scratch += [field(*packed)] * 5 + [field(*tile), field(2, *tile)] + fine
    scratch += [field(rows, m2)] * 7 + [field(rows // 4, m2 // 2)] * 9
    scratch += [field(rows // 16, m2 // 2), field(m0, m1, m2), field(b0 // 2 + 4, m1, m2)]
    scratch += [field(rows, m2), field(rows, m2), field(b0 + 2, b1 + 8, 2 * b2)]
    dma = pltpu.SemaphoreType.DMA
    scratch += [dma((len(names) + 1,))] + [dma((6,))] * 4
    for chosen in (everywhere(counts), close_by(counts), everywhere(counts)):
        scratch += [dma((len(chosen),))] * 2 + [dma((len(chosen) + 1,))] * 2
    return pl.pallas_call(
        functools.partial(fast_kernel, names, counts),
        out_shape=jax.ShapeDtypeStruct(source.shape, jnp.float32),
        in_specs=[pl.BlockSpec(memory_space=pltpu.HBM)] * len(names)
        + [pl.BlockSpec(memory_space=pltpu.SMEM), pl.BlockSpec(memory_space=pltpu.HBM)],
        out_specs=pl.BlockSpec(memory_space=pltpu.VMEM),
        scratch_shapes=scratch,
        compiler_params=pltpu.CompilerParams(
            vmem_limit_bytes=40 * 1024 * 1024, collective_id=0, has_side_effects=True
        ),
    )(*[in_hbm(jnp.asarray(table[name])) for name in names], shift, in_hbm(source))


def small_enough(counts, block):
    (nx, ny, nz), (b0, b1, b2) = counts, block
    rows = (b0 * nx // 2) * (b1 * nz // 2)
    return rows <= 512 and rows % 128 == 0 and (b0, b1, b2) == (16, 16, 128) and ny % 4 == 0 and min(counts) > 1


def dispatch(counts, source, shift):
    run = fast_per_device if small_enough(counts, source.shape) else per_device
    return run(counts, source, shift)


def solution(mesh):
    counts = tuple(mesh.shape[name] for name in NAMES)
    return jax.shard_map(
        functools.partial(dispatch, counts),
        mesh=mesh,
        in_specs=(P("gx", "gz", "gy"), P()),
        out_specs=P("gx", "gz", "gy"),
        check_vma=False,
    )
```

```python
import functools

import jax
import jax.numpy as jnp
import numpy as np
from jax import lax
from jax.experimental import pallas as pl
from jax.experimental.pallas import tpu as pltpu
from jax.sharding import PartitionSpec as P

LEVELS = 4
DAMPING = 6.0 / 7.0
PRECISE = lax.Precision.HIGHEST
CUBIC = (
    {-2: -5.0 / 128.0, -1: 35.0 / 128.0, 0: 105.0 / 128.0, 1: -7.0 / 128.0},
    {-1: -7.0 / 128.0, 0: 105.0 / 128.0, 1: 35.0 / 128.0, 2: -5.0 / 128.0},
)
LINEAR = ({-1: 0.25, 0: 0.75}, {0: 0.75, 1: 0.25})
NAMES = ("gx", "gy", "gz")
MESH = pl.DeviceIdType.MESH


def basis(count):
    cells = np.arange(count)
    columns, cosines = [], []
    for m in range(count):
        k = (m + 1) // 2
        angle = 2.0 * np.pi * k * cells / count
        column = np.cos(angle) if m % 2 == 1 or m == 0 else np.sin(angle)
        columns.append(column / np.sqrt(np.sum(column**2)))
        cosines.append(np.cos(2.0 * np.pi * k / count))
    return np.stack(columns, axis=1), np.array(cosines, np.float32)


def interpolation(coarse_count, fine_cells, weights):
    matrix = np.zeros((len(fine_cells), coarse_count))
    for row, cell in enumerate(fine_cells):
        for offset, weight in weights[cell % 2].items():
            matrix[row, (cell // 2 + offset) % coarse_count] += weight
    return matrix


def pairs(coarse_count):
    return np.kron(np.eye(coarse_count), np.ones((1, 2)))


def blocked(matrix):
    count = max(1, 128 // matrix.shape[1])
    return np.kron(np.eye(count), matrix)


def constants(block, sizes):
    b0, b1, b2 = block
    m0, m1, m2 = (size // 2 for size in sizes)
    q0, q1, q2 = (size // 4 for size in sizes)
    c0, c1, c2 = (size // 8 for size in sizes)
    table = {}
    table["own_rows"] = np.kron(np.eye(b0 // 2), pairs(b1 // 2))
    lanes = 0.125 * pairs(b2 // 2).T
    table["own_lo"] = np.concatenate([lanes, np.zeros_like(lanes)], axis=1)
    table["own_hi"] = np.concatenate([np.zeros_like(lanes), lanes], axis=1)
    table["down_rows"] = blocked(pairs(q1))
    table["down_lanes"] = 0.125 * pairs(q2).T
    window_lanes = [b2 + j for j in range(b2 // 2)] + [j - b2 for j in range(b2 // 2, 2 * b2)]
    window_rows = [j - 8 for j in range(b1 + 16)]
    for name, weights in (("cubic", CUBIC), ("linear", LINEAR)):
        table[name + "_rows1"] = blocked(interpolation(q1, range(m1), weights))
        table[name + "_lanes1"] = interpolation(q2, range(m2), weights).T
        table[name + "_rows0"] = blocked(interpolation(m1, window_rows, weights))
        table[name + "_lanes0"] = interpolation(m2, window_lanes, weights).T
    (u0, cos0), (u1, cos1), (u2, cos2) = basis(c0), basis(c1), basis(c2)
    table["spectrum_rows"] = np.kron(u0.T @ pairs(c0), u1.T @ pairs(c1))
    table["spectrum_lanes"] = 0.125 * pairs(c2).T @ u2
    for name, weights in (("cubic", CUBIC), ("linear", LINEAR)):
        table[name + "_rows2"] = np.kron(
            interpolation(c0, range(q0), weights) @ u0, interpolation(c1, range(q1), weights) @ u1
        )
        table[name + "_lanes2"] = u2.T @ interpolation(c2, range(q2), weights).T
    two = np.float32(2.0)
    eigen = (
        np.float32(6.0)
        - two * cos0[:, None, None]
        - two * cos1[None, :, None]
        - two * cos2[None, None, :]
    )
    table["eigen"] = (np.float32(0.25 ** (LEVELS - 1)) * eigen).reshape(c0 * c1, c2)
    wide = ("spectrum_rows", "spectrum_lanes", "eigen")
    return {
        name: np.asarray(
            value, np.float32 if name in wide or name.endswith("2") else jnp.bfloat16
        )
        for name, value in table.items()
    }


def dot(a, b):
    return jnp.dot(a, b, precision=PRECISE, preferred_element_type=jnp.float32)


def parts_of(values, pieces):
    parts = []
    for n in range(pieces):
        parts.append(values.astype(jnp.bfloat16))
        if n + 1 < pieces:
            values = values - parts[-1].astype(jnp.float32)
    return parts[::-1]


def right(values, matrix, pieces):
    terms = [
        jnp.dot(part, matrix, preferred_element_type=jnp.float32)
        for part in parts_of(values, pieces)
    ]
    return sum(terms[1:], terms[0])


def left(matrix, values, pieces):
    terms = [
        jnp.dot(matrix, part, preferred_element_type=jnp.float32)
        for part in parts_of(values, pieces)
    ]
    return sum(terms[1:], terms[0])


def around(plane):
    rows, lanes = plane.shape
    total = pltpu.roll(plane, 1, 0) + pltpu.roll(plane, rows - 1, 0)
    return total + (pltpu.roll(plane, 1, 1) + pltpu.roll(plane, lanes - 1, 1))


def around_all(values):
    first = jnp.concatenate([values[1:], values[:1]], axis=0)
    first = first + jnp.concatenate([values[-1:], values[:-1]], axis=0)
    for axis in (1, 2):
        first = first + pltpu.roll(values, 1, axis)
        first = first + pltpu.roll(values, values.shape[axis] - 1, axis)
    return first


def row_blocks(matrix, values, pieces):
    depth = matrix.shape[1]
    return jnp.concatenate(
        [left(matrix, values[i : i + depth], pieces) for i in range(0, values.shape[0], depth)], axis=0
    )


def loop(count, body):
    def step(i, carry):
        body(i)
        return carry

    lax.fori_loop(0, count, step, 0, unroll=4 if count % 4 == 0 else 2)


def close(ref):
    count = ref.shape[0] - 2
    ref[0] = ref[count]
    ref[count + 1] = ref[1]


def defect_plane(v, p, g, weight, diagonal):
    center = v[p]
    beside = v[p - 1] + v[p + 1] + around(center)
    return center, g - (diagonal * center - weight * beside)


def restrict_own(k, summed):
    b_half, rows, lanes = summed.shape
    folded = left(k["own_rows"][...], summed.reshape(b_half * rows, lanes), 3)
    half = folded.shape[0] // 2
    return right(folded[:half], k["own_lo"][...], 3) + right(folded[half:], k["own_hi"][...], 3)


def unpack(gathered, counts, g):
    nx, ny, nz = counts
    x, y, z = (lax.axis_index(name) for name in NAMES)
    half, rows, lanes = gathered.shape[1:]
    low = lax.broadcasted_iota(jnp.int32, (half, rows, lanes), 2) < lanes // 2
    for dx in range(nx):
        for dz in range(nz):
            for pair in range(ny // 2):
                parts = []
                for dy in (2 * pair, 2 * pair + 1):
                    index = (lax.rem(x + dx, nx) * ny + lax.rem(y + dy, ny)) * nz
                    parts.append(gathered[index + lax.rem(z + dz, nz)])
                turned = [pltpu.roll(part, lanes // 2, 2) for part in parts]
                where = (pl.ds(dz * rows, rows), pl.ds(pair * lanes, lanes))
                start = 2 * half * dx
                g[(pl.ds(start, half), *where)] = jnp.where(low, parts[0], turned[1])
                g[(pl.ds(start + half, half), *where)] = jnp.where(low, turned[0], parts[1])


def solve(k, kind, values, shift):
    shape = values.shape
    flat = values.reshape(shape[0] * shape[1], shape[2])
    spectrum = dot(k["spectrum_rows"][...], dot(flat, k["spectrum_lanes"][...]))
    spectrum = spectrum / (k["eigen"][...] + shift)
    fine = dot(k[kind + "_rows2"][...], dot(spectrum, k[kind + "_lanes2"][...]))
    return fine.reshape(shape)


def cycle2(k, v, g, shift):
    weight = 0.25**2
    diagonal = 6.0 * weight + shift
    damp = DAMPING / diagonal
    if v is None:
        v = damp * g
    else:
        v = v + damp * (g - (diagonal * v - weight * around_all(v)))
    v = v + solve(k, "linear", g - (diagonal * v - weight * around_all(v)), shift)
    return v + damp * (g - (diagonal * v - weight * around_all(v)))


def down(k, t, shape2):
    flat = row_blocks(k["down_rows"][...], t[...].reshape(-1, t.shape[2]), 3)
    return right(flat, k["down_lanes"][...], 3).reshape(shape2)


def up(k, kind, level, values, z):
    flat = right(values, k[kind + "_lanes" + level][...], 2)
    z[...] = row_blocks(k[kind + "_rows" + level][...], flat, 2).reshape(z.shape)


def blend(z, i, weights, count):
    total = None
    for offset, weight in weights.items():
        index = i + offset
        index = index if count is None else lax.rem(index + count, count)
        term = weight * z[index]
        total = term if total is None else total + term
    return total


def up1(k, kind, values, z, v, add):
    count = z.shape[0]
    up(k, kind, "1", values.reshape(-1, values.shape[2]), z)
    weights = CUBIC if kind == "cubic" else LINEAR

    def body(i):
        for odd in (0, 1):
            p = 2 * i + odd + 1
            value = blend(z, i, weights[odd], count)
            v[p] = v[p] + value if add else value

    loop(count, body)
    close(v)


def cycle1(k, v, u, g, t, z, shift, zero, shape2):
    weight = 0.25
    diagonal = 6.0 * weight + shift
    damp = DAMPING / diagonal
    count = g.shape[0]

    def before(p):
        if zero:
            u[p + 1] = damp * g[p]
        else:
            center, rest = defect_plane(v, p + 1, g[p], weight, diagonal)
            u[p + 1] = center + damp * rest

    loop(count, before)
    close(u)

    def residue(i):
        t[i] = (
            defect_plane(u, 2 * i + 1, g[2 * i], weight, diagonal)[1]
            + defect_plane(u, 2 * i + 2, g[2 * i + 1], weight, diagonal)[1]
        )

    loop(count // 2, residue)
    correction = cycle2(k, None, down(k, t, shape2), shift)
    up1(k, "linear", correction, z, u, True)

    def after(p):
        center, rest = defect_plane(u, p + 1, g[p], weight, diagonal)
        v[p + 1] = center + damp * rest

    loop(count, after)
    close(v)


def window(k, kind, v, zw, span, write):
    count = v.shape[0] - 2
    values = jnp.concatenate([v[count - 3 : count + 1], v[1 : span - 3]], axis=0)
    up(k, kind, "0", values.reshape(-1, values.shape[2]), zw)
    weights = CUBIC if kind == "cubic" else LINEAR

    def body(i):
        for odd in (0, 1):
            write(2 * i + odd, blend(zw, i + 3, weights[odd], None))

    loop(span - 6, body)


def own_defect(v, p, f, weight, diagonal):
    rows, lanes = f.shape
    inside = (pl.ds(8, rows), pl.ds(lanes, lanes))
    wide = v[p + 1, pl.ds(8, rows), :]
    center = wide[:, lanes:]
    beside = v[(p, *inside)] + v[(p + 2, *inside)]
    beside = beside + v[p + 1, pl.ds(7, rows), pl.ds(lanes, lanes)]
    beside = beside + v[p + 1, pl.ds(9, rows), pl.ds(lanes, lanes)]
    beside = beside + pltpu.roll(wide, 1, 1)[:, lanes:]
    beside = beside + pltpu.roll(wide, 2 * lanes - 1, 1)[:, lanes:]
    return center, f - (diagonal * center - weight * beside)


def position():
    return tuple(lax.axis_index(name) for name in NAMES)


def partner_of(place):
    x, y, z = place
    return (x, y + 1 - 2 * lax.rem(y, 2), z)


def shifted(place, counts, offset):
    return tuple(
        lax.rem(at + step + count, count) for at, step, count in zip(place, offset, counts)
    )


def slot(place, counts):
    return (place[0] * counts[1] + place[1]) * counts[2] + place[2]


def chip_offsets(counts):
    nx, ny, nz = counts
    offsets = [
        (dx, dy, dz) for dx in range(nx) for dy in range(0, ny, 2) for dz in range(nz)
    ]

    def hops(offset):
        return sum(min(step, count - step) for step, count in zip(offset, (nx, ny, nz)))

    return sorted(offsets[1:], key=hops, reverse=True)


def face_offsets(counts):
    faces = []
    for axis in range(3):
        for side, step in ((0, -1), (1, 1)):
            offset = [0, 0, 0]
            offset[axis] = step
            faces.append((tuple(offset), axis, side))
    return faces


def greet(barrier, places):
    for place in places:
        pl.semaphore_signal(barrier, inc=1, device_id=place, device_id_type=MESH)


def remote(src, dst, send, recv, place):
    return pltpu.make_async_remote_copy(
        src_ref=src, dst_ref=dst, send_sem=send, recv_sem=recv, device_id=place, device_id_type=MESH
    )


def spread(counts, block, gathered, sems):
    send, recv, relay_send, relay_recv = sems
    me = position()
    partner = partner_of(me)
    along, across = stages(counts)
    number = {offset: n for n, offset in enumerate(chip_offsets(counts))}
    mine = gathered.at[slot(me, counts)]
    copies, relays = {}, []

    def pass_on(offset, source, target, place):
        n = number[offset]
        copies[offset] = remote(source, target, send.at[n], recv.at[n], place)
        copies[offset].start()

    def relay(n, source, target):
        relays.append(remote(source, target, relay_send.at[n], relay_recv.at[n], partner))
        relays[-1].start()

    for offset in along + across:
        pass_on(offset, block, mine, shifted(me, counts, offset))
    relay(len(number), block, mine)

    def arrival(offset):
        copies[offset].wait_recv()
        source = shifted(me, counts, tuple(-step for step in offset))
        return gathered.at[slot(source, counts)]

    def finish():
        gathered[slot(me, counts)] = block[...]
        for first in along[::-1]:
            arrived = arrival(first)
            for second in across:
                place = shifted(me, counts, second)
                pass_on((first[0], second[1], second[2]), arrived, arrived, place)
            relay(number[first], arrived, arrived)
        for first in ((0, 0, 0), *along[::-1]):
            for second in across[::-1]:
                offset = (first[0], second[1], second[2])
                arrived = arrival(offset)
                relay(number[offset], arrived, arrived)
        for copy in copies.values():
            copy.wait_send()
        for copy in relays:
            copy.wait()

    return finish


def stages(counts):
    offsets = chip_offsets(counts)
    along = [offset for offset in offsets if offset[1:] == (0, 0)]
    across = [offset for offset in offsets if offset[0] == 0]
    return along, across


def gather_places(counts):
    me = position()
    along, across = stages(counts)
    return [shifted(me, counts, offset) for offset in along + across] + [partner_of(me)]


def first_part(k, counts, source, f, gathered, halos, block, owns, sems, face_sems):
    own_planes, own_rows, own_columns = owns
    planes, rows, columns = halos
    face_send, face_recv = face_sems
    me = position()
    barrier = pltpu.get_barrier_semaphore()
    faces = face_offsets(counts)
    places = gather_places(counts) + [shifted(me, counts, offset) for offset, _, _ in faces]
    greet(barrier, places)
    b0, b1, b2 = source.shape
    summed = source[...].reshape(b0 // 2, 2, b1, b2)
    block[...] = restrict_own(k, summed[:, 0] + summed[:, 1]).reshape(block.shape)
    own_planes[0] = source[0]
    own_planes[1] = source[b0 - 1]
    own_rows[0] = source[:, pl.ds(0, 1), :]
    own_rows[1] = source[:, pl.ds(b1 - 1, 1), :]
    turned = source[...].reshape(b0 * b1, b2).T
    own_columns[0] = turned[:8]
    own_columns[1] = turned[b2 - 8 :]
    pl.semaphore_wait(barrier, len(places))
    finish = spread(counts, block, gathered, sems)
    buffers = ((own_planes, planes), (own_rows, rows), (own_columns, columns))
    order = (0, 2, 1)
    copies = []
    for n, (offset, axis, side) in enumerate(faces):
        own, halo = buffers[order[axis]]
        place = shifted(me, counts, offset)
        copies.append(
            remote(own.at[side], halo.at[1 - side], face_send.at[n], face_recv.at[n], place)
        )
        copies[-1].start()
    f[...] = jnp.zeros_like(f)
    f[1 : b0 + 1, pl.ds(8, b1), pl.ds(b2, b2)] = source[...]
    finish()
    for copy in copies:
        copy.wait()


def second_part(k, counts, shape2, span, shift, gathered, source, halos, out, buffers):
    g, v, u, t, z, zw, v0, v1, f, summed = buffers
    plane_halo, row_halo, column_halo = halos
    unpack(gathered, counts, g)
    b0, b1, b2 = source.shape
    rows, lanes = pl.ds(8, b1), pl.ds(b2, b2)
    f[0, rows, lanes] = plane_halo[0]
    f[b0 + 1, rows, lanes] = plane_halo[1]
    f[1 : b0 + 1, pl.ds(7, 1), lanes] = row_halo[0]
    f[1 : b0 + 1, pl.ds(8 + b1, 1), lanes] = row_halo[1]
    middle = jnp.zeros((b2 - 16, b0 * b1), jnp.float32)
    turned = jnp.concatenate([column_halo[1], middle, column_halo[0]], axis=0)
    f[1 : b0 + 1, rows, pl.ds(0, b2)] = turned.T.reshape(b0, b1, b2)
    def pair_sum(i):
        t[i] = g[2 * i] + g[2 * i + 1]

    loop(g.shape[0] // 2, pair_sum)
    forcing2 = down(k, t, shape2)
    iterate2 = cycle2(k, solve(k, "cubic", forcing2, shift), forcing2, shift)
    up1(k, "cubic", iterate2, z, v, False)
    cycle1(k, v, u, g, t, z, shift, False, shape2)

    def put(p, value):
        v0[p] = value

    window(k, "cubic", v, zw, span, put)
    diagonal = 6.0 + shift
    damp = DAMPING / diagonal

    def before(p):
        center, rest = defect_plane(v0, p + 1, f[p], 1.0, diagonal)
        v1[p] = center + damp * rest

    loop(b0 + 2, before)

    def residue(i):
        summed[i] = (
            own_defect(v1, 2 * i, source[2 * i], 1.0, diagonal)[1]
            + own_defect(v1, 2 * i + 1, source[2 * i + 1], 1.0, diagonal)[1]
        )

    loop(b0 // 2, residue)
    out[...] = restrict_own(k, summed[...]).reshape(out.shape)


def third_part(k, counts, shape2, span, shift, gathered, source, out, buffers):
    g, v, u, t, z, zw, w, v1 = buffers[:8]
    unpack(gathered, counts, g)
    cycle1(k, v, u, g, t, z, shift, True, shape2)
    b0 = source.shape[0]

    def put(p, value):
        w[p] = value

    window(k, "linear", v, zw, span, put)

    def add(p):
        w[p] = v1[p] + w[p + 1]

    loop(b0 + 2, add)
    diagonal = 6.0 + shift
    damp = DAMPING / diagonal

    def after(p):
        center, rest = own_defect(w, p, source[p], 1.0, diagonal)
        out[p] = center + damp * rest

    loop(b0, after)


def kernel(names, counts, shape2, span, *refs):
    k = dict(zip(names, refs))
    shift_ref, source, out, *rest = refs[len(names) :]
    shift = shift_ref[0]
    landing, later, *halos = rest[:5]
    block, block_later, *owns = rest[5:10]
    buffers = rest[10:20]
    sems, sems_later, face_sems = rest[20:24], rest[24:28], rest[28:30]
    f = buffers[8]
    first_part(k, counts, source, f, landing, halos, block, owns, sems, face_sems)
    second_part(k, counts, shape2, span, shift, landing, source, halos, block_later, buffers)
    spread(counts, block_later, later, sems_later)()
    third_part(k, counts, shape2, span, shift, later, source, out, buffers)


def per_device(counts, source, shift):
    nx, ny, nz = counts
    b0, b1, b2 = source.shape
    sizes = (b0 * nx, b1 * nz, b2 * ny)
    table = constants(source.shape, sizes)
    m0, m1, m2 = (size // 2 for size in sizes)
    shape2 = tuple(size // 4 for size in sizes)
    span = b0 // 2 + 8
    wide = (b1 + 16, 2 * b2)
    packed = (b0 // 4, b1 // 2, b2)
    devices = nx * ny * nz
    chips = devices // 2
    vmem = pl.BlockSpec(memory_space=pltpu.VMEM)

    def field(*shape):
        return pltpu.VMEM(shape, jnp.float32)

    faces = [field(2, b1, b2), field(2, b0, 1, b2), field(2, 8, b0 * b1)]
    buffers = [
        field(m0, m1, m2),
        field(m0 + 2, m1, m2),
        field(m0 + 2, m1, m2),
        field(m0 // 2, m1, m2),
        field(m0 // 2, m1, m2),
        field(span, *wide),
        field(b0 + 4, *wide),
        field(b0 + 2, *wide),
        field(b0 + 2, *wide),
        field(b0 // 2, b1, b2),
    ]
    sems = [pltpu.SemaphoreType.DMA((max(chips - 1, 1),))] * 2
    sems += [pltpu.SemaphoreType.DMA((chips,))] * 2
    landing = [field(devices, *packed)] * 2 + faces
    names = tuple(table)
    return pl.pallas_call(
        functools.partial(kernel, names, counts, shape2, span),
        out_shape=jax.ShapeDtypeStruct(source.shape, jnp.float32),
        in_specs=[vmem] * len(names) + [pl.BlockSpec(memory_space=pltpu.SMEM), vmem],
        out_specs=vmem,
        scratch_shapes=landing
        + [field(*packed)] * 2
        + faces
        + buffers
        + sems * 2
        + [pltpu.SemaphoreType.DMA((6,))] * 2,
        compiler_params=pltpu.CompilerParams(
            vmem_limit_bytes=60 * 1024 * 1024, collective_id=0, has_side_effects=True
        ),
    )(*[jnp.asarray(table[name]) for name in names], shift, source)


def modes(count, depth):
    if depth == 0:
        return [(0, k) for k in range(count // 2)] + [(1, k) for k in range(1, count // 2 + 1)]
    half = count // 2
    low = modes(half, depth - 1)
    high = []
    for kind, k in low:
        if kind == 0:
            high.append((0, half - k if k else half // 2))
        else:
            high.append((1, half - k if k < half // 2 else half))
    return low + high


def waves(count, order):
    cells = (np.arange(count) + 0.5) * (2.0 * np.pi / count)
    return np.stack([np.sin(k * cells) if kind else np.cos(k * cells) for kind, k in order], axis=1)


def analysis(waves_):
    return waves_.T / np.sum(waves_**2, axis=0)[:, None]


def two_blocks(matrix, axis):
    first, second = np.split(matrix, 2, axis=axis)
    return np.concatenate([np.diag(first), np.diag(second)])


def factors(m):
    orders = modes(m, 2), modes(m // 2, 1), modes(m // 4, 0)
    bases = [waves(len(order), order) for order in orders]
    t = {"waves": bases[0]}
    for level, fine, coarse in (("1", bases[0], bases[1]), ("2", bases[1], bases[2])):
        n = fine.shape[0]
        t["r" + level] = two_blocks(analysis(coarse) @ (0.5 * pairs(n // 2)) @ fine, 1)
        for name, weights in (("p", LINEAR), ("q", CUBIC)):
            matrix = interpolation(n // 2, range(n), weights)
            t[name + level] = two_blocks(analysis(fine) @ matrix @ coarse, 0)
        order = orders[int(level) - 1]
        t["e" + level] = np.array([2.0 - 2.0 * np.cos(2.0 * np.pi * k / n) for _, k in order])
    t["c3"] = np.array([np.cos(2.0 * np.pi * k / (m // 4)) for _, k in orders[2]], np.float32)
    fine = np.eye(2 * m)
    lap = 2.0 * fine - np.roll(fine, 1, 0) - np.roll(fine, -1, 0)
    current = interpolation(m, range(2 * m), CUBIC) @ bases[0]
    for i in range(3):
        t[f"m{i}"] = np.sum(analysis(bases[0]).T * ((0.5 * pairs(m)) @ current), axis=0)
        current = lap @ current
    return t


def near(matrix, axis=0):
    return np.roll(matrix, 1, axis) + np.roll(matrix, -1, axis)


def synthesis(t, cells, weights, powers):
    m = t["waves"].shape[0]
    matrix = interpolation(m, range(2 * m), weights) @ t["waves"]
    result = []
    for _ in range(powers):
        result.append(matrix[np.array(cells) % (2 * m)])
        matrix = near(matrix)
    return result


def pick(matrix, rows, columns):
    return matrix[np.array(rows) % matrix.shape[0]][:, np.array(columns) % matrix.shape[1]]


def late_kinds(m, rows, columns):
    plain = interpolation(m, range(2 * m), LINEAR)
    return [pick(kind, rows, columns) for kind in (plain, near(plain), near(plain, 1), near(near(plain), 1))]


def mixed(p, r):
    return [
        np.kron(p[0], r[0]),
        np.kron(p[1], r[0]) + np.kron(p[0], r[1]),
        np.kron(p[2], r[0]) + np.kron(p[0], r[2]),
        np.kron(p[3], r[0]) + np.kron(p[0], r[3]) + np.kron(p[2], r[1]) + np.kron(p[1], r[2]),
    ]


def exact(matrix):
    result = np.asarray(matrix, jnp.bfloat16)
    assert np.all(result.astype(np.float64) == matrix)
    return result


def halves(matrix, axis):
    high = np.asarray(matrix, jnp.bfloat16)
    low = np.asarray(matrix - high.astype(np.float64), jnp.bfloat16)
    return np.concatenate([high, low], axis=axis)


def halved_rows(m0, m1):
    index = np.arange(m0 * m1).reshape(2, 2, 2, m0 // 8, 2, 2, m1 // 4)
    index = index.transpose(2, 0, 4, 1, 5, 3, 6).reshape(2, 4, -1)
    return index, index[:, 0].reshape(-1), index.reshape(-1)


def own_table(half):
    count = 2 * half
    four = sum(np.roll(np.kron(np.eye(half), np.eye(2)[:, :1]), s, axis=0) for s in (-1, 0, 1, 2))
    four[count - 1, 0] = 0.0
    four[0, half - 1] = 0.0
    beside = np.zeros((count, half))
    beside[count - 1, 0] = beside[0, half - 1] = 1.0
    own = np.zeros((2, count, 3, 2, half))
    for n, part in enumerate((pairs(half).T, beside, four)):
        for s in range(2):
            own[s, :, n, s] = 0.125 * part
    return np.asarray(own.reshape(2 * count, 3 * count), jnp.bfloat16)


def two_levels(count):
    whole = 2 * count
    fine, half = np.eye(whole), np.eye(whole // 2)
    near, near1 = (np.roll(e, 1, 0) + np.roll(e, -1, 0) for e in (fine, half))
    down, down1 = pairs(whole // 2), pairs(whole // 4)
    start = count // 2
    rows = range(start // 4 - 1, (start + count) // 4 + 1)
    kinds = (down1 @ down, down1 @ down @ near, down1 @ near1 @ down, down1 @ near1 @ down @ near)
    return [kind[rows, start : start + count] for kind in kinds]


def early_tables(block):
    b0, b1, b2 = block
    (p, r, c) = ([*two_levels(size)] for size in block)
    full = mixed(p, r)
    rows = np.zeros((4, 3, 16, b0 * b1))
    rows[:, :, : 2 * r[0].shape[0]] = np.stack(full).reshape(4, 3, 2 * r[0].shape[0], b0 * b1)
    lanes = np.zeros((4, b2, b2))
    for n in range(4):
        lanes[n, :, : c[n].shape[0]] = c[n].T / 64.0
    return exact(rows.reshape(-1, b0 * b1)), exact(lanes.reshape(-1, b2))


def fast_constants(counts, block, sizes):
    nx, ny, nz = counts
    b0, b1, b2 = block
    m0, m1, m2 = (size // 2 for size in sizes)
    t0, t1, t2 = (factors(m) for m in (m0, m1, m2))
    parts, index2, index1 = halved_rows(m0, m1)
    i0, i1 = index1 // m1, index1 % m1
    j0, j1 = index2 // m1, index2 % m1
    rows2 = len(index2)

    def across(name, k, l, op=np.multiply):
        return op(t0[name][k], t1[name][l])

    def joint(a, c):
        return t0[a][i0] * t1[c][i1]

    columns = [across("r1", i0, i1), across("p1", i0, i1), across("q1", i0, i1), across("e1", i0, i1, np.add)]
    columns += [joint("m0", "m0"), joint("m1", "m0") + joint("m0", "m1")]
    columns += [joint("m2", "m0") + joint("m0", "m2") + 2.0 * joint("m1", "m1")]
    by_row = np.zeros((m0 * m1, 128))
    by_row[:, : len(columns)] = np.stack(columns, axis=1)
    for n, name in enumerate(("r2", "p2", "q2", "e2")):
        by_row[:rows2, 8 + n] = across(name, j0, j1, np.add if name == "e2" else np.multiply)
    by_lane = np.zeros((16, m2))
    for n, name in enumerate(("r1", "p1", "q1", "e1", "m0", "m1", "m2")):
        by_lane[n] = t2[name]
    for n, name in enumerate(("r2", "p2", "q2", "e2")):
        by_lane[8 + n, : m2 // 2] = t2[name]
    two = np.float32(2.0)
    eigen = np.float32(6.0) - two * t0["c3"][:, None, None]
    eigen = eigen - two * t1["c3"][None, :, None] - two * t2["c3"][None, None, :]
    eigen = (np.float32(0.25 ** (LEVELS - 1)) * eigen).reshape(rows2 // 4, m2 // 4)
    early_rows, early_lanes = early_tables(block)
    table = {"own": own_table(b2 // 2), "early_rows": early_rows, "early_lanes": early_lanes}
    small = {"by_row": by_row, "by_lane": by_lane, "eigen": np.concatenate([eigen, eigen], axis=1)}
    table.update({name: np.asarray(value, np.float32) for name, value in small.items()})

    a0, a1 = (analysis(waves(m // 2, modes(m // 2, 1))) for m in (m0, m1))
    a2 = analysis(waves(m2 // 2, modes(m2 // 2, 1)))
    p0, p1, p2 = b0 // 4, b1 // 4, b2 // 4
    wide = p2 + 2
    lanes = np.zeros((ny, b2, 3, m2 // 2))
    for dy in range(ny):
        for n in range(3):
            lanes[dy, 42 * n : 42 * n + wide, n] = a2[:, np.arange(p2 * dy - 1, p2 * dy + p2 + 1) % (m2 // 2)].T
    table["level2_lanes"] = halves(lanes.reshape(ny * b2, -1), 0)
    n, dx, dz, c, r = np.meshgrid(*(range(k) for k in (3, nx, nz, 2, p1 + 2)), indexing="ij")
    planes = (p0 * dx + 2 * n + c - 1 - p0 // 2) % (m0 // 2)
    rows = (p1 * dz + r - 1) % (m1 // 2)
    full = np.zeros((rows2, 3, nx, nz, 16))
    full[..., : 2 * (p1 + 2)] = (a0[j0][:, planes] * a1[j1][:, rows]).reshape(rows2, 3, nx, nz, -1)
    table["level2_rows"] = halves(full.reshape(rows2, -1), 1)

    forward = analysis(t0["waves"])[i0][:, : m0 // 2, None] * analysis(t1["waves"])[i1][:, None, :]
    table["forward_rows"] = halves(forward.reshape(2, m0 * m1 // 2, -1), 2)
    table["forward_lanes"] = halves(analysis(t2["waves"]).T, 0)
    for name, weights, powers in (("cubic", CUBIC, 3), ("linear", LINEAR, 2)):
        p = synthesis(t0, range(b0 // 2), weights, powers)
        r = synthesis(t1, range(b1), weights, powers)
        full = []
        for part in parts.reshape(2, -1):
            q0 = [matrix[:, part // m1][:, None, :] for matrix in p]
            q1 = [matrix[:, part % m1][None, :, :] for matrix in r]
            kinds = [q0[0] * q1[0], q0[1] * q1[0] + q0[0] * q1[1]]
            if powers == 3:
                kinds.append(q0[2] * q1[0] + 2.0 * q0[1] * q1[1] + q0[0] * q1[2])
            full.append(np.stack(kinds).reshape(-1, part.size))
        table[name + "_rows"] = halves(np.stack(full), 2)
        lanes = [matrix.T for matrix in synthesis(t2, range(b2), weights, powers)]
        table[name + "_lanes"] = halves(np.concatenate(lanes), 0)
    p = late_kinds(m0, range(b0), range(-2, b0 // 2 + 2))
    r = late_kinds(m1, range(b1), range(m1))
    table["late_rows"] = exact(np.concatenate(mixed(p, r), axis=1))
    table["late_lanes"] = exact(np.concatenate([c.T for c in late_kinds(m2, range(b2), range(m2))], axis=1))
    return table


def split(values):
    high = values.astype(jnp.bfloat16)
    return high, (values - high.astype(jnp.float32)).astype(jnp.bfloat16)


def by_right(values, table):
    high, low = split(values)
    depth = values.shape[1]
    first, second = table[:depth], table[depth:]
    return jnp.dot(
        jnp.concatenate([high, low, high], axis=1),
        jnp.concatenate([first, first, second], axis=0),
        preferred_element_type=jnp.float32,
    )


def by_left(table, values):
    high, low = split(values)
    depth = values.shape[0]
    first, second = table[:, :depth], table[:, depth:]
    return jnp.dot(
        jnp.concatenate([first, first, second], axis=1),
        jnp.concatenate([high, low, high], axis=0),
        preferred_element_type=jnp.float32,
    )


def fold(values):
    n = values.shape[0] // 8
    parts = []
    for kind in range(2):
        quarter = [values[(4 * kind + i) * n : (4 * kind + i + 1) * n] for i in range(4)]
        parts.append((quarter[0] + quarter[1]) + (quarter[2] + quarter[3]))
    total = jnp.concatenate(parts, axis=0)
    return total + pltpu.roll(total, total.shape[1] // 2, 1)


def unfold(values):
    n = values.shape[0] // 2
    return jnp.concatenate([values[:n]] * 4 + [values[n:]] * 4, axis=0)


def own_parts(source, own, outs, alpha, beta):
    block, across, along_rows, along_planes, rest = outs
    b0, b1, b2 = source.shape
    h0, h1 = b0 // 2, b1 // 2
    first = [source[p, pl.ds(0, h1, stride=2), :] for p in range(b0)]
    second = [source[p, pl.ds(1, h1, stride=2), :] for p in range(b0)]
    summed = [a + b for a, b in zip(first, second)]
    row = lax.broadcasted_iota(jnp.int32, (h1, b2), 0)
    zero = jnp.zeros((h1, b2), jnp.float32)
    whole, faces, inner = [], [], []
    for c in range(h0):
        total = summed[2 * c] + summed[2 * c + 1]
        down = pltpu.roll(second[2 * c] + second[2 * c + 1], 1, 0)
        up = pltpu.roll(first[2 * c] + first[2 * c + 1], h1 - 1, 0)
        whole.append(total)
        faces.append(jnp.where(row == 0, down, jnp.where(row == h1 - 1, up, zero)))
        near = 2.0 * total + jnp.where(row > 0, down, zero) + jnp.where(row < h1 - 1, up, zero)
        if c > 0:
            near = near + summed[2 * c - 1]
        if c < h0 - 1:
            near = near + summed[2 * c + 2]
        inner.append(near)

    def pack(planes):
        half = len(planes) // 2
        return [jnp.concatenate([planes[i], planes[i + half]], axis=1) for i in range(half)]

    ends = [jnp.concatenate([summed[b0 - 1], summed[0]], axis=1)]
    stacked = jnp.concatenate(pack(whole) + pack(faces) + pack(inner) + ends + [jnp.zeros((8, 2 * b2), jnp.float32)], axis=0)
    parts = parts_of(stacked, 3)
    weights = own[...]
    result = jnp.dot(
        jnp.concatenate(parts, axis=1),
        jnp.concatenate([weights] * 3, axis=0),
        preferred_element_type=jnp.float32,
    )
    n = h0 // 2 * h1
    shape = block.shape
    mine = result[:n, :b2]
    block[...] = mine.reshape(shape)
    across[...] = result[:n, b2 : 2 * b2].reshape(shape)
    along_rows[...] = result[n : 2 * n, :b2].reshape(shape)
    along_planes[...] = result[3 * n : 3 * n + h1, :b2]
    rest[...] = (alpha * mine + beta * (result[2 * n : 3 * n, :b2] + result[:n, 2 * b2 :])).reshape(shape)


def early_part(source, rows_table, lanes_table, weights):
    keep0, near0, keep1, near1 = weights
    b0, b1, b2 = source.shape
    result = jnp.dot(
        jnp.concatenate([rows_table[...]] * 3, axis=1),
        jnp.concatenate(parts_of(source[...].reshape(b0 * b1, b2), 3), axis=0),
        preferred_element_type=jnp.float32,
    )
    n = result.shape[0] // 4
    plain, first, second, both = (result[i * n : (i + 1) * n] for i in range(4))
    joint = near0 * near1
    columns = (
        (keep0 * keep1) * plain + (keep1 * near0) * first + (keep0 * near1) * second + joint * both,
        (keep1 * near0) * plain + joint * second,
        (keep0 * near1) * plain + joint * first,
        joint * plain,
    )
    result = jnp.dot(
        jnp.concatenate(parts_of(jnp.concatenate(columns, axis=1), 3), axis=1),
        jnp.concatenate([lanes_table[...]] * 3, axis=0),
        preferred_element_type=jnp.float32,
    )
    total = result[:16] + pltpu.roll(result[16:32], 42, 1)
    return (total + pltpu.roll(result[32:], 84, 1)).reshape(2, 8, b2)


def beyond(place, counts):
    x, y, z = place
    return (x, lax.rem(y - 1 + 2 * lax.rem(y, 2) + counts[1], counts[1]), z)


def close_by(counts):
    chosen = []
    for offset in chip_offsets(counts):
        step = offset[0]
        if min(step, counts[0] - step) <= 1:
            part = 0 if step == 0 or counts[0] == 2 else (1 if step == 1 else -1)
            chosen.append((offset, part))
    return chosen


def wait_for(ref, sem):
    pltpu.make_async_copy(ref, ref, sem).wait()


class TwoStage:
    def __init__(self, counts, near, far, block, landing, sems):
        self.counts, self.near, self.far = counts, near, far
        self.block, self.landing = block, landing
        self.sent, self.arrived, self.relay_sent, self.relayed = sems
        self.count = 0

    def at(self, offset):
        source = shifted(position(), self.counts, tuple(-step for step in offset))
        return self.landing.at[slot(source, self.counts)]

    def send(self, source, target, step, sem):
        place = shifted(position(), self.counts, step)
        remote(source, target, self.sent.at[0], self.arrived.at[sem], place).start()
        self.count += 1

    def start(self, offsets):
        for offset in offsets:
            sem = self.near.index(offset) if offset in self.near else len(self.near)
            self.send(self.block, self.at((0, 0, 0)), offset, sem)

    def relay(self, source, target):
        remote(source, target, self.relay_sent.at[0], self.relayed.at[0], partner_of(position())).start()

    def own(self):
        self.relay(self.block, self.at((0, 0, 0)))

    def forward(self):
        for n, first in enumerate(self.near):
            arrived = self.at(first)
            wait_for(arrived, self.arrived.at[n])
            for second in self.far:
                self.send(arrived, arrived, second, len(self.near) + 1 + n)
            self.relay(arrived, arrived)

    def rest(self):
        for n, first in enumerate(((0, 0, 0), *self.near)):
            wait_for(self.landing.at[pl.ds(0, len(self.far))], self.arrived.at[len(self.near) + n])
            for second in self.far:
                arrived = self.at(tuple(a + b for a, b in zip(first, second)))
                self.relay(arrived, arrived)

    def end(self):
        self.landing[slot(position(), self.counts)] = self.block[...]
        wait_for(self.landing.at[pl.ds(0, self.count)], self.sent.at[0])
        for sem in (self.relay_sent, self.relayed):
            wait_for(self.landing.at[pl.ds(0, self.count + 1)], sem.at[0])

    @staticmethod
    def semaphores(near):
        dma = pltpu.SemaphoreType.DMA
        return [dma((1,)), dma((2 * len(near) + 1,)), dma((1,)), dma((1,))]


def piece(ref, part):
    if part == 0:
        return ref
    half = ref.shape[0] // 2
    return ref.at[pl.ds(half if part == 1 else 0, half)]


class Close:
    def __init__(self, counts, chosen, block, landing, sems):
        self.counts, self.chosen = counts, chosen
        self.block, self.landing = block, landing
        self.sent, self.arrived, self.relay_sent, self.relayed = (sem.at[0] for sem in sems)
        self.blocks = sum(2 if part == 0 else 1 for _, part in chosen) // 2

    def at(self, offset):
        source = shifted(position(), self.counts, tuple(-step for step in offset))
        return self.landing.at[slot(source, self.counts)]

    def relay(self, source, target):
        remote(source, target, self.relay_sent, self.relayed, partner_of(position())).start()

    def start(self):
        mine = self.at((0, 0, 0))
        for offset, part in self.chosen:
            place = shifted(position(), self.counts, offset)
            remote(piece(self.block, part), piece(mine, part), self.sent, self.arrived, place).start()
        self.relay(self.block, mine)

    def rest(self):
        wait_for(self.landing.at[pl.ds(0, self.blocks)], self.arrived)
        for offset, part in self.chosen:
            arrived = piece(self.at(offset), part)
            self.relay(arrived, arrived)

    def end(self):
        self.landing[slot(position(), self.counts)] = self.block[...]
        wait_for(self.landing.at[pl.ds(0, self.blocks)], self.sent)
        for sem in (self.relay_sent, self.relayed):
            wait_for(self.landing.at[pl.ds(0, self.blocks + 1)], sem)


def exchange(counts, sent, received, send, recv):
    me = position()
    order = (0, 2, 1)
    for offset, axis, side in face_offsets(counts):
        which = order[axis]
        mine = sent[which] if len(sent[which]) == 1 else [sent[which][side]]
        place = shifted(me, counts, offset)
        remote(mine[0], received[2 * which + 1 - side], send.at[0], recv.at[0], place).start()


def prepare(k, many, few, shift):
    diagonal0, diagonal1, diagonal2 = (6.0 * 0.25**level + shift for level in range(3))
    sigma0, sigma1, sigma2 = diagonal0 - 6.0, diagonal1 - 1.5, diagonal2 - 0.375
    damp0, damp1, damp2 = DAMPING / diagonal0, DAMPING / diagonal1, DAMPING / diagonal2
    down, pre, fine_q, out_q, out_g, out_e, cross = many
    by_row, by_lane = k["by_row"], k["by_lane"]
    lanes = by_lane.shape[1]

    def level1(i):
        rows = pl.ds(pl.multiple_of(8 * i, 8), 8)
        column = by_row[rows, :]

        def tall(n):
            return jnp.broadcast_to(column[:, n : n + 1], (8, lanes))

        def wide(n):
            return jnp.broadcast_to(by_lane[n : n + 1, :], (8, lanes))

        r, p, q = (tall(n) * wide(n) for n in range(3))
        a = 0.25 * (tall(3) + wide(3)) + sigma1
        s = 1.0 - damp1 * a
        down[rows, :] = r
        pre[rows, :] = r * s
        fine_q[rows, :] = a * q
        out_q[rows, :] = s * s * q
        out_g[rows, :] = damp1 * (1.0 + s)
        out_e[rows, :] = s * p
        c0, c1, c2 = tall(4), tall(5), tall(6)
        first = sigma0 * c0 + c1 - damp0 * ((sigma0 * sigma0) * c0 + (2.0 * sigma0) * c1 + c2)
        second = c0 - (2.0 * damp0) * (sigma0 * c0 + c1)
        cross[rows, :] = first * wide(4) + second * wide(5) - (damp0 * c0) * wide(6)

    loop(by_row.shape[0] // 8, level1)
    rows2, lanes2 = few[0].shape
    column = by_row[:rows2, :]

    def tall(n):
        return jnp.broadcast_to(column[:, n : n + 1], (rows2, lanes2))

    def wide(n):
        return jnp.broadcast_to(by_lane[n : n + 1, :lanes2], (rows2, lanes2))

    r, p, q = (tall(n) * wide(n) for n in (8, 9, 10))
    a = 0.0625 * (tall(11) + wide(11)) + sigma2
    s = 1.0 - damp2 * a
    values = (r, r * s, a * q, s * s * q, damp2 * (1.0 + s), s * p)
    for ref, value in zip(few, values):
        ref[...] = value
    k["inverse"][...] = 1.0 / (k["eigen"][...] + shift)


def level2(k, few, g):
    down, pre, fine_q, out_q, out_g, out_e = few
    e = unfold(fold(pre[...] * g) * k["inverse"][...])
    return out_g[...] * g + out_e[...] * e


def level2_full(k, few, g):
    down, pre, fine_q, out_q, out_g, out_e = few
    start = unfold(fold(down[...] * g) * k["inverse"][...])
    e = unfold(fold(pre[...] * (g - fine_q[...] * start)) * k["inverse"][...])
    return out_q[...] * start + out_g[...] * g + out_e[...] * e


def blocks_of(spectrum, i):
    rows2, lanes2 = spectrum.shape[0] // 4, spectrum.shape[1] // 2
    half = rows2 // 2
    base = 8 * i + 3 * half * lax.div(i, half // 8)
    for a in range(4):
        start = pl.multiple_of(base + a * half, 8)
        for c in range(2):
            yield (pl.ds(start, 8), pl.ds(c * lanes2, lanes2))


def spectral_u(k, many, few, spectrum, coupled, coarse):
    down, pre, fine_q, out_q, out_g, out_e, cross = many
    first, second, third = coarse
    steps = first.shape[0] // 8

    def at(i):
        return pl.ds(pl.multiple_of(8 * i, 8), 8)

    def restrict(i):
        first[at(i), :] = sum(down[w] * spectrum[w] for w in blocks_of(spectrum, i))

    loop(steps, restrict)
    second[...] = level2_full(k, few, first[...])

    def residue(i):
        u = second[at(i), :]
        first[at(i), :] = sum(pre[w] * (spectrum[w] - fine_q[w] * u) for w in blocks_of(spectrum, i))

    loop(steps, residue)
    third[...] = level2(k, few, first[...])

    def finish(i):
        u, e = second[at(i), :], third[at(i), :]
        total = None
        for w in blocks_of(spectrum, i):
            value = out_q[w] * u + out_g[w] * spectrum[w] + out_e[w] * e
            spectrum[w] = value
            value = cross[w] * value
            coupled[w] = value
            total = pre[w] * value if total is None else total + pre[w] * value
        first[at(i), :] = total

    loop(steps, finish)


def spectral_e(many, spectrum, coupled, e2):
    out_g, out_e = many[4], many[5]

    def finish(i):
        e = e2[pl.ds(pl.multiple_of(8 * i, 8), 8), :]
        for w in blocks_of(spectrum, i):
            spectrum[w] = out_e[w] * e - out_g[w] * coupled[w]

    loop(e2.shape[0] // 8, finish)


def unpack_centred(gathered, counts, g):
    nx, ny, nz = counts
    me = position()
    half, rows, lanes = gathered.shape[1:]
    planes = g.shape[0]
    low = lax.broadcasted_iota(jnp.int32, (half, rows, lanes), 2) < lanes // 2
    for dx in range(nx):
        for dz in range(nz):
            for pair in range(ny // 2):
                parts = [
                    gathered[slot(shifted(me, counts, (dx, dy, dz)), counts)] for dy in (2 * pair, 2 * pair + 1)
                ]
                turned = [pltpu.roll(part, lanes // 2, 2) for part in parts]
                where = (pl.ds(dz * rows, rows), pl.ds(pair * lanes, lanes))
                start = (2 * half * dx - half) % planes
                g[(pl.ds(start, half), *where)] = jnp.where(low, parts[0], turned[1])
                g[(pl.ds(2 * half * dx, half), *where)] = jnp.where(low, turned[0], parts[1])


def transform(k, counts, landing, g, spectrum):
    unpack_centred(landing, counts, g)
    m0, m1, m2 = g.shape
    half = m0 // 2
    depth = half * m1
    for kind in range(2):
        rows = [g[p] - g[m0 - 1 - p] if kind else g[p] + g[m0 - 1 - p] for p in range(half)]
        values = by_left(k["forward_rows"][kind], jnp.concatenate(rows, axis=0))
        spectrum[kind * depth : (kind + 1) * depth, :] = by_right(values, k["forward_lanes"])


def transform2(k, counts, landing):
    nx, ny, nz = counts
    me = position()
    columns = []
    for dy in range(ny):
        rows = [
            landing[slot(shifted(me, counts, (dx, dy, dz)), counts)].reshape(16, -1)
            for dx in range(nx)
            for dz in range(nz)
        ]
        columns.append(jnp.concatenate(rows, axis=0))
    values = by_right(jnp.concatenate(columns, axis=1), k["level2_lanes"])
    width = values.shape[1] // 3
    parts = [values[:, n * width : (n + 1) * width] for n in range(3)]
    return by_left(k["level2_rows"], jnp.concatenate(parts, axis=0))


def evaluate(k, kind, spectrum, mix, out):
    planes, rows, lanes = out.shape
    half = planes // 2
    depth = spectrum.shape[0] // 2
    parts = []
    for n in range(2):
        values = by_left(k[kind + "_rows"][n], spectrum[n * depth : (n + 1) * depth, :])
        pieces = [values[i : i + half * rows] for i in range(0, values.shape[0], half * rows)]
        columns = [sum(c * pieces[i] for i, c in enumerate(line) if c is not None) for line in mix]
        parts.append(by_right(jnp.concatenate(columns, axis=1), k[kind + "_lanes"]).reshape(half, rows, lanes))
    even, odd = parts
    for p in range(half):
        for index, value in ((half + p, even[p] + odd[p]), (half - 1 - p, even[p] - odd[p])):
            out[index] = out[index] + value


def unpack_near(gathered, counts, g):
    nx, ny, nz = counts
    me = position()
    half, rows, lanes = gathered.shape[1:]
    for dx, first, last in ((nx - 1, half - 2, half), (0, 0, half), (1, 0, 2)):
        shape = (last - first, rows, lanes)
        low = lax.broadcasted_iota(jnp.int32, shape, 2) < lanes // 2
        for dz in range(nz):
            for pair in range(ny // 2):
                parts = [
                    gathered[slot(shifted(me, counts, (dx, dy, dz)), counts), pl.ds(first, last - first)]
                    for dy in (2 * pair, 2 * pair + 1)
                ]
                turned = [pltpu.roll(part, lanes // 2, 2) for part in parts]
                where = (pl.ds(dz * rows, rows), pl.ds(pair * lanes, lanes))
                if dx != nx - 1:
                    start = 2 if dx == 0 else 2 + 2 * half
                    g[(pl.ds(start, last - first), *where)] = jnp.where(low, parts[0], turned[1])
                if dx != 1:
                    start = 2 + half if dx == 0 else 0
                    g[(pl.ds(start, last - first), *where)] = jnp.where(low, turned[0], parts[1])


def late_part(k, g, weights):
    keep0, near0, keep1, near1 = weights
    planes, m1, m2 = g.shape
    pieces = split(g[...].reshape(planes * m1, m2))
    table = k["late_lanes"][...]
    values = jnp.dot(
        jnp.concatenate(pieces, axis=1),
        jnp.concatenate([table, table], axis=0),
        preferred_element_type=jnp.float32,
    )
    lanes = values.shape[1] // 4
    a, b, c, d = (values[:, i * lanes : (i + 1) * lanes] for i in range(4))
    joint = near0 * near1
    stacked = (
        (keep0 * keep1) * a + (near0 * keep1) * b + (keep0 * near1) * c + joint * d,
        (near0 * keep1) * a + joint * c,
        (keep0 * near1) * a + joint * b,
        joint * a,
    )
    table = k["late_rows"][...]
    values = jnp.dot(
        jnp.concatenate([table, table], axis=1),
        jnp.concatenate(split(jnp.concatenate(stacked, axis=0)), axis=0),
        preferred_element_type=jnp.float32,
    )
    return values


def own_sweep(f, source, keep, damp, out):
    rows, lanes = source.shape[1:]

    def body(p):
        beside = f[p] + f[p + 2] + around(f[p + 1])
        out[p] = damp * ((1.0 + keep) * source[p] + damp * beside[:rows, :lanes])

    loop(source.shape[0], body)


def fast_kernel(names, counts, *refs):
    count = len(names)
    outside = dict(zip(names, refs))
    shift_ref, source_ref, out, *rest = refs[count:]

    def take(number):
        taken = rest[:number]
        del rest[:number]
        return taken

    k = dict(zip(names, take(count)))
    (source,) = take(1)
    landing_f, landing_h, landing_j = take(3)
    faces_in, halos = take(6), take(3)
    block_f, block_h, across, along_rows, local, along_planes = take(6)
    (block_j,) = take(1)
    own_planes, own_rows, own_columns = take(3)
    many, few, coarse = take(7), take(6), take(3)
    k["inverse"], g, near_h, spectrum, coupled, f = take(6)
    table_sems, *face_sems = take(5)
    sems_f, sems_h, sems_j = take(4), take(4), take(4)

    shift = shift_ref[0]
    me = position()
    barrier = pltpu.get_barrier_semaphore()
    places = [shifted(me, counts, offset) for offset in chip_offsets(counts)]
    places += [partner_of(me), beyond(me, counts)]
    greet(barrier, places)
    loads = {"source": pltpu.make_async_copy(source_ref, source, table_sems.at[count])}
    loads["source"].start()
    for n, name in enumerate(names):
        loads[name] = pltpu.make_async_copy(outside[name], k[name], table_sems.at[n])
        loads[name].start()

    b0, b1, b2 = source.shape
    diagonal, diagonal1 = 6.0 + shift, 1.5 + shift
    damp, damp1 = DAMPING / diagonal, DAMPING / diagonal1
    loads["source"].wait()
    loads["own"].wait()
    parts = (block_f, across, along_rows, along_planes, local)
    own_parts(source, k["own"], parts, 1.0 - damp * diagonal, damp)
    own_planes[0] = source[0]
    own_planes[1] = source[b0 - 1]
    own_rows[0] = source[:, pl.ds(0, 1), :]
    own_rows[1] = source[:, pl.ds(b1 - 1, 1), :]
    turned = source[...].reshape(b0 * b1, b2).T
    own_columns[0] = turned[:8]
    own_columns[1] = turned[b2 - 8 :]
    for name in ("early_rows", "early_lanes"):
        loads[name].wait()
    weights = (1.0 - damp * diagonal, damp, 1.0 - damp1 * diagonal1, 0.25 * damp1)
    block_j[...] = early_part(source, k["early_rows"], k["early_lanes"], weights)
    pl.semaphore_wait(barrier, len(places))

    exchange(counts, ([along_planes], [along_rows], [across]), faces_in, *face_sems[:2])
    along, across_all = stages(counts)
    gather_f = TwoStage(counts, along[::-1], across_all, block_f, landing_f, sems_f)
    gather_j = TwoStage(counts, across_all[::-1], along, block_j, landing_j, sems_j)
    gather_f.start(along + across_all)
    gather_j.start(across_all)
    gather_f.own()
    gather_j.own()

    for name in ("by_row", "by_lane", "eigen"):
        loads[name].wait()
    prepare(k, many, few, shift)
    for sem in face_sems[:2]:
        wait_for(f.at[pl.ds(0, 3)], sem.at[0])
    shape = local.shape
    lane = lax.rem(lax.broadcasted_iota(jnp.int32, shape, 2), b2 // 2)
    row = lax.broadcasted_iota(jnp.int32, shape, 1)
    from_planes, from_rows, from_lanes = faces_in[:2], faces_in[2:4], faces_in[4:6]
    total = jnp.where(lane == 0, from_lanes[0][...], 0.0) + jnp.where(lane == b2 // 2 - 1, from_lanes[1][...], 0.0)
    total = total + jnp.where(row == 0, from_rows[0][...], 0.0) + jnp.where(row == shape[1] - 1, from_rows[1][...], 0.0)
    block_h[...] = local[...] + damp * total
    low = lax.broadcasted_iota(jnp.int32, shape[1:], 1) < b2 // 2
    block_h[0] = block_h[0] + damp * jnp.where(low, from_planes[0][...], 0.0)
    end = shape[0] - 1
    block_h[end] = block_h[end] + damp * jnp.where(low, 0.0, from_planes[1][...])

    gather_f.forward()
    mine = [[own.at[side] for side in range(2)] for own in (own_planes, own_rows, own_columns)]
    exchange(counts, mine, [halo.at[side] for halo in halos for side in range(2)], *face_sems[2:4])
    gather_j.start(along)
    gather_j.forward()
    close_h = Close(counts, close_by(counts), block_h, landing_h, sems_h)
    close_h.start()
    gather_f.rest()
    for sem in face_sems[2:4]:
        wait_for(f.at[pl.ds(0, 2)], sem.at[0])
    f[...] = jnp.zeros_like(f)
    rows, lanes = pl.ds(0, b1), pl.ds(0, b2)
    f[1 : b0 + 1, rows, lanes] = source[...]
    f[0, rows, lanes] = halos[0][0]
    f[b0 + 1, rows, lanes] = halos[0][1]
    f[1 : b0 + 1, pl.ds(b1, 1), lanes] = halos[1][1]
    f[1 : b0 + 1, pl.ds(b1 + 7, 1), lanes] = halos[1][0]
    middle = jnp.zeros((b2 - 16, b0 * b1), jnp.float32)
    turned = jnp.concatenate([halos[2][1], middle, halos[2][0]], axis=0)
    f[1 : b0 + 1, rows, pl.ds(b2, b2)] = turned.T.reshape(b0, b1, b2)
    keep = 1.0 - damp * diagonal
    own_sweep(f, source, keep, damp, out)
    gather_f.end()
    for name in names:
        if name not in ("own", "early_rows", "early_lanes", "by_row", "by_lane", "eigen"):
            loads[name].wait()
    transform(k, counts, landing_f, g, spectrum)
    spectral_u(k, many, few, spectrum, coupled, coarse)
    gather_j.rest()
    close_h.rest()
    double = 2.0 * keep * damp
    square = damp * damp
    mix = ((keep * keep, double, square), (double, 2.0 * square, None), (square, None, None))
    evaluate(k, "cubic", spectrum, mix, out)
    close_h.end()
    gather_j.end()
    unpack_near(landing_h, counts, near_h)
    keep1 = 1.0 - damp1 * diagonal1
    coarse[1][...] = level2(k, few, transform2(k, counts, landing_j) - coarse[0][...])
    late = late_part(k, near_h, (keep, damp, damp1 * (1.0 + keep1), 0.25 * damp1 * damp1))
    out[...] = out[...] + late.reshape(out.shape)
    spectral_e(many, spectrum, coupled, coarse[1])
    evaluate(k, "linear", spectrum, ((keep, damp), (damp, None)), out)


def fast_per_device(counts, source, shift):
    nx, ny, nz = counts
    b0, b1, b2 = source.shape
    sizes = (b0 * nx, b1 * nz, b2 * ny)
    table = fast_constants(counts, source.shape, sizes)
    m0, m1, m2 = (size // 2 for size in sizes)
    rows = m0 * m1
    packed = (b0 // 4, b1 // 2, b2)
    devices = nx * ny * nz

    def field(*shape):
        return pltpu.VMEM(shape, jnp.float32)

    def in_hbm(value):
        return pltpu.with_memory_space_constraint(value, pltpu.HBM)

    names = tuple(table)
    tile = packed[1:]
    fine = [field(2, b1, b2), field(2, b0, 1, b2), field(2, 8, b0 * b1)]
    scratch = [pltpu.VMEM(table[name].shape, table[name].dtype) for name in names]
    scratch += [field(*source.shape), field(devices, *packed), field(devices, *packed), field(devices, 2, *tile)]
    scratch += [field(*tile)] * 2 + [field(*packed)] * 4 + fine
    scratch += [field(*packed)] * 5 + [field(*tile), field(2, *tile)] + fine
    scratch += [field(rows, m2)] * 7 + [field(rows // 4, m2 // 2)] * 9
    scratch += [field(rows // 16, m2 // 2), field(m0, m1, m2), field(b0 // 2 + 4, m1, m2)]
    scratch += [field(rows, m2), field(rows, m2), field(b0 + 2, b1 + 8, 2 * b2)]
    dma = pltpu.SemaphoreType.DMA
    scratch += [dma((len(names) + 1,))] + [dma((1,))] * 4
    along, across = stages(counts)
    scratch += TwoStage.semaphores(along) + [dma((1,))] * 4 + TwoStage.semaphores(across)
    return pl.pallas_call(
        functools.partial(fast_kernel, names, counts),
        out_shape=jax.ShapeDtypeStruct(source.shape, jnp.float32),
        in_specs=[pl.BlockSpec(memory_space=pltpu.HBM)] * len(names)
        + [pl.BlockSpec(memory_space=pltpu.SMEM), pl.BlockSpec(memory_space=pltpu.HBM)],
        out_specs=pl.BlockSpec(memory_space=pltpu.VMEM),
        scratch_shapes=scratch,
        compiler_params=pltpu.CompilerParams(
            vmem_limit_bytes=40 * 1024 * 1024, collective_id=0, has_side_effects=True
        ),
    )(*[in_hbm(jnp.asarray(table[name])) for name in names], shift, in_hbm(source))


def small_enough(counts, block):
    (nx, ny, nz), (b0, b1, b2) = counts, block
    rows = (b0 * nx // 2) * (b1 * nz // 2)
    return rows <= 512 and rows % 128 == 0 and (b0, b1, b2) == (16, 16, 128) and ny % 4 == 0 and min(counts) > 1


def dispatch(counts, source, shift):
    run = fast_per_device if small_enough(counts, source.shape) else per_device
    return run(counts, source, shift)


def solution(mesh):
    counts = tuple(mesh.shape[name] for name in NAMES)
    return jax.shard_map(
        functools.partial(dispatch, counts),
        mesh=mesh,
        in_specs=(P("gx", "gz", "gy"), P()),
        out_specs=P("gx", "gz", "gy"),
        check_vma=False,
    )
```

```python
import functools

import jax
import jax.numpy as jnp
import numpy as np
from jax import lax
from jax.experimental import pallas as pl
from jax.experimental.pallas import tpu as pltpu
from jax.sharding import PartitionSpec as P

LEVELS = 4
DAMPING = 6.0 / 7.0
PRECISE = lax.Precision.HIGHEST
CUBIC = (
    {-2: -5.0 / 128.0, -1: 35.0 / 128.0, 0: 105.0 / 128.0, 1: -7.0 / 128.0},
    {-1: -7.0 / 128.0, 0: 105.0 / 128.0, 1: 35.0 / 128.0, 2: -5.0 / 128.0},
)
LINEAR = ({-1: 0.25, 0: 0.75}, {0: 0.75, 1: 0.25})
NAMES = ("gx", "gy", "gz")
MESH = pl.DeviceIdType.MESH


def basis(count):
    cells = np.arange(count)
    columns, cosines = [], []
    for m in range(count):
        k = (m + 1) // 2
        angle = 2.0 * np.pi * k * cells / count
        column = np.cos(angle) if m % 2 == 1 or m == 0 else np.sin(angle)
        columns.append(column / np.sqrt(np.sum(column**2)))
        cosines.append(np.cos(2.0 * np.pi * k / count))
    return np.stack(columns, axis=1), np.array(cosines, np.float32)


def interpolation(coarse_count, fine_cells, weights):
    matrix = np.zeros((len(fine_cells), coarse_count))
    for row, cell in enumerate(fine_cells):
        for offset, weight in weights[cell % 2].items():
            matrix[row, (cell // 2 + offset) % coarse_count] += weight
    return matrix


def pairs(coarse_count):
    return np.kron(np.eye(coarse_count), np.ones((1, 2)))


def blocked(matrix):
    count = max(1, 128 // matrix.shape[1])
    return np.kron(np.eye(count), matrix)


def constants(block, sizes):
    b0, b1, b2 = block
    m0, m1, m2 = (size // 2 for size in sizes)
    q0, q1, q2 = (size // 4 for size in sizes)
    c0, c1, c2 = (size // 8 for size in sizes)
    table = {}
    table["own_rows"] = np.kron(np.eye(b0 // 2), pairs(b1 // 2))
    lanes = 0.125 * pairs(b2 // 2).T
    table["own_lo"] = np.concatenate([lanes, np.zeros_like(lanes)], axis=1)
    table["own_hi"] = np.concatenate([np.zeros_like(lanes), lanes], axis=1)
    table["down_rows"] = blocked(pairs(q1))
    table["down_lanes"] = 0.125 * pairs(q2).T
    window_lanes = [b2 + j for j in range(b2 // 2)] + [j - b2 for j in range(b2 // 2, 2 * b2)]
    window_rows = [j - 8 for j in range(b1 + 16)]
    for name, weights in (("cubic", CUBIC), ("linear", LINEAR)):
        table[name + "_rows1"] = blocked(interpolation(q1, range(m1), weights))
        table[name + "_lanes1"] = interpolation(q2, range(m2), weights).T
        table[name + "_rows0"] = blocked(interpolation(m1, window_rows, weights))
        table[name + "_lanes0"] = interpolation(m2, window_lanes, weights).T
    (u0, cos0), (u1, cos1), (u2, cos2) = basis(c0), basis(c1), basis(c2)
    table["spectrum_rows"] = np.kron(u0.T @ pairs(c0), u1.T @ pairs(c1))
    table["spectrum_lanes"] = 0.125 * pairs(c2).T @ u2
    for name, weights in (("cubic", CUBIC), ("linear", LINEAR)):
        table[name + "_rows2"] = np.kron(
            interpolation(c0, range(q0), weights) @ u0, interpolation(c1, range(q1), weights) @ u1
        )
        table[name + "_lanes2"] = u2.T @ interpolation(c2, range(q2), weights).T
    two = np.float32(2.0)
    eigen = (
        np.float32(6.0)
        - two * cos0[:, None, None]
        - two * cos1[None, :, None]
        - two * cos2[None, None, :]
    )
    table["eigen"] = (np.float32(0.25 ** (LEVELS - 1)) * eigen).reshape(c0 * c1, c2)
    wide = ("spectrum_rows", "spectrum_lanes", "eigen")
    return {
        name: np.asarray(
            value, np.float32 if name in wide or name.endswith("2") else jnp.bfloat16
        )
        for name, value in table.items()
    }


def dot(a, b):
    return jnp.dot(a, b, precision=PRECISE, preferred_element_type=jnp.float32)


def parts_of(values, pieces):
    parts = []
    for n in range(pieces):
        parts.append(values.astype(jnp.bfloat16))
        if n + 1 < pieces:
            values = values - parts[-1].astype(jnp.float32)
    return parts[::-1]


def right(values, matrix, pieces):
    terms = [
        jnp.dot(part, matrix, preferred_element_type=jnp.float32)
        for part in parts_of(values, pieces)
    ]
    return sum(terms[1:], terms[0])


def left(matrix, values, pieces):
    terms = [
        jnp.dot(matrix, part, preferred_element_type=jnp.float32)
        for part in parts_of(values, pieces)
    ]
    return sum(terms[1:], terms[0])


def around(plane):
    rows, lanes = plane.shape
    total = pltpu.roll(plane, 1, 0) + pltpu.roll(plane, rows - 1, 0)
    return total + (pltpu.roll(plane, 1, 1) + pltpu.roll(plane, lanes - 1, 1))


def around_all(values):
    first = jnp.concatenate([values[1:], values[:1]], axis=0)
    first = first + jnp.concatenate([values[-1:], values[:-1]], axis=0)
    for axis in (1, 2):
        first = first + pltpu.roll(values, 1, axis)
        first = first + pltpu.roll(values, values.shape[axis] - 1, axis)
    return first


def row_blocks(matrix, values, pieces):
    depth = matrix.shape[1]
    return jnp.concatenate(
        [left(matrix, values[i : i + depth], pieces) for i in range(0, values.shape[0], depth)], axis=0
    )


def loop(count, body):
    def step(i, carry):
        body(i)
        return carry

    lax.fori_loop(0, count, step, 0, unroll=4 if count % 4 == 0 else 2)


def close(ref):
    count = ref.shape[0] - 2
    ref[0] = ref[count]
    ref[count + 1] = ref[1]


def defect_plane(v, p, g, weight, diagonal):
    center = v[p]
    beside = v[p - 1] + v[p + 1] + around(center)
    return center, g - (diagonal * center - weight * beside)


def restrict_own(k, summed):
    b_half, rows, lanes = summed.shape
    folded = left(k["own_rows"][...], summed.reshape(b_half * rows, lanes), 3)
    half = folded.shape[0] // 2
    return right(folded[:half], k["own_lo"][...], 3) + right(folded[half:], k["own_hi"][...], 3)


def unpack(gathered, counts, g):
    nx, ny, nz = counts
    x, y, z = (lax.axis_index(name) for name in NAMES)
    half, rows, lanes = gathered.shape[1:]
    low = lax.broadcasted_iota(jnp.int32, (half, rows, lanes), 2) < lanes // 2
    for dx in range(nx):
        for dz in range(nz):
            for pair in range(ny // 2):
                parts = []
                for dy in (2 * pair, 2 * pair + 1):
                    index = (lax.rem(x + dx, nx) * ny + lax.rem(y + dy, ny)) * nz
                    parts.append(gathered[index + lax.rem(z + dz, nz)])
                turned = [pltpu.roll(part, lanes // 2, 2) for part in parts]
                where = (pl.ds(dz * rows, rows), pl.ds(pair * lanes, lanes))
                start = 2 * half * dx
                g[(pl.ds(start, half), *where)] = jnp.where(low, parts[0], turned[1])
                g[(pl.ds(start + half, half), *where)] = jnp.where(low, turned[0], parts[1])


def solve(k, kind, values, shift):
    shape = values.shape
    flat = values.reshape(shape[0] * shape[1], shape[2])
    spectrum = dot(k["spectrum_rows"][...], dot(flat, k["spectrum_lanes"][...]))
    spectrum = spectrum / (k["eigen"][...] + shift)
    fine = dot(k[kind + "_rows2"][...], dot(spectrum, k[kind + "_lanes2"][...]))
    return fine.reshape(shape)


def cycle2(k, v, g, shift):
    weight = 0.25**2
    diagonal = 6.0 * weight + shift
    damp = DAMPING / diagonal
    if v is None:
        v = damp * g
    else:
        v = v + damp * (g - (diagonal * v - weight * around_all(v)))
    v = v + solve(k, "linear", g - (diagonal * v - weight * around_all(v)), shift)
    return v + damp * (g - (diagonal * v - weight * around_all(v)))


def down(k, t, shape2):
    flat = row_blocks(k["down_rows"][...], t[...].reshape(-1, t.shape[2]), 3)
    return right(flat, k["down_lanes"][...], 3).reshape(shape2)


def up(k, kind, level, values, z):
    flat = right(values, k[kind + "_lanes" + level][...], 2)
    z[...] = row_blocks(k[kind + "_rows" + level][...], flat, 2).reshape(z.shape)


def blend(z, i, weights, count):
    total = None
    for offset, weight in weights.items():
        index = i + offset
        index = index if count is None else lax.rem(index + count, count)
        term = weight * z[index]
        total = term if total is None else total + term
    return total


def up1(k, kind, values, z, v, add):
    count = z.shape[0]
    up(k, kind, "1", values.reshape(-1, values.shape[2]), z)
    weights = CUBIC if kind == "cubic" else LINEAR

    def body(i):
        for odd in (0, 1):
            p = 2 * i + odd + 1
            value = blend(z, i, weights[odd], count)
            v[p] = v[p] + value if add else value

    loop(count, body)
    close(v)


def cycle1(k, v, u, g, t, z, shift, zero, shape2):
    weight = 0.25
    diagonal = 6.0 * weight + shift
    damp = DAMPING / diagonal
    count = g.shape[0]

    def before(p):
        if zero:
            u[p + 1] = damp * g[p]
        else:
            center, rest = defect_plane(v, p + 1, g[p], weight, diagonal)
            u[p + 1] = center + damp * rest

    loop(count, before)
    close(u)

    def residue(i):
        t[i] = (
            defect_plane(u, 2 * i + 1, g[2 * i], weight, diagonal)[1]
            + defect_plane(u, 2 * i + 2, g[2 * i + 1], weight, diagonal)[1]
        )

    loop(count // 2, residue)
    correction = cycle2(k, None, down(k, t, shape2), shift)
    up1(k, "linear", correction, z, u, True)

    def after(p):
        center, rest = defect_plane(u, p + 1, g[p], weight, diagonal)
        v[p + 1] = center + damp * rest

    loop(count, after)
    close(v)


def window(k, kind, v, zw, span, write):
    count = v.shape[0] - 2
    values = jnp.concatenate([v[count - 3 : count + 1], v[1 : span - 3]], axis=0)
    up(k, kind, "0", values.reshape(-1, values.shape[2]), zw)
    weights = CUBIC if kind == "cubic" else LINEAR

    def body(i):
        for odd in (0, 1):
            write(2 * i + odd, blend(zw, i + 3, weights[odd], None))

    loop(span - 6, body)


def own_defect(v, p, f, weight, diagonal):
    rows, lanes = f.shape
    inside = (pl.ds(8, rows), pl.ds(lanes, lanes))
    wide = v[p + 1, pl.ds(8, rows), :]
    center = wide[:, lanes:]
    beside = v[(p, *inside)] + v[(p + 2, *inside)]
    beside = beside + v[p + 1, pl.ds(7, rows), pl.ds(lanes, lanes)]
    beside = beside + v[p + 1, pl.ds(9, rows), pl.ds(lanes, lanes)]
    beside = beside + pltpu.roll(wide, 1, 1)[:, lanes:]
    beside = beside + pltpu.roll(wide, 2 * lanes - 1, 1)[:, lanes:]
    return center, f - (diagonal * center - weight * beside)


def position():
    return tuple(lax.axis_index(name) for name in NAMES)


def partner_of(place):
    x, y, z = place
    return (x, y + 1 - 2 * lax.rem(y, 2), z)


def shifted(place, counts, offset):
    return tuple(
        lax.rem(at + step + count, count) for at, step, count in zip(place, offset, counts)
    )


def slot(place, counts):
    return (place[0] * counts[1] + place[1]) * counts[2] + place[2]


def chip_offsets(counts):
    nx, ny, nz = counts
    offsets = [
        (dx, dy, dz) for dx in range(nx) for dy in range(0, ny, 2) for dz in range(nz)
    ]

    def hops(offset):
        return sum(min(step, count - step) for step, count in zip(offset, (nx, ny, nz)))

    return sorted(offsets[1:], key=hops, reverse=True)


def face_offsets(counts):
    faces = []
    for axis in range(3):
        for side, step in ((0, -1), (1, 1)):
            offset = [0, 0, 0]
            offset[axis] = step
            faces.append((tuple(offset), axis, side))
    return faces


def greet(barrier, places):
    for place in places:
        pl.semaphore_signal(barrier, inc=1, device_id=place, device_id_type=MESH)


def remote(src, dst, send, recv, place):
    return pltpu.make_async_remote_copy(
        src_ref=src, dst_ref=dst, send_sem=send, recv_sem=recv, device_id=place, device_id_type=MESH
    )


def spread(counts, block, gathered, sems):
    send, recv, relay_send, relay_recv = sems
    me = position()
    partner = partner_of(me)
    along, across = stages(counts)
    number = {offset: n for n, offset in enumerate(chip_offsets(counts))}
    mine = gathered.at[slot(me, counts)]
    copies, relays = {}, []

    def pass_on(offset, source, target, place):
        n = number[offset]
        copies[offset] = remote(source, target, send.at[n], recv.at[n], place)
        copies[offset].start()

    def relay(n, source, target):
        relays.append(remote(source, target, relay_send.at[n], relay_recv.at[n], partner))
        relays[-1].start()

    for offset in along + across:
        pass_on(offset, block, mine, shifted(me, counts, offset))
    relay(len(number), block, mine)

    def arrival(offset):
        copies[offset].wait_recv()
        source = shifted(me, counts, tuple(-step for step in offset))
        return gathered.at[slot(source, counts)]

    def finish():
        gathered[slot(me, counts)] = block[...]
        for first in along[::-1]:
            arrived = arrival(first)
            for second in across:
                place = shifted(me, counts, second)
                pass_on((first[0], second[1], second[2]), arrived, arrived, place)
            relay(number[first], arrived, arrived)
        for first in ((0, 0, 0), *along[::-1]):
            for second in across[::-1]:
                offset = (first[0], second[1], second[2])
                arrived = arrival(offset)
                relay(number[offset], arrived, arrived)
        for copy in copies.values():
            copy.wait_send()
        for copy in relays:
            copy.wait()

    return finish


def stages(counts):
    offsets = chip_offsets(counts)
    along = [offset for offset in offsets if offset[1:] == (0, 0)]
    across = [offset for offset in offsets if offset[0] == 0]
    return along, across


def gather_places(counts):
    me = position()
    along, across = stages(counts)
    return [shifted(me, counts, offset) for offset in along + across] + [partner_of(me)]


def first_part(k, counts, source, f, gathered, halos, block, owns, sems, face_sems):
    own_planes, own_rows, own_columns = owns
    planes, rows, columns = halos
    face_send, face_recv = face_sems
    me = position()
    barrier = pltpu.get_barrier_semaphore()
    faces = face_offsets(counts)
    places = gather_places(counts) + [shifted(me, counts, offset) for offset, _, _ in faces]
    greet(barrier, places)
    b0, b1, b2 = source.shape
    summed = source[...].reshape(b0 // 2, 2, b1, b2)
    block[...] = restrict_own(k, summed[:, 0] + summed[:, 1]).reshape(block.shape)
    own_planes[0] = source[0]
    own_planes[1] = source[b0 - 1]
    own_rows[0] = source[:, pl.ds(0, 1), :]
    own_rows[1] = source[:, pl.ds(b1 - 1, 1), :]
    turned = source[...].reshape(b0 * b1, b2).T
    own_columns[0] = turned[:8]
    own_columns[1] = turned[b2 - 8 :]
    pl.semaphore_wait(barrier, len(places))
    finish = spread(counts, block, gathered, sems)
    buffers = ((own_planes, planes), (own_rows, rows), (own_columns, columns))
    order = (0, 2, 1)
    copies = []
    for n, (offset, axis, side) in enumerate(faces):
        own, halo = buffers[order[axis]]
        place = shifted(me, counts, offset)
        copies.append(
            remote(own.at[side], halo.at[1 - side], face_send.at[n], face_recv.at[n], place)
        )
        copies[-1].start()
    f[...] = jnp.zeros_like(f)
    f[1 : b0 + 1, pl.ds(8, b1), pl.ds(b2, b2)] = source[...]
    finish()
    for copy in copies:
        copy.wait()


def second_part(k, counts, shape2, span, shift, gathered, source, halos, out, buffers):
    g, v, u, t, z, zw, v0, v1, f, summed = buffers
    plane_halo, row_halo, column_halo = halos
    unpack(gathered, counts, g)
    b0, b1, b2 = source.shape
    rows, lanes = pl.ds(8, b1), pl.ds(b2, b2)
    f[0, rows, lanes] = plane_halo[0]
    f[b0 + 1, rows, lanes] = plane_halo[1]
    f[1 : b0 + 1, pl.ds(7, 1), lanes] = row_halo[0]
    f[1 : b0 + 1, pl.ds(8 + b1, 1), lanes] = row_halo[1]
    middle = jnp.zeros((b2 - 16, b0 * b1), jnp.float32)
    turned = jnp.concatenate([column_halo[1], middle, column_halo[0]], axis=0)
    f[1 : b0 + 1, rows, pl.ds(0, b2)] = turned.T.reshape(b0, b1, b2)
    def pair_sum(i):
        t[i] = g[2 * i] + g[2 * i + 1]

    loop(g.shape[0] // 2, pair_sum)
    forcing2 = down(k, t, shape2)
    iterate2 = cycle2(k, solve(k, "cubic", forcing2, shift), forcing2, shift)
    up1(k, "cubic", iterate2, z, v, False)
    cycle1(k, v, u, g, t, z, shift, False, shape2)

    def put(p, value):
        v0[p] = value

    window(k, "cubic", v, zw, span, put)
    diagonal = 6.0 + shift
    damp = DAMPING / diagonal

    def before(p):
        center, rest = defect_plane(v0, p + 1, f[p], 1.0, diagonal)
        v1[p] = center + damp * rest

    loop(b0 + 2, before)

    def residue(i):
        summed[i] = (
            own_defect(v1, 2 * i, source[2 * i], 1.0, diagonal)[1]
            + own_defect(v1, 2 * i + 1, source[2 * i + 1], 1.0, diagonal)[1]
        )

    loop(b0 // 2, residue)
    out[...] = restrict_own(k, summed[...]).reshape(out.shape)


def third_part(k, counts, shape2, span, shift, gathered, source, out, buffers):
    g, v, u, t, z, zw, w, v1 = buffers[:8]
    unpack(gathered, counts, g)
    cycle1(k, v, u, g, t, z, shift, True, shape2)
    b0 = source.shape[0]

    def put(p, value):
        w[p] = value

    window(k, "linear", v, zw, span, put)

    def add(p):
        w[p] = v1[p] + w[p + 1]

    loop(b0 + 2, add)
    diagonal = 6.0 + shift
    damp = DAMPING / diagonal

    def after(p):
        center, rest = own_defect(w, p, source[p], 1.0, diagonal)
        out[p] = center + damp * rest

    loop(b0, after)


def kernel(names, counts, shape2, span, *refs):
    k = dict(zip(names, refs))
    shift_ref, source, out, *rest = refs[len(names) :]
    shift = shift_ref[0]
    landing, later, *halos = rest[:5]
    block, block_later, *owns = rest[5:10]
    buffers = rest[10:20]
    sems, sems_later, face_sems = rest[20:24], rest[24:28], rest[28:30]
    f = buffers[8]
    first_part(k, counts, source, f, landing, halos, block, owns, sems, face_sems)
    second_part(k, counts, shape2, span, shift, landing, source, halos, block_later, buffers)
    spread(counts, block_later, later, sems_later)()
    third_part(k, counts, shape2, span, shift, later, source, out, buffers)


def per_device(counts, source, shift):
    nx, ny, nz = counts
    b0, b1, b2 = source.shape
    sizes = (b0 * nx, b1 * nz, b2 * ny)
    table = constants(source.shape, sizes)
    m0, m1, m2 = (size // 2 for size in sizes)
    shape2 = tuple(size // 4 for size in sizes)
    span = b0 // 2 + 8
    wide = (b1 + 16, 2 * b2)
    packed = (b0 // 4, b1 // 2, b2)
    devices = nx * ny * nz
    chips = devices // 2
    vmem = pl.BlockSpec(memory_space=pltpu.VMEM)

    def field(*shape):
        return pltpu.VMEM(shape, jnp.float32)

    faces = [field(2, b1, b2), field(2, b0, 1, b2), field(2, 8, b0 * b1)]
    buffers = [
        field(m0, m1, m2),
        field(m0 + 2, m1, m2),
        field(m0 + 2, m1, m2),
        field(m0 // 2, m1, m2),
        field(m0 // 2, m1, m2),
        field(span, *wide),
        field(b0 + 4, *wide),
        field(b0 + 2, *wide),
        field(b0 + 2, *wide),
        field(b0 // 2, b1, b2),
    ]
    sems = [pltpu.SemaphoreType.DMA((max(chips - 1, 1),))] * 2
    sems += [pltpu.SemaphoreType.DMA((chips,))] * 2
    landing = [field(devices, *packed)] * 2 + faces
    names = tuple(table)
    return pl.pallas_call(
        functools.partial(kernel, names, counts, shape2, span),
        out_shape=jax.ShapeDtypeStruct(source.shape, jnp.float32),
        in_specs=[vmem] * len(names) + [pl.BlockSpec(memory_space=pltpu.SMEM), vmem],
        out_specs=vmem,
        scratch_shapes=landing
        + [field(*packed)] * 2
        + faces
        + buffers
        + sems * 2
        + [pltpu.SemaphoreType.DMA((6,))] * 2,
        compiler_params=pltpu.CompilerParams(
            vmem_limit_bytes=60 * 1024 * 1024, collective_id=0, has_side_effects=True
        ),
    )(*[jnp.asarray(table[name]) for name in names], shift, source)


def modes(count, depth):
    if depth == 0:
        return [(0, k) for k in range(count // 2)] + [(1, k) for k in range(1, count // 2 + 1)]
    half = count // 2
    low = modes(half, depth - 1)
    high = []
    for kind, k in low:
        if kind == 0:
            high.append((0, half - k if k else half // 2))
        else:
            high.append((1, half - k if k < half // 2 else half))
    return low + high


def waves(count, order):
    cells = (np.arange(count) + 0.5) * (2.0 * np.pi / count)
    return np.stack([np.sin(k * cells) if kind else np.cos(k * cells) for kind, k in order], axis=1)


def analysis(waves_):
    return waves_.T / np.sum(waves_**2, axis=0)[:, None]


def two_blocks(matrix, axis):
    first, second = np.split(matrix, 2, axis=axis)
    return np.concatenate([np.diag(first), np.diag(second)])


def factors(m):
    orders = modes(m, 2), modes(m // 2, 1), modes(m // 4, 0)
    bases = [waves(len(order), order) for order in orders]
    t = {"waves": bases[0]}
    for level, fine, coarse in (("1", bases[0], bases[1]), ("2", bases[1], bases[2])):
        n = fine.shape[0]
        t["r" + level] = two_blocks(analysis(coarse) @ (0.5 * pairs(n // 2)) @ fine, 1)
        for name, weights in (("p", LINEAR), ("q", CUBIC)):
            matrix = interpolation(n // 2, range(n), weights)
            t[name + level] = two_blocks(analysis(fine) @ matrix @ coarse, 0)
        order = orders[int(level) - 1]
        t["e" + level] = np.array([2.0 - 2.0 * np.cos(2.0 * np.pi * k / n) for _, k in order])
    t["c3"] = np.array([np.cos(2.0 * np.pi * k / (m // 4)) for _, k in orders[2]], np.float32)
    fine = np.eye(2 * m)
    lap = 2.0 * fine - np.roll(fine, 1, 0) - np.roll(fine, -1, 0)
    current = interpolation(m, range(2 * m), CUBIC) @ bases[0]
    for i in range(3):
        t[f"m{i}"] = np.sum(analysis(bases[0]).T * ((0.5 * pairs(m)) @ current), axis=0)
        current = lap @ current
    return t


def near(matrix, axis=0):
    return np.roll(matrix, 1, axis) + np.roll(matrix, -1, axis)


def synthesis(t, cells, weights, powers):
    m = t["waves"].shape[0]
    matrix = interpolation(m, range(2 * m), weights) @ t["waves"]
    result = []
    for _ in range(powers):
        result.append(matrix[np.array(cells) % (2 * m)])
        matrix = near(matrix)
    return result


def pick(matrix, rows, columns):
    return matrix[np.array(rows) % matrix.shape[0]][:, np.array(columns) % matrix.shape[1]]


def late_kinds(m, rows, columns):
    plain = interpolation(m, range(2 * m), LINEAR)
    return [pick(kind, rows, columns) for kind in (plain, near(plain), near(plain, 1), near(near(plain), 1))]


def mixed(p, r):
    return [
        np.kron(p[0], r[0]),
        np.kron(p[1], r[0]) + np.kron(p[0], r[1]),
        np.kron(p[2], r[0]) + np.kron(p[0], r[2]),
        np.kron(p[3], r[0]) + np.kron(p[0], r[3]) + np.kron(p[2], r[1]) + np.kron(p[1], r[2]),
    ]


def exact(matrix):
    result = np.asarray(matrix, jnp.bfloat16)
    assert np.all(result.astype(np.float64) == matrix)
    return result


def halves(matrix, axis):
    high = np.asarray(matrix, jnp.bfloat16)
    low = np.asarray(matrix - high.astype(np.float64), jnp.bfloat16)
    return np.concatenate([high, low], axis=axis)


def halved_rows(m0, m1):
    index = np.arange(m0 * m1).reshape(2, 2, 2, m0 // 8, 2, 2, m1 // 4)
    index = index.transpose(2, 0, 4, 1, 5, 3, 6).reshape(2, 4, -1)
    return index, index[:, 0].reshape(-1), index.reshape(-1)


def own_table(half):
    count = 2 * half
    four = sum(np.roll(np.kron(np.eye(half), np.eye(2)[:, :1]), s, axis=0) for s in (-1, 0, 1, 2))
    four[count - 1, 0] = 0.0
    four[0, half - 1] = 0.0
    beside = np.zeros((count, half))
    beside[count - 1, 0] = beside[0, half - 1] = 1.0
    own = np.zeros((2, count, 3, 2, half))
    for n, part in enumerate((pairs(half).T, beside, four)):
        for s in range(2):
            own[s, :, n, s] = 0.125 * part
    return np.asarray(own.reshape(2 * count, 3 * count), jnp.bfloat16)


def two_levels(count):
    whole = 2 * count
    fine, half = np.eye(whole), np.eye(whole // 2)
    near, near1 = (np.roll(e, 1, 0) + np.roll(e, -1, 0) for e in (fine, half))
    down, down1 = pairs(whole // 2), pairs(whole // 4)
    start = count // 2
    rows = range(start // 4 - 1, (start + count) // 4 + 1)
    kinds = (down1 @ down, down1 @ down @ near, down1 @ near1 @ down, down1 @ near1 @ down @ near)
    return [kind[rows, start : start + count] for kind in kinds]


def early_tables(block):
    b0, b1, b2 = block
    (p, r, c) = ([*two_levels(size)] for size in block)
    full = mixed(p, r)
    rows = np.zeros((4, 3, 16, b0 * b1))
    rows[:, :, : 2 * r[0].shape[0]] = np.stack(full).reshape(4, 3, 2 * r[0].shape[0], b0 * b1)
    lanes = np.zeros((4, b2, b2))
    for n in range(4):
        lanes[n, :, : c[n].shape[0]] = c[n].T / 64.0
    return exact(rows.reshape(-1, b0 * b1)), exact(lanes.reshape(-1, b2))


def fast_constants(counts, block, sizes):
    nx, ny, nz = counts
    b0, b1, b2 = block
    m0, m1, m2 = (size // 2 for size in sizes)
    t0, t1, t2 = (factors(m) for m in (m0, m1, m2))
    parts, index2, index1 = halved_rows(m0, m1)
    i0, i1 = index1 // m1, index1 % m1
    j0, j1 = index2 // m1, index2 % m1
    rows2 = len(index2)

    def across(name, k, l, op=np.multiply):
        return op(t0[name][k], t1[name][l])

    def joint(a, c):
        return t0[a][i0] * t1[c][i1]

    columns = [across("r1", i0, i1), across("p1", i0, i1), across("q1", i0, i1), across("e1", i0, i1, np.add)]
    columns += [joint("m0", "m0"), joint("m1", "m0") + joint("m0", "m1")]
    columns += [joint("m2", "m0") + joint("m0", "m2") + 2.0 * joint("m1", "m1")]
    by_row = np.zeros((m0 * m1, 128))
    by_row[:, : len(columns)] = np.stack(columns, axis=1)
    for n, name in enumerate(("r2", "p2", "q2", "e2")):
        by_row[:rows2, 8 + n] = across(name, j0, j1, np.add if name == "e2" else np.multiply)
    by_lane = np.zeros((16, m2))
    for n, name in enumerate(("r1", "p1", "q1", "e1", "m0", "m1", "m2")):
        by_lane[n] = t2[name]
    for n, name in enumerate(("r2", "p2", "q2", "e2")):
        by_lane[8 + n, : m2 // 2] = t2[name]
    two = np.float32(2.0)
    eigen = np.float32(6.0) - two * t0["c3"][:, None, None]
    eigen = eigen - two * t1["c3"][None, :, None] - two * t2["c3"][None, None, :]
    eigen = (np.float32(0.25 ** (LEVELS - 1)) * eigen).reshape(rows2 // 4, m2 // 4)
    early_rows, early_lanes = early_tables(block)
    table = {"own": own_table(b2 // 2), "early_rows": early_rows, "early_lanes": early_lanes}
    small = {"by_row": by_row, "by_lane": by_lane, "eigen": np.concatenate([eigen, eigen], axis=1)}
    table.update({name: np.asarray(value, np.float32) for name, value in small.items()})

    a0, a1 = (analysis(waves(m // 2, modes(m // 2, 1))) for m in (m0, m1))
    a2 = analysis(waves(m2 // 2, modes(m2 // 2, 1)))
    p0, p1, p2 = b0 // 4, b1 // 4, b2 // 4
    wide = p2 + 2
    lanes = np.zeros((ny, b2, 3, m2 // 2))
    for dy in range(ny):
        for n in range(3):
            lanes[dy, 42 * n : 42 * n + wide, n] = a2[:, np.arange(p2 * dy - 1, p2 * dy + p2 + 1) % (m2 // 2)].T
    table["level2_lanes"] = halves(lanes.reshape(ny * b2, -1), 0)
    n, dx, dz, c, r = np.meshgrid(*(range(k) for k in (3, nx, nz, 2, p1 + 2)), indexing="ij")
    planes = (p0 * dx + 2 * n + c - 1 - p0 // 2) % (m0 // 2)
    rows = (p1 * dz + r - 1) % (m1 // 2)
    full = np.zeros((rows2, 3, nx, nz, 16))
    full[..., : 2 * (p1 + 2)] = (a0[j0][:, planes] * a1[j1][:, rows]).reshape(rows2, 3, nx, nz, -1)
    table["level2_rows"] = halves(full.reshape(rows2, -1), 1)

    forward = analysis(t0["waves"])[i0][:, : m0 // 2, None] * analysis(t1["waves"])[i1][:, None, :]
    table["forward_rows"] = halves(forward.reshape(2, m0 * m1 // 2, -1), 2)
    table["forward_lanes"] = halves(analysis(t2["waves"]).T, 0)
    for name, weights, powers in (("cubic", CUBIC, 3), ("linear", LINEAR, 2)):
        p = synthesis(t0, range(b0 // 2), weights, powers)
        r = synthesis(t1, range(b1), weights, powers)
        full = []
        for part in parts.reshape(2, -1):
            q0 = [matrix[:, part // m1][:, None, :] for matrix in p]
            q1 = [matrix[:, part % m1][None, :, :] for matrix in r]
            kinds = [q0[0] * q1[0], q0[1] * q1[0] + q0[0] * q1[1]]
            if powers == 3:
                kinds.append(q0[2] * q1[0] + 2.0 * q0[1] * q1[1] + q0[0] * q1[2])
            full.append(np.stack(kinds).reshape(-1, part.size))
        table[name + "_rows"] = halves(np.stack(full), 2)
        lanes = [matrix.T for matrix in synthesis(t2, range(b2), weights, powers)]
        table[name + "_lanes"] = halves(np.concatenate(lanes), 0)
    p = late_kinds(m0, range(b0), range(-2, b0 // 2 + 2))
    r = late_kinds(m1, range(b1), range(m1))
    table["late_rows"] = exact(np.concatenate(mixed(p, r), axis=1))
    table["late_lanes"] = exact(np.concatenate([c.T for c in late_kinds(m2, range(b2), range(m2))], axis=1))
    return table


def split(values):
    high = values.astype(jnp.bfloat16)
    return high, (values - high.astype(jnp.float32)).astype(jnp.bfloat16)


def by_right(values, table):
    high, low = split(values)
    depth = values.shape[1]
    first, second = table[:depth], table[depth:]
    return jnp.dot(
        jnp.concatenate([high, low, high], axis=1),
        jnp.concatenate([first, first, second], axis=0),
        preferred_element_type=jnp.float32,
    )


def by_left(table, values):
    high, low = split(values)
    depth = values.shape[0]
    first, second = table[:, :depth], table[:, depth:]
    return jnp.dot(
        jnp.concatenate([first, first, second], axis=1),
        jnp.concatenate([high, low, high], axis=0),
        preferred_element_type=jnp.float32,
    )


def fold(values):
    n = values.shape[0] // 8
    parts = []
    for kind in range(2):
        quarter = [values[(4 * kind + i) * n : (4 * kind + i + 1) * n] for i in range(4)]
        parts.append((quarter[0] + quarter[1]) + (quarter[2] + quarter[3]))
    total = jnp.concatenate(parts, axis=0)
    return total + pltpu.roll(total, total.shape[1] // 2, 1)


def unfold(values):
    n = values.shape[0] // 2
    return jnp.concatenate([values[:n]] * 4 + [values[n:]] * 4, axis=0)


def own_parts(source, own, outs, alpha, beta):
    block, across, along_rows, along_planes, rest = outs
    b0, b1, b2 = source.shape
    h0, h1 = b0 // 2, b1 // 2
    first = [source[p, pl.ds(0, h1, stride=2), :] for p in range(b0)]
    second = [source[p, pl.ds(1, h1, stride=2), :] for p in range(b0)]
    summed = [a + b for a, b in zip(first, second)]
    row = lax.broadcasted_iota(jnp.int32, (h1, b2), 0)
    zero = jnp.zeros((h1, b2), jnp.float32)
    whole, faces, inner = [], [], []
    for c in range(h0):
        total = summed[2 * c] + summed[2 * c + 1]
        down = pltpu.roll(second[2 * c] + second[2 * c + 1], 1, 0)
        up = pltpu.roll(first[2 * c] + first[2 * c + 1], h1 - 1, 0)
        whole.append(total)
        faces.append(jnp.where(row == 0, down, jnp.where(row == h1 - 1, up, zero)))
        near = 2.0 * total + jnp.where(row > 0, down, zero) + jnp.where(row < h1 - 1, up, zero)
        if c > 0:
            near = near + summed[2 * c - 1]
        if c < h0 - 1:
            near = near + summed[2 * c + 2]
        inner.append(near)

    def pack(planes):
        half = len(planes) // 2
        return [jnp.concatenate([planes[i], planes[i + half]], axis=1) for i in range(half)]

    ends = [jnp.concatenate([summed[b0 - 1], summed[0]], axis=1)]
    stacked = jnp.concatenate(pack(whole) + pack(faces) + pack(inner) + ends + [jnp.zeros((8, 2 * b2), jnp.float32)], axis=0)
    parts = parts_of(stacked, 3)
    weights = own[...]
    result = jnp.dot(
        jnp.concatenate(parts, axis=1),
        jnp.concatenate([weights] * 3, axis=0),
        preferred_element_type=jnp.float32,
    )
    n = h0 // 2 * h1
    shape = block.shape
    mine = result[:n, :b2]
    block[...] = mine.reshape(shape)
    across[...] = result[:n, b2 : 2 * b2].reshape(shape)
    along_rows[...] = result[n : 2 * n, :b2].reshape(shape)
    along_planes[...] = result[3 * n : 3 * n + h1, :b2]
    rest[...] = (alpha * mine + beta * (result[2 * n : 3 * n, :b2] + result[:n, 2 * b2 :])).reshape(shape)


def early_part(source, rows_table, lanes_table, weights):
    keep0, near0, keep1, near1 = weights
    b0, b1, b2 = source.shape
    result = jnp.dot(
        jnp.concatenate([rows_table[...]] * 3, axis=1),
        jnp.concatenate(parts_of(source[...].reshape(b0 * b1, b2), 3), axis=0),
        preferred_element_type=jnp.float32,
    )
    n = result.shape[0] // 4
    plain, first, second, both = (result[i * n : (i + 1) * n] for i in range(4))
    joint = near0 * near1
    columns = (
        (keep0 * keep1) * plain + (keep1 * near0) * first + (keep0 * near1) * second + joint * both,
        (keep1 * near0) * plain + joint * second,
        (keep0 * near1) * plain + joint * first,
        joint * plain,
    )
    result = jnp.dot(
        jnp.concatenate(parts_of(jnp.concatenate(columns, axis=1), 3), axis=1),
        jnp.concatenate([lanes_table[...]] * 3, axis=0),
        preferred_element_type=jnp.float32,
    )
    total = result[:16] + pltpu.roll(result[16:32], 42, 1)
    return (total + pltpu.roll(result[32:], 84, 1)).reshape(2, 8, b2)


def beyond(place, counts):
    x, y, z = place
    return (x, lax.rem(y - 1 + 2 * lax.rem(y, 2) + counts[1], counts[1]), z)


def wait_for(ref, sem):
    pltpu.make_async_copy(ref, ref, sem).wait()


class TwoStage:
    def __init__(self, counts, near, far, block, landing, sems):
        self.counts, self.near, self.far = counts, near, far
        self.block, self.landing = block, landing
        self.sent, self.arrived, self.relay_sent, self.relayed = sems
        self.count = 0

    def at(self, offset):
        source = shifted(position(), self.counts, tuple(-step for step in offset))
        return self.landing.at[slot(source, self.counts)]

    def send(self, source, target, step, sem):
        place = shifted(position(), self.counts, step)
        remote(source, target, self.sent.at[0], self.arrived.at[sem], place).start()
        self.count += 1

    def start(self, offsets):
        for offset in offsets:
            sem = self.near.index(offset) if offset in self.near else len(self.near)
            self.send(self.block, self.at((0, 0, 0)), offset, sem)

    def relay(self, source, target):
        remote(source, target, self.relay_sent.at[0], self.relayed.at[0], partner_of(position())).start()

    def own(self):
        self.relay(self.block, self.at((0, 0, 0)))

    def forward(self, which):
        for n in which:
            arrived = self.at(self.near[n])
            wait_for(arrived, self.arrived.at[n])
            for second in self.far:
                self.send(arrived, arrived, second, len(self.near) + 1 + n)
            self.relay(arrived, arrived)

    def rest(self):
        for n, first in enumerate(((0, 0, 0), *self.near)):
            wait_for(self.landing.at[pl.ds(0, len(self.far))], self.arrived.at[len(self.near) + n])
            for second in self.far:
                arrived = self.at(tuple(a + b for a, b in zip(first, second)))
                self.relay(arrived, arrived)

    def end(self):
        self.landing[slot(position(), self.counts)] = self.block[...]
        wait_for(self.landing.at[pl.ds(0, self.count)], self.sent.at[0])
        for sem in (self.relay_sent, self.relayed):
            wait_for(self.landing.at[pl.ds(0, self.count + 1)], sem.at[0])

    @staticmethod
    def semaphores(near):
        dma = pltpu.SemaphoreType.DMA
        return [dma((1,)), dma((2 * len(near) + 1,)), dma((1,)), dma((1,))]


def piece(ref, part):
    if part == 0:
        return ref
    half = ref.shape[0] // 2
    return ref.at[pl.ds(half if part == 1 else 0, half)]


class Close:
    def __init__(self, counts, near, block, landing, sems):
        self.counts, self.near, self.block, self.landing = counts, near, block, landing
        self.far = [((1, 0, 0), 1), ((counts[0] - 1, 0, 0), -1)] if counts[0] > 2 else [((1, 0, 0), 0)]
        self.sent, self.arrived, self.relay_sent, self.relayed = sems
        self.blocks = 2 * len(near) + 1

    def at(self, offset):
        source = shifted(position(), self.counts, tuple(-step for step in offset))
        return self.landing.at[slot(source, self.counts)]

    def send(self, source, target, step, sem):
        place = shifted(position(), self.counts, step)
        remote(source, target, self.sent.at[0], self.arrived.at[sem], place).start()

    def relay(self, source, target):
        remote(source, target, self.relay_sent.at[0], self.relayed.at[0], partner_of(position())).start()

    def start(self):
        mine = self.at((0, 0, 0))
        for n, offset in enumerate(self.near):
            self.send(self.block, mine, offset, n)
        for step, part in self.far:
            self.send(piece(self.block, part), piece(mine, part), step, len(self.near))
        self.relay(self.block, mine)

    def forward(self):
        for n, first in enumerate(self.near):
            arrived = self.at(first)
            wait_for(arrived, self.arrived.at[n])
            for step, part in self.far:
                self.send(piece(arrived, part), piece(arrived, part), step, len(self.near) + 1 + n)
            self.relay(arrived, arrived)

    def rest(self):
        for n, first in enumerate(((0, 0, 0), *self.near)):
            wait_for(self.landing.at[0], self.arrived.at[len(self.near) + n])
            for step, part in self.far:
                arrived = piece(self.at(tuple(a + b for a, b in zip(first, step))), part)
                self.relay(arrived, arrived)

    def end(self):
        self.landing[slot(position(), self.counts)] = self.block[...]
        wait_for(self.landing.at[pl.ds(0, self.blocks)], self.sent.at[0])
        for sem in (self.relay_sent, self.relayed):
            wait_for(self.landing.at[pl.ds(0, self.blocks + 1)], sem.at[0])


def exchange(counts, sent, received, send, recv):
    me = position()
    order = (0, 2, 1)
    for offset, axis, side in face_offsets(counts):
        which = order[axis]
        mine = sent[which] if len(sent[which]) == 1 else [sent[which][side]]
        place = shifted(me, counts, offset)
        remote(mine[0], received[2 * which + 1 - side], send.at[0], recv.at[0], place).start()


def prepare(k, many, few, shift):
    diagonal0, diagonal1, diagonal2 = (6.0 * 0.25**level + shift for level in range(3))
    sigma0, sigma1, sigma2 = diagonal0 - 6.0, diagonal1 - 1.5, diagonal2 - 0.375
    damp0, damp1, damp2 = DAMPING / diagonal0, DAMPING / diagonal1, DAMPING / diagonal2
    down, pre, fine_q, out_q, out_g, out_e, cross = many
    by_row, by_lane = k["by_row"], k["by_lane"]
    lanes = by_lane.shape[1]

    def level1(i):
        rows = pl.ds(pl.multiple_of(8 * i, 8), 8)
        column = by_row[rows, :]

        def tall(n):
            return jnp.broadcast_to(column[:, n : n + 1], (8, lanes))

        def wide(n):
            return jnp.broadcast_to(by_lane[n : n + 1, :], (8, lanes))

        r, p, q = (tall(n) * wide(n) for n in range(3))
        a = 0.25 * (tall(3) + wide(3)) + sigma1
        s = 1.0 - damp1 * a
        down[rows, :] = r
        pre[rows, :] = r * s
        fine_q[rows, :] = a * q
        out_q[rows, :] = s * s * q
        out_g[rows, :] = damp1 * (1.0 + s)
        out_e[rows, :] = s * p
        c0, c1, c2 = tall(4), tall(5), tall(6)
        first = sigma0 * c0 + c1 - damp0 * ((sigma0 * sigma0) * c0 + (2.0 * sigma0) * c1 + c2)
        second = c0 - (2.0 * damp0) * (sigma0 * c0 + c1)
        cross[rows, :] = first * wide(4) + second * wide(5) - (damp0 * c0) * wide(6)

    loop(by_row.shape[0] // 8, level1)
    rows2, lanes2 = few[0].shape
    column = by_row[:rows2, :]

    def tall(n):
        return jnp.broadcast_to(column[:, n : n + 1], (rows2, lanes2))

    def wide(n):
        return jnp.broadcast_to(by_lane[n : n + 1, :lanes2], (rows2, lanes2))

    r, p, q = (tall(n) * wide(n) for n in (8, 9, 10))
    a = 0.0625 * (tall(11) + wide(11)) + sigma2
    s = 1.0 - damp2 * a
    values = (r, r * s, a * q, s * s * q, damp2 * (1.0 + s), s * p)
    for ref, value in zip(few, values):
        ref[...] = value
    k["inverse"][...] = 1.0 / (k["eigen"][...] + shift)


def level2(k, few, g):
    down, pre, fine_q, out_q, out_g, out_e = few
    e = unfold(fold(pre[...] * g) * k["inverse"][...])
    return out_g[...] * g + out_e[...] * e


def level2_full(k, few, g):
    down, pre, fine_q, out_q, out_g, out_e = few
    start = unfold(fold(down[...] * g) * k["inverse"][...])
    e = unfold(fold(pre[...] * (g - fine_q[...] * start)) * k["inverse"][...])
    return out_q[...] * start + out_g[...] * g + out_e[...] * e


def blocks_of(spectrum, i):
    rows2, lanes2 = spectrum.shape[0] // 4, spectrum.shape[1] // 2
    half = rows2 // 2
    base = 8 * i + 3 * half * lax.div(i, half // 8)
    for a in range(4):
        start = pl.multiple_of(base + a * half, 8)
        for c in range(2):
            yield (pl.ds(start, 8), pl.ds(c * lanes2, lanes2))


def spectral_u(k, many, few, spectrum, coupled, coarse):
    down, pre, fine_q, out_q, out_g, out_e, cross = many
    first, second, third = coarse
    steps = first.shape[0] // 8

    def at(i):
        return pl.ds(pl.multiple_of(8 * i, 8), 8)

    def restrict(i):
        first[at(i), :] = sum(down[w] * spectrum[w] for w in blocks_of(spectrum, i))

    loop(steps, restrict)
    second[...] = level2_full(k, few, first[...])

    def residue(i):
        u = second[at(i), :]
        first[at(i), :] = sum(pre[w] * (spectrum[w] - fine_q[w] * u) for w in blocks_of(spectrum, i))

    loop(steps, residue)
    third[...] = level2(k, few, first[...])

    def finish(i):
        u, e = second[at(i), :], third[at(i), :]
        total = None
        for w in blocks_of(spectrum, i):
            value = out_q[w] * u + out_g[w] * spectrum[w] + out_e[w] * e
            spectrum[w] = value
            value = cross[w] * value
            coupled[w] = value
            total = pre[w] * value if total is None else total + pre[w] * value
        first[at(i), :] = total

    loop(steps, finish)


def spectral_e(many, spectrum, coupled, e2):
    out_g, out_e = many[4], many[5]

    def finish(i):
        e = e2[pl.ds(pl.multiple_of(8 * i, 8), 8), :]
        for w in blocks_of(spectrum, i):
            spectrum[w] = out_e[w] * e - out_g[w] * coupled[w]

    loop(e2.shape[0] // 8, finish)


def unpack_centred(gathered, counts, g):
    nx, ny, nz = counts
    me = position()
    half, rows, lanes = gathered.shape[1:]
    planes = g.shape[0]
    low = lax.broadcasted_iota(jnp.int32, (half, rows, lanes), 2) < lanes // 2
    for dx in range(nx):
        for dz in range(nz):
            for pair in range(ny // 2):
                parts = [
                    gathered[slot(shifted(me, counts, (dx, dy, dz)), counts)] for dy in (2 * pair, 2 * pair + 1)
                ]
                turned = [pltpu.roll(part, lanes // 2, 2) for part in parts]
                where = (pl.ds(dz * rows, rows), pl.ds(pair * lanes, lanes))
                start = (2 * half * dx - half) % planes
                g[(pl.ds(start, half), *where)] = jnp.where(low, parts[0], turned[1])
                g[(pl.ds(2 * half * dx, half), *where)] = jnp.where(low, turned[0], parts[1])


def transform(k, counts, landing, g, spectrum):
    unpack_centred(landing, counts, g)
    m0, m1, m2 = g.shape
    half = m0 // 2
    depth = half * m1
    for kind in range(2):
        rows = [g[p] - g[m0 - 1 - p] if kind else g[p] + g[m0 - 1 - p] for p in range(half)]
        values = by_left(k["forward_rows"][kind], jnp.concatenate(rows, axis=0))
        spectrum[kind * depth : (kind + 1) * depth, :] = by_right(values, k["forward_lanes"])


def transform2(k, counts, landing):
    nx, ny, nz = counts
    me = position()
    columns = []
    for dy in range(ny):
        rows = [
            landing[slot(shifted(me, counts, (dx, dy, dz)), counts)].reshape(16, -1)
            for dx in range(nx)
            for dz in range(nz)
        ]
        columns.append(jnp.concatenate(rows, axis=0))
    values = by_right(jnp.concatenate(columns, axis=1), k["level2_lanes"])
    width = values.shape[1] // 3
    parts = [values[:, n * width : (n + 1) * width] for n in range(3)]
    return by_left(k["level2_rows"], jnp.concatenate(parts, axis=0))


def evaluate(k, kind, spectrum, mix, out):
    planes, rows, lanes = out.shape
    half = planes // 2
    depth = spectrum.shape[0] // 2
    parts = []
    for n in range(2):
        values = by_left(k[kind + "_rows"][n], spectrum[n * depth : (n + 1) * depth, :])
        pieces = [values[i : i + half * rows] for i in range(0, values.shape[0], half * rows)]
        columns = [sum(c * pieces[i] for i, c in enumerate(line) if c is not None) for line in mix]
        parts.append(by_right(jnp.concatenate(columns, axis=1), k[kind + "_lanes"]).reshape(half, rows, lanes))
    even, odd = parts
    for p in range(half):
        for index, value in ((half + p, even[p] + odd[p]), (half - 1 - p, even[p] - odd[p])):
            out[index] = out[index] + value


def unpack_near(gathered, counts, g):
    nx, ny, nz = counts
    me = position()
    half, rows, lanes = gathered.shape[1:]
    for dx, first, last in ((nx - 1, half - 2, half), (0, 0, half), (1, 0, 2)):
        shape = (last - first, rows, lanes)
        low = lax.broadcasted_iota(jnp.int32, shape, 2) < lanes // 2
        for dz in range(nz):
            for pair in range(ny // 2):
                parts = [
                    gathered[slot(shifted(me, counts, (dx, dy, dz)), counts), pl.ds(first, last - first)]
                    for dy in (2 * pair, 2 * pair + 1)
                ]
                turned = [pltpu.roll(part, lanes // 2, 2) for part in parts]
                where = (pl.ds(dz * rows, rows), pl.ds(pair * lanes, lanes))
                if dx != nx - 1:
                    start = 2 if dx == 0 else 2 + 2 * half
                    g[(pl.ds(start, last - first), *where)] = jnp.where(low, parts[0], turned[1])
                if dx != 1:
                    start = 2 + half if dx == 0 else 0
                    g[(pl.ds(start, last - first), *where)] = jnp.where(low, turned[0], parts[1])


def late_part(k, g, weights):
    keep0, near0, keep1, near1 = weights
    planes, m1, m2 = g.shape
    pieces = split(g[...].reshape(planes * m1, m2))
    table = k["late_lanes"][...]
    values = jnp.dot(
        jnp.concatenate(pieces, axis=1),
        jnp.concatenate([table, table], axis=0),
        preferred_element_type=jnp.float32,
    )
    lanes = values.shape[1] // 4
    a, b, c, d = (values[:, i * lanes : (i + 1) * lanes] for i in range(4))
    joint = near0 * near1
    stacked = (
        (keep0 * keep1) * a + (near0 * keep1) * b + (keep0 * near1) * c + joint * d,
        (near0 * keep1) * a + joint * c,
        (keep0 * near1) * a + joint * b,
        joint * a,
    )
    table = k["late_rows"][...]
    values = jnp.dot(
        jnp.concatenate([table, table], axis=1),
        jnp.concatenate(split(jnp.concatenate(stacked, axis=0)), axis=0),
        preferred_element_type=jnp.float32,
    )
    return values


def own_sweep(f, source, keep, damp, out):
    rows, lanes = source.shape[1:]

    def body(p):
        beside = f[p] + f[p + 2] + around(f[p + 1])
        out[p] = damp * ((1.0 + keep) * source[p] + damp * beside[:rows, :lanes])

    loop(source.shape[0], body)


def fast_kernel(names, counts, *refs):
    count = len(names)
    outside = dict(zip(names, refs))
    shift_ref, source_ref, out, *rest = refs[count:]

    def take(number):
        taken = rest[:number]
        del rest[:number]
        return taken

    k = dict(zip(names, take(count)))
    (source,) = take(1)
    landing_f, landing_h, landing_j = take(3)
    faces_in, halos = take(6), take(3)
    block_f, block_h, across, along_rows, local, along_planes = take(6)
    (block_j,) = take(1)
    own_planes, own_rows, own_columns = take(3)
    many, few, coarse = take(7), take(6), take(3)
    k["inverse"], g, near_h, spectrum, coupled, f = take(6)
    table_sems, *face_sems = take(5)
    sems_f, sems_h, sems_j = take(4), take(4), take(4)

    shift = shift_ref[0]
    me = position()
    barrier = pltpu.get_barrier_semaphore()
    along, across_all = stages(counts)
    places = [shifted(me, counts, offset) for offset in along + across_all]
    places += [partner_of(me), beyond(me, counts)]
    greet(barrier, places)
    loads = {"source": pltpu.make_async_copy(source_ref, source, table_sems.at[count])}
    loads["source"].start()
    for n, name in enumerate(names):
        loads[name] = pltpu.make_async_copy(outside[name], k[name], table_sems.at[n])
        loads[name].start()

    b0, b1, b2 = source.shape
    diagonal, diagonal1 = 6.0 + shift, 1.5 + shift
    damp, damp1 = DAMPING / diagonal, DAMPING / diagonal1
    loads["source"].wait()
    loads["own"].wait()
    parts = (block_f, across, along_rows, along_planes, local)
    own_parts(source, k["own"], parts, 1.0 - damp * diagonal, damp)
    pl.semaphore_wait(barrier, len(places))

    exchange(counts, ([along_planes], [along_rows], [across]), faces_in, *face_sems[:2])
    gather_f = TwoStage(counts, along[::-1], across_all, block_f, landing_f, sems_f)
    gather_j = TwoStage(counts, across_all[::-1], along, block_j, landing_j, sems_j)
    gather_f.start(along + across_all)
    gather_f.own()
    own_planes[0] = source[0]
    own_planes[1] = source[b0 - 1]
    own_rows[0] = source[:, pl.ds(0, 1), :]
    own_rows[1] = source[:, pl.ds(b1 - 1, 1), :]
    turned = source[...].reshape(b0 * b1, b2).T
    own_columns[0] = turned[:8]
    own_columns[1] = turned[b2 - 8 :]
    for name in ("early_rows", "early_lanes"):
        loads[name].wait()
    weights = (1.0 - damp * diagonal, damp, 1.0 - damp1 * diagonal1, 0.25 * damp1)
    block_j[...] = early_part(source, k["early_rows"], k["early_lanes"], weights)
    gather_j.start(across_all)
    gather_j.own()

    for name in ("by_row", "by_lane", "eigen"):
        loads[name].wait()
    prepare(k, many, few, shift)
    gather_f.forward(range(min(2, len(along))))
    for sem in face_sems[:2]:
        wait_for(f.at[pl.ds(0, 3)], sem.at[0])
    shape = local.shape
    lane = lax.rem(lax.broadcasted_iota(jnp.int32, shape, 2), b2 // 2)
    row = lax.broadcasted_iota(jnp.int32, shape, 1)
    from_planes, from_rows, from_lanes = faces_in[:2], faces_in[2:4], faces_in[4:6]
    total = jnp.where(lane == 0, from_lanes[0][...], 0.0) + jnp.where(lane == b2 // 2 - 1, from_lanes[1][...], 0.0)
    total = total + jnp.where(row == 0, from_rows[0][...], 0.0) + jnp.where(row == shape[1] - 1, from_rows[1][...], 0.0)
    block_h[...] = local[...] + damp * total
    low = lax.broadcasted_iota(jnp.int32, shape[1:], 1) < b2 // 2
    block_h[0] = block_h[0] + damp * jnp.where(low, from_planes[0][...], 0.0)
    end = shape[0] - 1
    block_h[end] = block_h[end] + damp * jnp.where(low, 0.0, from_planes[1][...])

    gather_f.forward(range(2, len(along)))
    mine = [[own.at[side] for side in range(2)] for own in (own_planes, own_rows, own_columns)]
    exchange(counts, mine, [halo.at[side] for halo in halos for side in range(2)], *face_sems[2:4])
    gather_j.start(along)
    gather_j.forward(range(len(across_all)))
    close_h = Close(counts, across_all[::-1], block_h, landing_h, sems_h)
    close_h.start()
    gather_f.rest()
    close_h.forward()
    for sem in face_sems[2:4]:
        wait_for(f.at[pl.ds(0, 2)], sem.at[0])
    f[...] = jnp.zeros_like(f)
    rows, lanes = pl.ds(0, b1), pl.ds(0, b2)
    f[1 : b0 + 1, rows, lanes] = source[...]
    f[0, rows, lanes] = halos[0][0]
    f[b0 + 1, rows, lanes] = halos[0][1]
    f[1 : b0 + 1, pl.ds(b1, 1), lanes] = halos[1][1]
    f[1 : b0 + 1, pl.ds(b1 + 7, 1), lanes] = halos[1][0]
    middle = jnp.zeros((b2 - 16, b0 * b1), jnp.float32)
    turned = jnp.concatenate([halos[2][1], middle, halos[2][0]], axis=0)
    f[1 : b0 + 1, rows, pl.ds(b2, b2)] = turned.T.reshape(b0, b1, b2)
    keep = 1.0 - damp * diagonal
    own_sweep(f, source, keep, damp, out)
    gather_f.end()
    for name in names:
        if name not in ("own", "early_rows", "early_lanes", "by_row", "by_lane", "eigen"):
            loads[name].wait()
    transform(k, counts, landing_f, g, spectrum)
    spectral_u(k, many, few, spectrum, coupled, coarse)
    gather_j.rest()
    double = 2.0 * keep * damp
    square = damp * damp
    mix = ((keep * keep, double, square), (double, 2.0 * square, None), (square, None, None))
    evaluate(k, "cubic", spectrum, mix, out)
    gather_j.end()
    coarse[1][...] = level2(k, few, transform2(k, counts, landing_j) - coarse[0][...])
    close_h.rest()
    spectral_e(many, spectrum, coupled, coarse[1])
    evaluate(k, "linear", spectrum, ((keep, damp), (damp, None)), out)
    close_h.end()
    unpack_near(landing_h, counts, near_h)
    keep1 = 1.0 - damp1 * diagonal1
    late = late_part(k, near_h, (keep, damp, damp1 * (1.0 + keep1), 0.25 * damp1 * damp1))
    out[...] = out[...] + late.reshape(out.shape)


def fast_per_device(counts, source, shift):
    nx, ny, nz = counts
    b0, b1, b2 = source.shape
    sizes = (b0 * nx, b1 * nz, b2 * ny)
    table = fast_constants(counts, source.shape, sizes)
    m0, m1, m2 = (size // 2 for size in sizes)
    rows = m0 * m1
    packed = (b0 // 4, b1 // 2, b2)
    devices = nx * ny * nz

    def field(*shape):
        return pltpu.VMEM(shape, jnp.float32)

    def in_hbm(value):
        return pltpu.with_memory_space_constraint(value, pltpu.HBM)

    names = tuple(table)
    tile = packed[1:]
    fine = [field(2, b1, b2), field(2, b0, 1, b2), field(2, 8, b0 * b1)]
    scratch = [pltpu.VMEM(table[name].shape, table[name].dtype) for name in names]
    scratch += [field(*source.shape), field(devices, *packed), field(devices, *packed), field(devices, 2, *tile)]
    scratch += [field(*tile)] * 2 + [field(*packed)] * 4 + fine
    scratch += [field(*packed)] * 5 + [field(*tile), field(2, *tile)] + fine
    scratch += [field(rows, m2)] * 7 + [field(rows // 4, m2 // 2)] * 9
    scratch += [field(rows // 16, m2 // 2), field(m0, m1, m2), field(b0 // 2 + 4, m1, m2)]
    scratch += [field(rows, m2), field(rows, m2), field(b0 + 2, b1 + 8, 2 * b2)]
    dma = pltpu.SemaphoreType.DMA
    scratch += [dma((len(names) + 1,))] + [dma((1,))] * 4
    along, across = stages(counts)
    scratch += TwoStage.semaphores(along) + TwoStage.semaphores(across) * 2
    return pl.pallas_call(
        functools.partial(fast_kernel, names, counts),
        out_shape=jax.ShapeDtypeStruct(source.shape, jnp.float32),
        in_specs=[pl.BlockSpec(memory_space=pltpu.HBM)] * len(names)
        + [pl.BlockSpec(memory_space=pltpu.SMEM), pl.BlockSpec(memory_space=pltpu.HBM)],
        out_specs=pl.BlockSpec(memory_space=pltpu.VMEM),
        scratch_shapes=scratch,
        compiler_params=pltpu.CompilerParams(
            vmem_limit_bytes=40 * 1024 * 1024, collective_id=0, has_side_effects=True
        ),
    )(*[in_hbm(jnp.asarray(table[name])) for name in names], shift, in_hbm(source))


def small_enough(counts, block):
    (nx, ny, nz), (b0, b1, b2) = counts, block
    rows = (b0 * nx // 2) * (b1 * nz // 2)
    return rows <= 512 and rows % 128 == 0 and (b0, b1, b2) == (16, 16, 128) and ny % 4 == 0 and min(counts) > 1


def dispatch(counts, source, shift):
    run = fast_per_device if small_enough(counts, source.shape) else per_device
    return run(counts, source, shift)


def solution(mesh):
    counts = tuple(mesh.shape[name] for name in NAMES)
    return jax.shard_map(
        functools.partial(dispatch, counts),
        mesh=mesh,
        in_specs=(P("gx", "gz", "gy"), P()),
        out_specs=P("gx", "gz", "gy"),
        check_vma=False,
    )
```

```python
import functools

import jax
import jax.numpy as jnp
import numpy as np
from jax import lax
from jax.experimental import pallas as pl
from jax.experimental.pallas import tpu as pltpu
from jax.sharding import PartitionSpec as P

LEVELS = 4
DAMPING = 6.0 / 7.0
PRECISE = lax.Precision.HIGHEST
CUBIC = (
    {-2: -5.0 / 128.0, -1: 35.0 / 128.0, 0: 105.0 / 128.0, 1: -7.0 / 128.0},
    {-1: -7.0 / 128.0, 0: 105.0 / 128.0, 1: 35.0 / 128.0, 2: -5.0 / 128.0},
)
LINEAR = ({-1: 0.25, 0: 0.75}, {0: 0.75, 1: 0.25})
NAMES = ("gx", "gy", "gz")
MESH = pl.DeviceIdType.MESH


def basis(count):
    cells = np.arange(count)
    columns, cosines = [], []
    for m in range(count):
        k = (m + 1) // 2
        angle = 2.0 * np.pi * k * cells / count
        column = np.cos(angle) if m % 2 == 1 or m == 0 else np.sin(angle)
        columns.append(column / np.sqrt(np.sum(column**2)))
        cosines.append(np.cos(2.0 * np.pi * k / count))
    return np.stack(columns, axis=1), np.array(cosines, np.float32)


def interpolation(coarse_count, fine_cells, weights):
    matrix = np.zeros((len(fine_cells), coarse_count))
    for row, cell in enumerate(fine_cells):
        for offset, weight in weights[cell % 2].items():
            matrix[row, (cell // 2 + offset) % coarse_count] += weight
    return matrix


def pairs(coarse_count):
    return np.kron(np.eye(coarse_count), np.ones((1, 2)))


def blocked(matrix):
    count = max(1, 128 // matrix.shape[1])
    return np.kron(np.eye(count), matrix)


def constants(block, sizes):
    b0, b1, b2 = block
    m0, m1, m2 = (size // 2 for size in sizes)
    q0, q1, q2 = (size // 4 for size in sizes)
    c0, c1, c2 = (size // 8 for size in sizes)
    table = {}
    table["own_rows"] = np.kron(np.eye(b0 // 2), pairs(b1 // 2))
    lanes = 0.125 * pairs(b2 // 2).T
    table["own_lo"] = np.concatenate([lanes, np.zeros_like(lanes)], axis=1)
    table["own_hi"] = np.concatenate([np.zeros_like(lanes), lanes], axis=1)
    table["down_rows"] = blocked(pairs(q1))
    table["down_lanes"] = 0.125 * pairs(q2).T
    window_lanes = [b2 + j for j in range(b2 // 2)] + [j - b2 for j in range(b2 // 2, 2 * b2)]
    window_rows = [j - 8 for j in range(b1 + 16)]
    for name, weights in (("cubic", CUBIC), ("linear", LINEAR)):
        table[name + "_rows1"] = blocked(interpolation(q1, range(m1), weights))
        table[name + "_lanes1"] = interpolation(q2, range(m2), weights).T
        table[name + "_rows0"] = blocked(interpolation(m1, window_rows, weights))
        table[name + "_lanes0"] = interpolation(m2, window_lanes, weights).T
    (u0, cos0), (u1, cos1), (u2, cos2) = basis(c0), basis(c1), basis(c2)
    table["spectrum_rows"] = np.kron(u0.T @ pairs(c0), u1.T @ pairs(c1))
    table["spectrum_lanes"] = 0.125 * pairs(c2).T @ u2
    for name, weights in (("cubic", CUBIC), ("linear", LINEAR)):
        table[name + "_rows2"] = np.kron(
            interpolation(c0, range(q0), weights) @ u0, interpolation(c1, range(q1), weights) @ u1
        )
        table[name + "_lanes2"] = u2.T @ interpolation(c2, range(q2), weights).T
    two = np.float32(2.0)
    eigen = (
        np.float32(6.0)
        - two * cos0[:, None, None]
        - two * cos1[None, :, None]
        - two * cos2[None, None, :]
    )
    table["eigen"] = (np.float32(0.25 ** (LEVELS - 1)) * eigen).reshape(c0 * c1, c2)
    wide = ("spectrum_rows", "spectrum_lanes", "eigen")
    return {
        name: np.asarray(
            value, np.float32 if name in wide or name.endswith("2") else jnp.bfloat16
        )
        for name, value in table.items()
    }


def dot(a, b):
    return jnp.dot(a, b, precision=PRECISE, preferred_element_type=jnp.float32)


def parts_of(values, pieces):
    parts = []
    for n in range(pieces):
        parts.append(values.astype(jnp.bfloat16))
        if n + 1 < pieces:
            values = values - parts[-1].astype(jnp.float32)
    return parts[::-1]


def right(values, matrix, pieces):
    terms = [
        jnp.dot(part, matrix, preferred_element_type=jnp.float32)
        for part in parts_of(values, pieces)
    ]
    return sum(terms[1:], terms[0])


def left(matrix, values, pieces):
    terms = [
        jnp.dot(matrix, part, preferred_element_type=jnp.float32)
        for part in parts_of(values, pieces)
    ]
    return sum(terms[1:], terms[0])


def around(plane):
    rows, lanes = plane.shape
    total = pltpu.roll(plane, 1, 0) + pltpu.roll(plane, rows - 1, 0)
    return total + (pltpu.roll(plane, 1, 1) + pltpu.roll(plane, lanes - 1, 1))


def around_all(values):
    first = jnp.concatenate([values[1:], values[:1]], axis=0)
    first = first + jnp.concatenate([values[-1:], values[:-1]], axis=0)
    for axis in (1, 2):
        first = first + pltpu.roll(values, 1, axis)
        first = first + pltpu.roll(values, values.shape[axis] - 1, axis)
    return first


def row_blocks(matrix, values, pieces):
    depth = matrix.shape[1]
    return jnp.concatenate(
        [left(matrix, values[i : i + depth], pieces) for i in range(0, values.shape[0], depth)], axis=0
    )


def loop(count, body, unroll=None):
    def step(i, carry):
        body(i)
        return carry

    lax.fori_loop(0, count, step, 0, unroll=unroll or (4 if count % 4 == 0 else 2))


def close(ref):
    count = ref.shape[0] - 2
    ref[0] = ref[count]
    ref[count + 1] = ref[1]


def defect_plane(v, p, g, weight, diagonal):
    center = v[p]
    beside = v[p - 1] + v[p + 1] + around(center)
    return center, g - (diagonal * center - weight * beside)


def restrict_own(k, summed):
    b_half, rows, lanes = summed.shape
    folded = left(k["own_rows"][...], summed.reshape(b_half * rows, lanes), 3)
    half = folded.shape[0] // 2
    return right(folded[:half], k["own_lo"][...], 3) + right(folded[half:], k["own_hi"][...], 3)


def unpack(gathered, counts, g):
    nx, ny, nz = counts
    x, y, z = (lax.axis_index(name) for name in NAMES)
    half, rows, lanes = gathered.shape[1:]
    low = lax.broadcasted_iota(jnp.int32, (half, rows, lanes), 2) < lanes // 2
    for dx in range(nx):
        for dz in range(nz):
            for pair in range(ny // 2):
                parts = []
                for dy in (2 * pair, 2 * pair + 1):
                    index = (lax.rem(x + dx, nx) * ny + lax.rem(y + dy, ny)) * nz
                    parts.append(gathered[index + lax.rem(z + dz, nz)])
                turned = [pltpu.roll(part, lanes // 2, 2) for part in parts]
                where = (pl.ds(dz * rows, rows), pl.ds(pair * lanes, lanes))
                start = 2 * half * dx
                g[(pl.ds(start, half), *where)] = jnp.where(low, parts[0], turned[1])
                g[(pl.ds(start + half, half), *where)] = jnp.where(low, turned[0], parts[1])


def solve(k, kind, values, shift):
    shape = values.shape
    flat = values.reshape(shape[0] * shape[1], shape[2])
    spectrum = dot(k["spectrum_rows"][...], dot(flat, k["spectrum_lanes"][...]))
    spectrum = spectrum / (k["eigen"][...] + shift)
    fine = dot(k[kind + "_rows2"][...], dot(spectrum, k[kind + "_lanes2"][...]))
    return fine.reshape(shape)


def cycle2(k, v, g, shift):
    weight = 0.25**2
    diagonal = 6.0 * weight + shift
    damp = DAMPING / diagonal
    if v is None:
        v = damp * g
    else:
        v = v + damp * (g - (diagonal * v - weight * around_all(v)))
    v = v + solve(k, "linear", g - (diagonal * v - weight * around_all(v)), shift)
    return v + damp * (g - (diagonal * v - weight * around_all(v)))


def down(k, t, shape2):
    flat = row_blocks(k["down_rows"][...], t[...].reshape(-1, t.shape[2]), 3)
    return right(flat, k["down_lanes"][...], 3).reshape(shape2)


def up(k, kind, level, values, z):
    flat = right(values, k[kind + "_lanes" + level][...], 2)
    z[...] = row_blocks(k[kind + "_rows" + level][...], flat, 2).reshape(z.shape)


def blend(z, i, weights, count):
    total = None
    for offset, weight in weights.items():
        index = i + offset
        index = index if count is None else lax.rem(index + count, count)
        term = weight * z[index]
        total = term if total is None else total + term
    return total


def up1(k, kind, values, z, v, add):
    count = z.shape[0]
    up(k, kind, "1", values.reshape(-1, values.shape[2]), z)
    weights = CUBIC if kind == "cubic" else LINEAR

    def body(i):
        for odd in (0, 1):
            p = 2 * i + odd + 1
            value = blend(z, i, weights[odd], count)
            v[p] = v[p] + value if add else value

    loop(count, body)
    close(v)


def cycle1(k, v, u, g, t, z, shift, zero, shape2):
    weight = 0.25
    diagonal = 6.0 * weight + shift
    damp = DAMPING / diagonal
    count = g.shape[0]

    def before(p):
        if zero:
            u[p + 1] = damp * g[p]
        else:
            center, rest = defect_plane(v, p + 1, g[p], weight, diagonal)
            u[p + 1] = center + damp * rest

    loop(count, before)
    close(u)

    def residue(i):
        t[i] = (
            defect_plane(u, 2 * i + 1, g[2 * i], weight, diagonal)[1]
            + defect_plane(u, 2 * i + 2, g[2 * i + 1], weight, diagonal)[1]
        )

    loop(count // 2, residue)
    correction = cycle2(k, None, down(k, t, shape2), shift)
    up1(k, "linear", correction, z, u, True)

    def after(p):
        center, rest = defect_plane(u, p + 1, g[p], weight, diagonal)
        v[p + 1] = center + damp * rest

    loop(count, after)
    close(v)


def window(k, kind, v, zw, span, write):
    count = v.shape[0] - 2
    values = jnp.concatenate([v[count - 3 : count + 1], v[1 : span - 3]], axis=0)
    up(k, kind, "0", values.reshape(-1, values.shape[2]), zw)
    weights = CUBIC if kind == "cubic" else LINEAR

    def body(i):
        for odd in (0, 1):
            write(2 * i + odd, blend(zw, i + 3, weights[odd], None))

    loop(span - 6, body)


def own_defect(v, p, f, weight, diagonal):
    rows, lanes = f.shape
    inside = (pl.ds(8, rows), pl.ds(lanes, lanes))
    wide = v[p + 1, pl.ds(8, rows), :]
    center = wide[:, lanes:]
    beside = v[(p, *inside)] + v[(p + 2, *inside)]
    beside = beside + v[p + 1, pl.ds(7, rows), pl.ds(lanes, lanes)]
    beside = beside + v[p + 1, pl.ds(9, rows), pl.ds(lanes, lanes)]
    beside = beside + pltpu.roll(wide, 1, 1)[:, lanes:]
    beside = beside + pltpu.roll(wide, 2 * lanes - 1, 1)[:, lanes:]
    return center, f - (diagonal * center - weight * beside)


def position():
    return tuple(lax.axis_index(name) for name in NAMES)


def partner_of(place):
    x, y, z = place
    return (x, y + 1 - 2 * lax.rem(y, 2), z)


def shifted(place, counts, offset):
    return tuple(
        lax.rem(at + step + count, count) for at, step, count in zip(place, offset, counts)
    )


def slot(place, counts):
    return (place[0] * counts[1] + place[1]) * counts[2] + place[2]


def chip_offsets(counts):
    nx, ny, nz = counts
    offsets = [
        (dx, dy, dz) for dx in range(nx) for dy in range(0, ny, 2) for dz in range(nz)
    ]

    def hops(offset):
        return sum(min(step, count - step) for step, count in zip(offset, (nx, ny, nz)))

    return sorted(offsets[1:], key=hops, reverse=True)


def face_offsets(counts):
    faces = []
    for axis in range(3):
        for side, step in ((0, -1), (1, 1)):
            offset = [0, 0, 0]
            offset[axis] = step
            faces.append((tuple(offset), axis, side))
    return faces


def greet(barrier, places):
    for place in places:
        pl.semaphore_signal(barrier, inc=1, device_id=place, device_id_type=MESH)


def remote(src, dst, send, recv, place):
    return pltpu.make_async_remote_copy(
        src_ref=src, dst_ref=dst, send_sem=send, recv_sem=recv, device_id=place, device_id_type=MESH
    )


def spread(counts, block, gathered, sems):
    send, recv, relay_send, relay_recv = sems
    me = position()
    partner = partner_of(me)
    along, across = stages(counts)
    number = {offset: n for n, offset in enumerate(chip_offsets(counts))}
    mine = gathered.at[slot(me, counts)]
    copies, relays = {}, []

    def pass_on(offset, source, target, place):
        n = number[offset]
        copies[offset] = remote(source, target, send.at[n], recv.at[n], place)
        copies[offset].start()

    def relay(n, source, target):
        relays.append(remote(source, target, relay_send.at[n], relay_recv.at[n], partner))
        relays[-1].start()

    for offset in along + across:
        pass_on(offset, block, mine, shifted(me, counts, offset))
    relay(len(number), block, mine)

    def arrival(offset):
        copies[offset].wait_recv()
        source = shifted(me, counts, tuple(-step for step in offset))
        return gathered.at[slot(source, counts)]

    def finish():
        gathered[slot(me, counts)] = block[...]
        for first in along[::-1]:
            arrived = arrival(first)
            for second in across:
                place = shifted(me, counts, second)
                pass_on((first[0], second[1], second[2]), arrived, arrived, place)
            relay(number[first], arrived, arrived)
        for first in ((0, 0, 0), *along[::-1]):
            for second in across[::-1]:
                offset = (first[0], second[1], second[2])
                arrived = arrival(offset)
                relay(number[offset], arrived, arrived)
        for copy in copies.values():
            copy.wait_send()
        for copy in relays:
            copy.wait()

    return finish


def stages(counts):
    offsets = chip_offsets(counts)
    along = [offset for offset in offsets if offset[1:] == (0, 0)]
    across = [offset for offset in offsets if offset[0] == 0]
    return along, across


def gather_places(counts):
    me = position()
    along, across = stages(counts)
    return [shifted(me, counts, offset) for offset in along + across] + [partner_of(me)]


def first_part(k, counts, source, f, gathered, halos, block, owns, sems, face_sems):
    own_planes, own_rows, own_columns = owns
    planes, rows, columns = halos
    face_send, face_recv = face_sems
    me = position()
    barrier = pltpu.get_barrier_semaphore()
    faces = face_offsets(counts)
    places = gather_places(counts) + [shifted(me, counts, offset) for offset, _, _ in faces]
    greet(barrier, places)
    b0, b1, b2 = source.shape
    summed = source[...].reshape(b0 // 2, 2, b1, b2)
    block[...] = restrict_own(k, summed[:, 0] + summed[:, 1]).reshape(block.shape)
    own_planes[0] = source[0]
    own_planes[1] = source[b0 - 1]
    own_rows[0] = source[:, pl.ds(0, 1), :]
    own_rows[1] = source[:, pl.ds(b1 - 1, 1), :]
    turned = source[...].reshape(b0 * b1, b2).T
    own_columns[0] = turned[:8]
    own_columns[1] = turned[b2 - 8 :]
    pl.semaphore_wait(barrier, len(places))
    finish = spread(counts, block, gathered, sems)
    buffers = ((own_planes, planes), (own_rows, rows), (own_columns, columns))
    order = (0, 2, 1)
    copies = []
    for n, (offset, axis, side) in enumerate(faces):
        own, halo = buffers[order[axis]]
        place = shifted(me, counts, offset)
        copies.append(
            remote(own.at[side], halo.at[1 - side], face_send.at[n], face_recv.at[n], place)
        )
        copies[-1].start()
    f[...] = jnp.zeros_like(f)
    f[1 : b0 + 1, pl.ds(8, b1), pl.ds(b2, b2)] = source[...]
    finish()
    for copy in copies:
        copy.wait()


def second_part(k, counts, shape2, span, shift, gathered, source, halos, out, buffers):
    g, v, u, t, z, zw, v0, v1, f, summed = buffers
    plane_halo, row_halo, column_halo = halos
    unpack(gathered, counts, g)
    b0, b1, b2 = source.shape
    rows, lanes = pl.ds(8, b1), pl.ds(b2, b2)
    f[0, rows, lanes] = plane_halo[0]
    f[b0 + 1, rows, lanes] = plane_halo[1]
    f[1 : b0 + 1, pl.ds(7, 1), lanes] = row_halo[0]
    f[1 : b0 + 1, pl.ds(8 + b1, 1), lanes] = row_halo[1]
    middle = jnp.zeros((b2 - 16, b0 * b1), jnp.float32)
    turned = jnp.concatenate([column_halo[1], middle, column_halo[0]], axis=0)
    f[1 : b0 + 1, rows, pl.ds(0, b2)] = turned.T.reshape(b0, b1, b2)
    def pair_sum(i):
        t[i] = g[2 * i] + g[2 * i + 1]

    loop(g.shape[0] // 2, pair_sum)
    forcing2 = down(k, t, shape2)
    iterate2 = cycle2(k, solve(k, "cubic", forcing2, shift), forcing2, shift)
    up1(k, "cubic", iterate2, z, v, False)
    cycle1(k, v, u, g, t, z, shift, False, shape2)

    def put(p, value):
        v0[p] = value

    window(k, "cubic", v, zw, span, put)
    diagonal = 6.0 + shift
    damp = DAMPING / diagonal

    def before(p):
        center, rest = defect_plane(v0, p + 1, f[p], 1.0, diagonal)
        v1[p] = center + damp * rest

    loop(b0 + 2, before)

    def residue(i):
        summed[i] = (
            own_defect(v1, 2 * i, source[2 * i], 1.0, diagonal)[1]
            + own_defect(v1, 2 * i + 1, source[2 * i + 1], 1.0, diagonal)[1]
        )

    loop(b0 // 2, residue)
    out[...] = restrict_own(k, summed[...]).reshape(out.shape)


def third_part(k, counts, shape2, span, shift, gathered, source, out, buffers):
    g, v, u, t, z, zw, w, v1 = buffers[:8]
    unpack(gathered, counts, g)
    cycle1(k, v, u, g, t, z, shift, True, shape2)
    b0 = source.shape[0]

    def put(p, value):
        w[p] = value

    window(k, "linear", v, zw, span, put)

    def add(p):
        w[p] = v1[p] + w[p + 1]

    loop(b0 + 2, add)
    diagonal = 6.0 + shift
    damp = DAMPING / diagonal

    def after(p):
        center, rest = own_defect(w, p, source[p], 1.0, diagonal)
        out[p] = center + damp * rest

    loop(b0, after)


def kernel(names, counts, shape2, span, *refs):
    k = dict(zip(names, refs))
    shift_ref, source, out, *rest = refs[len(names) :]
    shift = shift_ref[0]
    landing, later, *halos = rest[:5]
    block, block_later, *owns = rest[5:10]
    buffers = rest[10:20]
    sems, sems_later, face_sems = rest[20:24], rest[24:28], rest[28:30]
    f = buffers[8]
    first_part(k, counts, source, f, landing, halos, block, owns, sems, face_sems)
    second_part(k, counts, shape2, span, shift, landing, source, halos, block_later, buffers)
    spread(counts, block_later, later, sems_later)()
    third_part(k, counts, shape2, span, shift, later, source, out, buffers)


def per_device(counts, source, shift):
    nx, ny, nz = counts
    b0, b1, b2 = source.shape
    sizes = (b0 * nx, b1 * nz, b2 * ny)
    table = constants(source.shape, sizes)
    m0, m1, m2 = (size // 2 for size in sizes)
    shape2 = tuple(size // 4 for size in sizes)
    span = b0 // 2 + 8
    wide = (b1 + 16, 2 * b2)
    packed = (b0 // 4, b1 // 2, b2)
    devices = nx * ny * nz
    chips = devices // 2
    vmem = pl.BlockSpec(memory_space=pltpu.VMEM)

    def field(*shape):
        return pltpu.VMEM(shape, jnp.float32)

    faces = [field(2, b1, b2), field(2, b0, 1, b2), field(2, 8, b0 * b1)]
    buffers = [
        field(m0, m1, m2),
        field(m0 + 2, m1, m2),
        field(m0 + 2, m1, m2),
        field(m0 // 2, m1, m2),
        field(m0 // 2, m1, m2),
        field(span, *wide),
        field(b0 + 4, *wide),
        field(b0 + 2, *wide),
        field(b0 + 2, *wide),
        field(b0 // 2, b1, b2),
    ]
    sems = [pltpu.SemaphoreType.DMA((max(chips - 1, 1),))] * 2
    sems += [pltpu.SemaphoreType.DMA((chips,))] * 2
    landing = [field(devices, *packed)] * 2 + faces
    names = tuple(table)
    return pl.pallas_call(
        functools.partial(kernel, names, counts, shape2, span),
        out_shape=jax.ShapeDtypeStruct(source.shape, jnp.float32),
        in_specs=[vmem] * len(names) + [pl.BlockSpec(memory_space=pltpu.SMEM), vmem],
        out_specs=vmem,
        scratch_shapes=landing
        + [field(*packed)] * 2
        + faces
        + buffers
        + sems * 2
        + [pltpu.SemaphoreType.DMA((6,))] * 2,
        compiler_params=pltpu.CompilerParams(
            vmem_limit_bytes=60 * 1024 * 1024, collective_id=0, has_side_effects=True
        ),
    )(*[jnp.asarray(table[name]) for name in names], shift, source)


def modes(count, depth):
    if depth == 0:
        return [(0, k) for k in range(count // 2)] + [(1, k) for k in range(1, count // 2 + 1)]
    half = count // 2
    low = modes(half, depth - 1)
    high = []
    for kind, k in low:
        if kind == 0:
            high.append((0, half - k if k else half // 2))
        else:
            high.append((1, half - k if k < half // 2 else half))
    return low + high


def waves(count, order):
    cells = (np.arange(count) + 0.5) * (2.0 * np.pi / count)
    return np.stack([np.sin(k * cells) if kind else np.cos(k * cells) for kind, k in order], axis=1)


def analysis(waves_):
    return waves_.T / np.sum(waves_**2, axis=0)[:, None]


def two_blocks(matrix, axis):
    first, second = np.split(matrix, 2, axis=axis)
    return np.concatenate([np.diag(first), np.diag(second)])


def factors(m):
    orders = modes(m, 2), modes(m // 2, 1), modes(m // 4, 0)
    bases = [waves(len(order), order) for order in orders]
    t = {"waves": bases[0]}
    for level, fine, coarse in (("1", bases[0], bases[1]), ("2", bases[1], bases[2])):
        n = fine.shape[0]
        t["r" + level] = two_blocks(analysis(coarse) @ (0.5 * pairs(n // 2)) @ fine, 1)
        for name, weights in (("p", LINEAR), ("q", CUBIC)):
            matrix = interpolation(n // 2, range(n), weights)
            t[name + level] = two_blocks(analysis(fine) @ matrix @ coarse, 0)
        order = orders[int(level) - 1]
        t["e" + level] = np.array([2.0 - 2.0 * np.cos(2.0 * np.pi * k / n) for _, k in order])
    t["c3"] = np.array([np.cos(2.0 * np.pi * k / (m // 4)) for _, k in orders[2]], np.float32)
    fine = np.eye(2 * m)
    lap = 2.0 * fine - np.roll(fine, 1, 0) - np.roll(fine, -1, 0)
    current = interpolation(m, range(2 * m), CUBIC) @ bases[0]
    for i in range(3):
        t[f"m{i}"] = np.sum(analysis(bases[0]).T * ((0.5 * pairs(m)) @ current), axis=0)
        current = lap @ current
    return t


def near(matrix, axis=0):
    return np.roll(matrix, 1, axis) + np.roll(matrix, -1, axis)


def synthesis(t, cells, weights, powers):
    m = t["waves"].shape[0]
    matrix = interpolation(m, range(2 * m), weights) @ t["waves"]
    result = []
    for _ in range(powers):
        result.append(matrix[np.array(cells) % (2 * m)])
        matrix = near(matrix)
    return result


def pick(matrix, rows, columns):
    return matrix[np.array(rows) % matrix.shape[0]][:, np.array(columns) % matrix.shape[1]]


def late_kinds(m, rows, columns):
    plain = interpolation(m, range(2 * m), LINEAR)
    return [pick(kind, rows, columns) for kind in (plain, near(plain), near(plain, 1), near(near(plain), 1))]


def mixed(p, r):
    return [
        np.kron(p[0], r[0]),
        np.kron(p[1], r[0]) + np.kron(p[0], r[1]),
        np.kron(p[2], r[0]) + np.kron(p[0], r[2]),
        np.kron(p[3], r[0]) + np.kron(p[0], r[3]) + np.kron(p[2], r[1]) + np.kron(p[1], r[2]),
    ]


def exact(matrix):
    result = np.asarray(matrix, jnp.bfloat16)
    assert np.all(result.astype(np.float64) == matrix)
    return result


def halves(matrix, axis):
    high = np.asarray(matrix, jnp.bfloat16)
    low = np.asarray(matrix - high.astype(np.float64), jnp.bfloat16)
    return np.concatenate([high, low], axis=axis)


def halved_rows(m0, m1):
    index = np.arange(m0 * m1).reshape(2, 2, 2, m0 // 8, 2, 2, m1 // 4)
    index = index.transpose(2, 0, 4, 1, 5, 3, 6).reshape(2, 4, -1)
    return index, index[:, 0].reshape(-1), index.reshape(-1)


def own_table(half):
    count = 2 * half
    four = sum(np.roll(np.kron(np.eye(half), np.eye(2)[:, :1]), s, axis=0) for s in (-1, 0, 1, 2))
    four[count - 1, 0] = 0.0
    four[0, half - 1] = 0.0
    beside = np.zeros((count, half))
    beside[count - 1, 0] = beside[0, half - 1] = 1.0
    own = np.zeros((2, count, 3, 2, half))
    for n, part in enumerate((pairs(half).T, beside, four)):
        for s in range(2):
            own[s, :, n, s] = 0.125 * part
    return np.asarray(own.reshape(2 * count, 3 * count), jnp.bfloat16)


def two_levels(count):
    whole = 2 * count
    fine, half = np.eye(whole), np.eye(whole // 2)
    near, near1 = (np.roll(e, 1, 0) + np.roll(e, -1, 0) for e in (fine, half))
    down, down1 = pairs(whole // 2), pairs(whole // 4)
    start = count // 2
    rows = range(start // 4 - 1, (start + count) // 4 + 1)
    kinds = (down1 @ down, down1 @ down @ near, down1 @ near1 @ down, down1 @ near1 @ down @ near)
    return [kind[rows, start : start + count] for kind in kinds]


def early_tables(block):
    b0, b1, b2 = block
    (p, r, c) = ([*two_levels(size)] for size in block)
    full = mixed(p, r)
    rows = np.zeros((4, 3, 16, b0 * b1))
    rows[:, :, : 2 * r[0].shape[0]] = np.stack(full).reshape(4, 3, 2 * r[0].shape[0], b0 * b1)
    lanes = np.zeros((4, b2, b2))
    for n in range(4):
        lanes[n, :, : c[n].shape[0]] = c[n].T / 64.0
    return exact(rows.reshape(-1, b0 * b1)), exact(lanes.reshape(-1, b2))


def fast_constants(counts, block, sizes):
    nx, ny, nz = counts
    b0, b1, b2 = block
    m0, m1, m2 = (size // 2 for size in sizes)
    t0, t1, t2 = (factors(m) for m in (m0, m1, m2))
    parts, index2, index1 = halved_rows(m0, m1)
    i0, i1 = index1 // m1, index1 % m1
    j0, j1 = index2 // m1, index2 % m1
    rows2 = len(index2)

    def across(name, k, l, op=np.multiply):
        return op(t0[name][k], t1[name][l])

    def joint(a, c):
        return t0[a][i0] * t1[c][i1]

    columns = [across("r1", i0, i1), across("p1", i0, i1), across("q1", i0, i1), across("e1", i0, i1, np.add)]
    columns += [joint("m0", "m0"), joint("m1", "m0") + joint("m0", "m1")]
    columns += [joint("m2", "m0") + joint("m0", "m2") + 2.0 * joint("m1", "m1")]
    by_row = np.zeros((m0 * m1, 128))
    by_row[:, : len(columns)] = np.stack(columns, axis=1)
    for n, name in enumerate(("r2", "p2", "q2", "e2")):
        by_row[:rows2, 8 + n] = across(name, j0, j1, np.add if name == "e2" else np.multiply)
    by_lane = np.zeros((16, m2))
    for n, name in enumerate(("r1", "p1", "q1", "e1", "m0", "m1", "m2")):
        by_lane[n] = t2[name]
    for n, name in enumerate(("r2", "p2", "q2", "e2")):
        by_lane[8 + n, : m2 // 2] = t2[name]
    two = np.float32(2.0)
    eigen = np.float32(6.0) - two * t0["c3"][:, None, None]
    eigen = eigen - two * t1["c3"][None, :, None] - two * t2["c3"][None, None, :]
    eigen = (np.float32(0.25 ** (LEVELS - 1)) * eigen).reshape(rows2 // 4, m2 // 4)
    early_rows, early_lanes = early_tables(block)
    table = {"own": own_table(b2 // 2), "early_rows": early_rows, "early_lanes": early_lanes}
    small = {"by_row": by_row, "by_lane": by_lane, "eigen": np.concatenate([eigen, eigen], axis=1)}
    table.update({name: np.asarray(value, np.float32) for name, value in small.items()})

    a0, a1 = (analysis(waves(m // 2, modes(m // 2, 1))) for m in (m0, m1))
    a2 = analysis(waves(m2 // 2, modes(m2 // 2, 1)))
    p0, p1, p2 = b0 // 4, b1 // 4, b2 // 4
    wide = p2 + 2
    lanes = np.zeros((ny, b2, 3, m2 // 2))
    for dy in range(ny):
        for n in range(3):
            lanes[dy, 42 * n : 42 * n + wide, n] = a2[:, np.arange(p2 * dy - 1, p2 * dy + p2 + 1) % (m2 // 2)].T
    table["level2_lanes"] = halves(lanes.reshape(ny * b2, -1), 0)
    n, dx, dz, c, r = np.meshgrid(*(range(k) for k in (3, nx, nz, 2, p1 + 2)), indexing="ij")
    planes = (p0 * dx + 2 * n + c - 1 - p0 // 2) % (m0 // 2)
    rows = (p1 * dz + r - 1) % (m1 // 2)
    full = np.zeros((rows2, 3, nx, nz, 16))
    full[..., : 2 * (p1 + 2)] = (a0[j0][:, planes] * a1[j1][:, rows]).reshape(rows2, 3, nx, nz, -1)
    table["level2_rows"] = halves(full.reshape(rows2, -1), 1)

    forward = analysis(t0["waves"])[i0][:, : m0 // 2, None] * analysis(t1["waves"])[i1][:, None, :]
    table["forward_rows"] = halves(forward.reshape(2, m0 * m1 // 2, -1), 2)
    table["forward_lanes"] = halves(analysis(t2["waves"]).T, 0)
    for name, weights, powers in (("cubic", CUBIC, 3), ("linear", LINEAR, 2)):
        p = synthesis(t0, range(b0 // 2), weights, powers)
        r = synthesis(t1, range(b1), weights, powers)
        full = []
        for part in parts.reshape(2, -1):
            q0 = [matrix[:, part // m1][:, None, :] for matrix in p]
            q1 = [matrix[:, part % m1][None, :, :] for matrix in r]
            kinds = [q0[0] * q1[0], q0[1] * q1[0] + q0[0] * q1[1]]
            if powers == 3:
                kinds.append(q0[2] * q1[0] + 2.0 * q0[1] * q1[1] + q0[0] * q1[2])
            full.append(np.stack(kinds).reshape(-1, part.size))
        table[name + "_rows"] = halves(np.stack(full), 2)
        lanes = [matrix.T for matrix in synthesis(t2, range(b2), weights, powers)]
        table[name + "_lanes"] = halves(np.concatenate(lanes), 0)
    p = late_kinds(m0, range(b0), range(-2, b0 // 2 + 2))
    r = late_kinds(m1, range(b1), range(m1))
    table["late_rows"] = exact(np.concatenate(mixed(p, r), axis=1))
    table["late_lanes"] = exact(np.concatenate([c.T for c in late_kinds(m2, range(b2), range(m2))], axis=1))
    return table


def split(values):
    high = values.astype(jnp.bfloat16)
    return high, (values - high.astype(jnp.float32)).astype(jnp.bfloat16)


def by_right(values, table):
    high, low = split(values)
    depth = values.shape[1]
    first, second = table[:depth], table[depth:]
    return jnp.dot(
        jnp.concatenate([high, low, high], axis=1),
        jnp.concatenate([first, first, second], axis=0),
        preferred_element_type=jnp.float32,
    )


def by_left(table, values):
    high, low = split(values)
    depth = values.shape[0]
    first, second = table[:, :depth], table[:, depth:]
    return jnp.dot(
        jnp.concatenate([first, first, second], axis=1),
        jnp.concatenate([high, low, high], axis=0),
        preferred_element_type=jnp.float32,
    )


def fold(values):
    n = values.shape[0] // 8
    parts = []
    for kind in range(2):
        quarter = [values[(4 * kind + i) * n : (4 * kind + i + 1) * n] for i in range(4)]
        parts.append((quarter[0] + quarter[1]) + (quarter[2] + quarter[3]))
    total = jnp.concatenate(parts, axis=0)
    return total + pltpu.roll(total, total.shape[1] // 2, 1)


def unfold(values):
    n = values.shape[0] // 2
    return jnp.concatenate([values[:n]] * 4 + [values[n:]] * 4, axis=0)


def own_parts(source, own, outs, alpha, beta):
    block, across, along_rows, along_planes, rest = outs
    b0, b1, b2 = source.shape
    h0, h1 = b0 // 2, b1 // 2
    first = [source[p, pl.ds(0, h1, stride=2), :] for p in range(b0)]
    second = [source[p, pl.ds(1, h1, stride=2), :] for p in range(b0)]
    summed = [a + b for a, b in zip(first, second)]
    row = lax.broadcasted_iota(jnp.int32, (h1, b2), 0)
    zero = jnp.zeros((h1, b2), jnp.float32)
    whole, faces, inner = [], [], []
    for c in range(h0):
        total = summed[2 * c] + summed[2 * c + 1]
        down = pltpu.roll(second[2 * c] + second[2 * c + 1], 1, 0)
        up = pltpu.roll(first[2 * c] + first[2 * c + 1], h1 - 1, 0)
        whole.append(total)
        faces.append(jnp.where(row == 0, down, jnp.where(row == h1 - 1, up, zero)))
        near = 2.0 * total + jnp.where(row > 0, down, zero) + jnp.where(row < h1 - 1, up, zero)
        if c > 0:
            near = near + summed[2 * c - 1]
        if c < h0 - 1:
            near = near + summed[2 * c + 2]
        inner.append(near)

    def pack(planes):
        half = len(planes) // 2
        return [jnp.concatenate([planes[i], planes[i + half]], axis=1) for i in range(half)]

    ends = [jnp.concatenate([summed[b0 - 1], summed[0]], axis=1)]
    stacked = jnp.concatenate(pack(whole) + pack(faces) + pack(inner) + ends + [jnp.zeros((8, 2 * b2), jnp.float32)], axis=0)
    parts = parts_of(stacked, 3)
    weights = own[...]
    result = jnp.dot(
        jnp.concatenate(parts, axis=1),
        jnp.concatenate([weights] * 3, axis=0),
        preferred_element_type=jnp.float32,
    )
    n = h0 // 2 * h1
    shape = block.shape
    mine = result[:n, :b2]
    block[...] = mine.reshape(shape)
    across[...] = result[:n, b2 : 2 * b2].reshape(shape)
    along_rows[...] = result[n : 2 * n, :b2].reshape(shape)
    along_planes[...] = result[3 * n : 3 * n + h1, :b2]
    rest[...] = (alpha * mine + beta * (result[2 * n : 3 * n, :b2] + result[:n, 2 * b2 :])).reshape(shape)


def early_part(source, rows_table, lanes_table, weights):
    keep0, near0, keep1, near1 = weights
    b0, b1, b2 = source.shape
    result = jnp.dot(
        jnp.concatenate([rows_table[...]] * 3, axis=1),
        jnp.concatenate(parts_of(source[...].reshape(b0 * b1, b2), 3), axis=0),
        preferred_element_type=jnp.float32,
    )
    n = result.shape[0] // 4
    plain, first, second, both = (result[i * n : (i + 1) * n] for i in range(4))
    joint = near0 * near1
    columns = (
        (keep0 * keep1) * plain + (keep1 * near0) * first + (keep0 * near1) * second + joint * both,
        (keep1 * near0) * plain + joint * second,
        (keep0 * near1) * plain + joint * first,
        joint * plain,
    )
    result = jnp.dot(
        jnp.concatenate(parts_of(jnp.concatenate(columns, axis=1), 3), axis=1),
        jnp.concatenate([lanes_table[...]] * 3, axis=0),
        preferred_element_type=jnp.float32,
    )
    total = result[:16] + pltpu.roll(result[16:32], 42, 1)
    return (total + pltpu.roll(result[32:], 84, 1)).reshape(2, 8, b2)


def beyond(place, counts):
    x, y, z = place
    return (x, lax.rem(y - 1 + 2 * lax.rem(y, 2) + counts[1], counts[1]), z)


def wait_for(ref, sem):
    pltpu.make_async_copy(ref, ref, sem).wait()


class TwoStage:
    def __init__(self, counts, near, far, block, landing, sems):
        self.counts, self.near, self.far = counts, near, far
        self.block, self.landing = block, landing
        self.sent, self.arrived, self.relay_sent, self.relayed = sems
        self.count = 0

    def at(self, offset):
        source = shifted(position(), self.counts, tuple(-step for step in offset))
        return self.landing.at[slot(source, self.counts)]

    def send(self, source, target, step, sem):
        place = shifted(position(), self.counts, step)
        remote(source, target, self.sent.at[0], self.arrived.at[sem], place).start()
        self.count += 1

    def start(self, offsets):
        for offset in offsets:
            sem = self.near.index(offset) if offset in self.near else len(self.near)
            self.send(self.block, self.at((0, 0, 0)), offset, sem)

    def relay(self, source, target):
        remote(source, target, self.relay_sent.at[0], self.relayed.at[0], partner_of(position())).start()

    def own(self):
        self.relay(self.block, self.at((0, 0, 0)))

    def forward(self, which):
        for n in which:
            arrived = self.at(self.near[n])
            wait_for(arrived, self.arrived.at[n])
            for second in self.far:
                self.send(arrived, arrived, second, len(self.near) + 1 + n)
            self.relay(arrived, arrived)

    def rest(self, which=None):
        firsts = ((0, 0, 0), *self.near)
        for n in range(len(firsts)) if which is None else which:
            first = firsts[n]
            wait_for(self.landing.at[pl.ds(0, len(self.far))], self.arrived.at[len(self.near) + n])
            for second in self.far:
                arrived = self.at(tuple(a + b for a, b in zip(first, second)))
                self.relay(arrived, arrived)

    def end(self):
        self.landing[slot(position(), self.counts)] = self.block[...]
        wait_for(self.landing.at[pl.ds(0, self.count)], self.sent.at[0])
        for sem in (self.relay_sent, self.relayed):
            wait_for(self.landing.at[pl.ds(0, self.count + 1)], sem.at[0])

    @staticmethod
    def semaphores(near):
        dma = pltpu.SemaphoreType.DMA
        return [dma((1,)), dma((2 * len(near) + 1,)), dma((1,)), dma((1,))]


def piece(ref, part):
    if part == 0:
        return ref
    half = ref.shape[0] // 2
    return ref.at[pl.ds(half if part == 1 else 0, half)]


class Close:
    def __init__(self, counts, far, block, landing, sems):
        self.counts, self.far, self.block, self.landing = counts, far, block, landing
        self.near = [((1, 0, 0), 1), ((counts[0] - 1, 0, 0), -1)] if counts[0] > 2 else [((1, 0, 0), 0)]
        self.sent, self.arrived, self.relay_sent, self.relayed = sems
        self.blocks = 2 * len(far) + 1

    def at(self, offset):
        source = shifted(position(), self.counts, tuple(-step for step in offset))
        return self.landing.at[slot(source, self.counts)]

    def send(self, source, target, step, sem):
        place = shifted(position(), self.counts, step)
        remote(source, target, self.sent.at[0], self.arrived.at[sem], place).start()

    def relay(self, source, target):
        remote(source, target, self.relay_sent.at[0], self.relayed.at[0], partner_of(position())).start()

    def start(self):
        mine = self.at((0, 0, 0))
        for n, (step, part) in enumerate(self.near):
            self.send(piece(self.block, part), piece(mine, part), step, n)
        for step in self.far:
            self.send(self.block, mine, step, len(self.near))
        self.relay(self.block, mine)

    def forward(self):
        for n, (first, part) in enumerate(self.near):
            arrived = piece(self.at(first), part)
            wait_for(arrived, self.arrived.at[n])
            for step in self.far:
                self.send(arrived, arrived, step, len(self.near) + 1 + n)
            self.relay(arrived, arrived)

    def rest(self):
        count = len(self.far)
        wait_for(self.landing.at[pl.ds(0, count)], self.arrived.at[len(self.near)])
        for step in self.far:
            self.relay(self.at(step), self.at(step))
        for n, (first, part) in enumerate(self.near):
            size = self.landing.shape[1] // (2 if part else 1)
            wait_for(self.landing.at[pl.ds(0, count), pl.ds(0, size)], self.arrived.at[len(self.near) + 1 + n])
            for step in self.far:
                arrived = piece(self.at(tuple(a + b for a, b in zip(first, step))), part)
                self.relay(arrived, arrived)

    def end(self):
        self.landing[slot(position(), self.counts)] = self.block[...]
        wait_for(self.landing.at[pl.ds(0, self.blocks)], self.sent.at[0])
        for sem in (self.relay_sent, self.relayed):
            wait_for(self.landing.at[pl.ds(0, self.blocks + 1)], sem.at[0])


def exchange(counts, sent, received, send, recv):
    me = position()
    order = (0, 2, 1)
    for offset, axis, side in face_offsets(counts):
        which = order[axis]
        mine = sent[which] if len(sent[which]) == 1 else [sent[which][side]]
        place = shifted(me, counts, offset)
        remote(mine[0], received[2 * which + 1 - side], send.at[0], recv.at[0], place).start()


def prepare(k, many, few, shift):
    diagonal0, diagonal1, diagonal2 = (6.0 * 0.25**level + shift for level in range(3))
    sigma0, sigma1, sigma2 = diagonal0 - 6.0, diagonal1 - 1.5, diagonal2 - 0.375
    damp0, damp1, damp2 = DAMPING / diagonal0, DAMPING / diagonal1, DAMPING / diagonal2
    down, pre, fine_q, out_q, out_g, out_e, cross = many
    by_row, by_lane = k["by_row"], k["by_lane"]
    lanes = by_lane.shape[1]

    def level1(i):
        rows = pl.ds(pl.multiple_of(8 * i, 8), 8)
        column = by_row[rows, :]

        def tall(n):
            return jnp.broadcast_to(column[:, n : n + 1], (8, lanes))

        def wide(n):
            return jnp.broadcast_to(by_lane[n : n + 1, :], (8, lanes))

        r, p, q = (tall(n) * wide(n) for n in range(3))
        a = 0.25 * (tall(3) + wide(3)) + sigma1
        s = 1.0 - damp1 * a
        down[rows, :] = r
        pre[rows, :] = r * s
        fine_q[rows, :] = a * q
        out_q[rows, :] = s * s * q
        out_g[rows, :] = damp1 * (1.0 + s)
        out_e[rows, :] = s * p
        c0, c1, c2 = tall(4), tall(5), tall(6)
        first = sigma0 * c0 + c1 - damp0 * ((sigma0 * sigma0) * c0 + (2.0 * sigma0) * c1 + c2)
        second = c0 - (2.0 * damp0) * (sigma0 * c0 + c1)
        cross[rows, :] = first * wide(4) + second * wide(5) - (damp0 * c0) * wide(6)

    loop(by_row.shape[0] // 8, level1)
    rows2, lanes2 = few[0].shape
    column = by_row[:rows2, :]

    def tall(n):
        return jnp.broadcast_to(column[:, n : n + 1], (rows2, lanes2))

    def wide(n):
        return jnp.broadcast_to(by_lane[n : n + 1, :lanes2], (rows2, lanes2))

    r, p, q = (tall(n) * wide(n) for n in (8, 9, 10))
    a = 0.0625 * (tall(11) + wide(11)) + sigma2
    s = 1.0 - damp2 * a
    values = (r, r * s, a * q, s * s * q, damp2 * (1.0 + s), s * p)
    for ref, value in zip(few, values):
        ref[...] = value
    k["inverse"][...] = 1.0 / (k["eigen"][...] + shift)


def level2(k, few, g):
    down, pre, fine_q, out_q, out_g, out_e = few
    e = unfold(fold(pre[...] * g) * k["inverse"][...])
    return out_g[...] * g + out_e[...] * e


def level2_full(k, few, g):
    down, pre, fine_q, out_q, out_g, out_e = few
    start = unfold(fold(down[...] * g) * k["inverse"][...])
    e = unfold(fold(pre[...] * (g - fine_q[...] * start)) * k["inverse"][...])
    return out_q[...] * start + out_g[...] * g + out_e[...] * e


def blocks_of(spectrum, i):
    rows2, lanes2 = spectrum.shape[0] // 4, spectrum.shape[1] // 2
    half = rows2 // 2
    base = 8 * i + 3 * half * lax.div(i, half // 8)
    for a in range(4):
        start = pl.multiple_of(base + a * half, 8)
        for c in range(2):
            yield (pl.ds(start, 8), pl.ds(c * lanes2, lanes2))


def spectral_u(k, many, few, spectrum, coupled, coarse):
    down, pre, fine_q, out_q, out_g, out_e, cross = many
    first, second, third = coarse
    steps = first.shape[0] // 8

    def at(i):
        return pl.ds(pl.multiple_of(8 * i, 8), 8)

    def restrict(i):
        first[at(i), :] = sum(down[w] * spectrum[w] for w in blocks_of(spectrum, i))

    loop(steps, restrict, steps)
    second[...] = level2_full(k, few, first[...])

    def residue(i):
        u = second[at(i), :]
        first[at(i), :] = sum(pre[w] * (spectrum[w] - fine_q[w] * u) for w in blocks_of(spectrum, i))

    loop(steps, residue, steps)
    third[...] = level2(k, few, first[...])

    def finish(i):
        u, e = second[at(i), :], third[at(i), :]
        total = None
        for w in blocks_of(spectrum, i):
            value = out_q[w] * u + out_g[w] * spectrum[w] + out_e[w] * e
            spectrum[w] = value
            value = cross[w] * value
            coupled[w] = value
            total = pre[w] * value if total is None else total + pre[w] * value
        first[at(i), :] = total

    loop(steps, finish, steps)


def spectral_e(many, spectrum, coupled, e2):
    out_g, out_e = many[4], many[5]

    def finish(i):
        e = e2[pl.ds(pl.multiple_of(8 * i, 8), 8), :]
        for w in blocks_of(spectrum, i):
            spectrum[w] = out_e[w] * e - out_g[w] * coupled[w]

    loop(e2.shape[0] // 8, finish, e2.shape[0] // 8)


def unpack_centred(gathered, counts, g):
    nx, ny, nz = counts
    me = position()
    half, rows, lanes = gathered.shape[1:]
    planes = g.shape[0]
    low = lax.broadcasted_iota(jnp.int32, (half, rows, lanes), 2) < lanes // 2
    for dx in range(nx):
        for dz in range(nz):
            for pair in range(ny // 2):
                parts = [
                    gathered[slot(shifted(me, counts, (dx, dy, dz)), counts)] for dy in (2 * pair, 2 * pair + 1)
                ]
                turned = [pltpu.roll(part, lanes // 2, 2) for part in parts]
                where = (pl.ds(dz * rows, rows), pl.ds(pair * lanes, lanes))
                start = (2 * half * dx - half) % planes
                g[(pl.ds(start, half), *where)] = jnp.where(low, parts[0], turned[1])
                g[(pl.ds(2 * half * dx, half), *where)] = jnp.where(low, turned[0], parts[1])


def transform(k, counts, landing, g, spectrum):
    unpack_centred(landing, counts, g)
    m0, m1, m2 = g.shape
    half = m0 // 2
    depth = half * m1
    for kind in range(2):
        rows = [g[p] - g[m0 - 1 - p] if kind else g[p] + g[m0 - 1 - p] for p in range(half)]
        values = by_left(k["forward_rows"][kind], jnp.concatenate(rows, axis=0))
        spectrum[kind * depth : (kind + 1) * depth, :] = by_right(values, k["forward_lanes"])


def transform2(k, counts, landing):
    nx, ny, nz = counts
    me = position()
    columns = []
    for dy in range(ny):
        rows = [
            landing[slot(shifted(me, counts, (dx, dy, dz)), counts)].reshape(16, -1)
            for dx in range(nx)
            for dz in range(nz)
        ]
        columns.append(jnp.concatenate(rows, axis=0))
    values = by_right(jnp.concatenate(columns, axis=1), k["level2_lanes"])
    width = values.shape[1] // 3
    parts = [values[:, n * width : (n + 1) * width] for n in range(3)]
    return by_left(k["level2_rows"], jnp.concatenate(parts, axis=0))


def evaluate(k, kind, spectrum, mix, out):
    planes, rows, lanes = out.shape
    half = planes // 2
    depth = spectrum.shape[0] // 2
    parts = []
    for n in range(2):
        values = by_left(k[kind + "_rows"][n], spectrum[n * depth : (n + 1) * depth, :])
        pieces = [values[i : i + half * rows] for i in range(0, values.shape[0], half * rows)]
        columns = [sum(c * pieces[i] for i, c in enumerate(line) if c is not None) for line in mix]
        parts.append(by_right(jnp.concatenate(columns, axis=1), k[kind + "_lanes"]).reshape(half, rows, lanes))
    even, odd = parts
    for p in range(half):
        for index, value in ((half + p, even[p] + odd[p]), (half - 1 - p, even[p] - odd[p])):
            out[index] = out[index] + value


def unpack_near(gathered, counts, g):
    nx, ny, nz = counts
    me = position()
    half, rows, lanes = gathered.shape[1:]
    for dx, first, last in ((nx - 1, half - 2, half), (0, 0, half), (1, 0, 2)):
        shape = (last - first, rows, lanes)
        low = lax.broadcasted_iota(jnp.int32, shape, 2) < lanes // 2
        for dz in range(nz):
            for pair in range(ny // 2):
                parts = [
                    gathered[slot(shifted(me, counts, (dx, dy, dz)), counts), pl.ds(first, last - first)]
                    for dy in (2 * pair, 2 * pair + 1)
                ]
                turned = [pltpu.roll(part, lanes // 2, 2) for part in parts]
                where = (pl.ds(dz * rows, rows), pl.ds(pair * lanes, lanes))
                if dx != nx - 1:
                    start = 2 if dx == 0 else 2 + 2 * half
                    g[(pl.ds(start, last - first), *where)] = jnp.where(low, parts[0], turned[1])
                if dx != 1:
                    start = 2 + half if dx == 0 else 0
                    g[(pl.ds(start, last - first), *where)] = jnp.where(low, turned[0], parts[1])


def late_part(k, g, weights):
    keep0, near0, keep1, near1 = weights
    planes, m1, m2 = g.shape
    pieces = split(g[...].reshape(planes * m1, m2))
    table = k["late_lanes"][...]
    values = jnp.dot(
        jnp.concatenate(pieces, axis=1),
        jnp.concatenate([table, table], axis=0),
        preferred_element_type=jnp.float32,
    )
    lanes = values.shape[1] // 4
    a, b, c, d = (values[:, i * lanes : (i + 1) * lanes] for i in range(4))
    joint = near0 * near1
    stacked = (
        (keep0 * keep1) * a + (near0 * keep1) * b + (keep0 * near1) * c + joint * d,
        (near0 * keep1) * a + joint * c,
        (keep0 * near1) * a + joint * b,
        joint * a,
    )
    table = k["late_rows"][...]
    values = jnp.dot(
        jnp.concatenate([table, table], axis=1),
        jnp.concatenate(split(jnp.concatenate(stacked, axis=0)), axis=0),
        preferred_element_type=jnp.float32,
    )
    return values


def own_sweep(f, source, keep, damp, out):
    rows, lanes = source.shape[1:]

    def body(p):
        beside = f[p] + f[p + 2] + around(f[p + 1])
        out[p] = damp * ((1.0 + keep) * source[p] + damp * beside[:rows, :lanes])

    loop(source.shape[0], body, source.shape[0])


def fast_kernel(names, counts, *refs):
    count = len(names)
    outside = dict(zip(names, refs))
    shift_ref, source_ref, out, *rest = refs[count:]

    def take(number):
        taken = rest[:number]
        del rest[:number]
        return taken

    k = dict(zip(names, take(count)))
    (source,) = take(1)
    landing_f, landing_h, landing_j = take(3)
    faces_in, halos = take(6), take(3)
    block_f, block_h, across, along_rows, local, along_planes = take(6)
    (block_j,) = take(1)
    own_planes, own_rows, own_columns = take(3)
    many, few, coarse = take(7), take(6), take(3)
    k["inverse"], g, near_h, spectrum, coupled, f = take(6)
    table_sems, *face_sems = take(5)
    sems_f, sems_h, sems_j = take(4), take(4), take(4)

    shift = shift_ref[0]
    me = position()
    barrier = pltpu.get_barrier_semaphore()
    along, across_all = stages(counts)
    places = [shifted(me, counts, offset) for offset in along + across_all]
    places += [partner_of(me), beyond(me, counts)]
    greet(barrier, places)
    loads = {"source": pltpu.make_async_copy(source_ref, source, table_sems.at[count])}
    loads["source"].start()
    for n, name in enumerate(names):
        loads[name] = pltpu.make_async_copy(outside[name], k[name], table_sems.at[n])
        loads[name].start()

    b0, b1, b2 = source.shape
    diagonal, diagonal1 = 6.0 + shift, 1.5 + shift
    damp, damp1 = DAMPING / diagonal, DAMPING / diagonal1
    loads["source"].wait()
    loads["own"].wait()
    parts = (block_f, across, along_rows, along_planes, local)
    own_parts(source, k["own"], parts, 1.0 - damp * diagonal, damp)
    pl.semaphore_wait(barrier, len(places))

    exchange(counts, ([along_planes], [along_rows], [across]), faces_in, *face_sems[:2])
    gather_f = TwoStage(counts, along[::-1], across_all, block_f, landing_f, sems_f)
    gather_j = TwoStage(counts, across_all[::-1], along, block_j, landing_j, sems_j)
    gather_f.start(along[::-1] + across_all)
    gather_f.own()
    own_planes[0] = source[0]
    own_planes[1] = source[b0 - 1]
    own_rows[0] = source[:, pl.ds(0, 1), :]
    own_rows[1] = source[:, pl.ds(b1 - 1, 1), :]
    turned = source[...].reshape(b0 * b1, b2).T
    own_columns[0] = turned[:8]
    own_columns[1] = turned[b2 - 8 :]
    for name in ("early_rows", "early_lanes"):
        loads[name].wait()
    weights = (1.0 - damp * diagonal, damp, 1.0 - damp1 * diagonal1, 0.25 * damp1)
    block_j[...] = early_part(source, k["early_rows"], k["early_lanes"], weights)
    gather_j.start(across_all)
    gather_j.own()

    for name in ("by_row", "by_lane", "eigen"):
        loads[name].wait()
    prepare(k, many, few, shift)
    gather_f.forward(range(min(2, len(along))))
    for sem in face_sems[:2]:
        wait_for(f.at[pl.ds(0, 3)], sem.at[0])
    shape = local.shape
    lane = lax.rem(lax.broadcasted_iota(jnp.int32, shape, 2), b2 // 2)
    row = lax.broadcasted_iota(jnp.int32, shape, 1)
    from_planes, from_rows, from_lanes = faces_in[:2], faces_in[2:4], faces_in[4:6]
    total = jnp.where(lane == 0, from_lanes[0][...], 0.0) + jnp.where(lane == b2 // 2 - 1, from_lanes[1][...], 0.0)
    total = total + jnp.where(row == 0, from_rows[0][...], 0.0) + jnp.where(row == shape[1] - 1, from_rows[1][...], 0.0)
    block_h[...] = local[...] + damp * total
    low = lax.broadcasted_iota(jnp.int32, shape[1:], 1) < b2 // 2
    block_h[0] = block_h[0] + damp * jnp.where(low, from_planes[0][...], 0.0)
    end = shape[0] - 1
    block_h[end] = block_h[end] + damp * jnp.where(low, 0.0, from_planes[1][...])

    gather_f.forward(range(2, len(along)))
    mine = [[own.at[side] for side in range(2)] for own in (own_planes, own_rows, own_columns)]
    exchange(counts, mine, [halo.at[side] for halo in halos for side in range(2)], *face_sems[2:4])
    close_h = Close(counts, across_all[::-1], block_h, landing_h, sems_h)
    close_h.start()
    gather_j.start(along)
    gather_j.forward(range(len(across_all)))
    gather_f.rest(range(len(along)))
    close_h.forward()
    gather_f.rest(range(len(along), len(along) + 1))
    for sem in face_sems[2:4]:
        wait_for(f.at[pl.ds(0, 2)], sem.at[0])
    f[...] = jnp.zeros_like(f)
    rows, lanes = pl.ds(0, b1), pl.ds(0, b2)
    f[1 : b0 + 1, rows, lanes] = source[...]
    f[0, rows, lanes] = halos[0][0]
    f[b0 + 1, rows, lanes] = halos[0][1]
    f[1 : b0 + 1, pl.ds(b1, 1), lanes] = halos[1][1]
    f[1 : b0 + 1, pl.ds(b1 + 7, 1), lanes] = halos[1][0]
    middle = jnp.zeros((b2 - 16, b0 * b1), jnp.float32)
    turned = jnp.concatenate([halos[2][1], middle, halos[2][0]], axis=0)
    f[1 : b0 + 1, rows, pl.ds(b2, b2)] = turned.T.reshape(b0, b1, b2)
    keep = 1.0 - damp * diagonal
    own_sweep(f, source, keep, damp, out)
    gather_j.rest()
    gather_f.end()
    for name in names:
        if name not in ("own", "early_rows", "early_lanes", "by_row", "by_lane", "eigen"):
            loads[name].wait()
    transform(k, counts, landing_f, g, spectrum)
    spectral_u(k, many, few, spectrum, coupled, coarse)
    gather_j.end()
    double = 2.0 * keep * damp
    square = damp * damp
    mix = ((keep * keep, double, square), (double, 2.0 * square, None), (square, None, None))
    e2 = level2(k, few, transform2(k, counts, landing_j) - coarse[0][...])
    evaluate(k, "cubic", spectrum, mix, out)
    coarse[1][...] = e2
    close_h.rest()
    spectral_e(many, spectrum, coupled, coarse[1])
    evaluate(k, "linear", spectrum, ((keep, damp), (damp, None)), out)
    close_h.end()
    unpack_near(landing_h, counts, near_h)
    keep1 = 1.0 - damp1 * diagonal1
    late = late_part(k, near_h, (keep, damp, damp1 * (1.0 + keep1), 0.25 * damp1 * damp1))
    out[...] = out[...] + late.reshape(out.shape)


def fast_per_device(counts, source, shift):
    nx, ny, nz = counts
    b0, b1, b2 = source.shape
    sizes = (b0 * nx, b1 * nz, b2 * ny)
    table = fast_constants(counts, source.shape, sizes)
    m0, m1, m2 = (size // 2 for size in sizes)
    rows = m0 * m1
    packed = (b0 // 4, b1 // 2, b2)
    devices = nx * ny * nz

    def field(*shape):
        return pltpu.VMEM(shape, jnp.float32)

    def in_hbm(value):
        return pltpu.with_memory_space_constraint(value, pltpu.HBM)

    names = tuple(table)
    tile = packed[1:]
    fine = [field(2, b1, b2), field(2, b0, 1, b2), field(2, 8, b0 * b1)]
    scratch = [pltpu.VMEM(table[name].shape, table[name].dtype) for name in names]
    scratch += [field(*source.shape), field(devices, *packed), field(devices, *packed), field(devices, 2, *tile)]
    scratch += [field(*tile)] * 2 + [field(*packed)] * 4 + fine
    scratch += [field(*packed)] * 5 + [field(*tile), field(2, *tile)] + fine
    scratch += [field(rows, m2)] * 7 + [field(rows // 4, m2 // 2)] * 9
    scratch += [field(rows // 16, m2 // 2), field(m0, m1, m2), field(b0 // 2 + 4, m1, m2)]
    scratch += [field(rows, m2), field(rows, m2), field(b0 + 2, b1 + 8, 2 * b2)]
    dma = pltpu.SemaphoreType.DMA
    scratch += [dma((len(names) + 1,))] + [dma((1,))] * 4
    along, across = stages(counts)
    scratch += TwoStage.semaphores(along) * 2 + TwoStage.semaphores(across)
    return pl.pallas_call(
        functools.partial(fast_kernel, names, counts),
        out_shape=jax.ShapeDtypeStruct(source.shape, jnp.float32),
        in_specs=[pl.BlockSpec(memory_space=pltpu.HBM)] * len(names)
        + [pl.BlockSpec(memory_space=pltpu.SMEM), pl.BlockSpec(memory_space=pltpu.HBM)],
        out_specs=pl.BlockSpec(memory_space=pltpu.VMEM),
        scratch_shapes=scratch,
        compiler_params=pltpu.CompilerParams(
            vmem_limit_bytes=40 * 1024 * 1024, collective_id=0, has_side_effects=True
        ),
    )(*[in_hbm(jnp.asarray(table[name])) for name in names], shift, in_hbm(source))


def small_enough(counts, block):
    (nx, ny, nz), (b0, b1, b2) = counts, block
    rows = (b0 * nx // 2) * (b1 * nz // 2)
    return rows <= 512 and rows % 128 == 0 and (b0, b1, b2) == (16, 16, 128) and ny % 4 == 0 and min(counts) > 1


def dispatch(counts, source, shift):
    run = fast_per_device if small_enough(counts, source.shape) else per_device
    return run(counts, source, shift)


def solution(mesh):
    counts = tuple(mesh.shape[name] for name in NAMES)
    return jax.shard_map(
        functools.partial(dispatch, counts),
        mesh=mesh,
        in_specs=(P("gx", "gz", "gy"), P()),
        out_specs=P("gx", "gz", "gy"),
        check_vma=False,
    )
```

```python
import functools

import jax
import jax.numpy as jnp
import numpy as np
from jax import lax
from jax.experimental import pallas as pl
from jax.experimental.pallas import tpu as pltpu
from jax.sharding import PartitionSpec as P

LEVELS = 4
DAMPING = 6.0 / 7.0
PRECISE = lax.Precision.HIGHEST
CUBIC = (
    {-2: -5.0 / 128.0, -1: 35.0 / 128.0, 0: 105.0 / 128.0, 1: -7.0 / 128.0},
    {-1: -7.0 / 128.0, 0: 105.0 / 128.0, 1: 35.0 / 128.0, 2: -5.0 / 128.0},
)
LINEAR = ({-1: 0.25, 0: 0.75}, {0: 0.75, 1: 0.25})
NAMES = ("gx", "gy", "gz")
MESH = pl.DeviceIdType.MESH


def basis(count):
    cells = np.arange(count)
    columns, cosines = [], []
    for m in range(count):
        k = (m + 1) // 2
        angle = 2.0 * np.pi * k * cells / count
        column = np.cos(angle) if m % 2 == 1 or m == 0 else np.sin(angle)
        columns.append(column / np.sqrt(np.sum(column**2)))
        cosines.append(np.cos(2.0 * np.pi * k / count))
    return np.stack(columns, axis=1), np.array(cosines, np.float32)


def interpolation(coarse_count, fine_cells, weights):
    matrix = np.zeros((len(fine_cells), coarse_count))
    for row, cell in enumerate(fine_cells):
        for offset, weight in weights[cell % 2].items():
            matrix[row, (cell // 2 + offset) % coarse_count] += weight
    return matrix


def pairs(coarse_count):
    return np.kron(np.eye(coarse_count), np.ones((1, 2)))


def blocked(matrix):
    count = max(1, 128 // matrix.shape[1])
    return np.kron(np.eye(count), matrix)


def constants(block, sizes):
    b0, b1, b2 = block
    m0, m1, m2 = (size // 2 for size in sizes)
    q0, q1, q2 = (size // 4 for size in sizes)
    c0, c1, c2 = (size // 8 for size in sizes)
    table = {}
    table["own_rows"] = np.kron(np.eye(b0 // 2), pairs(b1 // 2))
    lanes = 0.125 * pairs(b2 // 2).T
    table["own_lo"] = np.concatenate([lanes, np.zeros_like(lanes)], axis=1)
    table["own_hi"] = np.concatenate([np.zeros_like(lanes), lanes], axis=1)
    table["down_rows"] = blocked(pairs(q1))
    table["down_lanes"] = 0.125 * pairs(q2).T
    window_lanes = [b2 + j for j in range(b2 // 2)] + [j - b2 for j in range(b2 // 2, 2 * b2)]
    window_rows = [j - 8 for j in range(b1 + 16)]
    for name, weights in (("cubic", CUBIC), ("linear", LINEAR)):
        table[name + "_rows1"] = blocked(interpolation(q1, range(m1), weights))
        table[name + "_lanes1"] = interpolation(q2, range(m2), weights).T
        table[name + "_rows0"] = blocked(interpolation(m1, window_rows, weights))
        table[name + "_lanes0"] = interpolation(m2, window_lanes, weights).T
    (u0, cos0), (u1, cos1), (u2, cos2) = basis(c0), basis(c1), basis(c2)
    table["spectrum_rows"] = np.kron(u0.T @ pairs(c0), u1.T @ pairs(c1))
    table["spectrum_lanes"] = 0.125 * pairs(c2).T @ u2
    for name, weights in (("cubic", CUBIC), ("linear", LINEAR)):
        table[name + "_rows2"] = np.kron(
            interpolation(c0, range(q0), weights) @ u0, interpolation(c1, range(q1), weights) @ u1
        )
        table[name + "_lanes2"] = u2.T @ interpolation(c2, range(q2), weights).T
    two = np.float32(2.0)
    eigen = (
        np.float32(6.0)
        - two * cos0[:, None, None]
        - two * cos1[None, :, None]
        - two * cos2[None, None, :]
    )
    table["eigen"] = (np.float32(0.25 ** (LEVELS - 1)) * eigen).reshape(c0 * c1, c2)
    wide = ("spectrum_rows", "spectrum_lanes", "eigen")
    return {
        name: np.asarray(
            value, np.float32 if name in wide or name.endswith("2") else jnp.bfloat16
        )
        for name, value in table.items()
    }


def dot(a, b):
    return jnp.dot(a, b, precision=PRECISE, preferred_element_type=jnp.float32)


def parts_of(values, pieces):
    parts = []
    for n in range(pieces):
        parts.append(values.astype(jnp.bfloat16))
        if n + 1 < pieces:
            values = values - parts[-1].astype(jnp.float32)
    return parts[::-1]


def right(values, matrix, pieces):
    terms = [
        jnp.dot(part, matrix, preferred_element_type=jnp.float32)
        for part in parts_of(values, pieces)
    ]
    return sum(terms[1:], terms[0])


def left(matrix, values, pieces):
    terms = [
        jnp.dot(matrix, part, preferred_element_type=jnp.float32)
        for part in parts_of(values, pieces)
    ]
    return sum(terms[1:], terms[0])


def around(plane):
    rows, lanes = plane.shape
    total = pltpu.roll(plane, 1, 0) + pltpu.roll(plane, rows - 1, 0)
    return total + (pltpu.roll(plane, 1, 1) + pltpu.roll(plane, lanes - 1, 1))


def around_all(values):
    first = jnp.concatenate([values[1:], values[:1]], axis=0)
    first = first + jnp.concatenate([values[-1:], values[:-1]], axis=0)
    for axis in (1, 2):
        first = first + pltpu.roll(values, 1, axis)
        first = first + pltpu.roll(values, values.shape[axis] - 1, axis)
    return first


def row_blocks(matrix, values, pieces):
    depth = matrix.shape[1]
    return jnp.concatenate(
        [left(matrix, values[i : i + depth], pieces) for i in range(0, values.shape[0], depth)], axis=0
    )


def loop(count, body, unroll=None):
    def step(i, carry):
        body(i)
        return carry

    lax.fori_loop(0, count, step, 0, unroll=unroll or (4 if count % 4 == 0 else 2))


def close(ref):
    count = ref.shape[0] - 2
    ref[0] = ref[count]
    ref[count + 1] = ref[1]


def defect_plane(v, p, g, weight, diagonal):
    center = v[p]
    beside = v[p - 1] + v[p + 1] + around(center)
    return center, g - (diagonal * center - weight * beside)


def restrict_own(k, summed):
    b_half, rows, lanes = summed.shape
    folded = left(k["own_rows"][...], summed.reshape(b_half * rows, lanes), 3)
    half = folded.shape[0] // 2
    return right(folded[:half], k["own_lo"][...], 3) + right(folded[half:], k["own_hi"][...], 3)


def unpack(gathered, counts, g):
    nx, ny, nz = counts
    x, y, z = (lax.axis_index(name) for name in NAMES)
    half, rows, lanes = gathered.shape[1:]
    low = lax.broadcasted_iota(jnp.int32, (half, rows, lanes), 2) < lanes // 2
    for dx in range(nx):
        for dz in range(nz):
            for pair in range(ny // 2):
                parts = []
                for dy in (2 * pair, 2 * pair + 1):
                    index = (lax.rem(x + dx, nx) * ny + lax.rem(y + dy, ny)) * nz
                    parts.append(gathered[index + lax.rem(z + dz, nz)])
                turned = [pltpu.roll(part, lanes // 2, 2) for part in parts]
                where = (pl.ds(dz * rows, rows), pl.ds(pair * lanes, lanes))
                start = 2 * half * dx
                g[(pl.ds(start, half), *where)] = jnp.where(low, parts[0], turned[1])
                g[(pl.ds(start + half, half), *where)] = jnp.where(low, turned[0], parts[1])


def solve(k, kind, values, shift):
    shape = values.shape
    flat = values.reshape(shape[0] * shape[1], shape[2])
    spectrum = dot(k["spectrum_rows"][...], dot(flat, k["spectrum_lanes"][...]))
    spectrum = spectrum / (k["eigen"][...] + shift)
    fine = dot(k[kind + "_rows2"][...], dot(spectrum, k[kind + "_lanes2"][...]))
    return fine.reshape(shape)


def cycle2(k, v, g, shift):
    weight = 0.25**2
    diagonal = 6.0 * weight + shift
    damp = DAMPING / diagonal
    if v is None:
        v = damp * g
    else:
        v = v + damp * (g - (diagonal * v - weight * around_all(v)))
    v = v + solve(k, "linear", g - (diagonal * v - weight * around_all(v)), shift)
    return v + damp * (g - (diagonal * v - weight * around_all(v)))


def down(k, t, shape2):
    flat = row_blocks(k["down_rows"][...], t[...].reshape(-1, t.shape[2]), 3)
    return right(flat, k["down_lanes"][...], 3).reshape(shape2)


def up(k, kind, level, values, z):
    flat = right(values, k[kind + "_lanes" + level][...], 2)
    z[...] = row_blocks(k[kind + "_rows" + level][...], flat, 2).reshape(z.shape)


def blend(z, i, weights, count):
    total = None
    for offset, weight in weights.items():
        index = i + offset
        index = index if count is None else lax.rem(index + count, count)
        term = weight * z[index]
        total = term if total is None else total + term
    return total


def up1(k, kind, values, z, v, add):
    count = z.shape[0]
    up(k, kind, "1", values.reshape(-1, values.shape[2]), z)
    weights = CUBIC if kind == "cubic" else LINEAR

    def body(i):
        for odd in (0, 1):
            p = 2 * i + odd + 1
            value = blend(z, i, weights[odd], count)
            v[p] = v[p] + value if add else value

    loop(count, body)
    close(v)


def cycle1(k, v, u, g, t, z, shift, zero, shape2):
    weight = 0.25
    diagonal = 6.0 * weight + shift
    damp = DAMPING / diagonal
    count = g.shape[0]

    def before(p):
        if zero:
            u[p + 1] = damp * g[p]
        else:
            center, rest = defect_plane(v, p + 1, g[p], weight, diagonal)
            u[p + 1] = center + damp * rest

    loop(count, before)
    close(u)

    def residue(i):
        t[i] = (
            defect_plane(u, 2 * i + 1, g[2 * i], weight, diagonal)[1]
            + defect_plane(u, 2 * i + 2, g[2 * i + 1], weight, diagonal)[1]
        )

    loop(count // 2, residue)
    correction = cycle2(k, None, down(k, t, shape2), shift)
    up1(k, "linear", correction, z, u, True)

    def after(p):
        center, rest = defect_plane(u, p + 1, g[p], weight, diagonal)
        v[p + 1] = center + damp * rest

    loop(count, after)
    close(v)


def window(k, kind, v, zw, span, write):
    count = v.shape[0] - 2
    values = jnp.concatenate([v[count - 3 : count + 1], v[1 : span - 3]], axis=0)
    up(k, kind, "0", values.reshape(-1, values.shape[2]), zw)
    weights = CUBIC if kind == "cubic" else LINEAR

    def body(i):
        for odd in (0, 1):
            write(2 * i + odd, blend(zw, i + 3, weights[odd], None))

    loop(span - 6, body)


def own_defect(v, p, f, weight, diagonal):
    rows, lanes = f.shape
    inside = (pl.ds(8, rows), pl.ds(lanes, lanes))
    wide = v[p + 1, pl.ds(8, rows), :]
    center = wide[:, lanes:]
    beside = v[(p, *inside)] + v[(p + 2, *inside)]
    beside = beside + v[p + 1, pl.ds(7, rows), pl.ds(lanes, lanes)]
    beside = beside + v[p + 1, pl.ds(9, rows), pl.ds(lanes, lanes)]
    beside = beside + pltpu.roll(wide, 1, 1)[:, lanes:]
    beside = beside + pltpu.roll(wide, 2 * lanes - 1, 1)[:, lanes:]
    return center, f - (diagonal * center - weight * beside)


def position():
    return tuple(lax.axis_index(name) for name in NAMES)


def partner_of(place):
    x, y, z = place
    return (x, y + 1 - 2 * lax.rem(y, 2), z)


def shifted(place, counts, offset):
    return tuple(
        lax.rem(at + step + count, count) for at, step, count in zip(place, offset, counts)
    )


def slot(place, counts):
    return (place[0] * counts[1] + place[1]) * counts[2] + place[2]


def chip_offsets(counts):
    nx, ny, nz = counts
    offsets = [
        (dx, dy, dz) for dx in range(nx) for dy in range(0, ny, 2) for dz in range(nz)
    ]

    def hops(offset):
        return sum(min(step, count - step) for step, count in zip(offset, (nx, ny, nz)))

    return sorted(offsets[1:], key=hops, reverse=True)


def face_offsets(counts):
    faces = []
    for axis in range(3):
        for side, step in ((0, -1), (1, 1)):
            offset = [0, 0, 0]
            offset[axis] = step
            faces.append((tuple(offset), axis, side))
    return faces


def greet(barrier, places):
    for place in places:
        pl.semaphore_signal(barrier, inc=1, device_id=place, device_id_type=MESH)


def remote(src, dst, send, recv, place):
    return pltpu.make_async_remote_copy(
        src_ref=src, dst_ref=dst, send_sem=send, recv_sem=recv, device_id=place, device_id_type=MESH
    )


def spread(counts, block, gathered, sems):
    send, recv, relay_send, relay_recv = sems
    me = position()
    partner = partner_of(me)
    along, across = stages(counts)
    number = {offset: n for n, offset in enumerate(chip_offsets(counts))}
    mine = gathered.at[slot(me, counts)]
    copies, relays = {}, []

    def pass_on(offset, source, target, place):
        n = number[offset]
        copies[offset] = remote(source, target, send.at[n], recv.at[n], place)
        copies[offset].start()

    def relay(n, source, target):
        relays.append(remote(source, target, relay_send.at[n], relay_recv.at[n], partner))
        relays[-1].start()

    for offset in along + across:
        pass_on(offset, block, mine, shifted(me, counts, offset))
    relay(len(number), block, mine)

    def arrival(offset):
        copies[offset].wait_recv()
        source = shifted(me, counts, tuple(-step for step in offset))
        return gathered.at[slot(source, counts)]

    def finish():
        gathered[slot(me, counts)] = block[...]
        for first in along[::-1]:
            arrived = arrival(first)
            for second in across:
                place = shifted(me, counts, second)
                pass_on((first[0], second[1], second[2]), arrived, arrived, place)
            relay(number[first], arrived, arrived)
        for first in ((0, 0, 0), *along[::-1]):
            for second in across[::-1]:
                offset = (first[0], second[1], second[2])
                arrived = arrival(offset)
                relay(number[offset], arrived, arrived)
        for copy in copies.values():
            copy.wait_send()
        for copy in relays:
            copy.wait()

    return finish


def stages(counts):
    offsets = chip_offsets(counts)
    along = [offset for offset in offsets if offset[1:] == (0, 0)]
    across = [offset for offset in offsets if offset[0] == 0]
    return along, across


def gather_places(counts):
    me = position()
    along, across = stages(counts)
    return [shifted(me, counts, offset) for offset in along + across] + [partner_of(me)]


def first_part(k, counts, source, f, gathered, halos, block, owns, sems, face_sems):
    own_planes, own_rows, own_columns = owns
    planes, rows, columns = halos
    face_send, face_recv = face_sems
    me = position()
    barrier = pltpu.get_barrier_semaphore()
    faces = face_offsets(counts)
    places = gather_places(counts) + [shifted(me, counts, offset) for offset, _, _ in faces]
    greet(barrier, places)
    b0, b1, b2 = source.shape
    summed = source[...].reshape(b0 // 2, 2, b1, b2)
    block[...] = restrict_own(k, summed[:, 0] + summed[:, 1]).reshape(block.shape)
    own_planes[0] = source[0]
    own_planes[1] = source[b0 - 1]
    own_rows[0] = source[:, pl.ds(0, 1), :]
    own_rows[1] = source[:, pl.ds(b1 - 1, 1), :]
    turned = source[...].reshape(b0 * b1, b2).T
    own_columns[0] = turned[:8]
    own_columns[1] = turned[b2 - 8 :]
    pl.semaphore_wait(barrier, len(places))
    finish = spread(counts, block, gathered, sems)
    buffers = ((own_planes, planes), (own_rows, rows), (own_columns, columns))
    order = (0, 2, 1)
    copies = []
    for n, (offset, axis, side) in enumerate(faces):
        own, halo = buffers[order[axis]]
        place = shifted(me, counts, offset)
        copies.append(
            remote(own.at[side], halo.at[1 - side], face_send.at[n], face_recv.at[n], place)
        )
        copies[-1].start()
    f[...] = jnp.zeros_like(f)
    f[1 : b0 + 1, pl.ds(8, b1), pl.ds(b2, b2)] = source[...]
    finish()
    for copy in copies:
        copy.wait()


def second_part(k, counts, shape2, span, shift, gathered, source, halos, out, buffers):
    g, v, u, t, z, zw, v0, v1, f, summed = buffers
    plane_halo, row_halo, column_halo = halos
    unpack(gathered, counts, g)
    b0, b1, b2 = source.shape
    rows, lanes = pl.ds(8, b1), pl.ds(b2, b2)
    f[0, rows, lanes] = plane_halo[0]
    f[b0 + 1, rows, lanes] = plane_halo[1]
    f[1 : b0 + 1, pl.ds(7, 1), lanes] = row_halo[0]
    f[1 : b0 + 1, pl.ds(8 + b1, 1), lanes] = row_halo[1]
    middle = jnp.zeros((b2 - 16, b0 * b1), jnp.float32)
    turned = jnp.concatenate([column_halo[1], middle, column_halo[0]], axis=0)
    f[1 : b0 + 1, rows, pl.ds(0, b2)] = turned.T.reshape(b0, b1, b2)
    def pair_sum(i):
        t[i] = g[2 * i] + g[2 * i + 1]

    loop(g.shape[0] // 2, pair_sum)
    forcing2 = down(k, t, shape2)
    iterate2 = cycle2(k, solve(k, "cubic", forcing2, shift), forcing2, shift)
    up1(k, "cubic", iterate2, z, v, False)
    cycle1(k, v, u, g, t, z, shift, False, shape2)

    def put(p, value):
        v0[p] = value

    window(k, "cubic", v, zw, span, put)
    diagonal = 6.0 + shift
    damp = DAMPING / diagonal

    def before(p):
        center, rest = defect_plane(v0, p + 1, f[p], 1.0, diagonal)
        v1[p] = center + damp * rest

    loop(b0 + 2, before)

    def residue(i):
        summed[i] = (
            own_defect(v1, 2 * i, source[2 * i], 1.0, diagonal)[1]
            + own_defect(v1, 2 * i + 1, source[2 * i + 1], 1.0, diagonal)[1]
        )

    loop(b0 // 2, residue)
    out[...] = restrict_own(k, summed[...]).reshape(out.shape)


def third_part(k, counts, shape2, span, shift, gathered, source, out, buffers):
    g, v, u, t, z, zw, w, v1 = buffers[:8]
    unpack(gathered, counts, g)
    cycle1(k, v, u, g, t, z, shift, True, shape2)
    b0 = source.shape[0]

    def put(p, value):
        w[p] = value

    window(k, "linear", v, zw, span, put)

    def add(p):
        w[p] = v1[p] + w[p + 1]

    loop(b0 + 2, add)
    diagonal = 6.0 + shift
    damp = DAMPING / diagonal

    def after(p):
        center, rest = own_defect(w, p, source[p], 1.0, diagonal)
        out[p] = center + damp * rest

    loop(b0, after)


def kernel(names, counts, shape2, span, *refs):
    k = dict(zip(names, refs))
    shift_ref, source, out, *rest = refs[len(names) :]
    shift = shift_ref[0]
    landing, later, *halos = rest[:5]
    block, block_later, *owns = rest[5:10]
    buffers = rest[10:20]
    sems, sems_later, face_sems = rest[20:24], rest[24:28], rest[28:30]
    f = buffers[8]
    first_part(k, counts, source, f, landing, halos, block, owns, sems, face_sems)
    second_part(k, counts, shape2, span, shift, landing, source, halos, block_later, buffers)
    spread(counts, block_later, later, sems_later)()
    third_part(k, counts, shape2, span, shift, later, source, out, buffers)


def per_device(counts, source, shift):
    nx, ny, nz = counts
    b0, b1, b2 = source.shape
    sizes = (b0 * nx, b1 * nz, b2 * ny)
    table = constants(source.shape, sizes)
    m0, m1, m2 = (size // 2 for size in sizes)
    shape2 = tuple(size // 4 for size in sizes)
    span = b0 // 2 + 8
    wide = (b1 + 16, 2 * b2)
    packed = (b0 // 4, b1 // 2, b2)
    devices = nx * ny * nz
    chips = devices // 2
    vmem = pl.BlockSpec(memory_space=pltpu.VMEM)

    def field(*shape):
        return pltpu.VMEM(shape, jnp.float32)

    faces = [field(2, b1, b2), field(2, b0, 1, b2), field(2, 8, b0 * b1)]
    buffers = [
        field(m0, m1, m2),
        field(m0 + 2, m1, m2),
        field(m0 + 2, m1, m2),
        field(m0 // 2, m1, m2),
        field(m0 // 2, m1, m2),
        field(span, *wide),
        field(b0 + 4, *wide),
        field(b0 + 2, *wide),
        field(b0 + 2, *wide),
        field(b0 // 2, b1, b2),
    ]
    sems = [pltpu.SemaphoreType.DMA((max(chips - 1, 1),))] * 2
    sems += [pltpu.SemaphoreType.DMA((chips,))] * 2
    landing = [field(devices, *packed)] * 2 + faces
    names = tuple(table)
    return pl.pallas_call(
        functools.partial(kernel, names, counts, shape2, span),
        out_shape=jax.ShapeDtypeStruct(source.shape, jnp.float32),
        in_specs=[vmem] * len(names) + [pl.BlockSpec(memory_space=pltpu.SMEM), vmem],
        out_specs=vmem,
        scratch_shapes=landing
        + [field(*packed)] * 2
        + faces
        + buffers
        + sems * 2
        + [pltpu.SemaphoreType.DMA((6,))] * 2,
        compiler_params=pltpu.CompilerParams(
            vmem_limit_bytes=60 * 1024 * 1024, collective_id=0, has_side_effects=True
        ),
    )(*[jnp.asarray(table[name]) for name in names], shift, source)


def modes(count, depth):
    if depth == 0:
        return [(0, k) for k in range(count // 2)] + [(1, k) for k in range(1, count // 2 + 1)]
    half = count // 2
    low = modes(half, depth - 1)
    high = []
    for kind, k in low:
        if kind == 0:
            high.append((0, half - k if k else half // 2))
        else:
            high.append((1, half - k if k < half // 2 else half))
    return low + high


def waves(count, order):
    cells = (np.arange(count) + 0.5) * (2.0 * np.pi / count)
    return np.stack([np.sin(k * cells) if kind else np.cos(k * cells) for kind, k in order], axis=1)


def analysis(waves_):
    return waves_.T / np.sum(waves_**2, axis=0)[:, None]


def two_blocks(matrix, axis):
    first, second = np.split(matrix, 2, axis=axis)
    return np.concatenate([np.diag(first), np.diag(second)])


def factors(m):
    orders = modes(m, 2), modes(m // 2, 1), modes(m // 4, 0)
    bases = [waves(len(order), order) for order in orders]
    t = {"waves": bases[0]}
    for level, fine, coarse in (("1", bases[0], bases[1]), ("2", bases[1], bases[2])):
        n = fine.shape[0]
        t["r" + level] = two_blocks(analysis(coarse) @ (0.5 * pairs(n // 2)) @ fine, 1)
        for name, weights in (("p", LINEAR), ("q", CUBIC)):
            matrix = interpolation(n // 2, range(n), weights)
            t[name + level] = two_blocks(analysis(fine) @ matrix @ coarse, 0)
        order = orders[int(level) - 1]
        t["e" + level] = np.array([2.0 - 2.0 * np.cos(2.0 * np.pi * k / n) for _, k in order])
    t["c3"] = np.array([np.cos(2.0 * np.pi * k / (m // 4)) for _, k in orders[2]], np.float32)
    fine = np.eye(2 * m)
    lap = 2.0 * fine - np.roll(fine, 1, 0) - np.roll(fine, -1, 0)
    current = interpolation(m, range(2 * m), CUBIC) @ bases[0]
    for i in range(3):
        t[f"m{i}"] = np.sum(analysis(bases[0]).T * ((0.5 * pairs(m)) @ current), axis=0)
        current = lap @ current
    return t


def near(matrix, axis=0):
    return np.roll(matrix, 1, axis) + np.roll(matrix, -1, axis)


def synthesis(t, cells, weights, powers):
    m = t["waves"].shape[0]
    matrix = interpolation(m, range(2 * m), weights) @ t["waves"]
    result = []
    for _ in range(powers):
        result.append(matrix[np.array(cells) % (2 * m)])
        matrix = near(matrix)
    return result


def pick(matrix, rows, columns):
    return matrix[np.array(rows) % matrix.shape[0]][:, np.array(columns) % matrix.shape[1]]


def late_kinds(m, rows, columns):
    plain = interpolation(m, range(2 * m), LINEAR)
    return [pick(kind, rows, columns) for kind in (plain, near(plain), near(plain, 1), near(near(plain), 1))]


def mixed(p, r):
    return [
        np.kron(p[0], r[0]),
        np.kron(p[1], r[0]) + np.kron(p[0], r[1]),
        np.kron(p[2], r[0]) + np.kron(p[0], r[2]),
        np.kron(p[3], r[0]) + np.kron(p[0], r[3]) + np.kron(p[2], r[1]) + np.kron(p[1], r[2]),
    ]


def exact(matrix):
    result = np.asarray(matrix, jnp.bfloat16)
    assert np.all(result.astype(np.float64) == matrix)
    return result


def halves(matrix, axis):
    high = np.asarray(matrix, jnp.bfloat16)
    low = np.asarray(matrix - high.astype(np.float64), jnp.bfloat16)
    return np.concatenate([high, low], axis=axis)


def halved_rows(m0, m1):
    index = np.arange(m0 * m1).reshape(2, 2, 2, m0 // 8, 2, 2, m1 // 4)
    index = index.transpose(2, 0, 4, 1, 5, 3, 6).reshape(2, 4, -1)
    return index, index[:, 0].reshape(-1), index.reshape(-1)


def own_table(half):
    count = 2 * half
    four = sum(np.roll(np.kron(np.eye(half), np.eye(2)[:, :1]), s, axis=0) for s in (-1, 0, 1, 2))
    four[count - 1, 0] = 0.0
    four[0, half - 1] = 0.0
    beside = np.zeros((count, half))
    beside[count - 1, 0] = beside[0, half - 1] = 1.0
    own = np.zeros((2, count, 3, 2, half))
    for n, part in enumerate((pairs(half).T, beside, four)):
        for s in range(2):
            own[s, :, n, s] = 0.125 * part
    return np.asarray(own.reshape(2 * count, 3 * count), jnp.bfloat16)


def two_levels(count):
    whole = 2 * count
    fine, half = np.eye(whole), np.eye(whole // 2)
    near, near1 = (np.roll(e, 1, 0) + np.roll(e, -1, 0) for e in (fine, half))
    down, down1 = pairs(whole // 2), pairs(whole // 4)
    start = count // 2
    rows = range(start // 4 - 1, (start + count) // 4 + 1)
    kinds = (down1 @ down, down1 @ down @ near, down1 @ near1 @ down, down1 @ near1 @ down @ near)
    return [kind[rows, start : start + count] for kind in kinds]


def early_tables(block):
    b0, b1, b2 = block
    (p, r, c) = ([*two_levels(size)] for size in block)
    full = mixed(p, r)
    rows = np.zeros((4, 3, 16, b0 * b1))
    rows[:, :, : 2 * r[0].shape[0]] = np.stack(full).reshape(4, 3, 2 * r[0].shape[0], b0 * b1)
    lanes = np.zeros((4, b2, b2))
    for n in range(4):
        lanes[n, :, : c[n].shape[0]] = c[n].T / 64.0
    return exact(rows.reshape(-1, b0 * b1)), exact(lanes.reshape(-1, b2))


def fast_constants(counts, block, sizes):
    nx, ny, nz = counts
    b0, b1, b2 = block
    m0, m1, m2 = (size // 2 for size in sizes)
    t0, t1, t2 = (factors(m) for m in (m0, m1, m2))
    parts, index2, index1 = halved_rows(m0, m1)
    i0, i1 = index1 // m1, index1 % m1
    j0, j1 = index2 // m1, index2 % m1
    rows2 = len(index2)

    def across(name, k, l, op=np.multiply):
        return op(t0[name][k], t1[name][l])

    def joint(a, c):
        return t0[a][i0] * t1[c][i1]

    columns = [across("r1", i0, i1), across("p1", i0, i1), across("q1", i0, i1), across("e1", i0, i1, np.add)]
    columns += [joint("m0", "m0"), joint("m1", "m0") + joint("m0", "m1")]
    columns += [joint("m2", "m0") + joint("m0", "m2") + 2.0 * joint("m1", "m1")]
    by_row = np.zeros((m0 * m1, 128))
    by_row[:, : len(columns)] = np.stack(columns, axis=1)
    for n, name in enumerate(("r2", "p2", "q2", "e2")):
        by_row[:rows2, 8 + n] = across(name, j0, j1, np.add if name == "e2" else np.multiply)
    by_lane = np.zeros((16, m2))
    for n, name in enumerate(("r1", "p1", "q1", "e1", "m0", "m1", "m2")):
        by_lane[n] = t2[name]
    for n, name in enumerate(("r2", "p2", "q2", "e2")):
        by_lane[8 + n, : m2 // 2] = t2[name]
    two = np.float32(2.0)
    eigen = np.float32(6.0) - two * t0["c3"][:, None, None]
    eigen = eigen - two * t1["c3"][None, :, None] - two * t2["c3"][None, None, :]
    eigen = (np.float32(0.25 ** (LEVELS - 1)) * eigen).reshape(rows2 // 4, m2 // 4)
    early_rows, early_lanes = early_tables(block)
    table = {"own": own_table(b2 // 2), "early_rows": early_rows, "early_lanes": early_lanes}
    small = {"by_row": by_row, "by_lane": by_lane, "eigen": np.concatenate([eigen, eigen], axis=1)}
    table.update({name: np.asarray(value, np.float32) for name, value in small.items()})

    a0, a1 = (analysis(waves(m // 2, modes(m // 2, 1))) for m in (m0, m1))
    a2 = analysis(waves(m2 // 2, modes(m2 // 2, 1)))
    p0, p1, p2 = b0 // 4, b1 // 4, b2 // 4
    wide = p2 + 2
    lanes = np.zeros((ny, b2, 3, m2 // 2))
    for dy in range(ny):
        for n in range(3):
            lanes[dy, 42 * n : 42 * n + wide, n] = a2[:, np.arange(p2 * dy - 1, p2 * dy + p2 + 1) % (m2 // 2)].T
    table["level2_lanes"] = halves(lanes.reshape(ny * b2, -1), 0)
    n, dx, dz, c, r = np.meshgrid(*(range(k) for k in (3, nx, nz, 2, p1 + 2)), indexing="ij")
    planes = (p0 * dx + 2 * n + c - 1 - p0 // 2) % (m0 // 2)
    rows = (p1 * dz + r - 1) % (m1 // 2)
    full = np.zeros((rows2, 3, nx, nz, 16))
    full[..., : 2 * (p1 + 2)] = (a0[j0][:, planes] * a1[j1][:, rows]).reshape(rows2, 3, nx, nz, -1)
    table["level2_rows"] = halves(full.reshape(rows2, -1), 1)

    forward = analysis(t0["waves"])[i0][:, : m0 // 2, None] * analysis(t1["waves"])[i1][:, None, :]
    table["forward_rows"] = halves(forward.reshape(2, m0 * m1 // 2, -1), 2)
    table["forward_lanes"] = halves(analysis(t2["waves"]).T, 0)
    for name, weights, powers in (("cubic", CUBIC, 3), ("linear", LINEAR, 2)):
        p = synthesis(t0, range(b0 // 2), weights, powers)
        r = synthesis(t1, range(b1), weights, powers)
        full = []
        for part in parts.reshape(2, -1):
            q0 = [matrix[:, part // m1][:, None, :] for matrix in p]
            q1 = [matrix[:, part % m1][None, :, :] for matrix in r]
            kinds = [q0[0] * q1[0], q0[1] * q1[0] + q0[0] * q1[1]]
            if powers == 3:
                kinds.append(q0[2] * q1[0] + 2.0 * q0[1] * q1[1] + q0[0] * q1[2])
            full.append(np.stack(kinds).reshape(-1, part.size))
        table[name + "_rows"] = halves(np.stack(full), 2)
        lanes = [matrix.T for matrix in synthesis(t2, range(b2), weights, powers)]
        table[name + "_lanes"] = halves(np.concatenate(lanes), 0)
    p = late_kinds(m0, range(b0), range(-2, b0 // 2 + 2))
    r = late_kinds(m1, range(b1), range(m1))
    table["late_rows"] = exact(np.concatenate(mixed(p, r), axis=1))
    table["late_lanes"] = exact(np.concatenate([c.T for c in late_kinds(m2, range(b2), range(m2))], axis=1))
    return table


def split(values):
    high = values.astype(jnp.bfloat16)
    return high, (values - high.astype(jnp.float32)).astype(jnp.bfloat16)


def by_right(values, table):
    high, low = split(values)
    depth = values.shape[1]
    first, second = table[:depth], table[depth:]
    return jnp.dot(
        jnp.concatenate([high, low, high], axis=1),
        jnp.concatenate([first, first, second], axis=0),
        preferred_element_type=jnp.float32,
    )


def by_left(table, values):
    high, low = split(values)
    depth = values.shape[0]
    first, second = table[:, :depth], table[:, depth:]
    return jnp.dot(
        jnp.concatenate([first, first, second], axis=1),
        jnp.concatenate([high, low, high], axis=0),
        preferred_element_type=jnp.float32,
    )


def fold(values):
    n = values.shape[0] // 8
    parts = []
    for kind in range(2):
        quarter = [values[(4 * kind + i) * n : (4 * kind + i + 1) * n] for i in range(4)]
        parts.append((quarter[0] + quarter[1]) + (quarter[2] + quarter[3]))
    total = jnp.concatenate(parts, axis=0)
    return total + pltpu.roll(total, total.shape[1] // 2, 1)


def unfold(values):
    n = values.shape[0] // 2
    return jnp.concatenate([values[:n]] * 4 + [values[n:]] * 4, axis=0)


def own_parts(source, own, outs, alpha, beta):
    block, across, along_rows, along_planes, rest = outs
    b0, b1, b2 = source.shape
    h0, h1 = b0 // 2, b1 // 2
    first = [source[p, pl.ds(0, h1, stride=2), :] for p in range(b0)]
    second = [source[p, pl.ds(1, h1, stride=2), :] for p in range(b0)]
    summed = [a + b for a, b in zip(first, second)]
    row = lax.broadcasted_iota(jnp.int32, (h1, b2), 0)
    zero = jnp.zeros((h1, b2), jnp.float32)
    whole, faces, inner = [], [], []
    for c in range(h0):
        total = summed[2 * c] + summed[2 * c + 1]
        down = pltpu.roll(second[2 * c] + second[2 * c + 1], 1, 0)
        up = pltpu.roll(first[2 * c] + first[2 * c + 1], h1 - 1, 0)
        whole.append(total)
        faces.append(jnp.where(row == 0, down, jnp.where(row == h1 - 1, up, zero)))
        near = 2.0 * total + jnp.where(row > 0, down, zero) + jnp.where(row < h1 - 1, up, zero)
        if c > 0:
            near = near + summed[2 * c - 1]
        if c < h0 - 1:
            near = near + summed[2 * c + 2]
        inner.append(near)

    def pack(planes):
        half = len(planes) // 2
        return [jnp.concatenate([planes[i], planes[i + half]], axis=1) for i in range(half)]

    ends = [jnp.concatenate([summed[b0 - 1], summed[0]], axis=1)]
    stacked = jnp.concatenate(pack(whole) + pack(faces) + pack(inner) + ends + [jnp.zeros((8, 2 * b2), jnp.float32)], axis=0)
    parts = parts_of(stacked, 3)
    weights = own[...]
    result = jnp.dot(
        jnp.concatenate(parts, axis=1),
        jnp.concatenate([weights] * 3, axis=0),
        preferred_element_type=jnp.float32,
    )
    n = h0 // 2 * h1
    shape = block.shape
    mine = result[:n, :b2]
    block[...] = mine.reshape(shape)
    across[...] = result[:n, b2 : 2 * b2].reshape(shape)
    along_rows[...] = result[n : 2 * n, :b2].reshape(shape)
    along_planes[...] = result[3 * n : 3 * n + h1, :b2]
    rest[...] = (alpha * mine + beta * (result[2 * n : 3 * n, :b2] + result[:n, 2 * b2 :])).reshape(shape)


def early_part(source, rows_table, lanes_table, weights):
    keep0, near0, keep1, near1 = weights
    b0, b1, b2 = source.shape
    result = jnp.dot(
        jnp.concatenate([rows_table[...]] * 3, axis=1),
        jnp.concatenate(parts_of(source[...].reshape(b0 * b1, b2), 3), axis=0),
        preferred_element_type=jnp.float32,
    )
    n = result.shape[0] // 4
    plain, first, second, both = (result[i * n : (i + 1) * n] for i in range(4))
    joint = near0 * near1
    columns = (
        (keep0 * keep1) * plain + (keep1 * near0) * first + (keep0 * near1) * second + joint * both,
        (keep1 * near0) * plain + joint * second,
        (keep0 * near1) * plain + joint * first,
        joint * plain,
    )
    result = jnp.dot(
        jnp.concatenate(parts_of(jnp.concatenate(columns, axis=1), 3), axis=1),
        jnp.concatenate([lanes_table[...]] * 3, axis=0),
        preferred_element_type=jnp.float32,
    )
    total = result[:16] + pltpu.roll(result[16:32], 42, 1)
    return (total + pltpu.roll(result[32:], 84, 1)).reshape(2, 8, b2)


def beyond(place, counts):
    x, y, z = place
    return (x, lax.rem(y - 1 + 2 * lax.rem(y, 2) + counts[1], counts[1]), z)


def wait_for(ref, sem):
    pltpu.make_async_copy(ref, ref, sem).wait()


class TwoStage:
    def __init__(self, counts, near, far, block, landing, sems):
        self.counts, self.near, self.far = counts, near, far
        self.block, self.landing = block, landing
        self.sent, self.arrived, self.relay_sent, self.relayed = sems
        self.count = 0

    def at(self, offset):
        source = shifted(position(), self.counts, tuple(-step for step in offset))
        return self.landing.at[slot(source, self.counts)]

    def send(self, source, target, step, sem):
        place = shifted(position(), self.counts, step)
        remote(source, target, self.sent.at[0], self.arrived.at[sem], place).start()
        self.count += 1

    def start(self, offsets):
        for offset in offsets:
            sem = self.near.index(offset) if offset in self.near else len(self.near)
            self.send(self.block, self.at((0, 0, 0)), offset, sem)

    def relay(self, source, target):
        remote(source, target, self.relay_sent.at[0], self.relayed.at[0], partner_of(position())).start()

    def own(self):
        self.relay(self.block, self.at((0, 0, 0)))

    def forward(self, which):
        for n in which:
            arrived = self.at(self.near[n])
            wait_for(arrived, self.arrived.at[n])
            for second in self.far:
                self.send(arrived, arrived, second, len(self.near) + 1 + n)
            self.relay(arrived, arrived)

    def rest(self, which=None):
        firsts = ((0, 0, 0), *self.near)
        for n in range(len(firsts)) if which is None else which:
            first = firsts[n]
            wait_for(self.landing.at[pl.ds(0, len(self.far))], self.arrived.at[len(self.near) + n])
            for second in self.far:
                arrived = self.at(tuple(a + b for a, b in zip(first, second)))
                self.relay(arrived, arrived)

    def end(self):
        self.landing[slot(position(), self.counts)] = self.block[...]
        wait_for(self.landing.at[pl.ds(0, self.count)], self.sent.at[0])
        for sem in (self.relay_sent, self.relayed):
            wait_for(self.landing.at[pl.ds(0, self.count + 1)], sem.at[0])

    @staticmethod
    def semaphores(near):
        dma = pltpu.SemaphoreType.DMA
        return [dma((1,)), dma((2 * len(near) + 1,)), dma((1,)), dma((1,))]


def piece(ref, part):
    if part == 0:
        return ref
    half = ref.shape[0] // 2
    return ref.at[pl.ds(half if part == 1 else 0, half)]


class Close:
    def __init__(self, counts, far, block, landing, sems):
        self.counts, self.far, self.block, self.landing = counts, far, block, landing
        self.near = [((1, 0, 0), 1), ((counts[0] - 1, 0, 0), -1)] if counts[0] > 2 else [((1, 0, 0), 0)]
        self.sent, self.arrived, self.relay_sent, self.relayed = sems
        self.blocks = 2 * len(far) + 1

    def at(self, offset):
        source = shifted(position(), self.counts, tuple(-step for step in offset))
        return self.landing.at[slot(source, self.counts)]

    def send(self, source, target, step, sem):
        place = shifted(position(), self.counts, step)
        remote(source, target, self.sent.at[0], self.arrived.at[sem], place).start()

    def relay(self, source, target):
        remote(source, target, self.relay_sent.at[0], self.relayed.at[0], partner_of(position())).start()

    def start(self):
        mine = self.at((0, 0, 0))
        for n, (step, part) in enumerate(self.near):
            self.send(piece(self.block, part), piece(mine, part), step, n)
        for step in self.far:
            self.send(self.block, mine, step, len(self.near))
        self.relay(self.block, mine)

    def forward(self):
        for n, (first, part) in enumerate(self.near):
            arrived = piece(self.at(first), part)
            wait_for(arrived, self.arrived.at[n])
            for step in self.far:
                self.send(arrived, arrived, step, len(self.near) + 1 + n)
            self.relay(arrived, arrived)

    def rest_own(self):
        wait_for(self.landing.at[pl.ds(0, len(self.far))], self.arrived.at[len(self.near)])
        for step in self.far:
            self.relay(self.at(step), self.at(step))

    def rest(self):
        count = len(self.far)
        for n, (first, part) in enumerate(self.near):
            size = self.landing.shape[1] // (2 if part else 1)
            wait_for(self.landing.at[pl.ds(0, count), pl.ds(0, size)], self.arrived.at[len(self.near) + 1 + n])
            for step in self.far:
                arrived = piece(self.at(tuple(a + b for a, b in zip(first, step))), part)
                self.relay(arrived, arrived)

    def end(self):
        self.landing[slot(position(), self.counts)] = self.block[...]
        wait_for(self.landing.at[pl.ds(0, self.blocks)], self.sent.at[0])
        for sem in (self.relay_sent, self.relayed):
            wait_for(self.landing.at[pl.ds(0, self.blocks + 1)], sem.at[0])


def exchange(counts, sent, received, send, recv):
    me = position()
    order = (0, 2, 1)
    for offset, axis, side in face_offsets(counts):
        which = order[axis]
        mine = sent[which] if len(sent[which]) == 1 else [sent[which][side]]
        place = shifted(me, counts, offset)
        remote(mine[0], received[2 * which + 1 - side], send.at[0], recv.at[0], place).start()


def prepare(k, many, few, shift):
    diagonal0, diagonal1, diagonal2 = (6.0 * 0.25**level + shift for level in range(3))
    sigma0, sigma1, sigma2 = diagonal0 - 6.0, diagonal1 - 1.5, diagonal2 - 0.375
    damp0, damp1, damp2 = DAMPING / diagonal0, DAMPING / diagonal1, DAMPING / diagonal2
    down, pre, fine_q, out_q, out_g, out_e, cross = many
    by_row, by_lane = k["by_row"], k["by_lane"]
    lanes = by_lane.shape[1]

    def level1(i):
        rows = pl.ds(pl.multiple_of(8 * i, 8), 8)
        column = by_row[rows, :]

        def tall(n):
            return jnp.broadcast_to(column[:, n : n + 1], (8, lanes))

        def wide(n):
            return jnp.broadcast_to(by_lane[n : n + 1, :], (8, lanes))

        r, p, q = (tall(n) * wide(n) for n in range(3))
        a = 0.25 * (tall(3) + wide(3)) + sigma1
        s = 1.0 - damp1 * a
        down[rows, :] = r
        pre[rows, :] = r * s
        fine_q[rows, :] = a * q
        out_q[rows, :] = s * s * q
        out_g[rows, :] = damp1 * (1.0 + s)
        out_e[rows, :] = s * p
        c0, c1, c2 = tall(4), tall(5), tall(6)
        first = sigma0 * c0 + c1 - damp0 * ((sigma0 * sigma0) * c0 + (2.0 * sigma0) * c1 + c2)
        second = c0 - (2.0 * damp0) * (sigma0 * c0 + c1)
        cross[rows, :] = first * wide(4) + second * wide(5) - (damp0 * c0) * wide(6)

    loop(by_row.shape[0] // 8, level1)
    rows2, lanes2 = few[0].shape
    column = by_row[:rows2, :]

    def tall(n):
        return jnp.broadcast_to(column[:, n : n + 1], (rows2, lanes2))

    def wide(n):
        return jnp.broadcast_to(by_lane[n : n + 1, :lanes2], (rows2, lanes2))

    r, p, q = (tall(n) * wide(n) for n in (8, 9, 10))
    a = 0.0625 * (tall(11) + wide(11)) + sigma2
    s = 1.0 - damp2 * a
    values = (r, r * s, a * q, s * s * q, damp2 * (1.0 + s), s * p)
    for ref, value in zip(few, values):
        ref[...] = value
    k["inverse"][...] = 1.0 / (k["eigen"][...] + shift)


def level2(k, few, g):
    down, pre, fine_q, out_q, out_g, out_e = few
    e = unfold(fold(pre[...] * g) * k["inverse"][...])
    return out_g[...] * g + out_e[...] * e


def level2_full(k, few, g):
    down, pre, fine_q, out_q, out_g, out_e = few
    start = unfold(fold(down[...] * g) * k["inverse"][...])
    e = unfold(fold(pre[...] * (g - fine_q[...] * start)) * k["inverse"][...])
    return out_q[...] * start + out_g[...] * g + out_e[...] * e


def blocks_of(spectrum, i):
    rows2, lanes2 = spectrum.shape[0] // 4, spectrum.shape[1] // 2
    half = rows2 // 2
    base = 8 * i + 3 * half * lax.div(i, half // 8)
    for a in range(4):
        start = pl.multiple_of(base + a * half, 8)
        for c in range(2):
            yield (pl.ds(start, 8), pl.ds(c * lanes2, lanes2))


def spectral_u(k, many, few, spectrum, coupled, coarse):
    down, pre, fine_q, out_q, out_g, out_e, cross = many
    first, second, third = coarse
    steps = first.shape[0] // 8

    def at(i):
        return pl.ds(pl.multiple_of(8 * i, 8), 8)

    def restrict(i):
        first[at(i), :] = sum(down[w] * spectrum[w] for w in blocks_of(spectrum, i))

    loop(steps, restrict, steps)
    second[...] = level2_full(k, few, first[...])

    def residue(i):
        u = second[at(i), :]
        first[at(i), :] = sum(pre[w] * (spectrum[w] - fine_q[w] * u) for w in blocks_of(spectrum, i))

    loop(steps, residue, steps)
    third[...] = level2(k, few, first[...])

    def finish(i):
        u, e = second[at(i), :], third[at(i), :]
        total = None
        for w in blocks_of(spectrum, i):
            value = out_q[w] * u + out_g[w] * spectrum[w] + out_e[w] * e
            spectrum[w] = value
            value = cross[w] * value
            coupled[w] = value
            total = pre[w] * value if total is None else total + pre[w] * value
        first[at(i), :] = total

    loop(steps, finish, steps)


def spectral_e(many, spectrum, coupled, e2):
    out_g, out_e = many[4], many[5]

    def finish(i):
        e = e2[pl.ds(pl.multiple_of(8 * i, 8), 8), :]
        for w in blocks_of(spectrum, i):
            spectrum[w] = out_e[w] * e - out_g[w] * coupled[w]

    loop(e2.shape[0] // 8, finish, e2.shape[0] // 8)


def unpack_centred(gathered, counts, g):
    nx, ny, nz = counts
    me = position()
    half, rows, lanes = gathered.shape[1:]
    planes = g.shape[0]
    low = lax.broadcasted_iota(jnp.int32, (half, rows, lanes), 2) < lanes // 2
    for dx in range(nx):
        for dz in range(nz):
            for pair in range(ny // 2):
                parts = [
                    gathered[slot(shifted(me, counts, (dx, dy, dz)), counts)] for dy in (2 * pair, 2 * pair + 1)
                ]
                turned = [pltpu.roll(part, lanes // 2, 2) for part in parts]
                where = (pl.ds(dz * rows, rows), pl.ds(pair * lanes, lanes))
                start = (2 * half * dx - half) % planes
                g[(pl.ds(start, half), *where)] = jnp.where(low, parts[0], turned[1])
                g[(pl.ds(2 * half * dx, half), *where)] = jnp.where(low, turned[0], parts[1])


def transform(k, counts, landing, g, spectrum):
    unpack_centred(landing, counts, g)
    m0, m1, m2 = g.shape
    half = m0 // 2
    depth = half * m1
    for kind in range(2):
        rows = [g[p] - g[m0 - 1 - p] if kind else g[p] + g[m0 - 1 - p] for p in range(half)]
        whole = jnp.concatenate(rows, axis=0)
        part = depth // 2
        for i in range(2):
            values = by_left(k["forward_rows"][kind, i * part : (i + 1) * part], whole)
            start = kind * depth + i * part
            spectrum[start : start + part, :] = by_right(values, k["forward_lanes"])


def transform2(k, counts, landing):
    nx, ny, nz = counts
    me = position()
    columns = []
    for dy in range(ny):
        rows = [
            landing[slot(shifted(me, counts, (dx, dy, dz)), counts)].reshape(16, -1)
            for dx in range(nx)
            for dz in range(nz)
        ]
        columns.append(jnp.concatenate(rows, axis=0))
    values = by_right(jnp.concatenate(columns, axis=1), k["level2_lanes"])
    width = values.shape[1] // 3
    parts = [values[:, n * width : (n + 1) * width] for n in range(3)]
    return by_left(k["level2_rows"], jnp.concatenate(parts, axis=0))


def evaluate(k, kind, spectrum, mix, out):
    planes, rows, lanes = out.shape
    half = planes // 2
    depth = spectrum.shape[0] // 2
    parts = []
    for n in range(2):
        values = by_left(k[kind + "_rows"][n], spectrum[n * depth : (n + 1) * depth, :])
        pieces = [values[i : i + half * rows] for i in range(0, values.shape[0], half * rows)]
        columns = [sum(c * pieces[i] for i, c in enumerate(line) if c is not None) for line in mix]
        parts.append(jnp.concatenate(columns, axis=1))
    values = by_right(jnp.concatenate(parts, axis=0), k[kind + "_lanes"]).reshape(2, half, rows, lanes)
    even, odd = values[0], values[1]
    for p in range(half):
        for index, value in ((half + p, even[p] + odd[p]), (half - 1 - p, even[p] - odd[p])):
            out[index] = out[index] + value


def unpack_near(gathered, counts, g):
    nx, ny, nz = counts
    me = position()
    half, rows, lanes = gathered.shape[1:]
    for dx, first, last in ((nx - 1, half - 2, half), (0, 0, half), (1, 0, 2)):
        shape = (last - first, rows, lanes)
        low = lax.broadcasted_iota(jnp.int32, shape, 2) < lanes // 2
        for dz in range(nz):
            for pair in range(ny // 2):
                parts = [
                    gathered[slot(shifted(me, counts, (dx, dy, dz)), counts), pl.ds(first, last - first)]
                    for dy in (2 * pair, 2 * pair + 1)
                ]
                turned = [pltpu.roll(part, lanes // 2, 2) for part in parts]
                where = (pl.ds(dz * rows, rows), pl.ds(pair * lanes, lanes))
                if dx != nx - 1:
                    start = 2 if dx == 0 else 2 + 2 * half
                    g[(pl.ds(start, last - first), *where)] = jnp.where(low, parts[0], turned[1])
                if dx != 1:
                    start = 2 + half if dx == 0 else 0
                    g[(pl.ds(start, last - first), *where)] = jnp.where(low, turned[0], parts[1])


def late_part(k, g, weights):
    keep0, near0, keep1, near1 = weights
    planes, m1, m2 = g.shape
    pieces = split(g[...].reshape(planes * m1, m2))
    table = k["late_lanes"][...]
    values = jnp.dot(
        jnp.concatenate(pieces, axis=1),
        jnp.concatenate([table, table], axis=0),
        preferred_element_type=jnp.float32,
    )
    lanes = values.shape[1] // 4
    a, b, c, d = (values[:, i * lanes : (i + 1) * lanes] for i in range(4))
    joint = near0 * near1
    stacked = (
        (keep0 * keep1) * a + (near0 * keep1) * b + (keep0 * near1) * c + joint * d,
        (near0 * keep1) * a + joint * c,
        (keep0 * near1) * a + joint * b,
        joint * a,
    )
    table = k["late_rows"][...]
    values = jnp.dot(
        jnp.concatenate([table, table], axis=1),
        jnp.concatenate(split(jnp.concatenate(stacked, axis=0)), axis=0),
        preferred_element_type=jnp.float32,
    )
    return values


def own_sweep(f, source, keep, damp, out):
    rows, lanes = source.shape[1:]

    def body(p):
        beside = f[p] + f[p + 2] + around(f[p + 1])
        out[p] = damp * ((1.0 + keep) * source[p] + damp * beside[:rows, :lanes])

    loop(source.shape[0], body, source.shape[0])


def fast_kernel(names, counts, *refs):
    count = len(names)
    outside = dict(zip(names, refs))
    shift_ref, source_ref, out, *rest = refs[count:]

    def take(number):
        taken = rest[:number]
        del rest[:number]
        return taken

    k = dict(zip(names, take(count)))
    (source,) = take(1)
    landing_f, landing_h, landing_j = take(3)
    faces_in, halos = take(6), take(3)
    block_f, block_h, across, along_rows, local, along_planes = take(6)
    (block_j,) = take(1)
    own_planes, own_rows, own_columns = take(3)
    many, few, coarse = take(7), take(6), take(3)
    k["inverse"], g, near_h, spectrum, coupled, f = take(6)
    table_sems, *face_sems = take(5)
    sems_f, sems_h, sems_j = take(4), take(4), take(4)

    shift = shift_ref[0]
    me = position()
    barrier = pltpu.get_barrier_semaphore()
    along, across_all = stages(counts)
    places = [shifted(me, counts, offset) for offset in along + across_all]
    places += [partner_of(me), beyond(me, counts)]
    greet(barrier, places)
    loads = {"source": pltpu.make_async_copy(source_ref, source, table_sems.at[count])}
    loads["source"].start()
    for n, name in enumerate(names):
        loads[name] = pltpu.make_async_copy(outside[name], k[name], table_sems.at[n])
        loads[name].start()

    b0, b1, b2 = source.shape
    diagonal, diagonal1 = 6.0 + shift, 1.5 + shift
    damp, damp1 = DAMPING / diagonal, DAMPING / diagonal1
    loads["source"].wait()
    loads["own"].wait()
    parts = (block_f, across, along_rows, along_planes, local)
    own_parts(source, k["own"], parts, 1.0 - damp * diagonal, damp)
    pl.semaphore_wait(barrier, len(places))

    exchange(counts, ([along_planes], [along_rows], [across]), faces_in, *face_sems[:2])
    gather_f = TwoStage(counts, along[::-1], across_all, block_f, landing_f, sems_f)
    gather_j = TwoStage(counts, across_all[::-1], along, block_j, landing_j, sems_j)
    gather_f.start(along[::-1] + across_all)
    gather_f.own()
    own_planes[0] = source[0]
    own_planes[1] = source[b0 - 1]
    own_rows[0] = source[:, pl.ds(0, 1), :]
    own_rows[1] = source[:, pl.ds(b1 - 1, 1), :]
    turned = source[...].reshape(b0 * b1, b2).T
    own_columns[0] = turned[:8]
    own_columns[1] = turned[b2 - 8 :]
    for name in ("early_rows", "early_lanes"):
        loads[name].wait()
    weights = (1.0 - damp * diagonal, damp, 1.0 - damp1 * diagonal1, 0.25 * damp1)
    block_j[...] = early_part(source, k["early_rows"], k["early_lanes"], weights)
    gather_j.start(across_all)
    gather_j.own()

    for name in ("by_row", "by_lane", "eigen"):
        loads[name].wait()
    prepare(k, many, few, shift)
    gather_f.forward(range(min(2, len(along))))
    for sem in face_sems[:2]:
        wait_for(f.at[pl.ds(0, 3)], sem.at[0])
    shape = local.shape
    lane = lax.rem(lax.broadcasted_iota(jnp.int32, shape, 2), b2 // 2)
    row = lax.broadcasted_iota(jnp.int32, shape, 1)
    from_planes, from_rows, from_lanes = faces_in[:2], faces_in[2:4], faces_in[4:6]
    total = jnp.where(lane == 0, from_lanes[0][...], 0.0) + jnp.where(lane == b2 // 2 - 1, from_lanes[1][...], 0.0)
    total = total + jnp.where(row == 0, from_rows[0][...], 0.0) + jnp.where(row == shape[1] - 1, from_rows[1][...], 0.0)
    block_h[...] = local[...] + damp * total
    low = lax.broadcasted_iota(jnp.int32, shape[1:], 1) < b2 // 2
    block_h[0] = block_h[0] + damp * jnp.where(low, from_planes[0][...], 0.0)
    end = shape[0] - 1
    block_h[end] = block_h[end] + damp * jnp.where(low, 0.0, from_planes[1][...])

    gather_f.forward(range(2, len(along)))
    close_h = Close(counts, across_all[::-1], block_h, landing_h, sems_h)
    close_h.start()
    mine = [[own.at[side] for side in range(2)] for own in (own_planes, own_rows, own_columns)]
    exchange(counts, mine, [halo.at[side] for halo in halos for side in range(2)], *face_sems[2:4])
    gather_j.start(along)
    gather_j.forward(range(len(across_all)))
    gather_f.rest(range(len(along)))
    close_h.forward()
    gather_f.rest(range(len(along), len(along) + 1))
    close_h.rest_own()
    for sem in face_sems[2:4]:
        wait_for(f.at[pl.ds(0, 2)], sem.at[0])
    f[...] = jnp.zeros_like(f)
    rows, lanes = pl.ds(0, b1), pl.ds(0, b2)
    f[1 : b0 + 1, rows, lanes] = source[...]
    f[0, rows, lanes] = halos[0][0]
    f[b0 + 1, rows, lanes] = halos[0][1]
    f[1 : b0 + 1, pl.ds(b1, 1), lanes] = halos[1][1]
    f[1 : b0 + 1, pl.ds(b1 + 7, 1), lanes] = halos[1][0]
    middle = jnp.zeros((b2 - 16, b0 * b1), jnp.float32)
    turned = jnp.concatenate([halos[2][1], middle, halos[2][0]], axis=0)
    f[1 : b0 + 1, rows, pl.ds(b2, b2)] = turned.T.reshape(b0, b1, b2)
    keep = 1.0 - damp * diagonal
    own_sweep(f, source, keep, damp, out)
    gather_j.rest()
    gather_f.end()
    for name in names:
        if name not in ("own", "early_rows", "early_lanes", "by_row", "by_lane", "eigen"):
            loads[name].wait()
    transform(k, counts, landing_f, g, spectrum)
    spectral_u(k, many, few, spectrum, coupled, coarse)
    gather_j.end()
    double = 2.0 * keep * damp
    square = damp * damp
    mix = ((keep * keep, double, square), (double, 2.0 * square, None), (square, None, None))
    e2 = level2(k, few, transform2(k, counts, landing_j) - coarse[0][...])
    evaluate(k, "cubic", spectrum, mix, out)
    coarse[1][...] = e2
    close_h.rest()
    spectral_e(many, spectrum, coupled, coarse[1])
    evaluate(k, "linear", spectrum, ((keep, damp), (damp, None)), out)
    close_h.end()
    unpack_near(landing_h, counts, near_h)
    keep1 = 1.0 - damp1 * diagonal1
    late = late_part(k, near_h, (keep, damp, damp1 * (1.0 + keep1), 0.25 * damp1 * damp1))
    out[...] = out[...] + late.reshape(out.shape)


def fast_per_device(counts, source, shift):
    nx, ny, nz = counts
    b0, b1, b2 = source.shape
    sizes = (b0 * nx, b1 * nz, b2 * ny)
    table = fast_constants(counts, source.shape, sizes)
    m0, m1, m2 = (size // 2 for size in sizes)
    rows = m0 * m1
    packed = (b0 // 4, b1 // 2, b2)
    devices = nx * ny * nz

    def field(*shape):
        return pltpu.VMEM(shape, jnp.float32)

    def in_hbm(value):
        return pltpu.with_memory_space_constraint(value, pltpu.HBM)

    names = tuple(table)
    tile = packed[1:]
    fine = [field(2, b1, b2), field(2, b0, 1, b2), field(2, 8, b0 * b1)]
    scratch = [pltpu.VMEM(table[name].shape, table[name].dtype) for name in names]
    scratch += [field(*source.shape), field(devices, *packed), field(devices, *packed), field(devices, 2, *tile)]
    scratch += [field(*tile)] * 2 + [field(*packed)] * 4 + fine
    scratch += [field(*packed)] * 5 + [field(*tile), field(2, *tile)] + fine
    scratch += [field(rows, m2)] * 7 + [field(rows // 4, m2 // 2)] * 9
    scratch += [field(rows // 16, m2 // 2), field(m0, m1, m2), field(b0 // 2 + 4, m1, m2)]
    scratch += [field(rows, m2), field(rows, m2), field(b0 + 2, b1 + 8, 2 * b2)]
    dma = pltpu.SemaphoreType.DMA
    scratch += [dma((len(names) + 1,))] + [dma((1,))] * 4
    along, across = stages(counts)
    scratch += TwoStage.semaphores(along) * 2 + TwoStage.semaphores(across)
    return pl.pallas_call(
        functools.partial(fast_kernel, names, counts),
        out_shape=jax.ShapeDtypeStruct(source.shape, jnp.float32),
        in_specs=[pl.BlockSpec(memory_space=pltpu.HBM)] * len(names)
        + [pl.BlockSpec(memory_space=pltpu.SMEM), pl.BlockSpec(memory_space=pltpu.HBM)],
        out_specs=pl.BlockSpec(memory_space=pltpu.VMEM),
        scratch_shapes=scratch,
        compiler_params=pltpu.CompilerParams(
            vmem_limit_bytes=40 * 1024 * 1024, collective_id=0, has_side_effects=True
        ),
    )(*[in_hbm(jnp.asarray(table[name])) for name in names], shift, in_hbm(source))


def small_enough(counts, block):
    (nx, ny, nz), (b0, b1, b2) = counts, block
    rows = (b0 * nx // 2) * (b1 * nz // 2)
    return rows <= 512 and rows % 128 == 0 and (b0, b1, b2) == (16, 16, 128) and ny % 4 == 0 and min(counts) > 1


def dispatch(counts, source, shift):
    run = fast_per_device if small_enough(counts, source.shape) else per_device
    return run(counts, source, shift)


def solution(mesh):
    counts = tuple(mesh.shape[name] for name in NAMES)
    return jax.shard_map(
        functools.partial(dispatch, counts),
        mesh=mesh,
        in_specs=(P("gx", "gz", "gy"), P()),
        out_specs=P("gx", "gz", "gy"),
        check_vma=False,
    )
```

```python
import functools

import jax
import jax.numpy as jnp
import numpy as np
from jax import lax
from jax.experimental import pallas as pl
from jax.experimental.pallas import tpu as pltpu
from jax.sharding import PartitionSpec as P

LEVELS = 4
DAMPING = 6.0 / 7.0
PRECISE = lax.Precision.HIGHEST
CUBIC = (
    {-2: -5.0 / 128.0, -1: 35.0 / 128.0, 0: 105.0 / 128.0, 1: -7.0 / 128.0},
    {-1: -7.0 / 128.0, 0: 105.0 / 128.0, 1: 35.0 / 128.0, 2: -5.0 / 128.0},
)
LINEAR = ({-1: 0.25, 0: 0.75}, {0: 0.75, 1: 0.25})
NAMES = ("gx", "gy", "gz")
MESH = pl.DeviceIdType.MESH


def basis(count):
    cells = np.arange(count)
    columns, cosines = [], []
    for m in range(count):
        k = (m + 1) // 2
        angle = 2.0 * np.pi * k * cells / count
        column = np.cos(angle) if m % 2 == 1 or m == 0 else np.sin(angle)
        columns.append(column / np.sqrt(np.sum(column**2)))
        cosines.append(np.cos(2.0 * np.pi * k / count))
    return np.stack(columns, axis=1), np.array(cosines, np.float32)


def interpolation(coarse_count, fine_cells, weights):
    matrix = np.zeros((len(fine_cells), coarse_count))
    for row, cell in enumerate(fine_cells):
        for offset, weight in weights[cell % 2].items():
            matrix[row, (cell // 2 + offset) % coarse_count] += weight
    return matrix


def pairs(coarse_count):
    return np.kron(np.eye(coarse_count), np.ones((1, 2)))


def blocked(matrix):
    count = max(1, 128 // matrix.shape[1])
    return np.kron(np.eye(count), matrix)


def constants(block, sizes):
    b0, b1, b2 = block
    m0, m1, m2 = (size // 2 for size in sizes)
    q0, q1, q2 = (size // 4 for size in sizes)
    c0, c1, c2 = (size // 8 for size in sizes)
    table = {}
    table["own_rows"] = np.kron(np.eye(b0 // 2), pairs(b1 // 2))
    lanes = 0.125 * pairs(b2 // 2).T
    table["own_lo"] = np.concatenate([lanes, np.zeros_like(lanes)], axis=1)
    table["own_hi"] = np.concatenate([np.zeros_like(lanes), lanes], axis=1)
    table["down_rows"] = blocked(pairs(q1))
    table["down_lanes"] = 0.125 * pairs(q2).T
    window_lanes = [b2 + j for j in range(b2 // 2)] + [j - b2 for j in range(b2 // 2, 2 * b2)]
    window_rows = [j - 8 for j in range(b1 + 16)]
    for name, weights in (("cubic", CUBIC), ("linear", LINEAR)):
        table[name + "_rows1"] = blocked(interpolation(q1, range(m1), weights))
        table[name + "_lanes1"] = interpolation(q2, range(m2), weights).T
        table[name + "_rows0"] = blocked(interpolation(m1, window_rows, weights))
        table[name + "_lanes0"] = interpolation(m2, window_lanes, weights).T
    (u0, cos0), (u1, cos1), (u2, cos2) = basis(c0), basis(c1), basis(c2)
    table["spectrum_rows"] = np.kron(u0.T @ pairs(c0), u1.T @ pairs(c1))
    table["spectrum_lanes"] = 0.125 * pairs(c2).T @ u2
    for name, weights in (("cubic", CUBIC), ("linear", LINEAR)):
        table[name + "_rows2"] = np.kron(
            interpolation(c0, range(q0), weights) @ u0, interpolation(c1, range(q1), weights) @ u1
        )
        table[name + "_lanes2"] = u2.T @ interpolation(c2, range(q2), weights).T
    two = np.float32(2.0)
    eigen = (
        np.float32(6.0)
        - two * cos0[:, None, None]
        - two * cos1[None, :, None]
        - two * cos2[None, None, :]
    )
    table["eigen"] = (np.float32(0.25 ** (LEVELS - 1)) * eigen).reshape(c0 * c1, c2)
    wide = ("spectrum_rows", "spectrum_lanes", "eigen")
    return {
        name: np.asarray(
            value, np.float32 if name in wide or name.endswith("2") else jnp.bfloat16
        )
        for name, value in table.items()
    }


def dot(a, b):
    return jnp.dot(a, b, precision=PRECISE, preferred_element_type=jnp.float32)


def parts_of(values, pieces):
    parts = []
    for n in range(pieces):
        parts.append(values.astype(jnp.bfloat16))
        if n + 1 < pieces:
            values = values - parts[-1].astype(jnp.float32)
    return parts[::-1]


def right(values, matrix, pieces):
    terms = [
        jnp.dot(part, matrix, preferred_element_type=jnp.float32)
        for part in parts_of(values, pieces)
    ]
    return sum(terms[1:], terms[0])


def left(matrix, values, pieces):
    terms = [
        jnp.dot(matrix, part, preferred_element_type=jnp.float32)
        for part in parts_of(values, pieces)
    ]
    return sum(terms[1:], terms[0])


def around(plane):
    rows, lanes = plane.shape
    total = pltpu.roll(plane, 1, 0) + pltpu.roll(plane, rows - 1, 0)
    return total + (pltpu.roll(plane, 1, 1) + pltpu.roll(plane, lanes - 1, 1))


def around_all(values):
    first = jnp.concatenate([values[1:], values[:1]], axis=0)
    first = first + jnp.concatenate([values[-1:], values[:-1]], axis=0)
    for axis in (1, 2):
        first = first + pltpu.roll(values, 1, axis)
        first = first + pltpu.roll(values, values.shape[axis] - 1, axis)
    return first


def row_blocks(matrix, values, pieces):
    depth = matrix.shape[1]
    return jnp.concatenate(
        [left(matrix, values[i : i + depth], pieces) for i in range(0, values.shape[0], depth)], axis=0
    )


def loop(count, body, unroll=None):
    def step(i, carry):
        body(i)
        return carry

    lax.fori_loop(0, count, step, 0, unroll=unroll or (4 if count % 4 == 0 else 2))


def close(ref):
    count = ref.shape[0] - 2
    ref[0] = ref[count]
    ref[count + 1] = ref[1]


def defect_plane(v, p, g, weight, diagonal):
    center = v[p]
    beside = v[p - 1] + v[p + 1] + around(center)
    return center, g - (diagonal * center - weight * beside)


def restrict_own(k, summed):
    b_half, rows, lanes = summed.shape
    folded = left(k["own_rows"][...], summed.reshape(b_half * rows, lanes), 3)
    half = folded.shape[0] // 2
    return right(folded[:half], k["own_lo"][...], 3) + right(folded[half:], k["own_hi"][...], 3)


def unpack(gathered, counts, g):
    nx, ny, nz = counts
    x, y, z = (lax.axis_index(name) for name in NAMES)
    half, rows, lanes = gathered.shape[1:]
    low = lax.broadcasted_iota(jnp.int32, (half, rows, lanes), 2) < lanes // 2
    for dx in range(nx):
        for dz in range(nz):
            for pair in range(ny // 2):
                parts = []
                for dy in (2 * pair, 2 * pair + 1):
                    index = (lax.rem(x + dx, nx) * ny + lax.rem(y + dy, ny)) * nz
                    parts.append(gathered[index + lax.rem(z + dz, nz)])
                turned = [pltpu.roll(part, lanes // 2, 2) for part in parts]
                where = (pl.ds(dz * rows, rows), pl.ds(pair * lanes, lanes))
                start = 2 * half * dx
                g[(pl.ds(start, half), *where)] = jnp.where(low, parts[0], turned[1])
                g[(pl.ds(start + half, half), *where)] = jnp.where(low, turned[0], parts[1])


def solve(k, kind, values, shift):
    shape = values.shape
    flat = values.reshape(shape[0] * shape[1], shape[2])
    spectrum = dot(k["spectrum_rows"][...], dot(flat, k["spectrum_lanes"][...]))
    spectrum = spectrum / (k["eigen"][...] + shift)
    fine = dot(k[kind + "_rows2"][...], dot(spectrum, k[kind + "_lanes2"][...]))
    return fine.reshape(shape)


def cycle2(k, v, g, shift):
    weight = 0.25**2
    diagonal = 6.0 * weight + shift
    damp = DAMPING / diagonal
    if v is None:
        v = damp * g
    else:
        v = v + damp * (g - (diagonal * v - weight * around_all(v)))
    v = v + solve(k, "linear", g - (diagonal * v - weight * around_all(v)), shift)
    return v + damp * (g - (diagonal * v - weight * around_all(v)))


def down(k, t, shape2):
    flat = row_blocks(k["down_rows"][...], t[...].reshape(-1, t.shape[2]), 3)
    return right(flat, k["down_lanes"][...], 3).reshape(shape2)


def up(k, kind, level, values, z):
    flat = right(values, k[kind + "_lanes" + level][...], 2)
    z[...] = row_blocks(k[kind + "_rows" + level][...], flat, 2).reshape(z.shape)


def blend(z, i, weights, count):
    total = None
    for offset, weight in weights.items():
        index = i + offset
        index = index if count is None else lax.rem(index + count, count)
        term = weight * z[index]
        total = term if total is None else total + term
    return total


def up1(k, kind, values, z, v, add):
    count = z.shape[0]
    up(k, kind, "1", values.reshape(-1, values.shape[2]), z)
    weights = CUBIC if kind == "cubic" else LINEAR

    def body(i):
        for odd in (0, 1):
            p = 2 * i + odd + 1
            value = blend(z, i, weights[odd], count)
            v[p] = v[p] + value if add else value

    loop(count, body)
    close(v)


def cycle1(k, v, u, g, t, z, shift, zero, shape2):
    weight = 0.25
    diagonal = 6.0 * weight + shift
    damp = DAMPING / diagonal
    count = g.shape[0]

    def before(p):
        if zero:
            u[p + 1] = damp * g[p]
        else:
            center, rest = defect_plane(v, p + 1, g[p], weight, diagonal)
            u[p + 1] = center + damp * rest

    loop(count, before)
    close(u)

    def residue(i):
        t[i] = (
            defect_plane(u, 2 * i + 1, g[2 * i], weight, diagonal)[1]
            + defect_plane(u, 2 * i + 2, g[2 * i + 1], weight, diagonal)[1]
        )

    loop(count // 2, residue)
    correction = cycle2(k, None, down(k, t, shape2), shift)
    up1(k, "linear", correction, z, u, True)

    def after(p):
        center, rest = defect_plane(u, p + 1, g[p], weight, diagonal)
        v[p + 1] = center + damp * rest

    loop(count, after)
    close(v)


def window(k, kind, v, zw, span, write):
    count = v.shape[0] - 2
    values = jnp.concatenate([v[count - 3 : count + 1], v[1 : span - 3]], axis=0)
    up(k, kind, "0", values.reshape(-1, values.shape[2]), zw)
    weights = CUBIC if kind == "cubic" else LINEAR

    def body(i):
        for odd in (0, 1):
            write(2 * i + odd, blend(zw, i + 3, weights[odd], None))

    loop(span - 6, body)


def own_defect(v, p, f, weight, diagonal):
    rows, lanes = f.shape
    inside = (pl.ds(8, rows), pl.ds(lanes, lanes))
    wide = v[p + 1, pl.ds(8, rows), :]
    center = wide[:, lanes:]
    beside = v[(p, *inside)] + v[(p + 2, *inside)]
    beside = beside + v[p + 1, pl.ds(7, rows), pl.ds(lanes, lanes)]
    beside = beside + v[p + 1, pl.ds(9, rows), pl.ds(lanes, lanes)]
    beside = beside + pltpu.roll(wide, 1, 1)[:, lanes:]
    beside = beside + pltpu.roll(wide, 2 * lanes - 1, 1)[:, lanes:]
    return center, f - (diagonal * center - weight * beside)


def position():
    return tuple(lax.axis_index(name) for name in NAMES)


def partner_of(place):
    x, y, z = place
    return (x, y + 1 - 2 * lax.rem(y, 2), z)


def shifted(place, counts, offset):
    return tuple(
        lax.rem(at + step + count, count) for at, step, count in zip(place, offset, counts)
    )


def slot(place, counts):
    return (place[0] * counts[1] + place[1]) * counts[2] + place[2]


def chip_offsets(counts):
    nx, ny, nz = counts
    offsets = [
        (dx, dy, dz) for dx in range(nx) for dy in range(0, ny, 2) for dz in range(nz)
    ]

    def hops(offset):
        return sum(min(step, count - step) for step, count in zip(offset, (nx, ny, nz)))

    return sorted(offsets[1:], key=hops, reverse=True)


def face_offsets(counts):
    faces = []
    for axis in range(3):
        for side, step in ((0, -1), (1, 1)):
            offset = [0, 0, 0]
            offset[axis] = step
            faces.append((tuple(offset), axis, side))
    return faces


def greet(barrier, places):
    for place in places:
        pl.semaphore_signal(barrier, inc=1, device_id=place, device_id_type=MESH)


def remote(src, dst, send, recv, place):
    return pltpu.make_async_remote_copy(
        src_ref=src, dst_ref=dst, send_sem=send, recv_sem=recv, device_id=place, device_id_type=MESH
    )


def spread(counts, block, gathered, sems):
    send, recv, relay_send, relay_recv = sems
    me = position()
    partner = partner_of(me)
    along, across = stages(counts)
    number = {offset: n for n, offset in enumerate(chip_offsets(counts))}
    mine = gathered.at[slot(me, counts)]
    copies, relays = {}, []

    def pass_on(offset, source, target, place):
        n = number[offset]
        copies[offset] = remote(source, target, send.at[n], recv.at[n], place)
        copies[offset].start()

    def relay(n, source, target):
        relays.append(remote(source, target, relay_send.at[n], relay_recv.at[n], partner))
        relays[-1].start()

    for offset in along + across:
        pass_on(offset, block, mine, shifted(me, counts, offset))
    relay(len(number), block, mine)

    def arrival(offset):
        copies[offset].wait_recv()
        source = shifted(me, counts, tuple(-step for step in offset))
        return gathered.at[slot(source, counts)]

    def finish():
        gathered[slot(me, counts)] = block[...]
        for first in along[::-1]:
            arrived = arrival(first)
            for second in across:
                place = shifted(me, counts, second)
                pass_on((first[0], second[1], second[2]), arrived, arrived, place)
            relay(number[first], arrived, arrived)
        for first in ((0, 0, 0), *along[::-1]):
            for second in across[::-1]:
                offset = (first[0], second[1], second[2])
                arrived = arrival(offset)
                relay(number[offset], arrived, arrived)
        for copy in copies.values():
            copy.wait_send()
        for copy in relays:
            copy.wait()

    return finish


def stages(counts):
    offsets = chip_offsets(counts)
    along = [offset for offset in offsets if offset[1:] == (0, 0)]
    across = [offset for offset in offsets if offset[0] == 0]
    return along, across


def gather_places(counts):
    me = position()
    along, across = stages(counts)
    return [shifted(me, counts, offset) for offset in along + across] + [partner_of(me)]


def first_part(k, counts, source, f, gathered, halos, block, owns, sems, face_sems):
    own_planes, own_rows, own_columns = owns
    planes, rows, columns = halos
    face_send, face_recv = face_sems
    me = position()
    barrier = pltpu.get_barrier_semaphore()
    faces = face_offsets(counts)
    places = gather_places(counts) + [shifted(me, counts, offset) for offset, _, _ in faces]
    greet(barrier, places)
    b0, b1, b2 = source.shape
    summed = source[...].reshape(b0 // 2, 2, b1, b2)
    block[...] = restrict_own(k, summed[:, 0] + summed[:, 1]).reshape(block.shape)
    own_planes[0] = source[0]
    own_planes[1] = source[b0 - 1]
    own_rows[0] = source[:, pl.ds(0, 1), :]
    own_rows[1] = source[:, pl.ds(b1 - 1, 1), :]
    turned = source[...].reshape(b0 * b1, b2).T
    own_columns[0] = turned[:8]
    own_columns[1] = turned[b2 - 8 :]
    pl.semaphore_wait(barrier, len(places))
    finish = spread(counts, block, gathered, sems)
    buffers = ((own_planes, planes), (own_rows, rows), (own_columns, columns))
    order = (0, 2, 1)
    copies = []
    for n, (offset, axis, side) in enumerate(faces):
        own, halo = buffers[order[axis]]
        place = shifted(me, counts, offset)
        copies.append(
            remote(own.at[side], halo.at[1 - side], face_send.at[n], face_recv.at[n], place)
        )
        copies[-1].start()
    f[...] = jnp.zeros_like(f)
    f[1 : b0 + 1, pl.ds(8, b1), pl.ds(b2, b2)] = source[...]
    finish()
    for copy in copies:
        copy.wait()


def second_part(k, counts, shape2, span, shift, gathered, source, halos, out, buffers):
    g, v, u, t, z, zw, v0, v1, f, summed = buffers
    plane_halo, row_halo, column_halo = halos
    unpack(gathered, counts, g)
    b0, b1, b2 = source.shape
    rows, lanes = pl.ds(8, b1), pl.ds(b2, b2)
    f[0, rows, lanes] = plane_halo[0]
    f[b0 + 1, rows, lanes] = plane_halo[1]
    f[1 : b0 + 1, pl.ds(7, 1), lanes] = row_halo[0]
    f[1 : b0 + 1, pl.ds(8 + b1, 1), lanes] = row_halo[1]
    middle = jnp.zeros((b2 - 16, b0 * b1), jnp.float32)
    turned = jnp.concatenate([column_halo[1], middle, column_halo[0]], axis=0)
    f[1 : b0 + 1, rows, pl.ds(0, b2)] = turned.T.reshape(b0, b1, b2)
    def pair_sum(i):
        t[i] = g[2 * i] + g[2 * i + 1]

    loop(g.shape[0] // 2, pair_sum)
    forcing2 = down(k, t, shape2)
    iterate2 = cycle2(k, solve(k, "cubic", forcing2, shift), forcing2, shift)
    up1(k, "cubic", iterate2, z, v, False)
    cycle1(k, v, u, g, t, z, shift, False, shape2)

    def put(p, value):
        v0[p] = value

    window(k, "cubic", v, zw, span, put)
    diagonal = 6.0 + shift
    damp = DAMPING / diagonal

    def before(p):
        center, rest = defect_plane(v0, p + 1, f[p], 1.0, diagonal)
        v1[p] = center + damp * rest

    loop(b0 + 2, before)

    def residue(i):
        summed[i] = (
            own_defect(v1, 2 * i, source[2 * i], 1.0, diagonal)[1]
            + own_defect(v1, 2 * i + 1, source[2 * i + 1], 1.0, diagonal)[1]
        )

    loop(b0 // 2, residue)
    out[...] = restrict_own(k, summed[...]).reshape(out.shape)


def third_part(k, counts, shape2, span, shift, gathered, source, out, buffers):
    g, v, u, t, z, zw, w, v1 = buffers[:8]
    unpack(gathered, counts, g)
    cycle1(k, v, u, g, t, z, shift, True, shape2)
    b0 = source.shape[0]

    def put(p, value):
        w[p] = value

    window(k, "linear", v, zw, span, put)

    def add(p):
        w[p] = v1[p] + w[p + 1]

    loop(b0 + 2, add)
    diagonal = 6.0 + shift
    damp = DAMPING / diagonal

    def after(p):
        center, rest = own_defect(w, p, source[p], 1.0, diagonal)
        out[p] = center + damp * rest

    loop(b0, after)


def kernel(names, counts, shape2, span, *refs):
    k = dict(zip(names, refs))
    shift_ref, source, out, *rest = refs[len(names) :]
    shift = shift_ref[0]
    landing, later, *halos = rest[:5]
    block, block_later, *owns = rest[5:10]
    buffers = rest[10:20]
    sems, sems_later, face_sems = rest[20:24], rest[24:28], rest[28:30]
    f = buffers[8]
    first_part(k, counts, source, f, landing, halos, block, owns, sems, face_sems)
    second_part(k, counts, shape2, span, shift, landing, source, halos, block_later, buffers)
    spread(counts, block_later, later, sems_later)()
    third_part(k, counts, shape2, span, shift, later, source, out, buffers)


def per_device(counts, source, shift):
    nx, ny, nz = counts
    b0, b1, b2 = source.shape
    sizes = (b0 * nx, b1 * nz, b2 * ny)
    table = constants(source.shape, sizes)
    m0, m1, m2 = (size // 2 for size in sizes)
    shape2 = tuple(size // 4 for size in sizes)
    span = b0 // 2 + 8
    wide = (b1 + 16, 2 * b2)
    packed = (b0 // 4, b1 // 2, b2)
    devices = nx * ny * nz
    chips = devices // 2
    vmem = pl.BlockSpec(memory_space=pltpu.VMEM)

    def field(*shape):
        return pltpu.VMEM(shape, jnp.float32)

    faces = [field(2, b1, b2), field(2, b0, 1, b2), field(2, 8, b0 * b1)]
    buffers = [
        field(m0, m1, m2),
        field(m0 + 2, m1, m2),
        field(m0 + 2, m1, m2),
        field(m0 // 2, m1, m2),
        field(m0 // 2, m1, m2),
        field(span, *wide),
        field(b0 + 4, *wide),
        field(b0 + 2, *wide),
        field(b0 + 2, *wide),
        field(b0 // 2, b1, b2),
    ]
    sems = [pltpu.SemaphoreType.DMA((max(chips - 1, 1),))] * 2
    sems += [pltpu.SemaphoreType.DMA((chips,))] * 2
    landing = [field(devices, *packed)] * 2 + faces
    names = tuple(table)
    return pl.pallas_call(
        functools.partial(kernel, names, counts, shape2, span),
        out_shape=jax.ShapeDtypeStruct(source.shape, jnp.float32),
        in_specs=[vmem] * len(names) + [pl.BlockSpec(memory_space=pltpu.SMEM), vmem],
        out_specs=vmem,
        scratch_shapes=landing
        + [field(*packed)] * 2
        + faces
        + buffers
        + sems * 2
        + [pltpu.SemaphoreType.DMA((6,))] * 2,
        compiler_params=pltpu.CompilerParams(
            vmem_limit_bytes=60 * 1024 * 1024, collective_id=0, has_side_effects=True
        ),
    )(*[jnp.asarray(table[name]) for name in names], shift, source)


def modes(count, depth):
    if depth == 0:
        return [(0, k) for k in range(count // 2)] + [(1, k) for k in range(1, count // 2 + 1)]
    half = count // 2
    low = modes(half, depth - 1)
    high = []
    for kind, k in low:
        if kind == 0:
            high.append((0, half - k if k else half // 2))
        else:
            high.append((1, half - k if k < half // 2 else half))
    return low + high


def waves(count, order):
    cells = (np.arange(count) + 0.5) * (2.0 * np.pi / count)
    return np.stack([np.sin(k * cells) if kind else np.cos(k * cells) for kind, k in order], axis=1)


def analysis(waves_):
    return waves_.T / np.sum(waves_**2, axis=0)[:, None]


def two_blocks(matrix, axis):
    first, second = np.split(matrix, 2, axis=axis)
    return np.concatenate([np.diag(first), np.diag(second)])


def factors(m):
    orders = modes(m, 2), modes(m // 2, 1), modes(m // 4, 0)
    bases = [waves(len(order), order) for order in orders]
    t = {"waves": bases[0]}
    for level, fine, coarse in (("1", bases[0], bases[1]), ("2", bases[1], bases[2])):
        n = fine.shape[0]
        t["r" + level] = two_blocks(analysis(coarse) @ (0.5 * pairs(n // 2)) @ fine, 1)
        for name, weights in (("p", LINEAR), ("q", CUBIC)):
            matrix = interpolation(n // 2, range(n), weights)
            t[name + level] = two_blocks(analysis(fine) @ matrix @ coarse, 0)
        order = orders[int(level) - 1]
        t["e" + level] = np.array([2.0 - 2.0 * np.cos(2.0 * np.pi * k / n) for _, k in order])
    t["c3"] = np.array([np.cos(2.0 * np.pi * k / (m // 4)) for _, k in orders[2]], np.float32)
    fine = np.eye(2 * m)
    lap = 2.0 * fine - np.roll(fine, 1, 0) - np.roll(fine, -1, 0)
    current = interpolation(m, range(2 * m), CUBIC) @ bases[0]
    for i in range(3):
        t[f"m{i}"] = np.sum(analysis(bases[0]).T * ((0.5 * pairs(m)) @ current), axis=0)
        current = lap @ current
    return t


def near(matrix, axis=0):
    return np.roll(matrix, 1, axis) + np.roll(matrix, -1, axis)


def synthesis(t, cells, weights, powers):
    m = t["waves"].shape[0]
    matrix = interpolation(m, range(2 * m), weights) @ t["waves"]
    result = []
    for _ in range(powers):
        result.append(matrix[np.array(cells) % (2 * m)])
        matrix = near(matrix)
    return result


def pick(matrix, rows, columns):
    return matrix[np.array(rows) % matrix.shape[0]][:, np.array(columns) % matrix.shape[1]]


def late_kinds(m, rows, columns):
    plain = interpolation(m, range(2 * m), LINEAR)
    return [pick(kind, rows, columns) for kind in (plain, near(plain), near(plain, 1), near(near(plain), 1))]


def mixed(p, r):
    return [
        np.kron(p[0], r[0]),
        np.kron(p[1], r[0]) + np.kron(p[0], r[1]),
        np.kron(p[2], r[0]) + np.kron(p[0], r[2]),
        np.kron(p[3], r[0]) + np.kron(p[0], r[3]) + np.kron(p[2], r[1]) + np.kron(p[1], r[2]),
    ]


def exact(matrix):
    result = np.asarray(matrix, jnp.bfloat16)
    assert np.all(result.astype(np.float64) == matrix)
    return result


def halves(matrix, axis):
    high = np.asarray(matrix, jnp.bfloat16)
    low = np.asarray(matrix - high.astype(np.float64), jnp.bfloat16)
    return np.concatenate([high, low], axis=axis)


def halved_rows(m0, m1):
    index = np.arange(m0 * m1).reshape(2, 2, 2, m0 // 8, 2, 2, m1 // 4)
    index = index.transpose(2, 0, 4, 1, 5, 3, 6).reshape(2, 4, -1)
    return index, index[:, 0].reshape(-1), index.reshape(-1)


def own_table(half):
    count = 2 * half
    four = sum(np.roll(np.kron(np.eye(half), np.eye(2)[:, :1]), s, axis=0) for s in (-1, 0, 1, 2))
    four[count - 1, 0] = 0.0
    four[0, half - 1] = 0.0
    beside = np.zeros((count, half))
    beside[count - 1, 0] = beside[0, half - 1] = 1.0
    own = np.zeros((2, count, 3, 2, half))
    for n, part in enumerate((pairs(half).T, beside, four)):
        for s in range(2):
            own[s, :, n, s] = 0.125 * part
    return np.asarray(own.reshape(2 * count, 3 * count), jnp.bfloat16)


def two_levels(count):
    whole = 2 * count
    fine, half = np.eye(whole), np.eye(whole // 2)
    near, near1 = (np.roll(e, 1, 0) + np.roll(e, -1, 0) for e in (fine, half))
    down, down1 = pairs(whole // 2), pairs(whole // 4)
    start = count // 2
    rows = range(start // 4 - 1, (start + count) // 4 + 1)
    kinds = (down1 @ down, down1 @ down @ near, down1 @ near1 @ down, down1 @ near1 @ down @ near)
    return [kind[rows, start : start + count] for kind in kinds]


def early_tables(block):
    b0, b1, b2 = block
    (p, r, c) = ([*two_levels(size)] for size in block)
    full = mixed(p, r)
    rows = np.zeros((4, 3, 16, b0 * b1))
    rows[:, :, : 2 * r[0].shape[0]] = np.stack(full).reshape(4, 3, 2 * r[0].shape[0], b0 * b1)
    lanes = np.zeros((4, b2, b2))
    for n in range(4):
        lanes[n, :, : c[n].shape[0]] = c[n].T / 64.0
    return exact(rows.reshape(-1, b0 * b1)), exact(lanes.reshape(-1, b2))


def fast_constants(counts, block, sizes):
    nx, ny, nz = counts
    b0, b1, b2 = block
    m0, m1, m2 = (size // 2 for size in sizes)
    t0, t1, t2 = (factors(m) for m in (m0, m1, m2))
    parts, index2, index1 = halved_rows(m0, m1)
    i0, i1 = index1 // m1, index1 % m1
    j0, j1 = index2 // m1, index2 % m1
    rows2 = len(index2)

    def across(name, k, l, op=np.multiply):
        return op(t0[name][k], t1[name][l])

    def joint(a, c):
        return t0[a][i0] * t1[c][i1]

    columns = [across("r1", i0, i1), across("p1", i0, i1), across("q1", i0, i1), across("e1", i0, i1, np.add)]
    columns += [joint("m0", "m0"), joint("m1", "m0") + joint("m0", "m1")]
    columns += [joint("m2", "m0") + joint("m0", "m2") + 2.0 * joint("m1", "m1")]
    by_row = np.zeros((m0 * m1, 128))
    by_row[:, : len(columns)] = np.stack(columns, axis=1)
    for n, name in enumerate(("r2", "p2", "q2", "e2")):
        by_row[:rows2, 8 + n] = across(name, j0, j1, np.add if name == "e2" else np.multiply)
    by_lane = np.zeros((16, m2))
    for n, name in enumerate(("r1", "p1", "q1", "e1", "m0", "m1", "m2")):
        by_lane[n] = t2[name]
    for n, name in enumerate(("r2", "p2", "q2", "e2")):
        by_lane[8 + n, : m2 // 2] = t2[name]
    two = np.float32(2.0)
    eigen = np.float32(6.0) - two * t0["c3"][:, None, None]
    eigen = eigen - two * t1["c3"][None, :, None] - two * t2["c3"][None, None, :]
    eigen = (np.float32(0.25 ** (LEVELS - 1)) * eigen).reshape(rows2 // 4, m2 // 4)
    early_rows, early_lanes = early_tables(block)
    table = {"own": own_table(b2 // 2), "early_rows": early_rows, "early_lanes": early_lanes}
    small = {"by_row": by_row, "by_lane": by_lane, "eigen": np.concatenate([eigen, eigen], axis=1)}
    table.update({name: np.asarray(value, np.float32) for name, value in small.items()})

    a0, a1 = (analysis(waves(m // 2, modes(m // 2, 1))) for m in (m0, m1))
    a2 = analysis(waves(m2 // 2, modes(m2 // 2, 1)))
    p0, p1, p2 = b0 // 4, b1 // 4, b2 // 4
    wide = p2 + 2
    lanes = np.zeros((ny, b2, 3, m2 // 2))
    for dy in range(ny):
        for n in range(3):
            lanes[dy, 42 * n : 42 * n + wide, n] = a2[:, np.arange(p2 * dy - 1, p2 * dy + p2 + 1) % (m2 // 2)].T
    table["level2_lanes"] = halves(lanes.reshape(ny * b2, -1), 0)
    n, dx, dz, c, r = np.meshgrid(*(range(k) for k in (3, nx, nz, 2, p1 + 2)), indexing="ij")
    planes = (p0 * dx + 2 * n + c - 1 - p0 // 2) % (m0 // 2)
    rows = (p1 * dz + r - 1) % (m1 // 2)
    full = np.zeros((rows2, 3, nx, nz, 16))
    full[..., : 2 * (p1 + 2)] = (a0[j0][:, planes] * a1[j1][:, rows]).reshape(rows2, 3, nx, nz, -1)
    table["level2_rows"] = halves(full.reshape(rows2, -1), 1)

    forward = analysis(t0["waves"])[i0][:, : m0 // 2, None] * analysis(t1["waves"])[i1][:, None, :]
    table["forward_rows"] = halves(forward.reshape(2, m0 * m1 // 2, -1), 2)
    table["forward_lanes"] = halves(analysis(t2["waves"]).T, 0)
    for name, weights, powers in (("cubic", CUBIC, 3), ("linear", LINEAR, 2)):
        p = synthesis(t0, range(b0 // 2), weights, powers)
        r = synthesis(t1, range(b1), weights, powers)
        full = []
        for part in parts.reshape(2, -1):
            q0 = [matrix[:, part // m1][:, None, :] for matrix in p]
            q1 = [matrix[:, part % m1][None, :, :] for matrix in r]
            kinds = [q0[0] * q1[0], q0[1] * q1[0] + q0[0] * q1[1]]
            if powers == 3:
                kinds.append(q0[2] * q1[0] + 2.0 * q0[1] * q1[1] + q0[0] * q1[2])
            full.append(np.stack(kinds).reshape(-1, part.size))
        table[name + "_rows"] = halves(np.stack(full), 2)
        lanes = [matrix.T for matrix in synthesis(t2, range(b2), weights, powers)]
        table[name + "_lanes"] = halves(np.concatenate(lanes), 0)
    p = late_kinds(m0, range(b0), range(-2, b0 // 2 + 2))
    r = late_kinds(m1, range(b1), range(m1))
    table["late_rows"] = exact(np.concatenate(mixed(p, r), axis=1))
    table["late_lanes"] = exact(np.concatenate([c.T for c in late_kinds(m2, range(b2), range(m2))], axis=1))
    return table


def split(values):
    high = values.astype(jnp.bfloat16)
    return high, (values - high.astype(jnp.float32)).astype(jnp.bfloat16)


def by_right(values, table):
    high, low = split(values)
    depth = values.shape[1]
    first, second = table[:depth], table[depth:]
    return jnp.dot(
        jnp.concatenate([high, low, high], axis=1),
        jnp.concatenate([first, first, second], axis=0),
        preferred_element_type=jnp.float32,
    )


def by_left(table, values):
    high, low = split(values)
    depth = values.shape[0]
    first, second = table[:, :depth], table[:, depth:]
    return jnp.dot(
        jnp.concatenate([first, first, second], axis=1),
        jnp.concatenate([high, low, high], axis=0),
        preferred_element_type=jnp.float32,
    )


def fold(values):
    n = values.shape[0] // 8
    parts = []
    for kind in range(2):
        quarter = [values[(4 * kind + i) * n : (4 * kind + i + 1) * n] for i in range(4)]
        parts.append((quarter[0] + quarter[1]) + (quarter[2] + quarter[3]))
    total = jnp.concatenate(parts, axis=0)
    return total + pltpu.roll(total, total.shape[1] // 2, 1)


def unfold(values):
    n = values.shape[0] // 2
    return jnp.concatenate([values[:n]] * 4 + [values[n:]] * 4, axis=0)


def own_parts(source, own, outs, alpha, beta):
    block, across, along_rows, along_planes, rest = outs
    b0, b1, b2 = source.shape
    h0, h1 = b0 // 2, b1 // 2
    first = [source[p, pl.ds(0, h1, stride=2), :] for p in range(b0)]
    second = [source[p, pl.ds(1, h1, stride=2), :] for p in range(b0)]
    summed = [a + b for a, b in zip(first, second)]
    row = lax.broadcasted_iota(jnp.int32, (h1, b2), 0)
    zero = jnp.zeros((h1, b2), jnp.float32)
    whole, faces, inner = [], [], []
    for c in range(h0):
        total = summed[2 * c] + summed[2 * c + 1]
        down = pltpu.roll(second[2 * c] + second[2 * c + 1], 1, 0)
        up = pltpu.roll(first[2 * c] + first[2 * c + 1], h1 - 1, 0)
        whole.append(total)
        faces.append(jnp.where(row == 0, down, jnp.where(row == h1 - 1, up, zero)))
        near = 2.0 * total + jnp.where(row > 0, down, zero) + jnp.where(row < h1 - 1, up, zero)
        if c > 0:
            near = near + summed[2 * c - 1]
        if c < h0 - 1:
            near = near + summed[2 * c + 2]
        inner.append(near)

    def pack(planes):
        half = len(planes) // 2
        return [jnp.concatenate([planes[i], planes[i + half]], axis=1) for i in range(half)]

    ends = [jnp.concatenate([summed[b0 - 1], summed[0]], axis=1)]
    stacked = jnp.concatenate(pack(whole) + pack(faces) + pack(inner) + ends + [jnp.zeros((8, 2 * b2), jnp.float32)], axis=0)
    parts = parts_of(stacked, 3)
    weights = own[...]
    result = jnp.dot(
        jnp.concatenate(parts, axis=1),
        jnp.concatenate([weights] * 3, axis=0),
        preferred_element_type=jnp.float32,
    )
    n = h0 // 2 * h1
    shape = block.shape
    mine = result[:n, :b2]
    block[...] = mine.reshape(shape)
    across[...] = result[:n, b2 : 2 * b2].reshape(shape)
    along_rows[...] = result[n : 2 * n, :b2].reshape(shape)
    along_planes[...] = result[3 * n : 3 * n + h1, :b2]
    rest[...] = (alpha * mine + beta * (result[2 * n : 3 * n, :b2] + result[:n, 2 * b2 :])).reshape(shape)


def early_part(source, rows_table, lanes_table, weights):
    keep0, near0, keep1, near1 = weights
    b0, b1, b2 = source.shape
    result = jnp.dot(
        jnp.concatenate([rows_table[...]] * 3, axis=1),
        jnp.concatenate(parts_of(source[...].reshape(b0 * b1, b2), 3), axis=0),
        preferred_element_type=jnp.float32,
    )
    n = result.shape[0] // 4
    plain, first, second, both = (result[i * n : (i + 1) * n] for i in range(4))
    joint = near0 * near1
    columns = (
        (keep0 * keep1) * plain + (keep1 * near0) * first + (keep0 * near1) * second + joint * both,
        (keep1 * near0) * plain + joint * second,
        (keep0 * near1) * plain + joint * first,
        joint * plain,
    )
    result = jnp.dot(
        jnp.concatenate(parts_of(jnp.concatenate(columns, axis=1), 3), axis=1),
        jnp.concatenate([lanes_table[...]] * 3, axis=0),
        preferred_element_type=jnp.float32,
    )
    total = result[:16] + pltpu.roll(result[16:32], 42, 1)
    return (total + pltpu.roll(result[32:], 84, 1)).reshape(2, 8, b2)


def beyond(place, counts):
    x, y, z = place
    return (x, lax.rem(y - 1 + 2 * lax.rem(y, 2) + counts[1], counts[1]), z)


def wait_for(ref, sem):
    pltpu.make_async_copy(ref, ref, sem).wait()


class TwoStage:
    def __init__(self, counts, near, far, block, landing, sems):
        self.counts, self.near, self.far = counts, near, far
        self.block, self.landing = block, landing
        self.sent, self.arrived, self.relayed = sems
        self.relay_sent = self.sent
        self.count = 0

    def at(self, offset):
        source = shifted(position(), self.counts, tuple(-step for step in offset))
        return self.landing.at[slot(source, self.counts)]

    def send(self, source, target, step, sem):
        place = shifted(position(), self.counts, step)
        remote(source, target, self.sent.at[0], self.arrived.at[sem], place).start()
        self.count += 1

    def start(self, offsets):
        for offset in offsets:
            sem = self.near.index(offset) if offset in self.near else len(self.near)
            self.send(self.block, self.at((0, 0, 0)), offset, sem)

    def relay(self, source, target):
        remote(source, target, self.relay_sent.at[0], self.relayed.at[0], partner_of(position())).start()

    def own(self):
        self.relay(self.block, self.at((0, 0, 0)))

    def forward(self, which):
        for n in which:
            arrived = self.at(self.near[n])
            wait_for(arrived, self.arrived.at[n])
            for second in self.far:
                self.send(arrived, arrived, second, len(self.near) + 1 + n)
            self.relay(arrived, arrived)

    def rest(self, which=None):
        firsts = ((0, 0, 0), *self.near)
        for n in range(len(firsts)) if which is None else which:
            first = firsts[n]
            wait_for(self.landing.at[pl.ds(0, len(self.far))], self.arrived.at[len(self.near) + n])
            for second in self.far:
                arrived = self.at(tuple(a + b for a, b in zip(first, second)))
                self.relay(arrived, arrived)

    def end(self):
        self.landing[slot(position(), self.counts)] = self.block[...]
        wait_for(self.landing.at[pl.ds(0, 2 * self.count + 1)], self.sent.at[0])
        wait_for(self.landing.at[pl.ds(0, self.count + 1)], self.relayed.at[0])

    @staticmethod
    def semaphores(near):
        dma = pltpu.SemaphoreType.DMA
        return [dma((1,)), dma((2 * len(near) + 1,)), dma((1,))]


def piece(ref, part):
    if part == 0:
        return ref
    half = ref.shape[0] // 2
    return ref.at[pl.ds(half if part == 1 else 0, half)]


class Close:
    def __init__(self, counts, far, block, landing, sems):
        self.counts, self.far, self.block, self.landing = counts, far, block, landing
        self.near = [((1, 0, 0), 1), ((counts[0] - 1, 0, 0), -1)] if counts[0] > 2 else [((1, 0, 0), 0)]
        self.sent, self.arrived, self.relayed = sems
        self.relay_sent = self.sent
        self.blocks = 2 * len(far) + 1

    def at(self, offset):
        source = shifted(position(), self.counts, tuple(-step for step in offset))
        return self.landing.at[slot(source, self.counts)]

    def send(self, source, target, step, sem):
        place = shifted(position(), self.counts, step)
        remote(source, target, self.sent.at[0], self.arrived.at[sem], place).start()

    def relay(self, source, target):
        remote(source, target, self.relay_sent.at[0], self.relayed.at[0], partner_of(position())).start()

    def start(self):
        mine = self.at((0, 0, 0))
        for n, (step, part) in enumerate(self.near):
            self.send(piece(self.block, part), piece(mine, part), step, n)
        for step in self.far:
            self.send(self.block, mine, step, len(self.near))
        self.relay(self.block, mine)

    def forward(self):
        for n, (first, part) in enumerate(self.near):
            arrived = piece(self.at(first), part)
            wait_for(arrived, self.arrived.at[n])
            for step in self.far:
                self.send(arrived, arrived, step, len(self.near) + 1 + n)
            self.relay(arrived, arrived)

    def rest_own(self):
        wait_for(self.landing.at[pl.ds(0, len(self.far))], self.arrived.at[len(self.near)])
        for step in self.far:
            self.relay(self.at(step), self.at(step))

    def rest(self):
        count = len(self.far)
        for n, (first, part) in enumerate(self.near):
            size = self.landing.shape[1] // (2 if part else 1)
            wait_for(self.landing.at[pl.ds(0, count), pl.ds(0, size)], self.arrived.at[len(self.near) + 1 + n])
            for step in self.far:
                arrived = piece(self.at(tuple(a + b for a, b in zip(first, step))), part)
                self.relay(arrived, arrived)

    def end(self):
        self.landing[slot(position(), self.counts)] = self.block[...]
        wait_for(self.landing.at[pl.ds(0, 2 * self.blocks + 1)], self.sent.at[0])
        wait_for(self.landing.at[pl.ds(0, self.blocks + 1)], self.relayed.at[0])


def exchange(counts, sent, received, send, recv):
    me = position()
    order = (0, 2, 1)
    for offset, axis, side in face_offsets(counts):
        which = order[axis]
        mine = sent[which] if len(sent[which]) == 1 else [sent[which][side]]
        place = shifted(me, counts, offset)
        remote(mine[0], received[2 * which + 1 - side], send.at[0], recv.at[0], place).start()


def prepare(k, many, few, shift):
    diagonal0, diagonal1, diagonal2 = (6.0 * 0.25**level + shift for level in range(3))
    sigma0, sigma1, sigma2 = diagonal0 - 6.0, diagonal1 - 1.5, diagonal2 - 0.375
    damp0, damp1, damp2 = DAMPING / diagonal0, DAMPING / diagonal1, DAMPING / diagonal2
    down, pre, fine_q, out_q, out_g, out_e, cross = many
    by_row, by_lane = k["by_row"], k["by_lane"]
    lanes = by_lane.shape[1]

    def level1(i):
        rows = pl.ds(pl.multiple_of(8 * i, 8), 8)
        column = by_row[rows, :]

        def tall(n):
            return jnp.broadcast_to(column[:, n : n + 1], (8, lanes))

        def wide(n):
            return jnp.broadcast_to(by_lane[n : n + 1, :], (8, lanes))

        r, p, q = (tall(n) * wide(n) for n in range(3))
        a = 0.25 * (tall(3) + wide(3)) + sigma1
        s = 1.0 - damp1 * a
        down[rows, :] = r
        pre[rows, :] = r * s
        fine_q[rows, :] = a * q
        out_q[rows, :] = s * s * q
        out_g[rows, :] = damp1 * (1.0 + s)
        out_e[rows, :] = s * p
        c0, c1, c2 = tall(4), tall(5), tall(6)
        first = sigma0 * c0 + c1 - damp0 * ((sigma0 * sigma0) * c0 + (2.0 * sigma0) * c1 + c2)
        second = c0 - (2.0 * damp0) * (sigma0 * c0 + c1)
        cross[rows, :] = first * wide(4) + second * wide(5) - (damp0 * c0) * wide(6)

    loop(by_row.shape[0] // 8, level1)
    rows2, lanes2 = few[0].shape
    column = by_row[:rows2, :]

    def tall(n):
        return jnp.broadcast_to(column[:, n : n + 1], (rows2, lanes2))

    def wide(n):
        return jnp.broadcast_to(by_lane[n : n + 1, :lanes2], (rows2, lanes2))

    r, p, q = (tall(n) * wide(n) for n in (8, 9, 10))
    a = 0.0625 * (tall(11) + wide(11)) + sigma2
    s = 1.0 - damp2 * a
    values = (r, r * s, a * q, s * s * q, damp2 * (1.0 + s), s * p)
    for ref, value in zip(few, values):
        ref[...] = value
    k["inverse"][...] = 1.0 / (k["eigen"][...] + shift)


def level2(k, few, g):
    down, pre, fine_q, out_q, out_g, out_e = few
    e = unfold(fold(pre[...] * g) * k["inverse"][...])
    return out_g[...] * g + out_e[...] * e


def level2_full(k, few, g):
    down, pre, fine_q, out_q, out_g, out_e = few
    start = unfold(fold(down[...] * g) * k["inverse"][...])
    e = unfold(fold(pre[...] * (g - fine_q[...] * start)) * k["inverse"][...])
    return out_q[...] * start + out_g[...] * g + out_e[...] * e


def blocks_of(spectrum, i):
    rows2, lanes2 = spectrum.shape[0] // 4, spectrum.shape[1] // 2
    half = rows2 // 2
    base = 8 * i + 3 * half * lax.div(i, half // 8)
    for a in range(4):
        start = pl.multiple_of(base + a * half, 8)
        for c in range(2):
            yield (pl.ds(start, 8), pl.ds(c * lanes2, lanes2))


def spectral_u(k, many, few, spectrum, coupled, coarse):
    down, pre, fine_q, out_q, out_g, out_e, cross = many
    first, second, third = coarse
    steps = first.shape[0] // 8

    def at(i):
        return pl.ds(pl.multiple_of(8 * i, 8), 8)

    def restrict(i):
        first[at(i), :] = sum(down[w] * spectrum[w] for w in blocks_of(spectrum, i))

    loop(steps, restrict, steps)
    second[...] = level2_full(k, few, first[...])

    def residue(i):
        u = second[at(i), :]
        first[at(i), :] = sum(pre[w] * (spectrum[w] - fine_q[w] * u) for w in blocks_of(spectrum, i))

    loop(steps, residue, steps)
    third[...] = level2(k, few, first[...])

    def finish(i):
        u, e = second[at(i), :], third[at(i), :]
        total = None
        for w in blocks_of(spectrum, i):
            value = out_q[w] * u + out_g[w] * spectrum[w] + out_e[w] * e
            spectrum[w] = value
            value = cross[w] * value
            coupled[w] = value
            total = pre[w] * value if total is None else total + pre[w] * value
        first[at(i), :] = total

    loop(steps, finish, steps)


def spectral_e(many, spectrum, coupled, e2):
    out_g, out_e = many[4], many[5]

    def finish(i):
        e = e2[pl.ds(pl.multiple_of(8 * i, 8), 8), :]
        for w in blocks_of(spectrum, i):
            spectrum[w] = out_e[w] * e - out_g[w] * coupled[w]

    loop(e2.shape[0] // 8, finish, e2.shape[0] // 8)


def unpack_centred(gathered, counts, g):
    nx, ny, nz = counts
    me = position()
    half, rows, lanes = gathered.shape[1:]
    planes = g.shape[0]
    low = lax.broadcasted_iota(jnp.int32, (half, rows, lanes), 2) < lanes // 2
    for dx in range(nx):
        for dz in range(nz):
            for pair in range(ny // 2):
                parts = [
                    gathered[slot(shifted(me, counts, (dx, dy, dz)), counts)] for dy in (2 * pair, 2 * pair + 1)
                ]
                turned = [pltpu.roll(part, lanes // 2, 2) for part in parts]
                where = (pl.ds(dz * rows, rows), pl.ds(pair * lanes, lanes))
                start = (2 * half * dx - half) % planes
                g[(pl.ds(start, half), *where)] = jnp.where(low, parts[0], turned[1])
                g[(pl.ds(2 * half * dx, half), *where)] = jnp.where(low, turned[0], parts[1])


def transform(k, counts, landing, g, spectrum):
    unpack_centred(landing, counts, g)
    m0, m1, m2 = g.shape
    half = m0 // 2
    depth = half * m1
    for kind in range(2):
        rows = [g[p] - g[m0 - 1 - p] if kind else g[p] + g[m0 - 1 - p] for p in range(half)]
        whole = jnp.concatenate(rows, axis=0)
        part = depth // 2
        for i in range(2):
            values = by_left(k["forward_rows"][kind, i * part : (i + 1) * part], whole)
            start = kind * depth + i * part
            spectrum[start : start + part, :] = by_right(values, k["forward_lanes"])


def transform2(k, counts, landing):
    nx, ny, nz = counts
    me = position()
    columns = []
    for dy in range(ny):
        rows = [
            landing[slot(shifted(me, counts, (dx, dy, dz)), counts)].reshape(16, -1)
            for dx in range(nx)
            for dz in range(nz)
        ]
        columns.append(jnp.concatenate(rows, axis=0))
    values = by_right(jnp.concatenate(columns, axis=1), k["level2_lanes"])
    width = values.shape[1] // 3
    parts = [values[:, n * width : (n + 1) * width] for n in range(3)]
    return by_left(k["level2_rows"], jnp.concatenate(parts, axis=0))


def evaluate(k, kind, spectrum, mix, out):
    planes, rows, lanes = out.shape
    half = planes // 2
    depth = spectrum.shape[0] // 2
    parts = []
    for n in range(2):
        values = by_left(k[kind + "_rows"][n], spectrum[n * depth : (n + 1) * depth, :])
        pieces = [values[i : i + half * rows] for i in range(0, values.shape[0], half * rows)]
        columns = [sum(c * pieces[i] for i, c in enumerate(line) if c is not None) for line in mix]
        parts.append(jnp.concatenate(columns, axis=1))
    values = by_right(jnp.concatenate(parts, axis=0), k[kind + "_lanes"]).reshape(2, half, rows, lanes)
    even, odd = values[0], values[1]
    for p in range(half):
        for index, value in ((half + p, even[p] + odd[p]), (half - 1 - p, even[p] - odd[p])):
            out[index] = out[index] + value


def unpack_near(gathered, counts, g):
    nx, ny, nz = counts
    me = position()
    half, rows, lanes = gathered.shape[1:]
    for dx, first, last in ((nx - 1, half - 2, half), (0, 0, half), (1, 0, 2)):
        shape = (last - first, rows, lanes)
        low = lax.broadcasted_iota(jnp.int32, shape, 2) < lanes // 2
        for dz in range(nz):
            for pair in range(ny // 2):
                parts = [
                    gathered[slot(shifted(me, counts, (dx, dy, dz)), counts), pl.ds(first, last - first)]
                    for dy in (2 * pair, 2 * pair + 1)
                ]
                turned = [pltpu.roll(part, lanes // 2, 2) for part in parts]
                where = (pl.ds(dz * rows, rows), pl.ds(pair * lanes, lanes))
                if dx != nx - 1:
                    start = 2 if dx == 0 else 2 + 2 * half
                    g[(pl.ds(start, last - first), *where)] = jnp.where(low, parts[0], turned[1])
                if dx != 1:
                    start = 2 + half if dx == 0 else 0
                    g[(pl.ds(start, last - first), *where)] = jnp.where(low, turned[0], parts[1])


def late_part(k, g, weights):
    keep0, near0, keep1, near1 = weights
    planes, m1, m2 = g.shape
    pieces = split(g[...].reshape(planes * m1, m2))
    table = k["late_lanes"][...]
    values = jnp.dot(
        jnp.concatenate(pieces, axis=1),
        jnp.concatenate([table, table], axis=0),
        preferred_element_type=jnp.float32,
    )
    lanes = values.shape[1] // 4
    a, b, c, d = (values[:, i * lanes : (i + 1) * lanes] for i in range(4))
    joint = near0 * near1
    stacked = (
        (keep0 * keep1) * a + (near0 * keep1) * b + (keep0 * near1) * c + joint * d,
        (near0 * keep1) * a + joint * c,
        (keep0 * near1) * a + joint * b,
        joint * a,
    )
    table = k["late_rows"][...]
    values = jnp.dot(
        jnp.concatenate([table, table], axis=1),
        jnp.concatenate(split(jnp.concatenate(stacked, axis=0)), axis=0),
        preferred_element_type=jnp.float32,
    )
    return values


def own_sweep(f, source, keep, damp, out):
    rows, lanes = source.shape[1:]

    def body(p):
        beside = f[p] + f[p + 2] + around(f[p + 1])
        out[p] = damp * ((1.0 + keep) * source[p] + damp * beside[:rows, :lanes])

    loop(source.shape[0], body, source.shape[0])


def fast_kernel(names, counts, *refs):
    count = len(names)
    outside = dict(zip(names, refs))
    shift_ref, source_ref, out, *rest = refs[count:]

    def take(number):
        taken = rest[:number]
        del rest[:number]
        return taken

    k = dict(zip(names, take(count)))
    (source,) = take(1)
    landing_f, landing_h, landing_j = take(3)
    faces_in, halos = take(6), take(3)
    block_f, block_h, across, along_rows, local, along_planes = take(6)
    (block_j,) = take(1)
    own_planes, own_rows, own_columns = take(3)
    many, few, coarse = take(7), take(6), take(3)
    k["inverse"], g, near_h, spectrum, coupled, f = take(6)
    table_sems, *face_sems = take(5)
    sems_f, sems_h, sems_j = take(3), take(3), take(3)

    shift = shift_ref[0]
    me = position()
    barrier = pltpu.get_barrier_semaphore()
    along, across_all = stages(counts)
    places = [shifted(me, counts, offset) for offset in along + across_all]
    places += [partner_of(me), beyond(me, counts)]
    greet(barrier, places)
    loads = {"source": pltpu.make_async_copy(source_ref, source, table_sems.at[count])}
    loads["source"].start()
    for n, name in enumerate(names):
        loads[name] = pltpu.make_async_copy(outside[name], k[name], table_sems.at[n])
        loads[name].start()

    b0, b1, b2 = source.shape
    diagonal, diagonal1 = 6.0 + shift, 1.5 + shift
    damp, damp1 = DAMPING / diagonal, DAMPING / diagonal1
    loads["source"].wait()
    loads["own"].wait()
    parts = (block_f, across, along_rows, along_planes, local)
    own_parts(source, k["own"], parts, 1.0 - damp * diagonal, damp)
    pl.semaphore_wait(barrier, len(places))

    exchange(counts, ([along_planes], [along_rows], [across]), faces_in, *face_sems[:2])
    gather_f = TwoStage(counts, along[::-1], across_all, block_f, landing_f, sems_f)
    gather_j = TwoStage(counts, across_all[::-1], along, block_j, landing_j, sems_j)
    gather_f.start(along[::-1] + across_all)
    gather_f.own()
    own_planes[0] = source[0]
    own_planes[1] = source[b0 - 1]
    own_rows[0] = source[:, pl.ds(0, 1), :]
    own_rows[1] = source[:, pl.ds(b1 - 1, 1), :]
    turned = source[...].reshape(b0 * b1, b2).T
    own_columns[0] = turned[:8]
    own_columns[1] = turned[b2 - 8 :]
    for name in ("early_rows", "early_lanes"):
        loads[name].wait()
    weights = (1.0 - damp * diagonal, damp, 1.0 - damp1 * diagonal1, 0.25 * damp1)
    block_j[...] = early_part(source, k["early_rows"], k["early_lanes"], weights)
    gather_j.start(across_all)
    gather_j.own()

    for name in ("by_row", "by_lane", "eigen"):
        loads[name].wait()
    prepare(k, many, few, shift)
    gather_f.forward(range(min(2, len(along))))
    for sem in face_sems[:2]:
        wait_for(f.at[pl.ds(0, 3)], sem.at[0])
    shape = local.shape
    lane = lax.rem(lax.broadcasted_iota(jnp.int32, shape, 2), b2 // 2)
    row = lax.broadcasted_iota(jnp.int32, shape, 1)
    from_planes, from_rows, from_lanes = faces_in[:2], faces_in[2:4], faces_in[4:6]
    total = jnp.where(lane == 0, from_lanes[0][...], 0.0) + jnp.where(lane == b2 // 2 - 1, from_lanes[1][...], 0.0)
    total = total + jnp.where(row == 0, from_rows[0][...], 0.0) + jnp.where(row == shape[1] - 1, from_rows[1][...], 0.0)
    block_h[...] = local[...] + damp * total
    low = lax.broadcasted_iota(jnp.int32, shape[1:], 1) < b2 // 2
    block_h[0] = block_h[0] + damp * jnp.where(low, from_planes[0][...], 0.0)
    end = shape[0] - 1
    block_h[end] = block_h[end] + damp * jnp.where(low, 0.0, from_planes[1][...])

    gather_f.forward(range(2, len(along)))
    close_h = Close(counts, across_all[::-1], block_h, landing_h, sems_h)
    close_h.start()
    mine = [[own.at[side] for side in range(2)] for own in (own_planes, own_rows, own_columns)]
    exchange(counts, mine, [halo.at[side] for halo in halos for side in range(2)], *face_sems[2:4])
    gather_j.start(along)
    gather_j.forward(range(len(across_all)))
    gather_f.rest(range(len(along)))
    close_h.forward()
    gather_f.rest(range(len(along), len(along) + 1))
    close_h.rest_own()
    for sem in face_sems[2:4]:
        wait_for(f.at[pl.ds(0, 2)], sem.at[0])
    f[...] = jnp.zeros_like(f)
    rows, lanes = pl.ds(0, b1), pl.ds(0, b2)
    f[1 : b0 + 1, rows, lanes] = source[...]
    f[0, rows, lanes] = halos[0][0]
    f[b0 + 1, rows, lanes] = halos[0][1]
    f[1 : b0 + 1, pl.ds(b1, 1), lanes] = halos[1][1]
    f[1 : b0 + 1, pl.ds(b1 + 7, 1), lanes] = halos[1][0]
    middle = jnp.zeros((b2 - 16, b0 * b1), jnp.float32)
    turned = jnp.concatenate([halos[2][1], middle, halos[2][0]], axis=0)
    f[1 : b0 + 1, rows, pl.ds(b2, b2)] = turned.T.reshape(b0, b1, b2)
    keep = 1.0 - damp * diagonal
    own_sweep(f, source, keep, damp, out)
    gather_j.rest()
    gather_f.end()
    for name in names:
        if name not in ("own", "early_rows", "early_lanes", "by_row", "by_lane", "eigen"):
            loads[name].wait()
    transform(k, counts, landing_f, g, spectrum)
    spectral_u(k, many, few, spectrum, coupled, coarse)
    gather_j.end()
    double = 2.0 * keep * damp
    square = damp * damp
    mix = ((keep * keep, double, square), (double, 2.0 * square, None), (square, None, None))
    e2 = level2(k, few, transform2(k, counts, landing_j) - coarse[0][...])
    evaluate(k, "cubic", spectrum, mix, out)
    coarse[1][...] = e2
    close_h.rest()
    spectral_e(many, spectrum, coupled, coarse[1])
    evaluate(k, "linear", spectrum, ((keep, damp), (damp, None)), out)
    close_h.end()
    unpack_near(landing_h, counts, near_h)
    keep1 = 1.0 - damp1 * diagonal1
    late = late_part(k, near_h, (keep, damp, damp1 * (1.0 + keep1), 0.25 * damp1 * damp1))
    out[...] = out[...] + late.reshape(out.shape)


def fast_per_device(counts, source, shift):
    nx, ny, nz = counts
    b0, b1, b2 = source.shape
    sizes = (b0 * nx, b1 * nz, b2 * ny)
    table = fast_constants(counts, source.shape, sizes)
    m0, m1, m2 = (size // 2 for size in sizes)
    rows = m0 * m1
    packed = (b0 // 4, b1 // 2, b2)
    devices = nx * ny * nz

    def field(*shape):
        return pltpu.VMEM(shape, jnp.float32)

    def in_hbm(value):
        return pltpu.with_memory_space_constraint(value, pltpu.HBM)

    names = tuple(table)
    tile = packed[1:]
    fine = [field(2, b1, b2), field(2, b0, 1, b2), field(2, 8, b0 * b1)]
    scratch = [pltpu.VMEM(table[name].shape, table[name].dtype) for name in names]
    scratch += [field(*source.shape), field(devices, *packed), field(devices, *packed), field(devices, 2, *tile)]
    scratch += [field(*tile)] * 2 + [field(*packed)] * 4 + fine
    scratch += [field(*packed)] * 5 + [field(*tile), field(2, *tile)] + fine
    scratch += [field(rows, m2)] * 7 + [field(rows // 4, m2 // 2)] * 9
    scratch += [field(rows // 16, m2 // 2), field(m0, m1, m2), field(b0 // 2 + 4, m1, m2)]
    scratch += [field(rows, m2), field(rows, m2), field(b0 + 2, b1 + 8, 2 * b2)]
    dma = pltpu.SemaphoreType.DMA
    scratch += [dma((len(names) + 1,))] + [dma((1,))] * 4
    along, across = stages(counts)
    scratch += TwoStage.semaphores(along) + TwoStage.semaphores(along[:2]) + TwoStage.semaphores(across)
    return pl.pallas_call(
        functools.partial(fast_kernel, names, counts),
        out_shape=jax.ShapeDtypeStruct(source.shape, jnp.float32),
        in_specs=[pl.BlockSpec(memory_space=pltpu.HBM)] * len(names)
        + [pl.BlockSpec(memory_space=pltpu.SMEM), pl.BlockSpec(memory_space=pltpu.HBM)],
        out_specs=pl.BlockSpec(memory_space=pltpu.VMEM),
        scratch_shapes=scratch,
        compiler_params=pltpu.CompilerParams(
            vmem_limit_bytes=40 * 1024 * 1024, collective_id=0, has_side_effects=True
        ),
    )(*[in_hbm(jnp.asarray(table[name])) for name in names], shift, in_hbm(source))


def small_enough(counts, block):
    (nx, ny, nz), (b0, b1, b2) = counts, block
    rows = (b0 * nx // 2) * (b1 * nz // 2)
    return rows <= 512 and rows % 128 == 0 and (b0, b1, b2) == (16, 16, 128) and ny % 4 == 0 and min(counts) > 1


def dispatch(counts, source, shift):
    run = fast_per_device if small_enough(counts, source.shape) else per_device
    return run(counts, source, shift)


def solution(mesh):
    counts = tuple(mesh.shape[name] for name in NAMES)
    return jax.shard_map(
        functools.partial(dispatch, counts),
        mesh=mesh,
        in_specs=(P("gx", "gz", "gy"), P()),
        out_specs=P("gx", "gz", "gy"),
        check_vma=False,
    )
```
